32 devices in a mesh: rep: 4 (over y, core), fsdp: 8 (over z, x).
Axes of the slice: x: 2, y: 2, z: 4, core: 2. Of those that a mesh axis runs over, the one named last changes fastest.
Arguments:
- token_ids: int32 [2, 32, 512], P(None, ('rep', 'fsdp')), may hold values from 0 to 30527
- segment_ids: int32 [2, 32, 512], P(None, ('rep', 'fsdp')), may hold values from 0 to 3, never falling along the last dimension, each value on 1 to 256 neighbouring positions
- masked_pos: int32 [2, 32, 128], P(None, ('rep', 'fsdp')), may hold values from 0 to 511, as said below
- labels: int32 [2, 32, 128], P(None, ('rep', 'fsdp')), may hold values from 0 to 30527
- blocks: float32 [32, 512, 512], P(None, 'fsdp')
- gains: float32 [6, 512], P(None, 'fsdp'), may hold values from 0.5 to 1.5
- embed: float32 [30528, 512], P('fsdp'), may hold values from -0.54 to 0.54
- embed_m: float32 [30528, 512], P('fsdp'), may hold values from -0.3 to 0.3
- embed_v: float32 [30528, 512], P('fsdp'), may hold values from 0.0005 to 0.05
- gains_m: float32 [6, 512], P(None, 'fsdp'), may hold values from -3 to 3
- gains_v: float32 [6, 512], P(None, 'fsdp'), may hold values from 0.01 to 1
- soap_m: float32 [48, 512, 512], P('fsdp'), may hold values from -0.3 to 0.3
- soap_v: float32 [48, 512, 512], P('fsdp'), may hold values from 0.0005 to 0.05
- left_basis: float32 [48, 512, 512], P('fsdp'), may hold values from -0.25 to 0.25
- right_basis: float32 [48, 512, 512], P('fsdp'), may hold values from -0.25 to 0.25
- block_slots: int32 [32], replicated, may hold values from 0 to 47, as said below
- step_count: int32 [1], replicated, may hold values from 1 to 20
Outputs:
- loss: float32 [1], replicated
- grad_norm: float32 [1], replicated
- blocks_new: float32 [32, 512, 512], P(None, 'fsdp')
- gains_new: float32 [6, 512], P(None, 'fsdp')
- embed_new: float32 [30528, 512], P('fsdp')
- embed_m_new: float32 [30528, 512], P('fsdp')
- embed_v_new: float32 [30528, 512], P('fsdp')
- gains_m_new: float32 [6, 512], P(None, 'fsdp')
- gains_v_new: float32 [6, 512], P(None, 'fsdp')
- soap_m_new: float32 [48, 512, 512], P('fsdp')
- soap_v_new: float32 [48, 512, 512], P('fsdp')
- blocks_new_low: bfloat16 [32, 512, 512], P(None, 'fsdp')
- embed_new_low: bfloat16 [30528, 512], P('fsdp')
The draws below stay inside these ranges and needn't reach their ends.
Inputs may be any that keep to these rules, and one draw needn't show every extreme that they name: `segment_ids`: never falling along a pack; every value present in every pack. `masked_pos`: the 128 positions of a pack are distinct. `block_slots`: distinct; slot sl belongs to fsdp index sl // 6; no fsdp index gets more than 6 blocks, and one gets exactly 6.
All inputs are finite; a program needn't handle non-finite values.
Results may differ from the reference program's by a relative error of at most 0.003.
The reference program's roundings to bfloat16 on the way count: a program that leaves them out, or rounds other values in their place, can miss the bound.
Values may be sent and summed in bfloat16 or wider, within the bound.
A program may use at most 448 MiB of HBM per device.

```python
import math
import jax
import jax.numpy as jnp
import numpy as np
from jax import lax

D = 512
HEADS = 8
HEAD_DIM = 64
FF = 2048
VOCAB = 30528
LAYERS = 2
MB = 2
PACK = 512
MASK_DEV = 128
PACKS = 32
BLOCKS = 32
NG = 6
CAP = 6
SLOTS = 48
N_FSDP = 8


def draw_masked_pos(key, part):
    noise = jax.random.randint(key, (MB, PACKS, PACK), 0, 2 ** 19)
    scores = noise * PACK + jnp.arange(PACK, dtype=jnp.int32)
    return jnp.argsort(scores, axis=-1)[:, :, :MASK_DEV].astype(jnp.int32)


def draw_blocks(key, part):
    pieces = FF // D
    per_layer = 4 + 3 * pieces
    normal_values = jax.random.normal(key, (BLOCKS, D, D), jnp.float32)
    block_kind = jnp.arange(BLOCKS) % per_layer
    block_scale = jnp.where(block_kind == 3, 4.0 / math.sqrt(D), jnp.where(block_kind >= 4 + 2 * pieces, 1.0 / math.sqrt(FF), 1.0 / math.sqrt(D)))
    return (normal_values * block_scale[:, None, None]).astype(jnp.float32)


def draw_block_slots(key, part):
    key_order = jax.random.fold_in(key, 11)
    key_owner = jax.random.fold_in(key, 12)
    key_shuffle = jax.random.fold_in(key, 13)
    slot_order = jax.random.permutation(key_order, SLOTS).astype(jnp.int32)
    chosen_owner = jax.random.randint(key_owner, (), 0, N_FSDP)
    slot_ids = jnp.arange(SLOTS, dtype=jnp.int32)
    scores = jnp.where(slot_ids // CAP == chosen_owner, slot_ids % CAP, CAP + slot_order)
    picked = jnp.argsort(scores)[:BLOCKS].astype(jnp.int32)
    shuffle = jax.random.permutation(key_shuffle, BLOCKS)
    return picked[shuffle].astype(jnp.int32)


def touch_ends(array, stream_key, smallest, high):
    longest = array.shape.index(max(array.shape))
    spots = []
    for shift in (0, 1):
        where = [jax.random.randint(jax.random.fold_in(stream_key, axis), (), 0, length) for axis, length in enumerate(array.shape)]
        where[longest] = (where[longest] + shift) % array.shape[longest]
        spots.append(tuple(where))
    return array.at[spots[0]].set(smallest).at[spots[1]].set(high)


def steps_of(stream_key, extent, cuts, smallest, largest):
    loudness = 1.0
    for axis_at, blocks in cuts:
        draws = jax.random.uniform(jax.random.fold_in(jax.random.fold_in(stream_key, 6), axis_at), (blocks,), jnp.float32, smallest / len(cuts), largest / len(cuts))
        loudness = loudness * jnp.repeat(jnp.exp(draws), extent[axis_at] // blocks).reshape((-1,) + (1,) * (len(extent) - 1 - axis_at))
    return loudness


def rank_table(amount, skew):
    loads = [(1 << 20) // math.isqrt(grade ** skew) + 1 for grade in range(1, amount + 1)]
    scale = 1 + sum(loads) // (1 << 30)
    return np.cumsum(np.array([max(1, weight // scale) for weight in loads]))


def skewed_ids(key, extent, amount, lean):
    table = rank_table(amount, lean)
    pick = jax.random.randint(jax.random.fold_in(key, 1), extent, 0, int(table[amount - 1]))
    grade = jnp.searchsorted(jnp.asarray(table, jnp.int32), pick, side="right")
    return jax.random.permutation(jax.random.fold_in(key, 2), amount)[grade].astype(jnp.int32)


def split_up(amount, total, most, skew):
    portions = [(1 << 20) // math.isqrt(rank ** skew) + 1 for rank in range(2, amount + 1)]
    surplus, counts = total - most - (amount - 1), [1] * (amount - 1)
    while surplus > 0:
        candidates = [i for i in range(amount - 1) if counts[i] < most]
        whole, budget = sum([portions[i] for i in candidates]), surplus
        for i in candidates:
            more = min(most - counts[i], max(1, budget * portions[i] // whole), surplus)
            counts[i] = counts[i] + more
            surplus = surplus - more
    return np.array([most] + counts)


def uneven(rng, amount, total, most, skew):
    if amount == 2:
        one = jax.random.randint(rng, (), max(1, total - most), min(most, total - 1) + 1)
        return jnp.stack([one, total - one])
    lengths = jnp.asarray(split_up(amount, total, most, skew), jnp.int32)
    pairs = (amount - 1) // 2
    source_of, receiver = lengths[1:1 + 2 * pairs:2], lengths[2:2 + 2 * pairs:2]
    slack = jnp.minimum(source_of - 1, most - receiver)
    moved = jax.random.randint(jax.random.fold_in(rng, 1), (pairs,), 0, 1 << 20) % (slack + 1)
    lengths = lengths.at[1:1 + 2 * pairs:2].set(source_of - moved).at[2:2 + 2 * pairs:2].set(receiver + moved)
    return lengths[jax.random.permutation(jax.random.fold_in(rng, 2), amount)]


def centred(own_key, shape, deviation, reach, split=(), held_as=jnp.bfloat16):
    entries = jax.random.normal(own_key, shape, jnp.float32) * deviation
    if len(split) > 0:
        entries = steps_of(own_key, shape, split, -0.22, 0.18) * entries
    return jnp.clip(entries, min=-reach, max=reach).astype(held_as)


def setup_inputs(seed: int = 0) -> dict:
    arg_keys = jax.random.split(jax.random.key(seed), 18)
    return {
        "token_ids": touch_ends(skewed_ids(arg_keys[0], (MB, PACKS, PACK), VOCAB, 2), jax.random.fold_in(arg_keys[0], 3), 0, VOCAB - 1).astype(jnp.int32),
        "segment_ids": jax.vmap(lambda own: jnp.searchsorted(jnp.cumsum(uneven(own, 4, PACK, PACK // 2, 2)), jnp.arange(PACK), side="right"))(jax.random.split(arg_keys[1], MB * PACKS)).reshape((MB, PACKS, PACK)).astype(jnp.int32),
        "masked_pos": draw_masked_pos(jax.random.fold_in(arg_keys[17], 71), 0),
        "labels": touch_ends(skewed_ids(arg_keys[3], (MB, PACKS, MASK_DEV), VOCAB, 2), jax.random.fold_in(arg_keys[3], 3), 0, VOCAB - 1).astype(jnp.int32),
        "blocks": draw_blocks(jax.random.fold_in(arg_keys[17], 71), 0),
        "gains": jnp.clip(1.0 + 0.1 * jax.random.normal(arg_keys[5], (NG, D), jnp.float32), 0.5, 1.5),
        "embed": centred(arg_keys[6], (VOCAB, D), 0.09, 0.54, ((0, 8),), jnp.float32),
        "embed_m": centred(arg_keys[7], (VOCAB, D), 0.05, 0.3, ((0, 8),), jnp.float32),
        "embed_v": jnp.clip(jnp.exp(math.log(0.05) - 4.6051702 * jax.random.uniform(arg_keys[8], (VOCAB, D), jnp.float32) ** steps_of(arg_keys[8], (VOCAB, D), ((0, 8),), -0.2, 0.2)), 0.0005, 0.05),
        "gains_m": centred(arg_keys[9], (NG, D), 0.5, 3.0, ((1, 8),), jnp.float32),
        "gains_v": jnp.clip(jnp.exp(math.log(1.0) - 4.6051702 * jax.random.uniform(arg_keys[10], (NG, D), jnp.float32) ** steps_of(arg_keys[10], (NG, D), ((1, 8),), -0.2, 0.2)), 0.01, 1.0),
        "soap_m": centred(arg_keys[11], (SLOTS, D, D), 0.05, 0.3, ((0, 8),), jnp.float32),
        "soap_v": jnp.clip(jnp.exp(math.log(0.05) - 4.6051702 * jax.random.uniform(arg_keys[12], (SLOTS, D, D), jnp.float32) ** steps_of(arg_keys[12], (SLOTS, D, D), ((0, 8),), -0.2, 0.2)), 0.0005, 0.05),
        "left_basis": centred(arg_keys[13], (SLOTS, D, D), D ** -0.5, 0.25, ((0, 8),), jnp.float32),
        "right_basis": centred(arg_keys[14], (SLOTS, D, D), D ** -0.5, 0.25, ((0, 8),), jnp.float32),
        "block_slots": draw_block_slots(jax.random.fold_in(arg_keys[17], 71), 0),
        "step_count": jax.random.randint(arg_keys[16], (1,), 1, 21).astype(jnp.int32),
    }


@jax.custom_vjp
def low(v):
    return lax.optimization_barrier(v.astype(jnp.bfloat16)).astype(jnp.float32)

@jax.custom_vjp
def low_back(v):
    return v

def low_keep(v):
    return (low(v), None)

def low_pass(kept, grad):
    return (grad,)

def back_keep(v):
    return (v, None)

def back_low(kept, grad):
    return (low(grad),)
low.defvjp(low_keep, low_pass)
low_back.defvjp(back_keep, back_low)
norm_epsilon = 1e-05
beta_first = 0.9
beta_second = 0.99
adam_epsilon = 1e-08
step_rate = 0.04
weight_decay = 0.1
clip_ratio = 12.0
masked_score = -1e+30
highest = lax.Precision.HIGHEST

def both_ways(value):
    return low_back(low(value))

def layer_norm(inputs, gain_row):
    centre = inputs - lax.optimization_barrier(jnp.mean(inputs, axis=-1, keepdims=True))
    spread = lax.optimization_barrier(jnp.mean(centre * centre, axis=-1, keepdims=True))
    return centre * lax.rsqrt(spread + norm_epsilon) * gain_row

def head_slopes():
    return 2.0 ** (-8.0 * (jnp.arange(HEADS, dtype=jnp.float32) + 1.0) / HEADS)

def attention_part(stream, gain_row, projections, output_matrix, segments):
    normed = low(layer_norm(stream, gain_row))
    mixed_rows = both_ways(jnp.einsum('td,bde->tbe', normed, projections, precision=highest))
    queries = mixed_rows[:, 0].reshape(PACK, HEADS, HEAD_DIM)
    keys_all = mixed_rows[:, 1].reshape(PACK, HEADS, HEAD_DIM)
    values_all = mixed_rows[:, 2].reshape(PACK, HEADS, HEAD_DIM)
    places = jnp.arange(PACK, dtype=jnp.float32)
    distance = jnp.abs(places[:, None] - places[None, :])
    same_doc = segments[:, None] == segments[None, :]
    scores = jnp.einsum('qhd,khd->hqk', queries, keys_all, precision=highest) * HEAD_DIM ** (-0.5)
    scores = low_back(scores - head_slopes()[:, None, None] * distance[None])
    scores = jnp.where(same_doc[None], scores, masked_score)
    shifted = jnp.exp(scores - lax.optimization_barrier(jnp.max(scores, axis=-1, keepdims=True)))
    weights = low(shifted / lax.optimization_barrier(jnp.sum(shifted, axis=-1, keepdims=True)))
    attended = both_ways(jnp.einsum('hqk,khd->qhd', weights, values_all, precision=highest).reshape(PACK, D))
    return stream + low_back(jnp.dot(attended, output_matrix, precision=highest))

def feed_part(stream, gain_row, gate_up, down_blocks):
    pieces = FF // D
    normed = low(layer_norm(stream, gain_row))
    mixed_rows = both_ways(jnp.einsum('td,bde->tbe', normed, gate_up, precision=highest))
    hidden = low(jax.nn.gelu(mixed_rows[:, :pieces]) * mixed_rows[:, pieces:])
    return stream + low_back(jnp.einsum('tbf,bfd->td', hidden, down_blocks, precision=highest))

def pack_loss(weights, pack_ids, pack_segments, pack_positions, pack_labels):
    matrices, gain_rows, table_rows = weights
    pieces = FF // D
    per_layer = 4 + 3 * pieces
    embedded = low_back(jnp.take(table_rows, pack_ids, axis=0))
    stream = layer_norm(embedded, gain_rows[0])
    for layer_index in range(LAYERS):
        base_index = layer_index * per_layer
        stream = attention_part(stream, gain_rows[1 + 2 * layer_index], matrices[base_index:base_index + 3], matrices[base_index + 3], pack_segments)
        stream = feed_part(stream, gain_rows[2 + 2 * layer_index], matrices[base_index + 4:base_index + 4 + 2 * pieces], matrices[base_index + 4 + 2 * pieces:base_index + per_layer])
    final_rows = layer_norm(stream, gain_rows[2 * LAYERS + 1])
    picked = low(jnp.take(final_rows, pack_positions, axis=0))
    logits = low_back(jnp.dot(picked, table_rows.T, precision=highest))
    top_value = lax.optimization_barrier(jnp.max(logits, axis=-1, keepdims=True))
    lse_total = jnp.log(lax.optimization_barrier(jnp.sum(jnp.exp(logits - top_value), axis=-1))) + top_value[:, 0]
    target = jnp.take_along_axis(logits, pack_labels[:, None], axis=1)[:, 0]
    return jnp.sum(lse_total - target)

def whole_loss(weights, flat_ids, flat_segments, flat_positions, flat_labels):
    checked = jax.checkpoint(pack_loss)

    def visit_pack(running, pack_items):
        return (running + checked(weights, *pack_items), None)
    total_loss, ignored = lax.scan(visit_pack, jnp.zeros((), jnp.float32), (flat_ids, flat_segments, flat_positions, flat_labels))
    return total_loss

def adam_moments(moment_old, second_old, gradient, first_fix, second_fix):
    moment_new = beta_first * moment_old + (1.0 - beta_first) * gradient
    second_new = beta_second * second_old + (1.0 - beta_second) * gradient * gradient
    step_value = moment_new / first_fix / (jnp.sqrt(second_new / second_fix) + adam_epsilon)
    return (moment_new, second_new, step_value)

def reference(token_ids, segment_ids, masked_pos, labels, blocks, gains, embed, embed_m, embed_v, gains_m, gains_v, soap_m, soap_v, left_basis, right_basis, block_slots, step_count):
    flat_ids = token_ids.reshape(MB * PACKS, PACK)
    flat_segments = segment_ids.reshape(MB * PACKS, PACK)
    flat_positions = masked_pos.reshape(MB * PACKS, MASK_DEV)
    flat_labels = labels.reshape(MB * PACKS, MASK_DEV)

    def objective(matrices, gain_rows, table_rows):
        weights = (low(matrices), low(gain_rows), low(table_rows))
        return whole_loss(weights, flat_ids, flat_segments, flat_positions, flat_labels)
    total_loss, pullback = jax.vjp(objective, blocks, gains, embed)
    grad_blocks, grad_gains, grad_table = pullback(jnp.ones((), jnp.float32))
    squares = jnp.sum(grad_blocks * grad_blocks) + jnp.sum(grad_gains * grad_gains) + jnp.sum(grad_table * grad_table)
    grad_norm = jnp.sqrt(squares)
    clip_limit = clip_ratio * math.sqrt(MB * PACKS * MASK_DEV)
    factor = jnp.minimum(1.0, clip_limit / grad_norm)
    steps_done = step_count[0].astype(jnp.float32)
    first_fix = 1.0 - beta_first ** steps_done
    second_fix = 1.0 - beta_second ** steps_done
    embed_m_new, embed_v_new, table_step = adam_moments(embed_m, embed_v, factor * grad_table, first_fix, second_fix)
    embed_new = embed - step_rate * (table_step + weight_decay * embed)
    gains_m_new, gains_v_new, gain_step = adam_moments(gains_m, gains_v, factor * grad_gains, first_fix, second_fix)
    gains_new = gains - step_rate * gain_step
    left_slots = left_basis[block_slots]
    right_slots = right_basis[block_slots]
    rotated = jnp.einsum('bji,bjk->bik', left_slots, factor * grad_blocks, precision=highest)
    rotated = jnp.einsum('bik,bkl->bil', rotated, right_slots, precision=highest)
    moment_first, moment_second, rotated_step = adam_moments(soap_m[block_slots], soap_v[block_slots], rotated, first_fix, second_fix)
    rotated_back = jnp.einsum('bij,bjk->bik', left_slots, rotated_step, precision=highest)
    rotated_back = jnp.einsum('bik,blk->bil', rotated_back, right_slots, precision=highest)
    blocks_new = blocks - step_rate * (rotated_back + weight_decay * blocks)
    soap_m_new = soap_m.at[block_slots].set(moment_first)
    soap_v_new = soap_v.at[block_slots].set(moment_second)
    loss = (total_loss / (MB * PACKS * MASK_DEV)).reshape(1)
    return (loss, grad_norm.reshape(1), blocks_new, gains_new, embed_new, embed_m_new, embed_v_new, gains_m_new, gains_v_new, soap_m_new, soap_v_new, blocks_new.astype(jnp.bfloat16), embed_new.astype(jnp.bfloat16))
```

```python
from functools import partial
import math

import jax
import jax.numpy as jnp
from jax import lax
from jax.experimental import pallas as pl
from jax.experimental.pallas import tpu as pltpu
from jax.sharding import PartitionSpec as P

HEADS = 8
FF = 2048
LAYERS = 2

norm_epsilon = 1e-05
beta_first = 0.9
beta_second = 0.99
adam_epsilon = 1e-08
step_rate = 0.04
weight_decay = 0.1
clip_ratio = 12.0
masked_score = -1e30
bf16 = jnp.bfloat16
f32 = jnp.float32
highest = lax.Precision.HIGHEST
high = lax.Precision.HIGH
MESH = pl.DeviceIdType.MESH
ANY = pl.BlockSpec(memory_space=pl.ANY)
VMEM = pl.BlockSpec(memory_space=pltpu.VMEM)
CAPACITY = 128


def pick(table, index):
    out = jnp.int32(table[0])
    for k in range(1, len(table)):
        out = jnp.where(index == k, jnp.int32(table[k]), out)
    return out


def ring_order(n):
    nz = 4
    nx = n // nz
    order = []
    for x in range(nx):
        zs = range(1, nz) if x % 2 == 0 else range(nz - 1, 0, -1)
        order += [z * nx + x for z in zs]
    order += [x for x in range(nx - 1, -1, -1)]
    return order


class Place:
    def __init__(self, n_rep, n_fsdp):
        self.r = lax.axis_index("rep")
        self.f = lax.axis_index("fsdp")
        self.n_rep, self.n = n_rep, n_fsdp
        self.c = lax.rem(self.r, 2)
        self.y = self.r // 2
        self.order = ring_order(n_fsdp)
        spot = [self.order.index(k) for k in range(n_fsdp)]
        self.pos = pick(spot, self.f)
        self.core = (self.r + 1 - 2 * self.c, self.f)
        self.next = (self.r, self.at(1))
        self.prev = (self.r, self.at(-1))

    def at(self, step):
        return pick(self.order, lax.rem(self.pos + step + 2 * self.n, self.n))


def enter(peers):
    barrier = pltpu.get_barrier_semaphore()
    for peer in peers:
        pl.semaphore_signal(barrier, inc=1, device_id=peer, device_id_type=MESH)
    pl.semaphore_wait(barrier, len(peers))


def remote(src, dst, send, recv, peer):
    return pltpu.make_async_remote_copy(
        src_ref=src, dst_ref=dst, send_sem=send, recv_sem=recv, device_id=peer, device_id_type=MESH
    )


def params(cid, limit=None):
    return pltpu.CompilerParams(
        collective_id=cid, has_side_effects=True, vmem_limit_bytes=limit
    )


def group_kernel(n_rep, n, spread, x_ref, o_ref, send, recv):
    here = Place(n_rep, n)
    me = here.f
    others = [lax.rem(me + k, n) for k in range(1, n)]
    enter([(here.r, o) for o in others])
    copies = []
    for k, o in enumerate(others):
        src = x_ref.at[o] if spread else x_ref
        cp = remote(src, o_ref.at[me], send.at[k], recv.at[k], (here.r, o))
        cp.start()
        copies.append(cp)
    o_ref[me] = x_ref[me] if spread else x_ref[...]
    for cp in copies:
        cp.wait()


def group_exchange(mesh_sizes, cid, x, spread):
    n_rep, n = mesh_sizes
    shape = x.shape if spread else (n,) + x.shape
    return pl.pallas_call(
        partial(group_kernel, n_rep, n, spread),
        out_shape=jax.ShapeDtypeStruct(shape, x.dtype),
        in_specs=[VMEM],
        out_specs=VMEM,
        scratch_shapes=[pltpu.SemaphoreType.DMA((n - 1,)), pltpu.SemaphoreType.DMA((n - 1,))],
        compiler_params=params(cid),
        name=f"group_{cid}",
    )(x)


def ask_kernel(n_rep, n, w_ref, facts_ref, gains_ref, asked, facts, gains, most, held, got, send, recv, send2, recv2):
    here = Place(n_rep, n)
    ypeer = (lax.rem(here.r + 2, 4), here.f)
    me = here.f
    others = [lax.rem(me + k, n) for k in range(1, n)]
    enter([(here.r, o) for o in others] + [here.core, ypeer])
    copies = []
    for k, o in enumerate(others):
        peer = (here.r, o)
        copies.append(remote(facts_ref, facts.at[me], send.at[0, k], recv.at[0, k], peer))
        copies.append(remote(w_ref.at[o], asked.at[me], send.at[1, k], recv.at[1, k], peer))
        copies.append(remote(gains_ref, gains.at[me], send.at[2, k], recv.at[2, k], peer))
    for cp in copies:
        cp.start()
    asked[me] = w_ref[me]
    facts[me] = facts_ref[...]
    gains[me] = gains_ref[...]
    for cp in copies:
        cp.wait_recv()
    top = facts[0]
    for k in range(1, n):
        top = jnp.maximum(top, facts[k])
    held[0] = top
    first = remote(held.at[0], got.at[0], send2.at[0], recv2.at[0], here.core)
    first.start()
    first.wait_recv()
    held[1] = jnp.maximum(top, got[0])
    second = remote(held.at[1], got.at[1], send2.at[1], recv2.at[1], ypeer)
    second.start()
    second.wait_recv()
    most[...] = jnp.maximum(held[1], got[1])
    first.wait_send()
    second.wait_send()
    for cp in copies:
        cp.wait_send()


def ask_group(mesh_sizes, cid, wanted, facts, gains):
    n_rep, n = mesh_sizes
    dma = pltpu.SemaphoreType.DMA
    return pl.pallas_call(
        partial(ask_kernel, n_rep, n),
        out_shape=[
            jax.ShapeDtypeStruct(wanted.shape, wanted.dtype),
            jax.ShapeDtypeStruct((n,) + facts.shape, facts.dtype),
            jax.ShapeDtypeStruct((n,) + gains.shape, gains.dtype),
            jax.ShapeDtypeStruct(facts.shape, facts.dtype),
        ],
        in_specs=[VMEM] * 3,
        out_specs=[VMEM] * 4,
        scratch_shapes=[pltpu.VMEM((2,) + facts.shape, facts.dtype)] * 2
        + [dma((3, n - 1)), dma((3, n - 1)), dma((2,)), dma((2,))],
        compiler_params=params(cid),
        name="ask_group",
    )(wanted, facts, gains)


def weights_kernel(n_rep, n, half, shared, x_ref, o_ref, ring_s, ring_r, core_s, core_r, y_s, y_r, over_s, over_r):
    here = Place(n_rep, n)
    ypeer = (lax.rem(here.r + 2, 4), here.f)
    rows = x_ref.shape[1]
    alone = (half - shared) // 2
    enter([here.next, here.prev, here.core, ypeer])
    mine = pl.ds(here.c * half + here.y * alone, alone + shared)
    given = pl.ds(here.c * half + here.y * (alone + shared), alone)
    taken = pl.ds(here.c * half + (1 - here.y) * (alone + shared), alone)
    hops = n // 2
    copies, sends = [], []

    def rows_of(origin, way, s):
        if s == hops - 1:
            return pl.ds(pl.multiple_of(origin * rows + way * (rows // 2), rows // 2), rows // 2)
        return pl.ds(pl.multiple_of(origin * rows, rows), rows)

    own = remote(
        x_ref, o_ref.at[:, rows_of(here.f, 0, -1)], core_s.at[0, 0], core_r.at[0, 0], here.core
    )
    own.start()
    copies.append(own)
    waiting = [None, None]
    across = []

    def pass_on(way, s):
        waiting[way].wait_recv()
        where = rows_of(here.at(-s - 1 if way == 0 else s + 1), way, s)
        held = o_ref.at[given, where]
        cp = remote(held, held, y_s.at[way, s], y_r.at[way, s], ypeer)
        cp.start()
        across.append((cp, o_ref.at[taken, where], way, s))
        held = o_ref.at[mine, where]
        cp = remote(held, held, core_s.at[way, s + 1], core_r.at[way, s + 1], here.core)
        cp.start()
        copies.append(cp)

    for s in range(hops):
        for way in range(2):
            if s > 0:
                pass_on(way, s - 1)
            origin = here.at(-s if way == 0 else s)
            where = rows_of(origin, way, s)
            if s == 0:
                src = x_ref.at[mine]
            else:
                src = o_ref.at[mine, where]
            cp = remote(
                src,
                o_ref.at[mine, where],
                ring_s.at[way, s],
                ring_r.at[way, s],
                here.next if way == 0 else here.prev,
            )
            cp.start()
            waiting[way] = cp
            sends.append(cp)
    for way in range(2):
        pass_on(way, hops - 1)
    for cp, held, way, s in across:
        cp.wait_recv()
        over = remote(held, held, over_s.at[way, s], over_r.at[way, s], here.core)
        over.start()
        copies.append(over)
        sends.append(cp)
    for cp in sends:
        cp.wait_send()
    for cp in copies:
        cp.wait()


def gather_weights(mesh_sizes, cid, shard):
    n_rep, n = mesh_sizes
    count, rows, width = shard.shape
    half = count // 2
    dma = pltpu.SemaphoreType.DMA
    return pl.pallas_call(
        partial(weights_kernel, n_rep, n, half, half - 2 * (half // 3)),
        out_shape=jax.ShapeDtypeStruct((count, rows * n, width), shard.dtype),
        in_specs=[ANY],
        out_specs=ANY,
        scratch_shapes=[
            dma((2, n // 2)),
            dma((2, n // 2)),
            dma((2, n // 2 + 1)),
            dma((2, n // 2 + 1)),
            dma((2, n // 2)),
            dma((2, n // 2)),
            dma((2, n // 2)),
            dma((2, n // 2)),
        ],
        compiler_params=params(cid),
        name="gather_weights",
    )(shard)


def ring_rows_kernel(n_rep, n, x_ref, o_ref, send, recv):
    here = Place(n_rep, n)
    enter([here.next, here.prev])
    rows = x_ref.shape[0]
    hops = n // 2
    copies = []
    waiting = [None, None]
    for s in range(hops):
        for way in range(2):
            peer = here.next if way == 0 else here.prev
            origin = here.at(-s if way == 0 else s)
            if s > 0:
                waiting[way].wait_recv()
            window = pl.ds(0, rows)
            if s == hops - 1:
                window = pl.ds(way * (rows // 2), rows // 2)
            src = x_ref.at[window] if s == 0 else o_ref.at[origin, window]
            cp = remote(src, o_ref.at[origin, window], send.at[way, s], recv.at[way, s], peer)
            cp.start()
            waiting[way] = cp
            copies.append(cp)
    o_ref[here.f] = x_ref[...]
    for way in range(2):
        waiting[way].wait_recv()
    for cp in copies:
        cp.wait_send()


def ring_rows(mesh_sizes, cid, x):
    n_rep, n = mesh_sizes
    return pl.pallas_call(
        partial(ring_rows_kernel, n_rep, n),
        out_shape=jax.ShapeDtypeStruct((n,) + x.shape, x.dtype),
        in_specs=[VMEM],
        out_specs=VMEM,
        scratch_shapes=[pltpu.SemaphoreType.DMA((2, n // 2)), pltpu.SemaphoreType.DMA((2, n // 2))],
        compiler_params=params(cid),
        name="ring_rows",
    )(x)


def reduce_kernel(
    n_rep, n, half, table_rows, each, *refs
):
    g_refs, refs = refs[: 2 * each], refs[2 * each :]
    (
    t_ref, o_ref, to_ref, sq_ref,
    own, part, got, fin, ysend, ygot, town, tpart, tsend, tgot,
    load_s, core_s, core_r, ring_s, ring_r, y_s, y_r, tload, tcs, tcr, tys, tyr, tos, tor,
    ) = refs
    here = Place(n_rep, n)
    c, y = here.c, here.y
    ypeer = (lax.rem(here.r + 2, 4), here.f)
    other_c, other_y = 1 - c, 1 - y
    enter([here.next, here.prev, here.core, ypeer])
    far = n // 2

    tl = pltpu.make_async_copy(t_ref.at[pl.ds(c * 2, 2)], town, tload)
    tl.start()
    tc = remote(t_ref.at[pl.ds(other_c * 2, 2)], tpart, tcs, tcr, here.core)
    tc.start()

    spots = {(0, far): 0, (1, far): 0}
    for d in range(far - 1, 0, -1):
        spots[0, d] = 1 + 2 * (far - 1 - d)
        spots[1, d] = 2 + 2 * (far - 1 - d)
    spots[0, 0] = spots[1, 0] = n - 1
    loads, cores = {}, {}
    done = set()
    for (way, d), spot in sorted(spots.items(), key=lambda item: item[1]):
        if spot in done:
            continue
        done.add(spot)
        to = here.f if d == 0 else here.at(d if way == 0 else -d)
        for h in (way, 1 - way):
            loads[spot, h], cores[spot, h] = [], []
            for j in range(each):
                g_ref = g_refs[h * each + j]
                into = pl.ds(j * (half // each), half // each)
                ld = pltpu.make_async_copy(g_ref.at[:, to, :, c], own.at[spot, h, into], load_s.at[spot, h, j])
                ld.start()
                loads[spot, h].append(ld)
                cp = remote(
                    g_ref.at[:, to, :, other_c],
                    part.at[spot, h, into],
                    core_s.at[spot, h, j],
                    core_r.at[spot, h, j],
                    here.core,
                )
                cp.start()
                cores[spot, h].append(cp)

    def ready(spot, h):
        for j in range(each):
            loads[spot, h][j].wait()
            cores[spot, h][j].wait_recv()

    ring = {}

    def came(way, h, s):
        return got.at[way, h, s]

    def lane(way, h, s):
        d = far - s
        spot = spots[way, d]
        ready(spot, h)
        before = ring.get((way, h, s - 1))
        if before is not None:
            before.wait_recv()
        target = own.at[spot, h]

        @pl.loop(0, half)
        def _(b):
            for k in range(2):
                total = own[spot, h, b, k].astype(f32) + part[spot, h, b, k].astype(f32)
                if before is not None:
                    total = total + came(way, h, s - 1)[b, k].astype(f32)
                target[b, k] = total.astype(target.dtype)

        cp = remote(
            target, came(way, h, s), ring_s.at[way, h, s], ring_r.at[way, h, s], here.next if way == 0 else here.prev
        )
        cp.start()
        ring[way, h, s] = cp

    step_rows = 48
    for s in range(far):
        for h_turn in range(2):
            for way in range(2):
                h = way if h_turn == 1 else 1 - way
                if s == 0 and h_turn == 0:
                    continue
                if s == 1 and h_turn == 0:
                    continue
                lane(way, h, s)
        if s == 0:
            for way in range(2):
                lane(way, 1 - way, 1)
            tl.wait()
            tc.wait_recv()

            @pl.loop(0, table_rows // step_rows)
            def _(i):
                at = pl.ds(pl.multiple_of(i * step_rows, step_rows), step_rows)
                town[y, at] = town[y, at] + tpart[y, at]
                tsend[at] = (town[other_y, at] + tpart[other_y, at]).astype(bf16)

            ty = remote(tsend, tgot, tys, tyr, ypeer)
            ty.start()
        if s == 2:
            ty.wait_recv()

            def add(i, acc):
                at = pl.ds(pl.multiple_of(i * step_rows, step_rows), step_rows)
                total = town[y, at] + tgot[at].astype(f32)
                town[y, at] = total
                square = total * total
                for k in range(step_rows // 8):
                    acc = acc + square[k * 8 : k * 8 + 8]
                return acc

            sq_ref[0] = lax.fori_loop(0, table_rows // step_rows, add, jnp.zeros((8, tgot.shape[1]), f32))
            mine = c * 2 + y
            near = c * 2 + other_y
            tkeep = pltpu.make_async_copy(town.at[y], to_ref.at[mine], tload)
            tkeep.start()
            t0 = remote(town.at[y], to_ref.at[mine], tos.at[0], tor.at[0], ypeer)
            t1 = remote(town.at[y], to_ref.at[mine], tos.at[1], tor.at[1], here.core)
            t0.start()
            t1.start()
    t0.wait_recv()
    t2 = remote(to_ref.at[near], to_ref.at[near], tos.at[2], tor.at[2], here.core)
    t2.start()
    ys = []
    spot = spots[0, 0]
    for h in range(2):
        ready(spot, h)
        for way in range(2):
            ring[way, h, far - 1].wait_recv()

        @pl.loop(0, half)
        def _(b, h=h):
            for keep in range(2):
                k = y if keep else other_y
                total = own[spot, h, b, k].astype(f32) + part[spot, h, b, k].astype(f32)
                for way in range(2):
                    total = total + got[way, h, far - 1, b, k].astype(f32)
                if keep:
                    fin[h, b] = total
                else:
                    ysend[h, b] = total.astype(bf16)

        cp = remote(ysend.at[h], ygot.at[h], y_s.at[h], y_r.at[h], ypeer)
        cp.start()
        ys.append(cp)

    acc = jnp.zeros((8, fin.shape[-1]), f32)
    for h in range(2):
        ys[h].wait_recv()

        def last(b, acc, h=h):
            total = fin[h, b] + ygot[h, b].astype(f32)
            o_ref[h * half + b] = total
            square = total * total
            return acc + square[:8] + square[8:]

        acc = lax.fori_loop(0, half, last, acc)
    sq_ref[1] = acc
    for cp in ys:
        cp.wait_send()
    for cp in ring.values():
        cp.wait_send()
    for group in cores.values():
        for cp in group:
            cp.wait_send()
    tc.wait_send()
    ty.wait_send()
    tkeep.wait()
    t0.wait_send()
    t1.wait()
    t2.wait()


def reduce_gradients(mesh_sizes, cid, grads, table):
    n_rep, n = mesh_sizes
    _, depth, width = grads[0].shape
    count = sum(g.shape[0] for g in grads)
    half = count // 2
    each = len(grads) // 2
    far = n // 2
    table_rows = table.shape[1]
    views = [g.reshape(g.shape[0], n, 2, 2, 16, width) for g in grads]
    dma = pltpu.SemaphoreType.DMA
    piece = (half, 2, 16, width)
    return pl.pallas_call(
        partial(reduce_kernel, n_rep, n, half, table_rows, each),
        out_shape=[
            jax.ShapeDtypeStruct((count, 16, width), f32),
            jax.ShapeDtypeStruct(table.shape, f32),
            jax.ShapeDtypeStruct((2, 8, width), f32),
        ],
        in_specs=[ANY] * (2 * each + 1),
        out_specs=[VMEM, ANY, VMEM],
        scratch_shapes=[
            pltpu.VMEM((n, 2) + piece, bf16),
            pltpu.VMEM((n, 2) + piece, bf16),
            pltpu.VMEM((2, 2, far) + piece, bf16),
            pltpu.VMEM((2, half, 16, width), f32),
            pltpu.VMEM((2, half, 16, width), bf16),
            pltpu.VMEM((2, half, 16, width), bf16),
            pltpu.VMEM((2, table_rows, width), f32),
            pltpu.VMEM((2, table_rows, width), f32),
            pltpu.VMEM((table_rows, width), bf16),
            pltpu.VMEM((table_rows, width), bf16),
            dma((n, 2, each)),
            dma((n, 2, each)),
            dma((n, 2, each)),
            dma((2, 2, far)),
            dma((2, 2, far)),
            dma((2,)),
            dma((2,)),
            dma,
            dma,
            dma,
            dma,
            dma,
            dma((3,)),
            dma((3,)),
        ],
        compiler_params=params(cid, 60 << 20),
        name="reduce_gradients",
    )(*views, table)


def rows_kernel(n_rep, n, x_ref, o_ref, held, got, send, recv):
    here = Place(n_rep, n)
    enter([here.next, here.prev])
    far = n // 2
    rows = x_ref.shape[1] // 2
    ring = {}

    def lane(way, h, s):
        d = far - s
        q = here.at(d if way == 0 else -d)
        before = ring.get((way, h, s - 1))
        if before is None:
            source = x_ref.at[q, pl.ds(h * rows, rows)]
        else:
            before.wait_recv()
            total = x_ref[q, pl.ds(h * rows, rows)].astype(f32) + got[way, h, s - 1].astype(f32)
            held[way, h, s - 1] = total.astype(held.dtype)
            source = held.at[way, h, s - 1]
        cp = remote(
            source, got.at[way, h, s], send.at[way, h, s], recv.at[way, h, s], here.next if way == 0 else here.prev
        )
        cp.start()
        ring[way, h, s] = cp

    for s in range(far):
        for turn in range(2):
            for way in range(2):
                h = way if turn == 1 else 1 - way
                if turn == 0 and s < 2:
                    continue
                lane(way, h, s)
        if s == 0:
            for way in range(2):
                lane(way, 1 - way, 1)
    for h in range(2):
        for way in range(2):
            ring[way, h, far - 1].wait_recv()
        at = pl.ds(h * rows, rows)
        total = x_ref[here.f, at].astype(f32)
        for way in range(2):
            total = total + got[way, h, far - 1].astype(f32)
        o_ref[at] = total
    for cp in ring.values():
        cp.wait_send()


def reduce_rows(mesh_sizes, cid, x):
    n_rep, n = mesh_sizes
    _, rows, width = x.shape
    far = n // 2
    dma = pltpu.SemaphoreType.DMA
    return pl.pallas_call(
        partial(rows_kernel, n_rep, n),
        out_shape=jax.ShapeDtypeStruct((rows, width), f32),
        in_specs=[VMEM],
        out_specs=VMEM,
        scratch_shapes=[
            pltpu.VMEM((2, 2, far - 1, rows // 2, width), x.dtype),
            pltpu.VMEM((2, 2, far, rows // 2, width), x.dtype),
            dma((2, 2, far)),
            dma((2, 2, far)),
        ],
        compiler_params=params(cid, 24 << 20),
        name="reduce_rows",
    )(x)


def total_kernel(n_rep, n, x_ref, o_ref, core_got, both, y_got, four, got, send, recv):
    here = Place(n_rep, n)
    ypeer = (lax.rem(here.r + 2, 4), here.f)
    others = [lax.rem(here.f + k, n) for k in range(1, n)]
    enter([(here.r, o) for o in others] + [here.core, ypeer])
    first = remote(x_ref, core_got, send.at[0], recv.at[0], here.core)
    first.start()
    first.wait_recv()
    both[...] = x_ref[...] + core_got[...]
    second = remote(both, y_got, send.at[1], recv.at[1], ypeer)
    second.start()
    second.wait_recv()
    four[...] = both[...] + y_got[...]
    copies = []
    for k, o in enumerate(others):
        cp = remote(four, got.at[here.f], send.at[2 + k], recv.at[2 + k], (here.r, o))
        cp.start()
        copies.append(cp)
    got[here.f] = four[...]
    for cp in copies:
        cp.wait_recv()
    total = got[0]
    for k in range(1, n):
        total = total + got[k]
    o_ref[...] = total
    first.wait_send()
    second.wait_send()
    for cp in copies:
        cp.wait_send()


def total_everyone(mesh_sizes, cid, x):
    n_rep, n = mesh_sizes
    dma = pltpu.SemaphoreType.DMA
    like = pltpu.VMEM(x.shape, x.dtype)
    return pl.pallas_call(
        partial(total_kernel, n_rep, n),
        out_shape=jax.ShapeDtypeStruct(x.shape, x.dtype),
        in_specs=[VMEM],
        out_specs=VMEM,
        scratch_shapes=[like] * 4 + [pltpu.VMEM((n,) + x.shape, x.dtype), dma((n + 1,)), dma((n + 1,))],
        compiler_params=params(cid),
        name=f"total_{cid}",
    )(x)


def slots_kernel(n_rep, n, to_slots, x_ref, o_ref, keep, a_s, a_r, f_s, f_r):
    here = Place(n_rep, n)
    ypeer = (lax.rem(here.r + 2, 4), here.f)
    me = here.f
    others = [lax.rem(me + k, n) for k in range(1, n)]
    enter([(here.r, o) for o in others] + [here.core, ypeer])

    def spot(source, r):
        return o_ref.at[:, source, r] if to_slots else o_ref.at[source, :, r]

    copies = []
    for k, o in enumerate(others):
        cp = remote(x_ref.at[o], spot(me, here.r), a_s.at[k], a_r.at[k], (here.r, o))
        cp.start()
        copies.append(cp)
    own = pltpu.make_async_copy(x_ref.at[me], spot(me, here.r), keep)
    own.start()
    sends, far = [], []
    for k in range(n):
        source = me if k == 0 else lax.rem(me - k + n, n)
        if k == 0:
            own.wait()
        else:
            copies[k - 1].wait_recv()
        held = spot(source, here.r)
        over = remote(held, held, f_s.at[0, k], f_r.at[0, k], ypeer)
        over.start()
        beside = remote(held, held, f_s.at[1, k], f_r.at[1, k], here.core)
        beside.start()
        far.append((over, source))
        sends.append(beside)
    yr = lax.rem(here.r + 2, 4)
    for k, (over, source) in enumerate(far):
        over.wait_recv()
        src = me if k == 0 else lax.rem(me - k + n, n)
        held = spot(src, yr)
        beside = remote(held, held, f_s.at[2, k], f_r.at[2, k], here.core)
        beside.start()
        sends.append(beside)
    for cp in copies:
        cp.wait_send()
    for over, _ in far:
        over.wait_send()
    for cp in sends:
        cp.wait()


def exchange_slots(mesh_sizes, cid, x, to_slots):
    n_rep, n = mesh_sizes
    _, cap, rows, width = x.shape
    shape = (cap, n, 4, rows, width) if to_slots else (n, cap, 4, rows, width)
    dma = pltpu.SemaphoreType.DMA
    return pl.pallas_call(
        partial(slots_kernel, n_rep, n, to_slots),
        out_shape=jax.ShapeDtypeStruct(shape, x.dtype),
        in_specs=[VMEM],
        out_specs=ANY,
        scratch_shapes=[dma, dma((n - 1,)), dma((n - 1,)), dma((3, n)), dma((3, n))],
        compiler_params=params(cid),
        name=f"slots_{cid}",
    )(x)


def layer_norm(inputs, gain_row):
    centre = inputs - jnp.mean(inputs, axis=-1, keepdims=True)
    spread = jnp.mean(centre * centre, axis=-1, keepdims=True)
    return centre * lax.rsqrt(spread + norm_epsilon) * gain_row


def adam_moments(moment_old, second_old, gradient, first_fix, second_fix):
    moment_new = beta_first * moment_old + (1.0 - beta_first) * gradient
    second_new = beta_second * second_old + (1.0 - beta_second) * gradient * gradient
    step_value = moment_new / first_fix / (jnp.sqrt(second_new / second_fix) + adam_epsilon)
    return (moment_new, second_new, step_value)


def head_slopes(head_count):
    return 2.0 ** (-8.0 * (jnp.arange(head_count, dtype=f32) + 1.0) / head_count)


NT = (((1,), (1,)), ((), ()))
TN = (((0,), (0,)), ((), ()))
masked_distance = 1e33


def mm(a, b, dims=None):
    if dims is None:
        return jnp.dot(a, b, preferred_element_type=f32)
    return lax.dot_general(a, b, dims, preferred_element_type=f32)


def norm_parts(x):
    centre = x - jnp.mean(x, axis=-1, keepdims=True)
    spread = jnp.mean(centre * centre, axis=-1, keepdims=True)
    rstd = lax.rsqrt(spread + norm_epsilon)
    return centre * rstd, rstd


def norm_back(x, gain, grad):
    hat, rstd = norm_parts(x)
    inner = grad * gain
    back = inner - jnp.mean(inner, axis=-1, keepdims=True) - hat * jnp.mean(inner * hat, axis=-1, keepdims=True)
    return rstd * back, grad * hat


def fold8(x):
    total = x[:8]
    for k in range(1, x.shape[0] // 8):
        total = total + x[k * 8 : k * 8 + 8]
    return total


def pair_bias(seg_row, seg_col, bias):
    length = bias.shape[0]
    i = lax.broadcasted_iota(jnp.int32, (length, length), 0)
    j = lax.broadcasted_iota(jnp.int32, (length, length), 1)
    apart = jnp.abs(i - j).astype(f32)
    bias[...] = jnp.where(seg_col == seg_row, apart, masked_distance)


def attend_kernel(slopes, x, gain, w, seg_row, seg_col, y, a, qkv, o, lse, bias):
    pair = pl.program_id(1)
    length, width = x.shape
    half = width // HEADS
    two = 2 * half
    rows = ROWS

    @pl.when(pair == 0)
    def _():
        pair_bias(seg_row[0], seg_col[0], bias)

        @pl.loop(0, length // rows)
        def _(i):
            at = pl.ds(pl.multiple_of(i * rows, rows), rows)
            hat, _ = norm_parts(x[at])
            low = (hat * gain[...]).astype(bf16)
            a[at] = low
            for k in range(3):
                part = mm(low, w[k])
                if k == 0:
                    part = part.astype(bf16).astype(f32) * half ** (-0.5)
                qkv[at, k * width : (k + 1) * width] = part.astype(bf16)

    lanes = pl.ds(pl.multiple_of(pair * two, two), two)
    q = qkv[:, pl.ds(pl.multiple_of(pair * two, two), two)]
    k = qkv[:, pl.ds(pl.multiple_of(width + pair * two, two), two)]
    v = qkv[:, pl.ds(pl.multiple_of(2 * width + pair * two, two), two)]
    v_t = v.astype(f32).T.astype(bf16)
    left = lax.broadcasted_iota(jnp.int32, (length, two), 1) < half
    zero = jnp.zeros_like(q)
    out = []
    for e in range(2):
        slope = slopes[2 * pair + e]
        q_e = jnp.where(left, q, zero) if e == 0 else jnp.where(left, zero, q)
        s = mm(k, q_e, NT) - slope * bias[...]
        top = jnp.max(s, axis=0, keepdims=True)
        p = jnp.exp(s - top)
        total = jnp.sum(p, axis=0, keepdims=True)
        low = (p * (1.0 / total)).astype(bf16)
        out.append(mm(v_t, low))
        lse[0, pl.ds(2 * pair + e, 1)] = top + jnp.log(total)
    upper = lax.broadcasted_iota(jnp.int32, (two, length), 0) < half
    o[:, lanes] = jnp.where(upper, out[0], out[1]).T.astype(bf16)

    @pl.when(pair == pl.num_programs(1) - 1)
    def _():
        @pl.loop(0, length // rows)
        def _(i):
            at = pl.ds(pl.multiple_of(i * rows, rows), rows)
            y[at] = x[at] + mm(o[at], w[3])


def attend(x, gain, weights, layer, seg):
    packs, length = seg.shape
    tokens, width = x.shape
    per_layer4 = weights.shape[0] // LAYERS // 4
    slopes = head_slopes(HEADS)
    whole = lambda shape: pl.BlockSpec(shape, lambda m, p: (m,) + (0,) * (len(shape) - 1))
    fixed = lambda shape, at: pl.BlockSpec(shape, lambda m, p: at)
    return pl.pallas_call(
        attend_kernel,
        grid=(packs, HEADS // 2),
        in_specs=[
            pl.BlockSpec(memory_space=pltpu.SMEM),
            whole((length, width)),
            fixed((1, width), (0, 0)),
            fixed((4, width, width), (per_layer4 * layer, 0, 0)),
            whole((1, 1, length)),
            whole((1, length, 1)),
        ],
        out_specs=[
            whole((length, width)),
            whole((length, width)),
            whole((length, 3 * width)),
            whole((length, width)),
            whole((1, HEADS, length)),
        ],
        out_shape=[
            jax.ShapeDtypeStruct((tokens, width), f32),
            jax.ShapeDtypeStruct((tokens, width), bf16),
            jax.ShapeDtypeStruct((tokens, 3 * width), bf16),
            jax.ShapeDtypeStruct((tokens, width), bf16),
            jax.ShapeDtypeStruct((packs, HEADS, length), f32),
        ],
        scratch_shapes=[pltpu.VMEM((length, length), f32)],
        compiler_params=pltpu.CompilerParams(vmem_limit_bytes=48 << 20),
        name="attend",
    )(slopes, x, gain.reshape(1, width), weights, seg.reshape(packs, 1, length), seg.reshape(packs, length, 1))


def attend_back_kernel(
    slopes, dx, x, gain, w, a, qkv, o, lse, seg_row, seg_col, new, dgain, gw, bias, do, dqkv, acc
):
    pack, pair = pl.program_id(0), pl.program_id(1)
    length, width = x.shape
    half = width // HEADS
    two = 2 * half
    rows = ROWS

    @pl.when(pair == 0)
    def _():
        pair_bias(seg_row[0], seg_col[0], bias)

        @pl.loop(0, length // rows)
        def _(i):
            at = pl.ds(pl.multiple_of(i * rows, rows), rows)
            do[at] = mm(dx[at].astype(bf16), w[3], NT).astype(bf16)

        part = mm(o[...], dx[...].astype(bf16), TN)

        @pl.when(pack == 0)
        def _():
            acc[3] = part

        @pl.when(pack > 0)
        def _():
            acc[3] += part

    lanes = [pl.ds(pl.multiple_of(n * width + pair * two, two), two) for n in range(3)]
    q, k, v = [qkv[:, at] for at in lanes]
    do_p = do[:, lanes[0]]
    k_t = k.astype(f32).T.astype(bf16)
    left = lax.broadcasted_iota(jnp.int32, (length, two), 1) < half
    upper = lax.broadcasted_iota(jnp.int32, (two, length), 0) < half
    zero = jnp.zeros_like(q)
    dq, dk, dv = [], [], []
    for e in range(2):
        slope = slopes[2 * pair + e]
        keep = (lambda t: jnp.where(left, t, zero)) if e == 0 else (lambda t: jnp.where(left, zero, t))
        s = mm(k, keep(q), NT) - slope * bias[...]
        p = jnp.exp(s - lse[0, pl.ds(2 * pair + e, 1)])
        dp = mm(v, keep(do_p), NT)
        inner = jnp.sum(p * dp, axis=0, keepdims=True)
        ds = (p * (dp - inner)).astype(bf16)
        dv.append(mm(p.astype(bf16), do_p))
        dk.append(mm(ds, q))
        dq.append(mm(k_t, ds))
    dqkv[:, lanes[0]] = (jnp.where(upper, dq[0], dq[1]).T * half ** (-0.5)).astype(bf16)
    dqkv[:, lanes[1]] = jnp.where(left, dk[0], dk[1]).astype(bf16)
    dqkv[:, lanes[2]] = jnp.where(left, dv[0], dv[1]).astype(bf16)

    @pl.when(pair == pl.num_programs(1) - 1)
    def _():
        def chunk(i, total):
            at = pl.ds(pl.multiple_of(i * rows, rows), rows)
            da = mm(dqkv[at, :width], w[0], NT)
            da = da + mm(dqkv[at, width : 2 * width], w[1], NT)
            da = da + mm(dqkv[at, 2 * width :], w[2], NT)
            back, extra = norm_back(x[at], gain[...], da)
            new[at] = dx[at] + back
            return total + fold8(extra)

        dgain[0] = lax.fori_loop(0, length // rows, chunk, jnp.zeros((8, width), f32))
        for n in range(3):
            part = mm(a[...], dqkv[:, n * width : (n + 1) * width], TN)

            @pl.when(pack == 0)
            def _(part=part, n=n):
                acc[n] = part

            @pl.when(pack > 0)
            def _(part=part, n=n):
                acc[n] += part

    @pl.when((pair == pl.num_programs(1) - 1) & (pack == pl.num_programs(0) - 1))
    def _():
        for n in range(4):
            gw[n] = acc[n].astype(bf16)


def attend_back(dx, x, gain, weights, layer, seg, kept):
    a, qkv, o, lse = kept
    packs, length = seg.shape
    tokens, width = x.shape
    per_layer4 = weights.shape[0] // LAYERS // 4
    whole = lambda shape: pl.BlockSpec(shape, lambda m, p: (m,) + (0,) * (len(shape) - 1))
    fixed = lambda shape, at: pl.BlockSpec(shape, lambda m, p: at)
    return pl.pallas_call(
        attend_back_kernel,
        grid=(packs, HEADS // 2),
        in_specs=[
            pl.BlockSpec(memory_space=pltpu.SMEM),
            whole((length, width)),
            whole((length, width)),
            fixed((1, width), (0, 0)),
            fixed((4, width, width), (per_layer4 * layer, 0, 0)),
            whole((length, width)),
            whole((length, 3 * width)),
            whole((length, width)),
            whole((1, HEADS, length)),
            whole((1, 1, length)),
            whole((1, length, 1)),
        ],
        out_specs=[
            whole((length, width)),
            whole((1, 8, width)),
            fixed((4, width, width), (0, 0, 0)),
        ],
        out_shape=[
            jax.ShapeDtypeStruct((tokens, width), f32),
            jax.ShapeDtypeStruct((packs, 8, width), f32),
            jax.ShapeDtypeStruct((4, width, width), bf16),
        ],
        scratch_shapes=[
            pltpu.VMEM((length, length), f32),
            pltpu.VMEM((length, width), bf16),
            pltpu.VMEM((length, 3 * width), bf16),
            pltpu.VMEM((4, width, width), f32),
        ],
        compiler_params=pltpu.CompilerParams(vmem_limit_bytes=56 << 20),
        name="attend_back",
    )(
        head_slopes(HEADS),
        dx,
        x,
        gain.reshape(1, width),
        weights,
        a,
        qkv,
        o,
        lse,
        seg.reshape(packs, 1, length),
        seg.reshape(packs, length, 1),
    )


ROWS = 512
gelu_c = math.sqrt(2.0 / math.pi)


def feed_kernel(x, gain, wg, wu, wd, y, f, gate, up):
    k = pl.program_id(0)
    tokens = x.shape[0]
    rows = ROWS

    @pl.loop(0, tokens // rows)
    def _(i):
        at = pl.ds(pl.multiple_of(i * rows, rows), rows)

        @pl.when(k == 0)
        def _():
            hat, _ = norm_parts(x[at])
            f[at] = (hat * gain[...]).astype(bf16)
            y[at] = x[at]

        low = f[at]
        g = mm(low, wg[0]).astype(bf16)
        u = mm(low, wu[0]).astype(bf16)
        gate[0, at] = g
        up[0, at] = u
        g, u = g.astype(f32), u.astype(f32)
        cdf = 0.5 * (1.0 + jnp.tanh(gelu_c * (g + 0.044715 * (g * g * g))))
        hidden = (g * cdf * u).astype(bf16)
        y[at] += mm(hidden, wd[0])


def feed(x, gain, weights, layer):
    tokens, width = x.shape
    per_layer = weights.shape[0] // LAYERS
    pieces = FF // width
    fixed = lambda shape: pl.BlockSpec(shape, lambda k: (0,) * len(shape))
    block = lambda skip: pl.BlockSpec((1, width, width), lambda k: (per_layer * layer + skip + k, 0, 0))
    each = pl.BlockSpec((1, tokens, width), lambda k: (k, 0, 0))
    return pl.pallas_call(
        feed_kernel,
        grid=(pieces,),
        in_specs=[fixed((tokens, width)), fixed((1, width)), block(4), block(4 + pieces), block(4 + 2 * pieces)],
        out_specs=[fixed((tokens, width)), fixed((tokens, width)), each, each],
        out_shape=[
            jax.ShapeDtypeStruct((tokens, width), f32),
            jax.ShapeDtypeStruct((tokens, width), bf16),
            jax.ShapeDtypeStruct((pieces, tokens, width), bf16),
            jax.ShapeDtypeStruct((pieces, tokens, width), bf16),
        ],
        compiler_params=pltpu.CompilerParams(vmem_limit_bytes=48 << 20),
        name="feed",
    )(x, gain.reshape(1, width), weights, weights, weights)


def feed_back_kernel(dx, x, gain, wg, wu, wd, f, gate, up, new, dgain, gg, gu, gd, f_t, dz, hid, dg, du):
    k = pl.program_id(0)
    tokens, width = x.shape
    rows = ROWS
    last = pl.num_programs(0) - 1

    @pl.when(k == 0)
    def _():
        @pl.loop(0, tokens // rows)
        def _(i):
            at = pl.ds(pl.multiple_of(i * rows, rows), rows)
            f_t[:, at] = f[at].astype(f32).T.astype(bf16)
            dz[at] = dx[at].astype(bf16)
            new[at] = jnp.zeros((rows, width), f32)

    def chunk(i, total):
        at = pl.ds(pl.multiple_of(i * rows, rows), rows)
        dh = mm(dz[at], wd[0], NT)
        g, u = gate[0, at].astype(f32), up[0, at].astype(f32)
        square = g * g
        t = jnp.tanh(gelu_c * (g + 0.044715 * (square * g)))
        cdf = 0.5 * (1.0 + t)
        act = g * cdf
        slope = cdf + 0.5 * g * (1.0 - t * t) * (gelu_c * (1.0 + 3 * 0.044715 * square))
        hid[at] = (act * u).astype(bf16)
        dgate = (dh * u * slope).astype(bf16)
        dup = (dh * act).astype(bf16)
        dg[at] = dgate
        du[at] = dup
        new[at] += mm(dgate, wg[0], NT) + mm(dup, wu[0], NT)
        return total

    lax.fori_loop(0, tokens // rows, chunk, 0)
    gg[0] = mm(f_t[...], dg[...]).astype(bf16)
    gu[0] = mm(f_t[...], du[...]).astype(bf16)
    gd[0] = mm(hid[...], dz[...], TN).astype(bf16)

    @pl.when(k == last)
    def _():
        def finish(i, total):
            at = pl.ds(pl.multiple_of(i * rows, rows), rows)
            back, extra = norm_back(x[at], gain[...], new[at])
            new[at] = dx[at] + back
            return total + fold8(extra)

        dgain[...] = lax.fori_loop(0, tokens // rows, finish, jnp.zeros((8, width), f32))


def feed_back(dx, x, gain, weights, layer, kept):
    f, gate, up = kept
    tokens, width = x.shape
    per_layer = weights.shape[0] // LAYERS
    pieces = FF // width
    fixed = lambda shape: pl.BlockSpec(shape, lambda k: (0,) * len(shape))
    block = lambda skip: pl.BlockSpec((1, width, width), lambda k: (per_layer * layer + skip + k, 0, 0))
    each = pl.BlockSpec((1, tokens, width), lambda k: (k, 0, 0))
    grad = pl.BlockSpec((1, width, width), lambda k: (k, 0, 0))
    return pl.pallas_call(
        feed_back_kernel,
        grid=(pieces,),
        in_specs=[
            fixed((tokens, width)),
            fixed((tokens, width)),
            fixed((1, width)),
            block(4),
            block(4 + pieces),
            block(4 + 2 * pieces),
            fixed((tokens, width)),
            each,
            each,
        ],
        out_specs=[fixed((tokens, width)), fixed((8, width)), grad, grad, grad],
        out_shape=[
            jax.ShapeDtypeStruct((tokens, width), f32),
            jax.ShapeDtypeStruct((8, width), f32),
        ]
        + [jax.ShapeDtypeStruct((pieces, width, width), bf16)] * 3,
        scratch_shapes=[
            pltpu.VMEM((width, tokens), bf16),
            pltpu.VMEM((tokens, width), bf16),
            pltpu.VMEM((tokens, width), bf16),
            pltpu.VMEM((tokens, width), bf16),
            pltpu.VMEM((tokens, width), bf16),
        ],
        compiler_params=pltpu.CompilerParams(vmem_limit_bytes=56 << 20),
        name="feed_back",
    )(dx, x, gain.reshape(1, width), weights, weights, weights, f, gate, up)


def two_parts(x):
    top = x.astype(bf16)
    return top, (x - top.astype(f32)).astype(bf16)


def mm3(a, b, dims=None):
    (a1, a2), (b1, b2) = a, b
    return mm(a1, b1, dims) + (mm(a1, b2, dims) + mm(a2, b1, dims))


def turn_kernel(scalars, numbers, left, right, some, grad, m, v, m_new, v_new, turned):
    slot = pl.program_id(0)
    factor, first_fix, second_fix = numbers[0], numbers[1], numbers[2]
    bases = two_parts(right[0])
    left_top, left_rest = two_parts(left[0])
    rotated = mm(left_top, grad[0], TN) + mm(left_rest, grad[0], TN)
    rotated = factor * mm3(two_parts(rotated), bases)
    moment, second, step = adam_moments(m[0], v[0], rotated, first_fix, second_fix)
    live = scalars[1 + slot] > 0
    m_new[0] = jnp.where(live, moment, m[0])
    v_new[0] = jnp.where(live, second, v[0])
    groups, _, rows, width = turned.shape
    rows_here = some[...].reshape(groups * rows, width)
    out = mm3(two_parts(rows_here), two_parts(step))
    out = mm3(two_parts(out), bases, NT)
    turned[...] = out.astype(turned.dtype).reshape(turned.shape)


def turn_slots(replica, live, numbers, left, right, grads, m, v):
    cap, width, _ = left.shape
    groups = width // 64
    scalars = jnp.concatenate([replica.reshape(1), live.astype(jnp.int32)])
    view = left.reshape(cap, groups, 4, 16, width)
    whole = pl.BlockSpec((1, width, width), lambda s, scalars: (s, 0, 0))
    grid_spec = pltpu.PrefetchScalarGridSpec(
        num_scalar_prefetch=1,
        grid=(cap,),
        in_specs=[
            pl.BlockSpec(memory_space=pltpu.SMEM),
            whole,
            whole,
            pl.BlockSpec((1, groups, 1, 16, width), lambda s, scalars: (s, 0, scalars[0], 0, 0)),
            whole,
            whole,
            whole,
        ],
        out_specs=[whole, whole, pl.BlockSpec((groups, 1, 16, width), lambda s, scalars: (0, s, 0, 0))],
    )
    return pl.pallas_call(
        turn_kernel,
        grid_spec=grid_spec,
        out_shape=[
            jax.ShapeDtypeStruct(m.shape, f32),
            jax.ShapeDtypeStruct(v.shape, f32),
            jax.ShapeDtypeStruct((groups, cap, 16, width), bf16),
        ],
        compiler_params=pltpu.CompilerParams(vmem_limit_bytes=56 << 20),
        name="turn_slots",
    )(scalars, numbers, left, right, view, grads, m, v)


class Transport:
    def __init__(self, n_rep, n_fsdp, shard_rows):
        self.sizes = (n_rep, n_fsdp)
        self.kernels = n_rep == 4 and n_fsdp == 8 and shard_rows == 64

    def ask(self, cid, wanted, facts, gains):
        if self.kernels:
            return ask_group(self.sizes, cid, wanted, facts, gains)
        asked = lax.all_to_all(wanted, "fsdp", split_axis=0, concat_axis=0, tiled=True)
        return asked, lax.all_gather(facts, "fsdp"), lax.all_gather(gains, "fsdp"), lax.pmax(facts, ("rep", "fsdp"))

    def spread(self, cid, x):
        if self.kernels:
            return group_exchange(self.sizes, cid, x, True)
        return lax.all_to_all(x, "fsdp", split_axis=0, concat_axis=0, tiled=True)

    def share(self, cid, x):
        if self.kernels:
            return group_exchange(self.sizes, cid, x, False)
        return lax.all_gather(x, "fsdp")

    def share_rows(self, cid, x):
        if self.kernels:
            return ring_rows(self.sizes, cid, x)
        return lax.all_gather(x, "fsdp")

    def sum_rows(self, cid, x):
        if self.kernels:
            return reduce_rows(self.sizes, cid, x)
        return lax.psum_scatter(x.astype(f32), "fsdp", scatter_dimension=0)

    def weights(self, cid, shard):
        if self.kernels:
            return gather_weights(self.sizes, cid, shard)
        return lax.all_gather(shard, "fsdp", axis=1, tiled=True)


def body(
    token_ids,
    segment_ids,
    masked_pos,
    labels,
    blocks,
    gains,
    embed,
    embed_m,
    embed_v,
    gains_m,
    gains_v,
    soap_m,
    soap_v,
    left_basis,
    right_basis,
    block_slots,
    step_count,
):
    groups = lax.axis_size("fsdp")
    replicas = lax.axis_size("rep")
    member = lax.axis_index("fsdp")
    replica = lax.axis_index("rep")
    micro_count = token_ids.shape[0]
    pack_length = token_ids.shape[2]
    pick_count = masked_pos.shape[2]
    vocab_rows, model_width = embed.shape
    block_count, shard_rows, _ = blocks.shape
    gain_count = gains.shape[0]
    tokens = micro_count * pack_length
    picks = micro_count * pick_count
    move = Transport(replicas, groups, shard_rows)
    table_low = embed.astype(bf16)

    ids = token_ids.reshape(tokens)
    index = jnp.arange(tokens, dtype=jnp.int32)
    owner = ids // vocab_rows
    local = ids - owner * vocab_rows
    first_at = jnp.min(jnp.where(ids[:, None] == ids[None, :], index[None, :], tokens), axis=1)
    is_first = first_at == index
    ahead = is_first[None, :] & (owner[:, None] == owner[None, :]) & (index[None, :] < first_at[:, None])
    rank = jnp.sum(ahead.astype(jnp.int32), axis=1)
    most = jnp.max(rank) + 1

    my_labels = labels.reshape(picks // 128, 128)
    facts = jnp.concatenate(
        [my_labels, jnp.full((8 - picks // 128, 128), most, jnp.int32)], axis=0
    )
    gain_pad = jnp.pad(gains, ((0, 8 - gain_count), (0, 128 - gains.shape[1])))
    slots = groups * CAPACITY
    most_rounds = (tokens + CAPACITY - 1) // CAPACITY
    slot_index = jnp.arange(slots, dtype=jnp.int32)

    def slot_of(k):
        here = rank - k * CAPACITY
        return jnp.where((here >= 0) & (here < CAPACITY), owner * CAPACITY + here, -1)

    def wanted_in(slot):
        wanted = jnp.where((slot[None, :] == slot_index[:, None]) & is_first[None, :], local[None, :], 0)
        return jnp.sum(wanted, axis=1).reshape(groups, 1, CAPACITY)

    def rows_for(cid, slot, asked):
        rows = jnp.take(table_low, asked.reshape(slots), axis=0)
        rows = move.spread(cid, rows.reshape(groups, CAPACITY, model_width)).reshape(slots, model_width)
        return jnp.dot((slot[:, None] == slot_index[None, :]).astype(bf16), rows, preferred_element_type=f32)

    slot = slot_of(0)
    asked, group_facts, gain_rows, most_facts = move.ask(0, wanted_in(slot), facts, gain_pad)
    rounds = (most_facts[7, 0] + CAPACITY - 1) // CAPACITY
    all_labels = group_facts[:, : picks // 128].reshape(groups * picks)
    gain_rows = gain_rows[:, :gain_count, : gains.shape[1]].transpose(1, 0, 2).reshape(gain_count, model_width)
    gain_rows = lax.reduce_precision(gain_rows, exponent_bits=8, mantissa_bits=7)
    embedded = rows_for(2, slot, asked)
    asked_all = jnp.zeros((most_rounds, slots), jnp.int32).at[0].set(asked.reshape(slots))

    def look(state):
        k, rows_so_far, asked_all = state
        slot = slot_of(k)
        asked = move.spread(1, wanted_in(slot))
        asked_all = lax.dynamic_update_index_in_dim(asked_all, asked.reshape(slots), k, 0)
        return k + 1, rows_so_far + rows_for(12, slot, asked), asked_all

    _, embedded, asked_all = lax.while_loop(lambda s: s[0] < rounds, look, (jnp.int32(1), embedded, asked_all))

    full_blocks = move.weights(3, blocks.astype(bf16))

    segments = segment_ids.reshape(micro_count, pack_length)
    stream, first_pull = jax.vjp(layer_norm, embedded, gain_rows[0])
    saved_layers = []
    for layer in range(LAYERS):
        middle, *attention_kept = attend(stream, gain_rows[1 + 2 * layer], full_blocks, layer, segments)
        after, *feed_kept = feed(middle, gain_rows[2 + 2 * layer], full_blocks, layer)
        saved_layers.append((stream, attention_kept, middle, feed_kept))
        stream = after
    final_rows, final_pull = jax.vjp(layer_norm, stream, gain_rows[gain_count - 1])

    positions = masked_pos.reshape(micro_count, pick_count)
    flat_positions = (positions + jnp.arange(micro_count, dtype=jnp.int32)[:, None] * pack_length).reshape(picks)
    picked = jnp.take(final_rows, flat_positions, axis=0).astype(bf16)
    all_picked = move.share_rows(4, picked).reshape(groups * picks, model_width)
    logits = jnp.einsum("td,vd->tv", all_picked, table_low, preferred_element_type=f32)
    top_value = jnp.max(logits, axis=-1)
    exp_total = jnp.sum(jnp.exp(logits - top_value[:, None]), axis=-1)
    label_local = all_labels - member * vocab_rows
    columns = jnp.arange(vocab_rows, dtype=jnp.int32)
    label_hits = columns[None, :] == label_local[:, None]
    target = jnp.sum(jnp.where(label_hits, logits, 0.0), axis=-1)
    stats = move.share(5, jnp.stack([top_value, exp_total, target]))
    top_all = jnp.max(stats[:, 0], axis=0)
    total_all = jnp.sum(stats[:, 1] * jnp.exp(stats[:, 0] - top_all[None]), axis=0)
    target_all = jnp.sum(stats[:, 2], axis=0)
    entropy = top_all + jnp.log(total_all) - target_all
    loss_local = jnp.sum(lax.dynamic_slice_in_dim(entropy, member * picks, picks))
    grad_logits = (
        jnp.exp(logits - top_all[:, None]) / total_all[:, None] - label_hits.astype(f32)
    ).astype(bf16)
    grad_table = jnp.einsum("tv,td->vd", grad_logits, all_picked, preferred_element_type=f32)
    grad_picked = jnp.einsum("tv,vd->td", grad_logits, table_low, preferred_element_type=f32)
    grad_picked = move.sum_rows(6, grad_picked.astype(bf16).reshape(groups, picks, model_width))

    match = flat_positions[None, :] == index[:, None]
    place = jnp.sum(jnp.where(match, jnp.arange(picks, dtype=jnp.int32)[None, :] + 1, 0), axis=1)
    grad_final = jnp.where(
        (place > 0)[:, None], jnp.take(grad_picked, jnp.maximum(place - 1, 0), axis=0), 0.0
    )
    grad_stream, grad_final_gain = final_pull(grad_final)
    gain_grads = [None] * gain_count
    gain_grads[gain_count - 1] = grad_final_gain
    layer_grads = [None] * LAYERS
    for layer in reversed(range(LAYERS)):
        before, attention_kept, middle, feed_kept = saved_layers[layer]
        grad_stream, feed_gain, *grads_feed = feed_back(
            grad_stream, middle, gain_rows[2 + 2 * layer], full_blocks, layer, feed_kept
        )
        grad_stream, attention_gain, grads_attention = attend_back(
            grad_stream, before, gain_rows[1 + 2 * layer], full_blocks, layer, segments, attention_kept
        )
        gain_grads[1 + 2 * layer] = jnp.sum(attention_gain, axis=(0, 1))
        gain_grads[2 + 2 * layer] = jnp.sum(feed_gain, axis=0)
        layer_grads[layer] = [grads_attention] + grads_feed
    grad_embedded, gain_grads[0] = first_pull(grad_stream)
    grad_rows = grad_embedded.astype(bf16)
    padded_rows = -(-vocab_rows // 384) * 384
    grad_table = jnp.pad(grad_table, ((0, padded_rows - vocab_rows), (0, 0)))
    row_index = jnp.arange(padded_rows, dtype=jnp.int32)

    def given(cid, k, grad_table):
        chosen = (slot_index[:, None] == slot_of(k)[None, :]).astype(bf16)
        rows = jnp.dot(chosen, grad_rows, preferred_element_type=f32).astype(bf16)
        rows = move.spread(cid, rows.reshape(groups, CAPACITY, model_width)).reshape(slots, model_width)
        asked = lax.dynamic_index_in_dim(asked_all, k, 0, keepdims=False)
        target_rows = (row_index[:, None] == asked[None, :]).astype(bf16)
        return grad_table + jnp.dot(target_rows, rows, preferred_element_type=f32)

    grad_table = given(7, 0, grad_table)
    _, grad_table = lax.while_loop(
        lambda s: s[0] < rounds, lambda s: (s[0] + 1, given(13, s[0], s[1])), (jnp.int32(1), grad_table)
    )
    grad_blocks = [g for grads in layer_grads for g in grads]
    grad_gains = jnp.stack(gain_grads, axis=0)

    position_count = micro_count * replicas * groups * pick_count
    clip_limit = clip_ratio * math.sqrt(position_count)
    steps_done = step_count[0].astype(f32)
    first_fix = 1.0 - beta_first**steps_done
    second_fix = 1.0 - beta_second**steps_done
    slot_cap = soap_m.shape[0]
    slot_total = slot_cap * groups
    named = jnp.arange(slot_total, dtype=jnp.int32)[:, None] == block_slots[None, :]
    taken = jnp.any(named, axis=1)
    block_of = jnp.sum(jnp.where(named, jnp.arange(block_count, dtype=jnp.int32)[None, :], 0), axis=1)

    small = jnp.zeros((8, model_width), f32).at[:gain_count].set(grad_gains)
    small = small.at[7, 0].set(loss_local)
    if move.kernels:
        mine, grad_table, squares = reduce_gradients(
            move.sizes, 8, grad_blocks, grad_table.reshape(4, padded_rows // 4, model_width)
        )
        grad_table = grad_table.reshape(padded_rows, model_width)[:vocab_rows]
        small = total_everyone(move.sizes, 9, small.at[6].set(jnp.sum(squares, axis=(0, 1))))
        squares = jnp.sum(small[6])
        outgoing = jnp.where(taken[:, None, None], jnp.take(mine.astype(bf16), block_of, axis=0), 0)
        owned = exchange_slots(move.sizes, 10, outgoing.reshape(groups, slot_cap, 16, model_width), True)
        owned = owned.reshape(slot_cap, model_width, model_width)
    else:
        grad_blocks = jnp.concatenate([g.astype(f32) for g in grad_blocks], axis=0)
        mine = lax.psum_scatter(grad_blocks, "fsdp", scatter_dimension=1, tiled=True)
        mine, grad_table = lax.psum((mine, grad_table[:vocab_rows]), "rep")
        small = lax.psum(small, ("rep", "fsdp"))
        squares = lax.psum(jnp.sum(mine * mine) + jnp.sum(grad_table * grad_table), "fsdp")
        outgoing = jnp.where(taken[:, None, None], jnp.take(mine, block_of, axis=0), 0)
        owned = lax.all_to_all(outgoing, "fsdp", split_axis=0, concat_axis=1, tiled=True)
    loss_all = small[7, 0]
    grad_gains = small[:gain_count]
    grad_norm = jnp.sqrt(squares + jnp.sum(grad_gains * grad_gains))
    factor = jnp.minimum(1.0, clip_limit / grad_norm)
    grad_gains = lax.dynamic_slice_in_dim(grad_gains, member * gains.shape[1], gains.shape[1], axis=1)

    live = lax.dynamic_slice_in_dim(taken, member * slot_cap, slot_cap)
    if move.kernels:
        soap_m_new, soap_v_new, turned = turn_slots(
            replica,
            live,
            jnp.stack([factor, first_fix, second_fix]),
            left_basis,
            right_basis,
            owned,
            soap_m,
            soap_v,
        )
        returned = exchange_slots(move.sizes, 11, turned, False)
        returned = returned.reshape(slot_total, shard_rows, model_width)
    else:
        rotated = jnp.einsum("bji,bjk->bik", left_basis, owned, precision=high)
        rotated = factor * jnp.einsum("bik,bkl->bil", rotated, right_basis, precision=high)
        moment_first, moment_second, rotated_step = adam_moments(soap_m, soap_v, rotated, first_fix, second_fix)
        soap_m_new = jnp.where(live[:, None, None], moment_first, soap_m)
        soap_v_new = jnp.where(live[:, None, None], moment_second, soap_v)
        turned = jnp.einsum("bij,bjk->bik", left_basis, rotated_step, precision=high)
        turned = jnp.einsum("bik,blk->bil", turned, right_basis, precision=high)
        returned = lax.all_to_all(turned, "fsdp", split_axis=1, concat_axis=0, tiled=True)
    update = jnp.take(returned, block_slots, axis=0).astype(f32)
    blocks_new = blocks - step_rate * (update + weight_decay * blocks)

    embed_m_new, embed_v_new, table_step = adam_moments(
        embed_m, embed_v, factor * grad_table, first_fix, second_fix
    )
    embed_new = embed - step_rate * (table_step + weight_decay * embed)
    gains_m_new, gains_v_new, gain_step = adam_moments(
        gains_m, gains_v, factor * grad_gains, first_fix, second_fix
    )
    gains_new = gains - step_rate * gain_step
    loss = (loss_all / position_count).reshape(1)
    return (
        loss,
        grad_norm.reshape(1),
        blocks_new,
        gains_new,
        embed_new,
        embed_m_new,
        embed_v_new,
        gains_m_new,
        gains_v_new,
        soap_m_new,
        soap_v_new,
        blocks_new.astype(bf16),
        embed_new.astype(bf16),
    )


def solution(mesh):
    packs = P(None, ("rep", "fsdp"), None)
    rows = P(None, "fsdp", None)
    columns = P(None, "fsdp")
    table = P("fsdp", None)
    slots = P("fsdp", None, None)
    return jax.shard_map(
        body,
        mesh=mesh,
        in_specs=(packs,) * 4
        + (rows, columns)
        + (table,) * 3
        + (columns,) * 2
        + (slots,) * 4
        + (P(), P()),
        out_specs=(P(), P(), rows, columns)
        + (table,) * 3
        + (columns,) * 2
        + (slots,) * 2
        + (rows, table),
        check_vma=False,
    )
```

```python
from functools import partial
import math

import jax
import jax.numpy as jnp
from jax import lax
from jax.experimental import pallas as pl
from jax.experimental.pallas import tpu as pltpu
from jax.sharding import PartitionSpec as P

HEADS = 8
FF = 2048
LAYERS = 2

norm_epsilon = 1e-05
beta_first = 0.9
beta_second = 0.99
adam_epsilon = 1e-08
step_rate = 0.04
weight_decay = 0.1
clip_ratio = 12.0
masked_score = -1e30
bf16 = jnp.bfloat16
f32 = jnp.float32
highest = lax.Precision.HIGHEST
high = lax.Precision.HIGH
MESH = pl.DeviceIdType.MESH
ANY = pl.BlockSpec(memory_space=pl.ANY)
VMEM = pl.BlockSpec(memory_space=pltpu.VMEM)
CAPACITY = 128


def pick(table, index):
    out = jnp.int32(table[0])
    for k in range(1, len(table)):
        out = jnp.where(index == k, jnp.int32(table[k]), out)
    return out


def ring_order(n):
    nz = 4
    nx = n // nz
    order = []
    for x in range(nx):
        zs = range(1, nz) if x % 2 == 0 else range(nz - 1, 0, -1)
        order += [z * nx + x for z in zs]
    order += [x for x in range(nx - 1, -1, -1)]
    return order


class Place:
    def __init__(self, n_rep, n_fsdp):
        self.r = lax.axis_index("rep")
        self.f = lax.axis_index("fsdp")
        self.n_rep, self.n = n_rep, n_fsdp
        self.c = lax.rem(self.r, 2)
        self.y = self.r // 2
        self.order = ring_order(n_fsdp)
        spot = [self.order.index(k) for k in range(n_fsdp)]
        self.pos = pick(spot, self.f)
        self.core = (self.r + 1 - 2 * self.c, self.f)
        self.next = (self.r, self.at(1))
        self.prev = (self.r, self.at(-1))

    def at(self, step):
        return pick(self.order, lax.rem(self.pos + step + 2 * self.n, self.n))


def enter(peers):
    barrier = pltpu.get_barrier_semaphore()
    for peer in peers:
        pl.semaphore_signal(barrier, inc=1, device_id=peer, device_id_type=MESH)
    pl.semaphore_wait(barrier, len(peers))


def remote(src, dst, send, recv, peer):
    return pltpu.make_async_remote_copy(
        src_ref=src, dst_ref=dst, send_sem=send, recv_sem=recv, device_id=peer, device_id_type=MESH
    )


def params(cid, limit=None):
    return pltpu.CompilerParams(
        collective_id=cid, has_side_effects=True, vmem_limit_bytes=limit
    )


def group_kernel(n_rep, n, spread, x_ref, o_ref, send, recv):
    here = Place(n_rep, n)
    me = here.f
    others = [lax.rem(me + k, n) for k in range(1, n)]
    enter([(here.r, o) for o in others])
    copies = []
    for k, o in enumerate(others):
        src = x_ref.at[o] if spread else x_ref
        cp = remote(src, o_ref.at[me], send.at[k], recv.at[k], (here.r, o))
        cp.start()
        copies.append(cp)
    o_ref[me] = x_ref[me] if spread else x_ref[...]
    for cp in copies:
        cp.wait()


def group_exchange(mesh_sizes, cid, x, spread):
    n_rep, n = mesh_sizes
    shape = x.shape if spread else (n,) + x.shape
    return pl.pallas_call(
        partial(group_kernel, n_rep, n, spread),
        out_shape=jax.ShapeDtypeStruct(shape, x.dtype),
        in_specs=[VMEM],
        out_specs=VMEM,
        scratch_shapes=[pltpu.SemaphoreType.DMA((n - 1,)), pltpu.SemaphoreType.DMA((n - 1,))],
        compiler_params=params(cid),
        name=f"group_{cid}",
    )(x)


def opening_kernel(
    n_rep, n, half, shared, x_ref, t_ref, w_ref, facts_ref, gains_ref, o_ref, rows_ref, asked, facts, gains, most,
    table, index, stage, ready, held, got,
    t_s, ring_s, ring_r, core_s, core_r, y_s, y_r, over_s, over_r, ask_s, ask_r, top_s, top_r, rows_s, rows_r,
):
    here = Place(n_rep, n)
    me = here.f
    ypeer = (lax.rem(here.r + 2, 4), here.f)
    others = [lax.rem(me + k, n) for k in range(1, n)]
    rows = x_ref.shape[1]
    alone = (half - shared) // 2
    enter([(here.r, o) for o in others] + [here.core, ypeer])
    load = pltpu.make_async_copy(t_ref, table, t_s.at[0])
    load.start()
    asks = []
    for k, o in enumerate(others):
        peer = (here.r, o)
        asks.append(remote(w_ref.at[o], asked.at[me], ask_s.at[0, k], ask_r.at[0, k], peer))
        asks.append(remote(facts_ref, facts.at[me], ask_s.at[1, k], ask_r.at[1, k], peer))
        asks.append(remote(gains_ref, gains.at[me], ask_s.at[2, k], ask_r.at[2, k], peer))
    for cp in asks:
        cp.start()

    mine = pl.ds(here.c * half + here.y * alone, alone + shared)
    given = pl.ds(here.c * half + here.y * (alone + shared), alone)
    taken = pl.ds(here.c * half + (1 - here.y) * (alone + shared), alone)
    hops = n // 2
    copies, sends = [], []

    def rows_of(origin, way, s):
        if s == hops - 1:
            return pl.ds(pl.multiple_of(origin * rows + way * (rows // 2), rows // 2), rows // 2)
        return pl.ds(pl.multiple_of(origin * rows, rows), rows)

    own = remote(x_ref, o_ref.at[:, rows_of(here.f, 0, -1)], core_s.at[0, 0], core_r.at[0, 0], here.core)
    own.start()
    copies.append(own)
    waiting = [None, None]
    across = []

    def pass_on(way, s):
        waiting[way].wait_recv()
        where = rows_of(here.at(-s - 1 if way == 0 else s + 1), way, s)
        kept = o_ref.at[given, where]
        cp = remote(kept, kept, y_s.at[way, s], y_r.at[way, s], ypeer)
        cp.start()
        across.append((cp, o_ref.at[taken, where], way, s))
        kept = o_ref.at[mine, where]
        cp = remote(kept, kept, core_s.at[way, s + 1], core_r.at[way, s + 1], here.core)
        cp.start()
        copies.append(cp)

    def hop(way, s):
        where = rows_of(here.at(-s if way == 0 else s), way, s)
        src = x_ref.at[mine] if s == 0 else o_ref.at[mine, where]
        cp = remote(
            src, o_ref.at[mine, where], ring_s.at[way, s], ring_r.at[way, s], here.next if way == 0 else here.prev
        )
        cp.start()
        waiting[way] = cp
        sends.append(cp)

    for way in range(2):
        hop(way, 0)

    asked[me] = w_ref[me]
    facts[me] = facts_ref[...]
    gains[me] = gains_ref[...]
    for cp in asks:
        cp.wait_recv()
    listed = pltpu.make_async_copy(asked, index, t_s.at[1])
    listed.start()
    top = facts[0]
    for k in range(1, n):
        top = jnp.maximum(top, facts[k])
    held[0] = top
    first = remote(held.at[0], got.at[0], top_s.at[0], top_r.at[0], here.core)
    first.start()
    listed.wait()
    load.wait()
    places = rows_ref.shape[1]

    def collect(o):
        def one(i, carry):
            stage[pl.ds(i, 1)] = table[pl.ds(index[o, 0, i], 1)]
            return carry

        lax.fori_loop(0, places, one, 0, unroll=8)
        return stage[...].astype(bf16)

    for k, o in enumerate(others):
        ready[o] = collect(o)
        cp = remote(ready.at[o], rows_ref.at[me], rows_s.at[k], rows_r.at[k], (here.r, o))
        cp.start()
        asks.append(cp)
    rows_ref[me] = collect(me)
    first.wait_recv()
    held[1] = jnp.maximum(top, got[0])
    second = remote(held.at[1], got.at[1], top_s.at[1], top_r.at[1], ypeer)
    second.start()

    for s in range(1, hops):
        for way in range(2):
            pass_on(way, s - 1)
            hop(way, s)
    second.wait_recv()
    most[...] = jnp.maximum(held[1], got[1])
    for way in range(2):
        pass_on(way, hops - 1)
    for cp, kept, way, s in across:
        cp.wait_recv()
        over = remote(kept, kept, over_s.at[way, s], over_r.at[way, s], here.core)
        over.start()
        copies.append(over)
        sends.append(cp)
    for cp in asks[3 * (n - 1) :]:
        cp.wait_recv()
    for cp in asks + [first, second] + sends:
        cp.wait_send()
    for cp in copies:
        cp.wait()


def open_step(mesh_sizes, cid, shard, table, wanted, facts, gains):
    n_rep, n = mesh_sizes
    count, rows, width = shard.shape
    half = count // 2
    places = wanted.shape[2]
    dma = pltpu.SemaphoreType.DMA
    return pl.pallas_call(
        partial(opening_kernel, n_rep, n, half, half - 2 * (half // 3)),
        out_shape=[
            jax.ShapeDtypeStruct((count, rows * n, width), shard.dtype),
            jax.ShapeDtypeStruct((n, places, width), bf16),
            jax.ShapeDtypeStruct(wanted.shape, wanted.dtype),
            jax.ShapeDtypeStruct((n,) + facts.shape, facts.dtype),
            jax.ShapeDtypeStruct((n,) + gains.shape, gains.dtype),
            jax.ShapeDtypeStruct(facts.shape, facts.dtype),
        ],
        in_specs=[ANY, ANY] + [VMEM] * 3,
        out_specs=[ANY] + [VMEM] * 5,
        scratch_shapes=[
            pltpu.VMEM(table.shape, table.dtype),
            pltpu.SMEM(wanted.shape, wanted.dtype),
            pltpu.VMEM((places, width), table.dtype),
            pltpu.VMEM((n, places, width), bf16),
            pltpu.VMEM((2,) + facts.shape, facts.dtype),
            pltpu.VMEM((2,) + facts.shape, facts.dtype),
            dma((2,)),
            dma((2, n // 2)),
            dma((2, n // 2)),
            dma((2, n // 2 + 1)),
            dma((2, n // 2 + 1)),
            dma((2, n // 2)),
            dma((2, n // 2)),
            dma((2, n // 2)),
            dma((2, n // 2)),
            dma((3, n - 1)),
            dma((3, n - 1)),
            dma((2,)),
            dma((2,)),
            dma((n - 1,)),
            dma((n - 1,)),
        ],
        compiler_params=params(cid, 24 << 20),
        name="open_step",
    )(shard, table, wanted, facts, gains)


def ring_rows_kernel(n_rep, n, x_ref, o_ref, send, recv):
    here = Place(n_rep, n)
    enter([here.next, here.prev])
    rows = x_ref.shape[0]
    hops = n // 2
    copies = []
    waiting = [None, None]
    for s in range(hops):
        for way in range(2):
            peer = here.next if way == 0 else here.prev
            origin = here.at(-s if way == 0 else s)
            if s > 0:
                waiting[way].wait_recv()
            window = pl.ds(0, rows)
            if s == hops - 1:
                window = pl.ds(way * (rows // 2), rows // 2)
            src = x_ref.at[window] if s == 0 else o_ref.at[origin, window]
            cp = remote(src, o_ref.at[origin, window], send.at[way, s], recv.at[way, s], peer)
            cp.start()
            waiting[way] = cp
            copies.append(cp)
    o_ref[here.f] = x_ref[...]
    for way in range(2):
        waiting[way].wait_recv()
    for cp in copies:
        cp.wait_send()


def ring_rows(mesh_sizes, cid, x):
    n_rep, n = mesh_sizes
    return pl.pallas_call(
        partial(ring_rows_kernel, n_rep, n),
        out_shape=jax.ShapeDtypeStruct((n,) + x.shape, x.dtype),
        in_specs=[VMEM],
        out_specs=VMEM,
        scratch_shapes=[pltpu.SemaphoreType.DMA((2, n // 2)), pltpu.SemaphoreType.DMA((2, n // 2))],
        compiler_params=params(cid),
        name="ring_rows",
    )(x)


def squares_row(square):
    row = jnp.sum(square, axis=0, keepdims=True)
    return jnp.where(lax.broadcasted_iota(jnp.int32, square.shape, 0) == 6, row, 0.0)


def reduce_kernel(
    n_rep, n, half, table_rows, each, *refs
):
    g_refs, refs = refs[: 2 * each], refs[2 * each :]
    (
    t_ref, small_ref, block_of, taken, o_ref, to_ref, sum_ref, mine, outgoing, held, hgot, four, fours, squares,
    own, part, got, fin, ysend, ygot, town, tpart, tsend, tgot,
    load_s, core_s, core_r, ring_s, ring_r, y_s, y_r, tload, tcs, tcr, tys, tyr, tos, tor,
    keep, a_s, a_r, f_s, f_r, sum_s, sum_r,
    ) = refs
    here = Place(n_rep, n)
    c, y = here.c, here.y
    ypeer = (lax.rem(here.r + 2, 4), here.f)
    other_c, other_y = 1 - c, 1 - y
    me = here.f
    others = [lax.rem(me + k, n) for k in range(1, n)]
    enter([(here.r, o) for o in others] + [here.core, ypeer])
    far = n // 2

    tl = pltpu.make_async_copy(t_ref.at[pl.ds(c * 2, 2)], town, tload)
    tl.start()
    tc = remote(t_ref.at[pl.ds(other_c * 2, 2)], tpart, tcs, tcr, here.core)
    tc.start()

    spots = {(0, far): 0, (1, far): 0}
    for d in range(far - 1, 0, -1):
        spots[0, d] = 1 + 2 * (far - 1 - d)
        spots[1, d] = 2 + 2 * (far - 1 - d)
    spots[0, 0] = spots[1, 0] = n - 1
    loads, cores = {}, {}
    done = set()
    for (way, d), spot in sorted(spots.items(), key=lambda item: item[1]):
        if spot in done:
            continue
        done.add(spot)
        to = here.f if d == 0 else here.at(d if way == 0 else -d)
        for h in (way, 1 - way):
            loads[spot, h], cores[spot, h] = [], []
            for j in range(each):
                g_ref = g_refs[h * each + j]
                into = pl.ds(j * (half // each), half // each)
                ld = pltpu.make_async_copy(g_ref.at[:, to, :, c], own.at[spot, h, into], load_s.at[spot, h, j])
                ld.start()
                loads[spot, h].append(ld)
                cp = remote(
                    g_ref.at[:, to, :, other_c],
                    part.at[spot, h, into],
                    core_s.at[spot, h, j],
                    core_r.at[spot, h, j],
                    here.core,
                )
                cp.start()
                cores[spot, h].append(cp)

    def ready(spot, h):
        for j in range(each):
            loads[spot, h][j].wait()
            cores[spot, h][j].wait_recv()

    ring = {}

    def came(way, h, s):
        return got.at[way, h, s]

    def lane(way, h, s):
        d = far - s
        spot = spots[way, d]
        ready(spot, h)
        before = ring.get((way, h, s - 1))
        if before is not None:
            before.wait_recv()
        target = own.at[spot, h]

        @pl.loop(0, half)
        def _(b):
            for k in range(2):
                total = own[spot, h, b, k].astype(f32) + part[spot, h, b, k].astype(f32)
                if before is not None:
                    total = total + came(way, h, s - 1)[b, k].astype(f32)
                target[b, k] = total.astype(target.dtype)

        cp = remote(
            target, came(way, h, s), ring_s.at[way, h, s], ring_r.at[way, h, s], here.next if way == 0 else here.prev
        )
        cp.start()
        ring[way, h, s] = cp

    step_rows = 48
    for s in range(far):
        for h_turn in range(2):
            for way in range(2):
                h = way if h_turn == 1 else 1 - way
                if s == 0 and h_turn == 0:
                    continue
                if s == 1 and h_turn == 0:
                    continue
                lane(way, h, s)
        if s == 0:
            for way in range(2):
                lane(way, 1 - way, 1)
            tl.wait()
            tc.wait_recv()

            @pl.loop(0, table_rows // step_rows)
            def _(i):
                at = pl.ds(pl.multiple_of(i * step_rows, step_rows), step_rows)
                town[y, at] = town[y, at] + tpart[y, at]
                tsend[at] = (town[other_y, at] + tpart[other_y, at]).astype(bf16)

            ty = remote(tsend, tgot, tys, tyr, ypeer)
            ty.start()
        if s == 2:
            ty.wait_recv()

            def add(i, acc):
                at = pl.ds(pl.multiple_of(i * step_rows, step_rows), step_rows)
                total = town[y, at] + tgot[at].astype(f32)
                town[y, at] = total
                square = total * total
                for k in range(step_rows // 8):
                    acc = acc + square[k * 8 : k * 8 + 8]
                return acc

            squares[...] = lax.fori_loop(0, table_rows // step_rows, add, jnp.zeros((8, tgot.shape[1]), f32))
            quarter = c * 2 + y
            near = c * 2 + other_y
            tkeep = pltpu.make_async_copy(town.at[y], to_ref.at[quarter], tload)
            tkeep.start()
            t0 = remote(town.at[y], to_ref.at[quarter], tos.at[0], tor.at[0], ypeer)
            t1 = remote(town.at[y], to_ref.at[quarter], tos.at[1], tor.at[1], here.core)
            t0.start()
            t1.start()
    ys = []
    spot = spots[0, 0]
    for h in range(2):
        ready(spot, h)
        for way in range(2):
            ring[way, h, far - 1].wait_recv()

        @pl.loop(0, half)
        def _(b, h=h):
            for keep in range(2):
                k = y if keep else other_y
                total = own[spot, h, b, k].astype(f32) + part[spot, h, b, k].astype(f32)
                for way in range(2):
                    total = total + got[way, h, far - 1, b, k].astype(f32)
                if keep:
                    fin[h, b] = total
                else:
                    ysend[h, b] = total.astype(bf16)

        cp = remote(ysend.at[h], ygot.at[h], y_s.at[h], y_r.at[h], ypeer)
        cp.start()
        ys.append(cp)

    acc = jnp.zeros((8, fin.shape[-1]), f32)
    for h in range(2):
        ys[h].wait_recv()

        def last(b, acc, h=h):
            total = fin[h, b] + ygot[h, b].astype(f32)
            mine[h * half + b] = total.astype(bf16)
            square = total * total
            return acc + square[:8] + square[8:]

        acc = lax.fori_loop(0, half, last, acc)

    held[0] = small_ref[...] + squares_row(acc + squares[...])
    first = remote(held.at[0], hgot.at[0], sum_s.at[0], sum_r.at[0], here.core)
    first.start()

    cap = o_ref.shape[0]

    @pl.loop(0, n * cap)
    def _(k):
        value = mine[block_of[k]]
        outgoing[k] = jnp.where(taken[k] > 0, value, jnp.zeros_like(value))

    def spot_of(source, r):
        return o_ref.at[:, source, r]

    moves = []
    for k, o in enumerate(others):
        cp = remote(outgoing.at[pl.ds(o * cap, cap)], spot_of(me, here.r), a_s.at[k], a_r.at[k], (here.r, o))
        cp.start()
        moves.append(cp)
    kept = pltpu.make_async_copy(outgoing.at[pl.ds(me * cap, cap)], spot_of(me, here.r), keep)
    kept.start()
    first.wait_recv()
    held[1] = held[0] + hgot[0]
    second = remote(held.at[1], hgot.at[1], sum_s.at[1], sum_r.at[1], ypeer)
    second.start()
    t0.wait_recv()
    t2 = remote(to_ref.at[near], to_ref.at[near], tos.at[2], tor.at[2], here.core)
    t2.start()
    second.wait_recv()
    four[...] = held[1] + hgot[1]
    totals = []
    for k, o in enumerate(others):
        cp = remote(four, fours.at[me], sum_s.at[2 + k], sum_r.at[2 + k], (here.r, o))
        cp.start()
        totals.append(cp)
    fours[me] = four[...]
    beside, distant = [], []
    for k in range(n):
        source = me if k == 0 else lax.rem(me - k + n, n)
        if k == 0:
            kept.wait()
        else:
            moves[k - 1].wait_recv()
        piece = spot_of(source, here.r)
        over = remote(piece, piece, f_s.at[0, k], f_r.at[0, k], ypeer)
        over.start()
        cp = remote(piece, piece, f_s.at[1, k], f_r.at[1, k], here.core)
        cp.start()
        distant.append((over, source))
        beside.append(cp)
    for cp in totals:
        cp.wait_recv()
    total = fours[0]
    for k in range(1, n):
        total = total + fours[k]
    sum_ref[...] = total
    yr = lax.rem(here.r + 2, 4)
    for k, (over, source) in enumerate(distant):
        over.wait_recv()
        piece = spot_of(source, yr)
        cp = remote(piece, piece, f_s.at[2, k], f_r.at[2, k], here.core)
        cp.start()
        beside.append(cp)
    for cp in moves + totals + [first, second] + [over for over, _ in distant]:
        cp.wait_send()
    for cp in beside:
        cp.wait()
    for cp in ys:
        cp.wait_send()
    for cp in ring.values():
        cp.wait_send()
    for group in cores.values():
        for cp in group:
            cp.wait_send()
    tc.wait_send()
    ty.wait_send()
    tkeep.wait()
    t0.wait_send()
    t1.wait()
    t2.wait()


def settle_gradients(mesh_sizes, cid, grads, table, small, block_of, taken, cap):
    n_rep, n = mesh_sizes
    _, depth, width = grads[0].shape
    count = sum(g.shape[0] for g in grads)
    half = count // 2
    each = len(grads) // 2
    far = n // 2
    table_rows = table.shape[1]
    views = [g.reshape(g.shape[0], n, 2, 2, 16, width) for g in grads]
    dma = pltpu.SemaphoreType.DMA
    piece = (half, 2, 16, width)
    smem = pl.BlockSpec(memory_space=pltpu.SMEM)
    like = small.shape
    return pl.pallas_call(
        partial(reduce_kernel, n_rep, n, half, table_rows, each),
        out_shape=[
            jax.ShapeDtypeStruct((cap, n, 4, 16, width), bf16),
            jax.ShapeDtypeStruct(table.shape, f32),
            jax.ShapeDtypeStruct(like, f32),
        ],
        in_specs=[ANY] * (2 * each + 1) + [VMEM, smem, smem],
        out_specs=[ANY, ANY, VMEM],
        scratch_shapes=[
            pltpu.VMEM((count, 16, width), bf16),
            pltpu.VMEM((n * cap, 16, width), bf16),
            pltpu.VMEM((2,) + like, f32),
            pltpu.VMEM((2,) + like, f32),
            pltpu.VMEM(like, f32),
            pltpu.VMEM((n,) + like, f32),
            pltpu.VMEM(like, f32),
            pltpu.VMEM((n, 2) + piece, bf16),
            pltpu.VMEM((n, 2) + piece, bf16),
            pltpu.VMEM((2, 2, far) + piece, bf16),
            pltpu.VMEM((2, half, 16, width), f32),
            pltpu.VMEM((2, half, 16, width), bf16),
            pltpu.VMEM((2, half, 16, width), bf16),
            pltpu.VMEM((2, table_rows, width), f32),
            pltpu.VMEM((2, table_rows, width), f32),
            pltpu.VMEM((table_rows, width), bf16),
            pltpu.VMEM((table_rows, width), bf16),
            dma((n, 2, each)),
            dma((n, 2, each)),
            dma((n, 2, each)),
            dma((2, 2, far)),
            dma((2, 2, far)),
            dma((2,)),
            dma((2,)),
            dma,
            dma,
            dma,
            dma,
            dma,
            dma((3,)),
            dma((3,)),
            dma,
            dma((n - 1,)),
            dma((n - 1,)),
            dma((3, n)),
            dma((3, n)),
            dma((n + 1,)),
            dma((n + 1,)),
        ],
        compiler_params=params(cid, 56 << 20),
        name="settle_gradients",
    )(*views, table, small, block_of, taken)


def rows_kernel(n_rep, n, x_ref, o_ref, held, got, send, recv):
    here = Place(n_rep, n)
    enter([here.next, here.prev])
    far = n // 2
    rows = x_ref.shape[1] // 2
    ring = {}

    def lane(way, h, s):
        d = far - s
        q = here.at(d if way == 0 else -d)
        before = ring.get((way, h, s - 1))
        if before is None:
            source = x_ref.at[q, pl.ds(h * rows, rows)]
        else:
            before.wait_recv()
            total = x_ref[q, pl.ds(h * rows, rows)].astype(f32) + got[way, h, s - 1].astype(f32)
            held[way, h, s - 1] = total.astype(held.dtype)
            source = held.at[way, h, s - 1]
        cp = remote(
            source, got.at[way, h, s], send.at[way, h, s], recv.at[way, h, s], here.next if way == 0 else here.prev
        )
        cp.start()
        ring[way, h, s] = cp

    for s in range(far):
        for turn in range(2):
            for way in range(2):
                h = way if turn == 1 else 1 - way
                if turn == 0 and s < 2:
                    continue
                lane(way, h, s)
        if s == 0:
            for way in range(2):
                lane(way, 1 - way, 1)
    for h in range(2):
        for way in range(2):
            ring[way, h, far - 1].wait_recv()
        at = pl.ds(h * rows, rows)
        total = x_ref[here.f, at].astype(f32)
        for way in range(2):
            total = total + got[way, h, far - 1].astype(f32)
        o_ref[at] = total
    for cp in ring.values():
        cp.wait_send()


def reduce_rows(mesh_sizes, cid, x):
    n_rep, n = mesh_sizes
    _, rows, width = x.shape
    far = n // 2
    dma = pltpu.SemaphoreType.DMA
    return pl.pallas_call(
        partial(rows_kernel, n_rep, n),
        out_shape=jax.ShapeDtypeStruct((rows, width), f32),
        in_specs=[VMEM],
        out_specs=VMEM,
        scratch_shapes=[
            pltpu.VMEM((2, 2, far - 1, rows // 2, width), x.dtype),
            pltpu.VMEM((2, 2, far, rows // 2, width), x.dtype),
            dma((2, 2, far)),
            dma((2, 2, far)),
        ],
        compiler_params=params(cid, 24 << 20),
        name="reduce_rows",
    )(x)


def slots_kernel(n_rep, n, to_slots, x_ref, o_ref, keep, a_s, a_r, f_s, f_r):
    here = Place(n_rep, n)
    ypeer = (lax.rem(here.r + 2, 4), here.f)
    me = here.f
    others = [lax.rem(me + k, n) for k in range(1, n)]
    enter([(here.r, o) for o in others] + [here.core, ypeer])

    def spot(source, r):
        return o_ref.at[:, source, r] if to_slots else o_ref.at[source, :, r]

    copies = []
    for k, o in enumerate(others):
        cp = remote(x_ref.at[o], spot(me, here.r), a_s.at[k], a_r.at[k], (here.r, o))
        cp.start()
        copies.append(cp)
    own = pltpu.make_async_copy(x_ref.at[me], spot(me, here.r), keep)
    own.start()
    sends, far = [], []
    for k in range(n):
        source = me if k == 0 else lax.rem(me - k + n, n)
        if k == 0:
            own.wait()
        else:
            copies[k - 1].wait_recv()
        held = spot(source, here.r)
        over = remote(held, held, f_s.at[0, k], f_r.at[0, k], ypeer)
        over.start()
        beside = remote(held, held, f_s.at[1, k], f_r.at[1, k], here.core)
        beside.start()
        far.append((over, source))
        sends.append(beside)
    yr = lax.rem(here.r + 2, 4)
    for k, (over, source) in enumerate(far):
        over.wait_recv()
        src = me if k == 0 else lax.rem(me - k + n, n)
        held = spot(src, yr)
        beside = remote(held, held, f_s.at[2, k], f_r.at[2, k], here.core)
        beside.start()
        sends.append(beside)
    for cp in copies:
        cp.wait_send()
    for over, _ in far:
        over.wait_send()
    for cp in sends:
        cp.wait()


def exchange_slots(mesh_sizes, cid, x, to_slots):
    n_rep, n = mesh_sizes
    _, cap, rows, width = x.shape
    shape = (cap, n, 4, rows, width) if to_slots else (n, cap, 4, rows, width)
    dma = pltpu.SemaphoreType.DMA
    return pl.pallas_call(
        partial(slots_kernel, n_rep, n, to_slots),
        out_shape=jax.ShapeDtypeStruct(shape, x.dtype),
        in_specs=[VMEM],
        out_specs=ANY,
        scratch_shapes=[dma, dma((n - 1,)), dma((n - 1,)), dma((3, n)), dma((3, n))],
        compiler_params=params(cid),
        name=f"slots_{cid}",
    )(x)


def layer_norm(inputs, gain_row):
    centre = inputs - jnp.mean(inputs, axis=-1, keepdims=True)
    spread = jnp.mean(centre * centre, axis=-1, keepdims=True)
    return centre * lax.rsqrt(spread + norm_epsilon) * gain_row


def adam_moments(moment_old, second_old, gradient, first_fix, second_fix):
    moment_new = beta_first * moment_old + (1.0 - beta_first) * gradient
    second_new = beta_second * second_old + (1.0 - beta_second) * gradient * gradient
    step_value = moment_new / first_fix / (jnp.sqrt(second_new / second_fix) + adam_epsilon)
    return (moment_new, second_new, step_value)


def head_slopes(head_count):
    return 2.0 ** (-8.0 * (jnp.arange(head_count, dtype=f32) + 1.0) / head_count)


NT = (((1,), (1,)), ((), ()))
TN = (((0,), (0,)), ((), ()))
masked_distance = 1e33


def mm(a, b, dims=None):
    if dims is None:
        return jnp.dot(a, b, preferred_element_type=f32)
    return lax.dot_general(a, b, dims, preferred_element_type=f32)


def norm_parts(x):
    centre = x - jnp.mean(x, axis=-1, keepdims=True)
    spread = jnp.mean(centre * centre, axis=-1, keepdims=True)
    rstd = lax.rsqrt(spread + norm_epsilon)
    return centre * rstd, rstd


def norm_back(x, gain, grad):
    hat, rstd = norm_parts(x)
    inner = grad * gain
    back = inner - jnp.mean(inner, axis=-1, keepdims=True) - hat * jnp.mean(inner * hat, axis=-1, keepdims=True)
    return rstd * back, grad * hat


def fold8(x):
    total = x[:8]
    for k in range(1, x.shape[0] // 8):
        total = total + x[k * 8 : k * 8 + 8]
    return total


def pair_bias(seg_row, seg_col, bias):
    length = bias.shape[0]
    i = lax.broadcasted_iota(jnp.int32, (length, length), 0)
    j = lax.broadcasted_iota(jnp.int32, (length, length), 1)
    apart = jnp.abs(i - j).astype(f32)
    bias[...] = jnp.where(seg_col == seg_row, apart, masked_distance)


def attend_kernel(slopes, x, gain, w, seg_row, seg_col, y, a, qkv, o, lse, bias):
    pair = pl.program_id(1)
    length, width = x.shape
    half = width // HEADS
    two = 2 * half
    rows = ROWS

    @pl.when(pair == 0)
    def _():
        pair_bias(seg_row[0], seg_col[0], bias)

        @pl.loop(0, length // rows)
        def _(i):
            at = pl.ds(pl.multiple_of(i * rows, rows), rows)
            hat, _ = norm_parts(x[at])
            low = (hat * gain[...]).astype(bf16)
            a[at] = low
            for k in range(3):
                part = mm(low, w[k])
                if k == 0:
                    part = part.astype(bf16).astype(f32) * half ** (-0.5)
                qkv[at, k * width : (k + 1) * width] = part.astype(bf16)

    lanes = pl.ds(pl.multiple_of(pair * two, two), two)
    q = qkv[:, pl.ds(pl.multiple_of(pair * two, two), two)]
    k = qkv[:, pl.ds(pl.multiple_of(width + pair * two, two), two)]
    v = qkv[:, pl.ds(pl.multiple_of(2 * width + pair * two, two), two)]
    v_t = v.astype(f32).T.astype(bf16)
    left = lax.broadcasted_iota(jnp.int32, (length, two), 1) < half
    zero = jnp.zeros_like(q)
    out = []
    for e in range(2):
        slope = slopes[2 * pair + e]
        q_e = jnp.where(left, q, zero) if e == 0 else jnp.where(left, zero, q)
        s = mm(k, q_e, NT) - slope * bias[...]
        top = jnp.max(s, axis=0, keepdims=True)
        p = jnp.exp(s - top)
        total = jnp.sum(p, axis=0, keepdims=True)
        low = (p * (1.0 / total)).astype(bf16)
        out.append(mm(v_t, low))
        lse[0, pl.ds(2 * pair + e, 1)] = top + jnp.log(total)
    upper = lax.broadcasted_iota(jnp.int32, (two, length), 0) < half
    o[:, lanes] = jnp.where(upper, out[0], out[1]).T.astype(bf16)

    @pl.when(pair == pl.num_programs(1) - 1)
    def _():
        @pl.loop(0, length // rows)
        def _(i):
            at = pl.ds(pl.multiple_of(i * rows, rows), rows)
            y[at] = x[at] + mm(o[at], w[3])


def attend(x, gain, weights, layer, seg):
    packs, length = seg.shape
    tokens, width = x.shape
    per_layer4 = weights.shape[0] // LAYERS // 4
    slopes = head_slopes(HEADS)
    whole = lambda shape: pl.BlockSpec(shape, lambda m, p: (m,) + (0,) * (len(shape) - 1))
    fixed = lambda shape, at: pl.BlockSpec(shape, lambda m, p: at)
    return pl.pallas_call(
        attend_kernel,
        grid=(packs, HEADS // 2),
        in_specs=[
            pl.BlockSpec(memory_space=pltpu.SMEM),
            whole((length, width)),
            fixed((1, width), (0, 0)),
            fixed((4, width, width), (per_layer4 * layer, 0, 0)),
            whole((1, 1, length)),
            whole((1, length, 1)),
        ],
        out_specs=[
            whole((length, width)),
            whole((length, width)),
            whole((length, 3 * width)),
            whole((length, width)),
            whole((1, HEADS, length)),
        ],
        out_shape=[
            jax.ShapeDtypeStruct((tokens, width), f32),
            jax.ShapeDtypeStruct((tokens, width), bf16),
            jax.ShapeDtypeStruct((tokens, 3 * width), bf16),
            jax.ShapeDtypeStruct((tokens, width), bf16),
            jax.ShapeDtypeStruct((packs, HEADS, length), f32),
        ],
        scratch_shapes=[pltpu.VMEM((length, length), f32)],
        compiler_params=pltpu.CompilerParams(vmem_limit_bytes=48 << 20),
        name="attend",
    )(slopes, x, gain.reshape(1, width), weights, seg.reshape(packs, 1, length), seg.reshape(packs, length, 1))


def attend_back_kernel(
    slopes, dx, x, gain, w, a, qkv, o, lse, seg_row, seg_col, new, dgain, gw, bias, do, dqkv, acc
):
    pack, pair = pl.program_id(0), pl.program_id(1)
    length, width = x.shape
    half = width // HEADS
    two = 2 * half
    rows = ROWS

    @pl.when(pair == 0)
    def _():
        pair_bias(seg_row[0], seg_col[0], bias)

        @pl.loop(0, length // rows)
        def _(i):
            at = pl.ds(pl.multiple_of(i * rows, rows), rows)
            do[at] = mm(dx[at].astype(bf16), w[3], NT).astype(bf16)

        part = mm(o[...], dx[...].astype(bf16), TN)

        @pl.when(pack == 0)
        def _():
            acc[3] = part

        @pl.when(pack > 0)
        def _():
            acc[3] += part

    lanes = [pl.ds(pl.multiple_of(n * width + pair * two, two), two) for n in range(3)]
    q, k, v = [qkv[:, at] for at in lanes]
    do_p = do[:, lanes[0]]
    k_t = k.astype(f32).T.astype(bf16)
    left = lax.broadcasted_iota(jnp.int32, (length, two), 1) < half
    upper = lax.broadcasted_iota(jnp.int32, (two, length), 0) < half
    zero = jnp.zeros_like(q)
    dq, dk, dv = [], [], []
    for e in range(2):
        slope = slopes[2 * pair + e]
        keep = (lambda t: jnp.where(left, t, zero)) if e == 0 else (lambda t: jnp.where(left, zero, t))
        s = mm(k, keep(q), NT) - slope * bias[...]
        p = jnp.exp(s - lse[0, pl.ds(2 * pair + e, 1)])
        dp = mm(v, keep(do_p), NT)
        inner = jnp.sum(p * dp, axis=0, keepdims=True)
        ds = (p * (dp - inner)).astype(bf16)
        dv.append(mm(p.astype(bf16), do_p))
        dk.append(mm(ds, q))
        dq.append(mm(k_t, ds))
    dqkv[:, lanes[0]] = (jnp.where(upper, dq[0], dq[1]).T * half ** (-0.5)).astype(bf16)
    dqkv[:, lanes[1]] = jnp.where(left, dk[0], dk[1]).astype(bf16)
    dqkv[:, lanes[2]] = jnp.where(left, dv[0], dv[1]).astype(bf16)

    @pl.when(pair == pl.num_programs(1) - 1)
    def _():
        def chunk(i, total):
            at = pl.ds(pl.multiple_of(i * rows, rows), rows)
            da = mm(dqkv[at, :width], w[0], NT)
            da = da + mm(dqkv[at, width : 2 * width], w[1], NT)
            da = da + mm(dqkv[at, 2 * width :], w[2], NT)
            back, extra = norm_back(x[at], gain[...], da)
            new[at] = dx[at] + back
            return total + fold8(extra)

        dgain[0] = lax.fori_loop(0, length // rows, chunk, jnp.zeros((8, width), f32))
        for n in range(3):
            part = mm(a[...], dqkv[:, n * width : (n + 1) * width], TN)

            @pl.when(pack == 0)
            def _(part=part, n=n):
                acc[n] = part

            @pl.when(pack > 0)
            def _(part=part, n=n):
                acc[n] += part

    @pl.when((pair == pl.num_programs(1) - 1) & (pack == pl.num_programs(0) - 1))
    def _():
        for n in range(4):
            gw[n] = acc[n].astype(bf16)


def attend_back(dx, x, gain, weights, layer, seg, kept):
    a, qkv, o, lse = kept
    packs, length = seg.shape
    tokens, width = x.shape
    per_layer4 = weights.shape[0] // LAYERS // 4
    whole = lambda shape: pl.BlockSpec(shape, lambda m, p: (m,) + (0,) * (len(shape) - 1))
    fixed = lambda shape, at: pl.BlockSpec(shape, lambda m, p: at)
    return pl.pallas_call(
        attend_back_kernel,
        grid=(packs, HEADS // 2),
        in_specs=[
            pl.BlockSpec(memory_space=pltpu.SMEM),
            whole((length, width)),
            whole((length, width)),
            fixed((1, width), (0, 0)),
            fixed((4, width, width), (per_layer4 * layer, 0, 0)),
            whole((length, width)),
            whole((length, 3 * width)),
            whole((length, width)),
            whole((1, HEADS, length)),
            whole((1, 1, length)),
            whole((1, length, 1)),
        ],
        out_specs=[
            whole((length, width)),
            whole((1, 8, width)),
            fixed((4, width, width), (0, 0, 0)),
        ],
        out_shape=[
            jax.ShapeDtypeStruct((tokens, width), f32),
            jax.ShapeDtypeStruct((packs, 8, width), f32),
            jax.ShapeDtypeStruct((4, width, width), bf16),
        ],
        scratch_shapes=[
            pltpu.VMEM((length, length), f32),
            pltpu.VMEM((length, width), bf16),
            pltpu.VMEM((length, 3 * width), bf16),
            pltpu.VMEM((4, width, width), f32),
        ],
        compiler_params=pltpu.CompilerParams(vmem_limit_bytes=56 << 20),
        name="attend_back",
    )(
        head_slopes(HEADS),
        dx,
        x,
        gain.reshape(1, width),
        weights,
        a,
        qkv,
        o,
        lse,
        seg.reshape(packs, 1, length),
        seg.reshape(packs, length, 1),
    )


ROWS = 512
gelu_c = math.sqrt(2.0 / math.pi)


def feed_kernel(x, gain, wg, wu, wd, y, f, gate, up):
    k = pl.program_id(0)
    tokens = x.shape[0]
    rows = ROWS

    @pl.loop(0, tokens // rows)
    def _(i):
        at = pl.ds(pl.multiple_of(i * rows, rows), rows)

        @pl.when(k == 0)
        def _():
            hat, _ = norm_parts(x[at])
            f[at] = (hat * gain[...]).astype(bf16)
            y[at] = x[at]

        low = f[at]
        g = mm(low, wg[0]).astype(bf16)
        u = mm(low, wu[0]).astype(bf16)
        gate[0, at] = g
        up[0, at] = u
        g, u = g.astype(f32), u.astype(f32)
        cdf = 0.5 * (1.0 + jnp.tanh(gelu_c * (g + 0.044715 * (g * g * g))))
        hidden = (g * cdf * u).astype(bf16)
        y[at] += mm(hidden, wd[0])


def feed(x, gain, weights, layer):
    tokens, width = x.shape
    per_layer = weights.shape[0] // LAYERS
    pieces = FF // width
    fixed = lambda shape: pl.BlockSpec(shape, lambda k: (0,) * len(shape))
    block = lambda skip: pl.BlockSpec((1, width, width), lambda k: (per_layer * layer + skip + k, 0, 0))
    each = pl.BlockSpec((1, tokens, width), lambda k: (k, 0, 0))
    return pl.pallas_call(
        feed_kernel,
        grid=(pieces,),
        in_specs=[fixed((tokens, width)), fixed((1, width)), block(4), block(4 + pieces), block(4 + 2 * pieces)],
        out_specs=[fixed((tokens, width)), fixed((tokens, width)), each, each],
        out_shape=[
            jax.ShapeDtypeStruct((tokens, width), f32),
            jax.ShapeDtypeStruct((tokens, width), bf16),
            jax.ShapeDtypeStruct((pieces, tokens, width), bf16),
            jax.ShapeDtypeStruct((pieces, tokens, width), bf16),
        ],
        compiler_params=pltpu.CompilerParams(vmem_limit_bytes=48 << 20),
        name="feed",
    )(x, gain.reshape(1, width), weights, weights, weights)


def feed_back_kernel(dx, x, gain, wg, wu, wd, f, gate, up, new, dgain, gg, gu, gd, f_t, dz, hid, dg, du):
    k = pl.program_id(0)
    tokens, width = x.shape
    rows = ROWS
    last = pl.num_programs(0) - 1

    @pl.when(k == 0)
    def _():
        @pl.loop(0, tokens // rows)
        def _(i):
            at = pl.ds(pl.multiple_of(i * rows, rows), rows)
            f_t[:, at] = f[at].astype(f32).T.astype(bf16)
            dz[at] = dx[at].astype(bf16)
            new[at] = jnp.zeros((rows, width), f32)

    def chunk(i, total):
        at = pl.ds(pl.multiple_of(i * rows, rows), rows)
        dh = mm(dz[at], wd[0], NT)
        g, u = gate[0, at].astype(f32), up[0, at].astype(f32)
        square = g * g
        t = jnp.tanh(gelu_c * (g + 0.044715 * (square * g)))
        cdf = 0.5 * (1.0 + t)
        act = g * cdf
        slope = cdf + 0.5 * g * (1.0 - t * t) * (gelu_c * (1.0 + 3 * 0.044715 * square))
        hid[at] = (act * u).astype(bf16)
        dgate = (dh * u * slope).astype(bf16)
        dup = (dh * act).astype(bf16)
        dg[at] = dgate
        du[at] = dup
        new[at] += mm(dgate, wg[0], NT) + mm(dup, wu[0], NT)
        return total

    lax.fori_loop(0, tokens // rows, chunk, 0)
    gg[0] = mm(f_t[...], dg[...]).astype(bf16)
    gu[0] = mm(f_t[...], du[...]).astype(bf16)
    gd[0] = mm(hid[...], dz[...], TN).astype(bf16)

    @pl.when(k == last)
    def _():
        def finish(i, total):
            at = pl.ds(pl.multiple_of(i * rows, rows), rows)
            back, extra = norm_back(x[at], gain[...], new[at])
            new[at] = dx[at] + back
            return total + fold8(extra)

        dgain[...] = lax.fori_loop(0, tokens // rows, finish, jnp.zeros((8, width), f32))


def feed_back(dx, x, gain, weights, layer, kept):
    f, gate, up = kept
    tokens, width = x.shape
    per_layer = weights.shape[0] // LAYERS
    pieces = FF // width
    fixed = lambda shape: pl.BlockSpec(shape, lambda k: (0,) * len(shape))
    block = lambda skip: pl.BlockSpec((1, width, width), lambda k: (per_layer * layer + skip + k, 0, 0))
    each = pl.BlockSpec((1, tokens, width), lambda k: (k, 0, 0))
    grad = pl.BlockSpec((1, width, width), lambda k: (k, 0, 0))
    return pl.pallas_call(
        feed_back_kernel,
        grid=(pieces,),
        in_specs=[
            fixed((tokens, width)),
            fixed((tokens, width)),
            fixed((1, width)),
            block(4),
            block(4 + pieces),
            block(4 + 2 * pieces),
            fixed((tokens, width)),
            each,
            each,
        ],
        out_specs=[fixed((tokens, width)), fixed((8, width)), grad, grad, grad],
        out_shape=[
            jax.ShapeDtypeStruct((tokens, width), f32),
            jax.ShapeDtypeStruct((8, width), f32),
        ]
        + [jax.ShapeDtypeStruct((pieces, width, width), bf16)] * 3,
        scratch_shapes=[
            pltpu.VMEM((width, tokens), bf16),
            pltpu.VMEM((tokens, width), bf16),
            pltpu.VMEM((tokens, width), bf16),
            pltpu.VMEM((tokens, width), bf16),
            pltpu.VMEM((tokens, width), bf16),
        ],
        compiler_params=pltpu.CompilerParams(vmem_limit_bytes=56 << 20),
        name="feed_back",
    )(dx, x, gain.reshape(1, width), weights, weights, weights, f, gate, up)


def two_parts(x):
    top = x.astype(bf16)
    return top, (x - top.astype(f32)).astype(bf16)


def mm3(a, b, dims=None):
    (a1, a2), (b1, b2) = a, b
    return mm(a1, b1, dims) + (mm(a1, b2, dims) + mm(a2, b1, dims))


def turn_kernel(scalars, numbers, left, right, some, grad, m, v, m_new, v_new, turned):
    slot = pl.program_id(0)
    factor, first_fix, second_fix = numbers[0], numbers[1], numbers[2]
    bases = two_parts(right[0])
    left_top, left_rest = two_parts(left[0])
    rotated = mm(left_top, grad[0], TN) + mm(left_rest, grad[0], TN)
    rotated = factor * mm3(two_parts(rotated), bases)
    moment, second, step = adam_moments(m[0], v[0], rotated, first_fix, second_fix)
    live = scalars[1 + slot] > 0
    m_new[0] = jnp.where(live, moment, m[0])
    v_new[0] = jnp.where(live, second, v[0])
    groups, _, rows, width = turned.shape
    rows_here = some[...].reshape(groups * rows, width)
    out = mm3(two_parts(rows_here), two_parts(step))
    out = mm3(two_parts(out), bases, NT)
    turned[...] = out.astype(turned.dtype).reshape(turned.shape)


def turn_slots(replica, live, numbers, left, right, grads, m, v):
    cap, width, _ = left.shape
    groups = width // 64
    scalars = jnp.concatenate([replica.reshape(1), live.astype(jnp.int32)])
    view = left.reshape(cap, groups, 4, 16, width)
    whole = pl.BlockSpec((1, width, width), lambda s, scalars: (s, 0, 0))
    grid_spec = pltpu.PrefetchScalarGridSpec(
        num_scalar_prefetch=1,
        grid=(cap,),
        in_specs=[
            pl.BlockSpec(memory_space=pltpu.SMEM),
            whole,
            whole,
            pl.BlockSpec((1, groups, 1, 16, width), lambda s, scalars: (s, 0, scalars[0], 0, 0)),
            whole,
            whole,
            whole,
        ],
        out_specs=[whole, whole, pl.BlockSpec((groups, 1, 16, width), lambda s, scalars: (0, s, 0, 0))],
    )
    return pl.pallas_call(
        turn_kernel,
        grid_spec=grid_spec,
        out_shape=[
            jax.ShapeDtypeStruct(m.shape, f32),
            jax.ShapeDtypeStruct(v.shape, f32),
            jax.ShapeDtypeStruct((groups, cap, 16, width), bf16),
        ],
        compiler_params=pltpu.CompilerParams(vmem_limit_bytes=56 << 20),
        name="turn_slots",
    )(scalars, numbers, left, right, view, grads, m, v)


class Transport:
    def __init__(self, n_rep, n_fsdp, shard_rows):
        self.sizes = (n_rep, n_fsdp)
        self.kernels = n_rep == 4 and n_fsdp == 8 and shard_rows == 64

    def open(self, cid, shard, table, wanted, facts, gains):
        if self.kernels:
            return open_step(self.sizes, cid, shard, table, wanted, facts, gains)
        asked = lax.all_to_all(wanted, "fsdp", split_axis=0, concat_axis=0, tiled=True)
        rows = jnp.take(table.astype(bf16), asked.reshape(-1), axis=0)
        rows = rows.reshape(wanted.shape[0], wanted.shape[2], table.shape[1])
        return (
            lax.all_gather(shard, "fsdp", axis=1, tiled=True),
            self.spread(cid, rows),
            asked,
            lax.all_gather(facts, "fsdp"),
            lax.all_gather(gains, "fsdp"),
            lax.pmax(facts, ("rep", "fsdp")),
        )

    def spread(self, cid, x):
        if self.kernels:
            return group_exchange(self.sizes, cid, x, True)
        return lax.all_to_all(x, "fsdp", split_axis=0, concat_axis=0, tiled=True)

    def share(self, cid, x):
        if self.kernels:
            return group_exchange(self.sizes, cid, x, False)
        return lax.all_gather(x, "fsdp")

    def share_rows(self, cid, x):
        if self.kernels:
            return ring_rows(self.sizes, cid, x)
        return lax.all_gather(x, "fsdp")

    def sum_rows(self, cid, x):
        if self.kernels:
            return reduce_rows(self.sizes, cid, x)
        return lax.psum_scatter(x.astype(f32), "fsdp", scatter_dimension=0)


def body(
    token_ids,
    segment_ids,
    masked_pos,
    labels,
    blocks,
    gains,
    embed,
    embed_m,
    embed_v,
    gains_m,
    gains_v,
    soap_m,
    soap_v,
    left_basis,
    right_basis,
    block_slots,
    step_count,
):
    groups = lax.axis_size("fsdp")
    replicas = lax.axis_size("rep")
    member = lax.axis_index("fsdp")
    replica = lax.axis_index("rep")
    micro_count = token_ids.shape[0]
    pack_length = token_ids.shape[2]
    pick_count = masked_pos.shape[2]
    vocab_rows, model_width = embed.shape
    block_count, shard_rows, _ = blocks.shape
    gain_count = gains.shape[0]
    tokens = micro_count * pack_length
    picks = micro_count * pick_count
    move = Transport(replicas, groups, shard_rows)
    table_low = embed.astype(bf16)

    ids = token_ids.reshape(tokens)
    index = jnp.arange(tokens, dtype=jnp.int32)
    owner = ids // vocab_rows
    local = ids - owner * vocab_rows
    first_at = jnp.min(jnp.where(ids[:, None] == ids[None, :], index[None, :], tokens), axis=1)
    is_first = first_at == index
    ahead = is_first[None, :] & (owner[:, None] == owner[None, :]) & (index[None, :] < first_at[:, None])
    rank = jnp.sum(ahead.astype(jnp.int32), axis=1)
    most = jnp.max(rank) + 1

    my_labels = labels.reshape(picks // 128, 128)
    facts = jnp.concatenate(
        [my_labels, jnp.full((8 - picks // 128, 128), most, jnp.int32)], axis=0
    )
    gain_pad = jnp.pad(gains, ((0, 8 - gain_count), (0, 128 - gains.shape[1])))
    slots = groups * CAPACITY
    most_rounds = (tokens + CAPACITY - 1) // CAPACITY
    slot_index = jnp.arange(slots, dtype=jnp.int32)

    def slot_of(k):
        here = rank - k * CAPACITY
        return jnp.where((here >= 0) & (here < CAPACITY), owner * CAPACITY + here, -1)

    def wanted_in(slot):
        wanted = jnp.where((slot[None, :] == slot_index[:, None]) & is_first[None, :], local[None, :], 0)
        return jnp.sum(wanted, axis=1).reshape(groups, 1, CAPACITY)

    def placed(slot, rows):
        chosen = (slot[:, None] == slot_index[None, :]).astype(bf16)
        return jnp.dot(chosen, rows.reshape(slots, model_width), preferred_element_type=f32)

    slot = slot_of(0)
    full_blocks, rows, asked, group_facts, gain_rows, most_facts = move.open(
        0, blocks.astype(bf16), embed, wanted_in(slot), facts, gain_pad
    )
    rounds = (most_facts[7, 0] + CAPACITY - 1) // CAPACITY
    all_labels = group_facts[:, : picks // 128].reshape(groups * picks)
    gain_rows = gain_rows[:, :gain_count, : gains.shape[1]].transpose(1, 0, 2).reshape(gain_count, model_width)
    gain_rows = lax.reduce_precision(gain_rows, exponent_bits=8, mantissa_bits=7)
    embedded = placed(slot, rows)
    asked_all = jnp.zeros((most_rounds, slots), jnp.int32).at[0].set(asked.reshape(slots))

    def look(state):
        k, rows_so_far, asked_all = state
        slot = slot_of(k)
        asked = move.spread(1, wanted_in(slot))
        asked_all = lax.dynamic_update_index_in_dim(asked_all, asked.reshape(slots), k, 0)
        rows = jnp.take(table_low, asked.reshape(slots), axis=0).reshape(groups, CAPACITY, model_width)
        return k + 1, rows_so_far + placed(slot, move.spread(2, rows)), asked_all

    _, embedded, asked_all = lax.while_loop(lambda s: s[0] < rounds, look, (jnp.int32(1), embedded, asked_all))

    segments = segment_ids.reshape(micro_count, pack_length)
    stream, first_pull = jax.vjp(layer_norm, embedded, gain_rows[0])
    saved_layers = []
    for layer in range(LAYERS):
        middle, *attention_kept = attend(stream, gain_rows[1 + 2 * layer], full_blocks, layer, segments)
        after, *feed_kept = feed(middle, gain_rows[2 + 2 * layer], full_blocks, layer)
        saved_layers.append((stream, attention_kept, middle, feed_kept))
        stream = after
    final_rows, final_pull = jax.vjp(layer_norm, stream, gain_rows[gain_count - 1])

    positions = masked_pos.reshape(micro_count, pick_count)
    flat_positions = (positions + jnp.arange(micro_count, dtype=jnp.int32)[:, None] * pack_length).reshape(picks)
    picked = jnp.take(final_rows, flat_positions, axis=0).astype(bf16)
    all_picked = move.share_rows(4, picked).reshape(groups * picks, model_width)
    logits = jnp.einsum("td,vd->tv", all_picked, table_low, preferred_element_type=f32)
    top_value = jnp.max(logits, axis=-1)
    exp_total = jnp.sum(jnp.exp(logits - top_value[:, None]), axis=-1)
    label_local = all_labels - member * vocab_rows
    columns = jnp.arange(vocab_rows, dtype=jnp.int32)
    label_hits = columns[None, :] == label_local[:, None]
    target = jnp.sum(jnp.where(label_hits, logits, 0.0), axis=-1)
    stats = move.share(5, jnp.stack([top_value, exp_total, target]))
    top_all = jnp.max(stats[:, 0], axis=0)
    total_all = jnp.sum(stats[:, 1] * jnp.exp(stats[:, 0] - top_all[None]), axis=0)
    target_all = jnp.sum(stats[:, 2], axis=0)
    entropy = top_all + jnp.log(total_all) - target_all
    loss_local = jnp.sum(lax.dynamic_slice_in_dim(entropy, member * picks, picks))
    grad_logits = (
        jnp.exp(logits - top_all[:, None]) / total_all[:, None] - label_hits.astype(f32)
    ).astype(bf16)
    grad_table = jnp.einsum("tv,td->vd", grad_logits, all_picked, preferred_element_type=f32)
    grad_picked = jnp.einsum("tv,vd->td", grad_logits, table_low, preferred_element_type=f32)
    grad_picked = move.sum_rows(6, grad_picked.astype(bf16).reshape(groups, picks, model_width))

    match = flat_positions[None, :] == index[:, None]
    place = jnp.sum(jnp.where(match, jnp.arange(picks, dtype=jnp.int32)[None, :] + 1, 0), axis=1)
    grad_final = jnp.where(
        (place > 0)[:, None], jnp.take(grad_picked, jnp.maximum(place - 1, 0), axis=0), 0.0
    )
    grad_stream, grad_final_gain = final_pull(grad_final)
    gain_grads = [None] * gain_count
    gain_grads[gain_count - 1] = grad_final_gain
    layer_grads = [None] * LAYERS
    for layer in reversed(range(LAYERS)):
        before, attention_kept, middle, feed_kept = saved_layers[layer]
        grad_stream, feed_gain, *grads_feed = feed_back(
            grad_stream, middle, gain_rows[2 + 2 * layer], full_blocks, layer, feed_kept
        )
        grad_stream, attention_gain, grads_attention = attend_back(
            grad_stream, before, gain_rows[1 + 2 * layer], full_blocks, layer, segments, attention_kept
        )
        gain_grads[1 + 2 * layer] = jnp.sum(attention_gain, axis=(0, 1))
        gain_grads[2 + 2 * layer] = jnp.sum(feed_gain, axis=0)
        layer_grads[layer] = [grads_attention] + grads_feed
    grad_embedded, gain_grads[0] = first_pull(grad_stream)
    grad_rows = grad_embedded.astype(bf16)
    padded_rows = -(-vocab_rows // 384) * 384
    grad_table = jnp.pad(grad_table, ((0, padded_rows - vocab_rows), (0, 0)))
    row_index = jnp.arange(padded_rows, dtype=jnp.int32)

    def given(cid, k, grad_table):
        chosen = (slot_index[:, None] == slot_of(k)[None, :]).astype(bf16)
        rows = jnp.dot(chosen, grad_rows, preferred_element_type=f32).astype(bf16)
        rows = move.spread(cid, rows.reshape(groups, CAPACITY, model_width)).reshape(slots, model_width)
        asked = lax.dynamic_index_in_dim(asked_all, k, 0, keepdims=False)
        target_rows = (row_index[:, None] == asked[None, :]).astype(bf16)
        return grad_table + jnp.dot(target_rows, rows, preferred_element_type=f32)

    grad_table = given(7, 0, grad_table)
    _, grad_table = lax.while_loop(
        lambda s: s[0] < rounds, lambda s: (s[0] + 1, given(13, s[0], s[1])), (jnp.int32(1), grad_table)
    )
    grad_blocks = [g for grads in layer_grads for g in grads]
    grad_gains = jnp.stack(gain_grads, axis=0)

    position_count = micro_count * replicas * groups * pick_count
    clip_limit = clip_ratio * math.sqrt(position_count)
    steps_done = step_count[0].astype(f32)
    first_fix = 1.0 - beta_first**steps_done
    second_fix = 1.0 - beta_second**steps_done
    slot_cap = soap_m.shape[0]
    slot_total = slot_cap * groups
    named = jnp.arange(slot_total, dtype=jnp.int32)[:, None] == block_slots[None, :]
    taken = jnp.any(named, axis=1)
    block_of = jnp.sum(jnp.where(named, jnp.arange(block_count, dtype=jnp.int32)[None, :], 0), axis=1)

    small = jnp.zeros((8, model_width), f32).at[:gain_count].set(grad_gains)
    small = small.at[7, 0].set(loss_local)
    if move.kernels:
        owned, grad_table, small = settle_gradients(
            move.sizes,
            8,
            grad_blocks,
            grad_table.reshape(4, padded_rows // 4, model_width),
            small,
            block_of,
            taken.astype(jnp.int32),
            slot_cap,
        )
        grad_table = grad_table.reshape(padded_rows, model_width)[:vocab_rows]
        squares = jnp.sum(small[6])
        owned = owned.reshape(slot_cap, model_width, model_width)
    else:
        grad_blocks = jnp.concatenate([g.astype(f32) for g in grad_blocks], axis=0)
        mine = lax.psum_scatter(grad_blocks, "fsdp", scatter_dimension=1, tiled=True)
        mine, grad_table = lax.psum((mine, grad_table[:vocab_rows]), "rep")
        small = lax.psum(small, ("rep", "fsdp"))
        squares = lax.psum(jnp.sum(mine * mine) + jnp.sum(grad_table * grad_table), "fsdp")
        outgoing = jnp.where(taken[:, None, None], jnp.take(mine, block_of, axis=0), 0)
        owned = lax.all_to_all(outgoing, "fsdp", split_axis=0, concat_axis=1, tiled=True)
    loss_all = small[7, 0]
    grad_gains = small[:gain_count]
    grad_norm = jnp.sqrt(squares + jnp.sum(grad_gains * grad_gains))
    factor = jnp.minimum(1.0, clip_limit / grad_norm)
    grad_gains = lax.dynamic_slice_in_dim(grad_gains, member * gains.shape[1], gains.shape[1], axis=1)

    live = lax.dynamic_slice_in_dim(taken, member * slot_cap, slot_cap)
    if move.kernels:
        soap_m_new, soap_v_new, turned = turn_slots(
            replica,
            live,
            jnp.stack([factor, first_fix, second_fix]),
            left_basis,
            right_basis,
            owned,
            soap_m,
            soap_v,
        )
        returned = exchange_slots(move.sizes, 11, turned, False)
        returned = returned.reshape(slot_total, shard_rows, model_width)
    else:
        rotated = jnp.einsum("bji,bjk->bik", left_basis, owned, precision=high)
        rotated = factor * jnp.einsum("bik,bkl->bil", rotated, right_basis, precision=high)
        moment_first, moment_second, rotated_step = adam_moments(soap_m, soap_v, rotated, first_fix, second_fix)
        soap_m_new = jnp.where(live[:, None, None], moment_first, soap_m)
        soap_v_new = jnp.where(live[:, None, None], moment_second, soap_v)
        turned = jnp.einsum("bij,bjk->bik", left_basis, rotated_step, precision=high)
        turned = jnp.einsum("bik,blk->bil", turned, right_basis, precision=high)
        returned = lax.all_to_all(turned, "fsdp", split_axis=1, concat_axis=0, tiled=True)
    update = jnp.take(returned, block_slots, axis=0).astype(f32)
    blocks_new = blocks - step_rate * (update + weight_decay * blocks)

    embed_m_new, embed_v_new, table_step = adam_moments(
        embed_m, embed_v, factor * grad_table, first_fix, second_fix
    )
    embed_new = embed - step_rate * (table_step + weight_decay * embed)
    gains_m_new, gains_v_new, gain_step = adam_moments(
        gains_m, gains_v, factor * grad_gains, first_fix, second_fix
    )
    gains_new = gains - step_rate * gain_step
    loss = (loss_all / position_count).reshape(1)
    return (
        loss,
        grad_norm.reshape(1),
        blocks_new,
        gains_new,
        embed_new,
        embed_m_new,
        embed_v_new,
        gains_m_new,
        gains_v_new,
        soap_m_new,
        soap_v_new,
        blocks_new.astype(bf16),
        embed_new.astype(bf16),
    )


def solution(mesh):
    packs = P(None, ("rep", "fsdp"), None)
    rows = P(None, "fsdp", None)
    columns = P(None, "fsdp")
    table = P("fsdp", None)
    slots = P("fsdp", None, None)
    return jax.shard_map(
        body,
        mesh=mesh,
        in_specs=(packs,) * 4
        + (rows, columns)
        + (table,) * 3
        + (columns,) * 2
        + (slots,) * 4
        + (P(), P()),
        out_specs=(P(), P(), rows, columns)
        + (table,) * 3
        + (columns,) * 2
        + (slots,) * 2
        + (rows, table),
        check_vma=False,
    )
```

```python
from functools import partial
import math

import jax
import jax.numpy as jnp
from jax import lax
from jax.experimental import pallas as pl
from jax.experimental.pallas import tpu as pltpu
from jax.sharding import PartitionSpec as P

HEADS = 8
FF = 2048
LAYERS = 2

norm_epsilon = 1e-05
beta_first = 0.9
beta_second = 0.99
adam_epsilon = 1e-08
step_rate = 0.04
weight_decay = 0.1
clip_ratio = 12.0
masked_score = -1e30
bf16 = jnp.bfloat16
f32 = jnp.float32
highest = lax.Precision.HIGHEST
high = lax.Precision.HIGH
MESH = pl.DeviceIdType.MESH
ANY = pl.BlockSpec(memory_space=pl.ANY)
VMEM = pl.BlockSpec(memory_space=pltpu.VMEM)
CAPACITY = 128


def pick(table, index):
    out = jnp.int32(table[0])
    for k in range(1, len(table)):
        out = jnp.where(index == k, jnp.int32(table[k]), out)
    return out


def ring_order(n):
    nz = 4
    nx = n // nz
    order = []
    for x in range(nx):
        zs = range(1, nz) if x % 2 == 0 else range(nz - 1, 0, -1)
        order += [z * nx + x for z in zs]
    order += [x for x in range(nx - 1, -1, -1)]
    return order


class Place:
    def __init__(self, n_rep, n_fsdp):
        self.r = lax.axis_index("rep")
        self.f = lax.axis_index("fsdp")
        self.n_rep, self.n = n_rep, n_fsdp
        self.c = lax.rem(self.r, 2)
        self.y = self.r // 2
        self.order = ring_order(n_fsdp)
        spot = [self.order.index(k) for k in range(n_fsdp)]
        self.pos = pick(spot, self.f)
        self.core = (self.r + 1 - 2 * self.c, self.f)
        self.next = (self.r, self.at(1))
        self.prev = (self.r, self.at(-1))

    def at(self, step):
        return pick(self.order, lax.rem(self.pos + step + 2 * self.n, self.n))


def enter(peers):
    barrier = pltpu.get_barrier_semaphore()
    for peer in peers:
        pl.semaphore_signal(barrier, inc=1, device_id=peer, device_id_type=MESH)
    pl.semaphore_wait(barrier, len(peers))


def remote(src, dst, send, recv, peer):
    return pltpu.make_async_remote_copy(
        src_ref=src, dst_ref=dst, send_sem=send, recv_sem=recv, device_id=peer, device_id_type=MESH
    )


def params(cid, limit=None):
    return pltpu.CompilerParams(
        collective_id=cid, has_side_effects=True, vmem_limit_bytes=limit
    )


def group_kernel(n_rep, n, spread, x_ref, o_ref, send, recv):
    here = Place(n_rep, n)
    me = here.f
    others = [lax.rem(me + k, n) for k in range(1, n)]
    enter([(here.r, o) for o in others])
    copies = []
    for k, o in enumerate(others):
        src = x_ref.at[o] if spread else x_ref
        cp = remote(src, o_ref.at[me], send.at[k], recv.at[k], (here.r, o))
        cp.start()
        copies.append(cp)
    o_ref[me] = x_ref[me] if spread else x_ref[...]
    for cp in copies:
        cp.wait()


def group_exchange(mesh_sizes, cid, x, spread):
    n_rep, n = mesh_sizes
    shape = x.shape if spread else (n,) + x.shape
    return pl.pallas_call(
        partial(group_kernel, n_rep, n, spread),
        out_shape=jax.ShapeDtypeStruct(shape, x.dtype),
        in_specs=[VMEM],
        out_specs=VMEM,
        scratch_shapes=[pltpu.SemaphoreType.DMA((n - 1,)), pltpu.SemaphoreType.DMA((n - 1,))],
        compiler_params=params(cid),
        name=f"group_{cid}",
    )(x)


def opening_kernel(
    n_rep, n, half, shared, x_ref, t_ref, w_ref, facts_ref, gains_ref, o_ref, rows_ref, asked, facts, gains, most,
    table, index, stage, ready, held, got,
    t_s, ring_s, ring_r, core_s, core_r, y_s, y_r, over_s, over_r, ask_s, ask_r, top_s, top_r, rows_s, rows_r,
):
    here = Place(n_rep, n)
    me = here.f
    ypeer = (lax.rem(here.r + 2, 4), here.f)
    others = [lax.rem(me + k, n) for k in range(1, n)]
    rows = x_ref.shape[1]
    alone = (half - shared) // 2
    enter([(here.r, o) for o in others] + [here.core, ypeer])
    load = pltpu.make_async_copy(t_ref, table, t_s.at[0])
    load.start()
    asks = []
    for k, o in enumerate(others):
        peer = (here.r, o)
        asks.append(remote(w_ref.at[o], asked.at[me], ask_s.at[0, k], ask_r.at[0, k], peer))
        asks.append(remote(facts_ref, facts.at[me], ask_s.at[1, k], ask_r.at[1, k], peer))
        asks.append(remote(gains_ref, gains.at[me], ask_s.at[2, k], ask_r.at[2, k], peer))
    for cp in asks:
        cp.start()

    mine = pl.ds(here.c * half + here.y * alone, alone + shared)
    given = pl.ds(here.c * half + here.y * (alone + shared), alone)
    taken = pl.ds(here.c * half + (1 - here.y) * (alone + shared), alone)
    hops = n // 2
    copies, sends = [], []

    def rows_of(origin, way, s):
        if s == hops - 1:
            return pl.ds(pl.multiple_of(origin * rows + way * (rows // 2), rows // 2), rows // 2)
        return pl.ds(pl.multiple_of(origin * rows, rows), rows)

    own = remote(x_ref, o_ref.at[:, rows_of(here.f, 0, -1)], core_s.at[0, 0], core_r.at[0, 0], here.core)
    own.start()
    copies.append(own)
    waiting = [None, None]
    across = []

    def pass_on(way, s):
        waiting[way].wait_recv()
        where = rows_of(here.at(-s - 1 if way == 0 else s + 1), way, s)
        kept = o_ref.at[given, where]
        cp = remote(kept, kept, y_s.at[way, s], y_r.at[way, s], ypeer)
        cp.start()
        across.append((cp, o_ref.at[taken, where], way, s))
        kept = o_ref.at[mine, where]
        cp = remote(kept, kept, core_s.at[way, s + 1], core_r.at[way, s + 1], here.core)
        cp.start()
        copies.append(cp)

    def hop(way, s):
        where = rows_of(here.at(-s if way == 0 else s), way, s)
        src = x_ref.at[mine] if s == 0 else o_ref.at[mine, where]
        cp = remote(
            src, o_ref.at[mine, where], ring_s.at[way, s], ring_r.at[way, s], here.next if way == 0 else here.prev
        )
        cp.start()
        waiting[way] = cp
        sends.append(cp)

    for way in range(2):
        hop(way, 0)

    asked[me] = w_ref[me]
    facts[me] = facts_ref[...]
    gains[me] = gains_ref[...]
    for cp in asks:
        cp.wait_recv()
    listed = pltpu.make_async_copy(asked, index, t_s.at[1])
    listed.start()
    top = facts[0]
    for k in range(1, n):
        top = jnp.maximum(top, facts[k])
    held[0] = top
    first = remote(held.at[0], got.at[0], top_s.at[0], top_r.at[0], here.core)
    first.start()
    listed.wait()
    load.wait()
    places = rows_ref.shape[1]

    def collect(o):
        def one(i, carry):
            stage[pl.ds(i, 1)] = table[pl.ds(index[o, 0, i], 1)]
            return carry

        lax.fori_loop(0, places, one, 0, unroll=8)
        return stage[...].astype(bf16)

    for k, o in enumerate(others):
        ready[o] = collect(o)
        cp = remote(ready.at[o], rows_ref.at[me], rows_s.at[k], rows_r.at[k], (here.r, o))
        cp.start()
        asks.append(cp)
    rows_ref[me] = collect(me)
    first.wait_recv()
    held[1] = jnp.maximum(top, got[0])
    second = remote(held.at[1], got.at[1], top_s.at[1], top_r.at[1], ypeer)
    second.start()

    for s in range(1, hops):
        for way in range(2):
            pass_on(way, s - 1)
            hop(way, s)
    second.wait_recv()
    most[...] = jnp.maximum(held[1], got[1])
    for way in range(2):
        pass_on(way, hops - 1)
    for cp, kept, way, s in across:
        cp.wait_recv()
        over = remote(kept, kept, over_s.at[way, s], over_r.at[way, s], here.core)
        over.start()
        copies.append(over)
        sends.append(cp)
    for cp in asks[3 * (n - 1) :]:
        cp.wait_recv()
    for cp in asks + [first, second] + sends:
        cp.wait_send()
    for cp in copies:
        cp.wait()


def open_step(mesh_sizes, cid, shard, table, wanted, facts, gains):
    n_rep, n = mesh_sizes
    count, rows, width = shard.shape
    half = count // 2
    places = wanted.shape[2]
    dma = pltpu.SemaphoreType.DMA
    return pl.pallas_call(
        partial(opening_kernel, n_rep, n, half, half - 2 * (half // 3)),
        out_shape=[
            jax.ShapeDtypeStruct((count, rows * n, width), shard.dtype),
            jax.ShapeDtypeStruct((n, places, width), bf16),
            jax.ShapeDtypeStruct(wanted.shape, wanted.dtype),
            jax.ShapeDtypeStruct((n,) + facts.shape, facts.dtype),
            jax.ShapeDtypeStruct((n,) + gains.shape, gains.dtype),
            jax.ShapeDtypeStruct(facts.shape, facts.dtype),
        ],
        in_specs=[ANY, ANY] + [VMEM] * 3,
        out_specs=[ANY] + [VMEM] * 5,
        scratch_shapes=[
            pltpu.VMEM(table.shape, table.dtype),
            pltpu.SMEM(wanted.shape, wanted.dtype),
            pltpu.VMEM((places, width), table.dtype),
            pltpu.VMEM((n, places, width), bf16),
            pltpu.VMEM((2,) + facts.shape, facts.dtype),
            pltpu.VMEM((2,) + facts.shape, facts.dtype),
            dma((2,)),
            dma((2, n // 2)),
            dma((2, n // 2)),
            dma((2, n // 2 + 1)),
            dma((2, n // 2 + 1)),
            dma((2, n // 2)),
            dma((2, n // 2)),
            dma((2, n // 2)),
            dma((2, n // 2)),
            dma((3, n - 1)),
            dma((3, n - 1)),
            dma((2,)),
            dma((2,)),
            dma((n - 1,)),
            dma((n - 1,)),
        ],
        compiler_params=params(cid, 24 << 20),
        name="open_step",
    )(shard, table, wanted, facts, gains)


def squares_row(square):
    row = jnp.sum(square, axis=0, keepdims=True)
    return jnp.where(lax.broadcasted_iota(jnp.int32, square.shape, 0) == 6, row, 0.0)


def reduce_kernel(
    n_rep, n, half, table_rows, each, *refs
):
    g_refs, refs = refs[: 2 * each], refs[2 * each :]
    (
    t_ref, small_ref, block_of, taken, o_ref, to_ref, sum_ref, mine, outgoing, held, hgot, four, fours, squares,
    own, part, got, fin, ysend, ygot, town, tpart, tsend, tgot,
    load_s, core_s, core_r, ring_s, ring_r, y_s, y_r, tload, tcs, tcr, tys, tyr, tos, tor,
    keep, a_s, a_r, f_s, f_r, sum_s, sum_r,
    ) = refs
    here = Place(n_rep, n)
    c, y = here.c, here.y
    ypeer = (lax.rem(here.r + 2, 4), here.f)
    other_c, other_y = 1 - c, 1 - y
    me = here.f
    others = [lax.rem(me + k, n) for k in range(1, n)]
    enter([(here.r, o) for o in others] + [here.core, ypeer])
    far = n // 2

    tl = pltpu.make_async_copy(t_ref.at[pl.ds(c * 2, 2)], town, tload)
    tl.start()
    tc = remote(t_ref.at[pl.ds(other_c * 2, 2)], tpart, tcs, tcr, here.core)
    tc.start()

    spots = {(0, far): 0, (1, far): 0}
    for d in range(far - 1, 0, -1):
        spots[0, d] = 1 + 2 * (far - 1 - d)
        spots[1, d] = 2 + 2 * (far - 1 - d)
    spots[0, 0] = spots[1, 0] = n - 1
    loads, cores = {}, {}
    done = set()
    for (way, d), spot in sorted(spots.items(), key=lambda item: item[1]):
        if spot in done:
            continue
        done.add(spot)
        to = here.f if d == 0 else here.at(d if way == 0 else -d)
        for h in (way, 1 - way):
            loads[spot, h], cores[spot, h] = [], []
            for j in range(each):
                g_ref = g_refs[h * each + j]
                into = pl.ds(j * (half // each), half // each)
                ld = pltpu.make_async_copy(g_ref.at[:, to, :, c], own.at[spot, h, into], load_s.at[spot, h, j])
                ld.start()
                loads[spot, h].append(ld)
                cp = remote(
                    g_ref.at[:, to, :, other_c],
                    part.at[spot, h, into],
                    core_s.at[spot, h, j],
                    core_r.at[spot, h, j],
                    here.core,
                )
                cp.start()
                cores[spot, h].append(cp)

    def ready(spot, h):
        for j in range(each):
            loads[spot, h][j].wait()
            cores[spot, h][j].wait_recv()

    ring = {}

    def came(way, h, s):
        return got.at[way, h, s]

    def lane(way, h, s):
        d = far - s
        spot = spots[way, d]
        ready(spot, h)
        before = ring.get((way, h, s - 1))
        if before is not None:
            before.wait_recv()
        target = own.at[spot, h]

        @pl.loop(0, half)
        def _(b):
            for k in range(2):
                total = own[spot, h, b, k].astype(f32) + part[spot, h, b, k].astype(f32)
                if before is not None:
                    total = total + came(way, h, s - 1)[b, k].astype(f32)
                target[b, k] = total.astype(target.dtype)

        cp = remote(
            target, came(way, h, s), ring_s.at[way, h, s], ring_r.at[way, h, s], here.next if way == 0 else here.prev
        )
        cp.start()
        ring[way, h, s] = cp

    step_rows = 48
    for s in range(far):
        for h_turn in range(2):
            for way in range(2):
                h = way if h_turn == 1 else 1 - way
                if s == 0 and h_turn == 0:
                    continue
                if s == 1 and h_turn == 0:
                    continue
                lane(way, h, s)
        if s == 0:
            for way in range(2):
                lane(way, 1 - way, 1)
            tl.wait()
            tc.wait_recv()

            @pl.loop(0, table_rows // step_rows)
            def _(i):
                at = pl.ds(pl.multiple_of(i * step_rows, step_rows), step_rows)
                town[y, at] = town[y, at] + tpart[y, at]
                tsend[at] = (town[other_y, at] + tpart[other_y, at]).astype(bf16)

            ty = remote(tsend, tgot, tys, tyr, ypeer)
            ty.start()
        if s == 2:
            ty.wait_recv()

            def add(i, acc):
                at = pl.ds(pl.multiple_of(i * step_rows, step_rows), step_rows)
                total = town[y, at] + tgot[at].astype(f32)
                town[y, at] = total
                square = total * total
                for k in range(step_rows // 8):
                    acc = acc + square[k * 8 : k * 8 + 8]
                return acc

            squares[...] = lax.fori_loop(0, table_rows // step_rows, add, jnp.zeros((8, tgot.shape[1]), f32))
            quarter = c * 2 + y
            near = c * 2 + other_y
            tkeep = pltpu.make_async_copy(town.at[y], to_ref.at[quarter], tload)
            tkeep.start()
            t0 = remote(town.at[y], to_ref.at[quarter], tos.at[0], tor.at[0], ypeer)
            t1 = remote(town.at[y], to_ref.at[quarter], tos.at[1], tor.at[1], here.core)
            t0.start()
            t1.start()
    ys = []
    spot = spots[0, 0]
    for h in range(2):
        ready(spot, h)
        for way in range(2):
            ring[way, h, far - 1].wait_recv()

        @pl.loop(0, half)
        def _(b, h=h):
            for keep in range(2):
                k = y if keep else other_y
                total = own[spot, h, b, k].astype(f32) + part[spot, h, b, k].astype(f32)
                for way in range(2):
                    total = total + got[way, h, far - 1, b, k].astype(f32)
                if keep:
                    fin[h, b] = total
                else:
                    ysend[h, b] = total.astype(bf16)

        cp = remote(ysend.at[h], ygot.at[h], y_s.at[h], y_r.at[h], ypeer)
        cp.start()
        ys.append(cp)

    acc = jnp.zeros((8, fin.shape[-1]), f32)
    for h in range(2):
        ys[h].wait_recv()

        def last(b, acc, h=h):
            total = fin[h, b] + ygot[h, b].astype(f32)
            mine[h * half + b] = total.astype(bf16)
            square = total * total
            return acc + square[:8] + square[8:]

        acc = lax.fori_loop(0, half, last, acc)

    held[0] = small_ref[...] + squares_row(acc + squares[...])
    first = remote(held.at[0], hgot.at[0], sum_s.at[0], sum_r.at[0], here.core)
    first.start()

    cap = o_ref.shape[0]

    @pl.loop(0, n * cap)
    def _(k):
        value = mine[block_of[k]]
        outgoing[k] = jnp.where(taken[k] > 0, value, jnp.zeros_like(value))

    def spot_of(source, r):
        return o_ref.at[:, source, r]

    moves = []
    for k, o in enumerate(others):
        cp = remote(outgoing.at[pl.ds(o * cap, cap)], spot_of(me, here.r), a_s.at[k], a_r.at[k], (here.r, o))
        cp.start()
        moves.append(cp)
    kept = pltpu.make_async_copy(outgoing.at[pl.ds(me * cap, cap)], spot_of(me, here.r), keep)
    kept.start()
    first.wait_recv()
    held[1] = held[0] + hgot[0]
    second = remote(held.at[1], hgot.at[1], sum_s.at[1], sum_r.at[1], ypeer)
    second.start()
    t0.wait_recv()
    t2 = remote(to_ref.at[near], to_ref.at[near], tos.at[2], tor.at[2], here.core)
    t2.start()
    second.wait_recv()
    four[...] = held[1] + hgot[1]
    totals = []
    for k, o in enumerate(others):
        cp = remote(four, fours.at[me], sum_s.at[2 + k], sum_r.at[2 + k], (here.r, o))
        cp.start()
        totals.append(cp)
    fours[me] = four[...]
    beside, distant = [], []
    for k in range(n):
        source = me if k == 0 else lax.rem(me - k + n, n)
        if k == 0:
            kept.wait()
        else:
            moves[k - 1].wait_recv()
        piece = spot_of(source, here.r)
        over = remote(piece, piece, f_s.at[0, k], f_r.at[0, k], ypeer)
        over.start()
        cp = remote(piece, piece, f_s.at[1, k], f_r.at[1, k], here.core)
        cp.start()
        distant.append((over, source))
        beside.append(cp)
    for cp in totals:
        cp.wait_recv()
    total = fours[0]
    for k in range(1, n):
        total = total + fours[k]
    sum_ref[...] = total
    yr = lax.rem(here.r + 2, 4)
    for k, (over, source) in enumerate(distant):
        over.wait_recv()
        piece = spot_of(source, yr)
        cp = remote(piece, piece, f_s.at[2, k], f_r.at[2, k], here.core)
        cp.start()
        beside.append(cp)
    for cp in moves + totals + [first, second] + [over for over, _ in distant]:
        cp.wait_send()
    for cp in beside:
        cp.wait()
    for cp in ys:
        cp.wait_send()
    for cp in ring.values():
        cp.wait_send()
    for group in cores.values():
        for cp in group:
            cp.wait_send()
    tc.wait_send()
    ty.wait_send()
    tkeep.wait()
    t0.wait_send()
    t1.wait()
    t2.wait()


def settle_gradients(mesh_sizes, cid, grads, table, small, block_of, taken, cap):
    n_rep, n = mesh_sizes
    _, depth, width = grads[0].shape
    count = sum(g.shape[0] for g in grads)
    half = count // 2
    each = len(grads) // 2
    far = n // 2
    table_rows = table.shape[1]
    views = [g.reshape(g.shape[0], n, 2, 2, 16, width) for g in grads]
    dma = pltpu.SemaphoreType.DMA
    piece = (half, 2, 16, width)
    smem = pl.BlockSpec(memory_space=pltpu.SMEM)
    like = small.shape
    return pl.pallas_call(
        partial(reduce_kernel, n_rep, n, half, table_rows, each),
        out_shape=[
            jax.ShapeDtypeStruct((cap, n, 4, 16, width), bf16),
            jax.ShapeDtypeStruct(table.shape, f32),
            jax.ShapeDtypeStruct(like, f32),
        ],
        in_specs=[ANY] * (2 * each + 1) + [VMEM, smem, smem],
        out_specs=[ANY, ANY, VMEM],
        scratch_shapes=[
            pltpu.VMEM((count, 16, width), bf16),
            pltpu.VMEM((n * cap, 16, width), bf16),
            pltpu.VMEM((2,) + like, f32),
            pltpu.VMEM((2,) + like, f32),
            pltpu.VMEM(like, f32),
            pltpu.VMEM((n,) + like, f32),
            pltpu.VMEM(like, f32),
            pltpu.VMEM((n, 2) + piece, bf16),
            pltpu.VMEM((n, 2) + piece, bf16),
            pltpu.VMEM((2, 2, far) + piece, bf16),
            pltpu.VMEM((2, half, 16, width), f32),
            pltpu.VMEM((2, half, 16, width), bf16),
            pltpu.VMEM((2, half, 16, width), bf16),
            pltpu.VMEM((2, table_rows, width), f32),
            pltpu.VMEM((2, table_rows, width), f32),
            pltpu.VMEM((table_rows, width), bf16),
            pltpu.VMEM((table_rows, width), bf16),
            dma((n, 2, each)),
            dma((n, 2, each)),
            dma((n, 2, each)),
            dma((2, 2, far)),
            dma((2, 2, far)),
            dma((2,)),
            dma((2,)),
            dma,
            dma,
            dma,
            dma,
            dma,
            dma((3,)),
            dma((3,)),
            dma,
            dma((n - 1,)),
            dma((n - 1,)),
            dma((3, n)),
            dma((3, n)),
            dma((n + 1,)),
            dma((n + 1,)),
        ],
        compiler_params=params(cid, 56 << 20),
        name="settle_gradients",
    )(*views, table, small, block_of, taken)


def slots_kernel(n_rep, n, to_slots, x_ref, o_ref, keep, a_s, a_r, f_s, f_r):
    here = Place(n_rep, n)
    ypeer = (lax.rem(here.r + 2, 4), here.f)
    me = here.f
    others = [lax.rem(me + k, n) for k in range(1, n)]
    enter([(here.r, o) for o in others] + [here.core, ypeer])

    def spot(source, r):
        return o_ref.at[:, source, r] if to_slots else o_ref.at[source, :, r]

    copies = []
    for k, o in enumerate(others):
        cp = remote(x_ref.at[o], spot(me, here.r), a_s.at[k], a_r.at[k], (here.r, o))
        cp.start()
        copies.append(cp)
    own = pltpu.make_async_copy(x_ref.at[me], spot(me, here.r), keep)
    own.start()
    sends, far = [], []
    for k in range(n):
        source = me if k == 0 else lax.rem(me - k + n, n)
        if k == 0:
            own.wait()
        else:
            copies[k - 1].wait_recv()
        held = spot(source, here.r)
        over = remote(held, held, f_s.at[0, k], f_r.at[0, k], ypeer)
        over.start()
        beside = remote(held, held, f_s.at[1, k], f_r.at[1, k], here.core)
        beside.start()
        far.append((over, source))
        sends.append(beside)
    yr = lax.rem(here.r + 2, 4)
    for k, (over, source) in enumerate(far):
        over.wait_recv()
        src = me if k == 0 else lax.rem(me - k + n, n)
        held = spot(src, yr)
        beside = remote(held, held, f_s.at[2, k], f_r.at[2, k], here.core)
        beside.start()
        sends.append(beside)
    for cp in copies:
        cp.wait_send()
    for over, _ in far:
        over.wait_send()
    for cp in sends:
        cp.wait()


def exchange_slots(mesh_sizes, cid, x, to_slots):
    n_rep, n = mesh_sizes
    _, cap, rows, width = x.shape
    shape = (cap, n, 4, rows, width) if to_slots else (n, cap, 4, rows, width)
    dma = pltpu.SemaphoreType.DMA
    return pl.pallas_call(
        partial(slots_kernel, n_rep, n, to_slots),
        out_shape=jax.ShapeDtypeStruct(shape, x.dtype),
        in_specs=[VMEM],
        out_specs=ANY,
        scratch_shapes=[dma, dma((n - 1,)), dma((n - 1,)), dma((3, n)), dma((3, n))],
        compiler_params=params(cid),
        name=f"slots_{cid}",
    )(x)


def layer_norm(inputs, gain_row):
    centre = inputs - jnp.mean(inputs, axis=-1, keepdims=True)
    spread = jnp.mean(centre * centre, axis=-1, keepdims=True)
    return centre * lax.rsqrt(spread + norm_epsilon) * gain_row


def adam_moments(moment_old, second_old, gradient, first_fix, second_fix):
    moment_new = beta_first * moment_old + (1.0 - beta_first) * gradient
    second_new = beta_second * second_old + (1.0 - beta_second) * gradient * gradient
    step_value = moment_new / first_fix / (jnp.sqrt(second_new / second_fix) + adam_epsilon)
    return (moment_new, second_new, step_value)


def head_slopes(head_count):
    return 2.0 ** (-8.0 * (jnp.arange(head_count, dtype=f32) + 1.0) / head_count)


NT = (((1,), (1,)), ((), ()))
TN = (((0,), (0,)), ((), ()))
masked_distance = 1e33


def mm(a, b, dims=None):
    if dims is None:
        return jnp.dot(a, b, preferred_element_type=f32)
    return lax.dot_general(a, b, dims, preferred_element_type=f32)


def norm_parts(x):
    centre = x - jnp.mean(x, axis=-1, keepdims=True)
    spread = jnp.mean(centre * centre, axis=-1, keepdims=True)
    rstd = lax.rsqrt(spread + norm_epsilon)
    return centre * rstd, rstd


def norm_back(x, gain, grad):
    hat, rstd = norm_parts(x)
    inner = grad * gain
    back = inner - jnp.mean(inner, axis=-1, keepdims=True) - hat * jnp.mean(inner * hat, axis=-1, keepdims=True)
    return rstd * back, grad * hat


def fold8(x):
    total = x[:8]
    for k in range(1, x.shape[0] // 8):
        total = total + x[k * 8 : k * 8 + 8]
    return total


def pair_bias(seg_row, seg_col, bias):
    length = bias.shape[0]
    i = lax.broadcasted_iota(jnp.int32, (length, length), 0)
    j = lax.broadcasted_iota(jnp.int32, (length, length), 1)
    apart = jnp.abs(i - j).astype(f32)
    bias[...] = jnp.where(seg_col == seg_row, apart, masked_distance)


def attend_kernel(slopes, x, gain, w, seg_row, seg_col, y, a, qkv, o, lse, bias):
    pair = pl.program_id(1)
    length, width = x.shape
    half = width // HEADS
    two = 2 * half
    rows = ROWS

    @pl.when(pair == 0)
    def _():
        pair_bias(seg_row[0], seg_col[0], bias)

        @pl.loop(0, length // rows)
        def _(i):
            at = pl.ds(pl.multiple_of(i * rows, rows), rows)
            hat, _ = norm_parts(x[at])
            low = (hat * gain[...]).astype(bf16)
            a[at] = low
            for k in range(3):
                part = mm(low, w[k])
                if k == 0:
                    part = part.astype(bf16).astype(f32) * half ** (-0.5)
                qkv[at, k * width : (k + 1) * width] = part.astype(bf16)

    lanes = pl.ds(pl.multiple_of(pair * two, two), two)
    q = qkv[:, pl.ds(pl.multiple_of(pair * two, two), two)]
    k = qkv[:, pl.ds(pl.multiple_of(width + pair * two, two), two)]
    v = qkv[:, pl.ds(pl.multiple_of(2 * width + pair * two, two), two)]
    v_t = v.astype(f32).T.astype(bf16)
    left = lax.broadcasted_iota(jnp.int32, (length, two), 1) < half
    zero = jnp.zeros_like(q)
    out = []
    for e in range(2):
        slope = slopes[2 * pair + e]
        q_e = jnp.where(left, q, zero) if e == 0 else jnp.where(left, zero, q)
        s = mm(k, q_e, NT) - slope * bias[...]
        top = jnp.max(s, axis=0, keepdims=True)
        p = jnp.exp(s - top)
        total = jnp.sum(p, axis=0, keepdims=True)
        low = (p * (1.0 / total)).astype(bf16)
        out.append(mm(v_t, low))
        lse[0, pl.ds(2 * pair + e, 1)] = top + jnp.log(total)
    upper = lax.broadcasted_iota(jnp.int32, (two, length), 0) < half
    o[:, lanes] = jnp.where(upper, out[0], out[1]).T.astype(bf16)

    @pl.when(pair == pl.num_programs(1) - 1)
    def _():
        @pl.loop(0, length // rows)
        def _(i):
            at = pl.ds(pl.multiple_of(i * rows, rows), rows)
            y[at] = x[at] + mm(o[at], w[3])


def attend(x, gain, weights, layer, seg):
    packs, length = seg.shape
    tokens, width = x.shape
    per_layer4 = weights.shape[0] // LAYERS // 4
    slopes = head_slopes(HEADS)
    whole = lambda shape: pl.BlockSpec(shape, lambda m, p: (m,) + (0,) * (len(shape) - 1))
    fixed = lambda shape, at: pl.BlockSpec(shape, lambda m, p: at)
    return pl.pallas_call(
        attend_kernel,
        grid=(packs, HEADS // 2),
        in_specs=[
            pl.BlockSpec(memory_space=pltpu.SMEM),
            whole((length, width)),
            fixed((1, width), (0, 0)),
            fixed((4, width, width), (per_layer4 * layer, 0, 0)),
            whole((1, 1, length)),
            whole((1, length, 1)),
        ],
        out_specs=[
            whole((length, width)),
            whole((length, width)),
            whole((length, 3 * width)),
            whole((length, width)),
            whole((1, HEADS, length)),
        ],
        out_shape=[
            jax.ShapeDtypeStruct((tokens, width), f32),
            jax.ShapeDtypeStruct((tokens, width), bf16),
            jax.ShapeDtypeStruct((tokens, 3 * width), bf16),
            jax.ShapeDtypeStruct((tokens, width), bf16),
            jax.ShapeDtypeStruct((packs, HEADS, length), f32),
        ],
        scratch_shapes=[pltpu.VMEM((length, length), f32)],
        compiler_params=pltpu.CompilerParams(vmem_limit_bytes=48 << 20),
        name="attend",
    )(slopes, x, gain.reshape(1, width), weights, seg.reshape(packs, 1, length), seg.reshape(packs, length, 1))


def attend_back_kernel(
    slopes, dx, x, gain, w, a, qkv, o, lse, seg_row, seg_col, new, dgain, gw, bias, do, dqkv, acc
):
    pack, pair = pl.program_id(0), pl.program_id(1)
    length, width = x.shape
    half = width // HEADS
    two = 2 * half
    rows = ROWS

    @pl.when(pair == 0)
    def _():
        pair_bias(seg_row[0], seg_col[0], bias)

        @pl.loop(0, length // rows)
        def _(i):
            at = pl.ds(pl.multiple_of(i * rows, rows), rows)
            do[at] = mm(dx[at].astype(bf16), w[3], NT).astype(bf16)

        part = mm(o[...], dx[...].astype(bf16), TN)

        @pl.when(pack == 0)
        def _():
            acc[3] = part

        @pl.when(pack > 0)
        def _():
            acc[3] += part

    lanes = [pl.ds(pl.multiple_of(n * width + pair * two, two), two) for n in range(3)]
    q, k, v = [qkv[:, at] for at in lanes]
    do_p = do[:, lanes[0]]
    k_t = k.astype(f32).T.astype(bf16)
    left = lax.broadcasted_iota(jnp.int32, (length, two), 1) < half
    upper = lax.broadcasted_iota(jnp.int32, (two, length), 0) < half
    zero = jnp.zeros_like(q)
    dq, dk, dv = [], [], []
    for e in range(2):
        slope = slopes[2 * pair + e]
        keep = (lambda t: jnp.where(left, t, zero)) if e == 0 else (lambda t: jnp.where(left, zero, t))
        s = mm(k, keep(q), NT) - slope * bias[...]
        p = jnp.exp(s - lse[0, pl.ds(2 * pair + e, 1)])
        dp = mm(v, keep(do_p), NT)
        inner = jnp.sum(p * dp, axis=0, keepdims=True)
        ds = (p * (dp - inner)).astype(bf16)
        dv.append(mm(p.astype(bf16), do_p))
        dk.append(mm(ds, q))
        dq.append(mm(k_t, ds))
    dqkv[:, lanes[0]] = (jnp.where(upper, dq[0], dq[1]).T * half ** (-0.5)).astype(bf16)
    dqkv[:, lanes[1]] = jnp.where(left, dk[0], dk[1]).astype(bf16)
    dqkv[:, lanes[2]] = jnp.where(left, dv[0], dv[1]).astype(bf16)

    @pl.when(pair == pl.num_programs(1) - 1)
    def _():
        def chunk(i, total):
            at = pl.ds(pl.multiple_of(i * rows, rows), rows)
            da = mm(dqkv[at, :width], w[0], NT)
            da = da + mm(dqkv[at, width : 2 * width], w[1], NT)
            da = da + mm(dqkv[at, 2 * width :], w[2], NT)
            back, extra = norm_back(x[at], gain[...], da)
            new[at] = dx[at] + back
            return total + fold8(extra)

        dgain[0] = lax.fori_loop(0, length // rows, chunk, jnp.zeros((8, width), f32))
        for n in range(3):
            part = mm(a[...], dqkv[:, n * width : (n + 1) * width], TN)

            @pl.when(pack == 0)
            def _(part=part, n=n):
                acc[n] = part

            @pl.when(pack > 0)
            def _(part=part, n=n):
                acc[n] += part

    @pl.when((pair == pl.num_programs(1) - 1) & (pack == pl.num_programs(0) - 1))
    def _():
        for n in range(4):
            gw[n] = acc[n].astype(bf16)


def attend_back(dx, x, gain, weights, layer, seg, kept):
    a, qkv, o, lse = kept
    packs, length = seg.shape
    tokens, width = x.shape
    per_layer4 = weights.shape[0] // LAYERS // 4
    whole = lambda shape: pl.BlockSpec(shape, lambda m, p: (m,) + (0,) * (len(shape) - 1))
    fixed = lambda shape, at: pl.BlockSpec(shape, lambda m, p: at)
    return pl.pallas_call(
        attend_back_kernel,
        grid=(packs, HEADS // 2),
        in_specs=[
            pl.BlockSpec(memory_space=pltpu.SMEM),
            whole((length, width)),
            whole((length, width)),
            fixed((1, width), (0, 0)),
            fixed((4, width, width), (per_layer4 * layer, 0, 0)),
            whole((length, width)),
            whole((length, 3 * width)),
            whole((length, width)),
            whole((1, HEADS, length)),
            whole((1, 1, length)),
            whole((1, length, 1)),
        ],
        out_specs=[
            whole((length, width)),
            whole((1, 8, width)),
            fixed((4, width, width), (0, 0, 0)),
        ],
        out_shape=[
            jax.ShapeDtypeStruct((tokens, width), f32),
            jax.ShapeDtypeStruct((packs, 8, width), f32),
            jax.ShapeDtypeStruct((4, width, width), bf16),
        ],
        scratch_shapes=[
            pltpu.VMEM((length, length), f32),
            pltpu.VMEM((length, width), bf16),
            pltpu.VMEM((length, 3 * width), bf16),
            pltpu.VMEM((4, width, width), f32),
        ],
        compiler_params=pltpu.CompilerParams(vmem_limit_bytes=56 << 20),
        name="attend_back",
    )(
        head_slopes(HEADS),
        dx,
        x,
        gain.reshape(1, width),
        weights,
        a,
        qkv,
        o,
        lse,
        seg.reshape(packs, 1, length),
        seg.reshape(packs, length, 1),
    )


ROWS = 512
gelu_c = math.sqrt(2.0 / math.pi)


def feed_kernel(x, gain, wg, wu, wd, y, f, gate, up):
    k = pl.program_id(0)
    tokens = x.shape[0]
    rows = ROWS

    @pl.loop(0, tokens // rows)
    def _(i):
        at = pl.ds(pl.multiple_of(i * rows, rows), rows)

        @pl.when(k == 0)
        def _():
            hat, _ = norm_parts(x[at])
            f[at] = (hat * gain[...]).astype(bf16)
            y[at] = x[at]

        low = f[at]
        g = mm(low, wg[0]).astype(bf16)
        u = mm(low, wu[0]).astype(bf16)
        gate[0, at] = g
        up[0, at] = u
        g, u = g.astype(f32), u.astype(f32)
        cdf = 0.5 * (1.0 + jnp.tanh(gelu_c * (g + 0.044715 * (g * g * g))))
        hidden = (g * cdf * u).astype(bf16)
        y[at] += mm(hidden, wd[0])


def feed(x, gain, weights, layer):
    tokens, width = x.shape
    per_layer = weights.shape[0] // LAYERS
    pieces = FF // width
    fixed = lambda shape: pl.BlockSpec(shape, lambda k: (0,) * len(shape))
    block = lambda skip: pl.BlockSpec((1, width, width), lambda k: (per_layer * layer + skip + k, 0, 0))
    each = pl.BlockSpec((1, tokens, width), lambda k: (k, 0, 0))
    return pl.pallas_call(
        feed_kernel,
        grid=(pieces,),
        in_specs=[fixed((tokens, width)), fixed((1, width)), block(4), block(4 + pieces), block(4 + 2 * pieces)],
        out_specs=[fixed((tokens, width)), fixed((tokens, width)), each, each],
        out_shape=[
            jax.ShapeDtypeStruct((tokens, width), f32),
            jax.ShapeDtypeStruct((tokens, width), bf16),
            jax.ShapeDtypeStruct((pieces, tokens, width), bf16),
            jax.ShapeDtypeStruct((pieces, tokens, width), bf16),
        ],
        compiler_params=pltpu.CompilerParams(vmem_limit_bytes=48 << 20),
        name="feed",
    )(x, gain.reshape(1, width), weights, weights, weights)


def feed_back_kernel(dx, x, gain, wg, wu, wd, f, gate, up, new, dgain, gg, gu, gd, f_t, dz, hid, dg, du):
    k = pl.program_id(0)
    tokens, width = x.shape
    rows = ROWS
    last = pl.num_programs(0) - 1

    @pl.when(k == 0)
    def _():
        @pl.loop(0, tokens // rows)
        def _(i):
            at = pl.ds(pl.multiple_of(i * rows, rows), rows)
            f_t[:, at] = f[at].astype(f32).T.astype(bf16)
            dz[at] = dx[at].astype(bf16)
            new[at] = jnp.zeros((rows, width), f32)

    def chunk(i, total):
        at = pl.ds(pl.multiple_of(i * rows, rows), rows)
        dh = mm(dz[at], wd[0], NT)
        g, u = gate[0, at].astype(f32), up[0, at].astype(f32)
        square = g * g
        t = jnp.tanh(gelu_c * (g + 0.044715 * (square * g)))
        cdf = 0.5 * (1.0 + t)
        act = g * cdf
        slope = cdf + 0.5 * g * (1.0 - t * t) * (gelu_c * (1.0 + 3 * 0.044715 * square))
        hid[at] = (act * u).astype(bf16)
        dgate = (dh * u * slope).astype(bf16)
        dup = (dh * act).astype(bf16)
        dg[at] = dgate
        du[at] = dup
        new[at] += mm(dgate, wg[0], NT) + mm(dup, wu[0], NT)
        return total

    lax.fori_loop(0, tokens // rows, chunk, 0)
    gg[0] = mm(f_t[...], dg[...]).astype(bf16)
    gu[0] = mm(f_t[...], du[...]).astype(bf16)
    gd[0] = mm(hid[...], dz[...], TN).astype(bf16)

    @pl.when(k == last)
    def _():
        def finish(i, total):
            at = pl.ds(pl.multiple_of(i * rows, rows), rows)
            back, extra = norm_back(x[at], gain[...], new[at])
            new[at] = dx[at] + back
            return total + fold8(extra)

        dgain[...] = lax.fori_loop(0, tokens // rows, finish, jnp.zeros((8, width), f32))


def feed_back(dx, x, gain, weights, layer, kept):
    f, gate, up = kept
    tokens, width = x.shape
    per_layer = weights.shape[0] // LAYERS
    pieces = FF // width
    fixed = lambda shape: pl.BlockSpec(shape, lambda k: (0,) * len(shape))
    block = lambda skip: pl.BlockSpec((1, width, width), lambda k: (per_layer * layer + skip + k, 0, 0))
    each = pl.BlockSpec((1, tokens, width), lambda k: (k, 0, 0))
    grad = pl.BlockSpec((1, width, width), lambda k: (k, 0, 0))
    return pl.pallas_call(
        feed_back_kernel,
        grid=(pieces,),
        in_specs=[
            fixed((tokens, width)),
            fixed((tokens, width)),
            fixed((1, width)),
            block(4),
            block(4 + pieces),
            block(4 + 2 * pieces),
            fixed((tokens, width)),
            each,
            each,
        ],
        out_specs=[fixed((tokens, width)), fixed((8, width)), grad, grad, grad],
        out_shape=[
            jax.ShapeDtypeStruct((tokens, width), f32),
            jax.ShapeDtypeStruct((8, width), f32),
        ]
        + [jax.ShapeDtypeStruct((pieces, width, width), bf16)] * 3,
        scratch_shapes=[
            pltpu.VMEM((width, tokens), bf16),
            pltpu.VMEM((tokens, width), bf16),
            pltpu.VMEM((tokens, width), bf16),
            pltpu.VMEM((tokens, width), bf16),
            pltpu.VMEM((tokens, width), bf16),
        ],
        compiler_params=pltpu.CompilerParams(vmem_limit_bytes=56 << 20),
        name="feed_back",
    )(dx, x, gain.reshape(1, width), weights, weights, weights, f, gate, up)


def two_parts(x):
    top = x.astype(bf16)
    return top, (x - top.astype(f32)).astype(bf16)


def mm3(a, b, dims=None):
    (a1, a2), (b1, b2) = a, b
    return mm(a1, b1, dims) + (mm(a1, b2, dims) + mm(a2, b1, dims))


def turn_kernel(scalars, numbers, left, right, some, grad, m, v, m_new, v_new, turned):
    slot = pl.program_id(0)
    factor, first_fix, second_fix = numbers[0], numbers[1], numbers[2]
    bases = two_parts(right[0])
    left_top, left_rest = two_parts(left[0])
    rotated = mm(left_top, grad[0], TN) + mm(left_rest, grad[0], TN)
    rotated = factor * mm3(two_parts(rotated), bases)
    moment, second, step = adam_moments(m[0], v[0], rotated, first_fix, second_fix)
    live = scalars[1 + slot] > 0
    m_new[0] = jnp.where(live, moment, m[0])
    v_new[0] = jnp.where(live, second, v[0])
    groups, _, rows, width = turned.shape
    rows_here = some[...].reshape(groups * rows, width)
    out = mm3(two_parts(rows_here), two_parts(step))
    out = mm3(two_parts(out), bases, NT)
    turned[...] = out.astype(turned.dtype).reshape(turned.shape)


def turn_slots(replica, live, numbers, left, right, grads, m, v):
    cap, width, _ = left.shape
    groups = width // 64
    scalars = jnp.concatenate([replica.reshape(1), live.astype(jnp.int32)])
    view = left.reshape(cap, groups, 4, 16, width)
    whole = pl.BlockSpec((1, width, width), lambda s, scalars: (s, 0, 0))
    grid_spec = pltpu.PrefetchScalarGridSpec(
        num_scalar_prefetch=1,
        grid=(cap,),
        in_specs=[
            pl.BlockSpec(memory_space=pltpu.SMEM),
            whole,
            whole,
            pl.BlockSpec((1, groups, 1, 16, width), lambda s, scalars: (s, 0, scalars[0], 0, 0)),
            whole,
            whole,
            whole,
        ],
        out_specs=[whole, whole, pl.BlockSpec((groups, 1, 16, width), lambda s, scalars: (0, s, 0, 0))],
    )
    return pl.pallas_call(
        turn_kernel,
        grid_spec=grid_spec,
        out_shape=[
            jax.ShapeDtypeStruct(m.shape, f32),
            jax.ShapeDtypeStruct(v.shape, f32),
            jax.ShapeDtypeStruct((groups, cap, 16, width), bf16),
        ],
        compiler_params=pltpu.CompilerParams(vmem_limit_bytes=56 << 20),
        name="turn_slots",
    )(scalars, numbers, left, right, view, grads, m, v)


def head_kernel(
    n_rep, n, vocab, tile, x_ref, e_ref, label_ref, picked_ref, table_ref, loss_ref,
    table, rows_all, logits, stats, shared, held, got,
    load_s, ring_s, ring_r, stat_s, stat_r, back_s, back_r,
):
    here = Place(n_rep, n)
    me = here.f
    others = [lax.rem(me + k, n) for k in range(1, n)]
    enter([(here.r, o) for o in others])
    picks, width = x_ref.shape
    half = picks // 2
    tiles = table.shape[0] // tile
    far = n // 2
    load = pltpu.make_async_copy(e_ref, table, load_s)
    load.start()
    sends = []
    waiting = {}

    def hop(way, s):
        origin = here.at(-s if way == 0 else s)
        window = pl.ds(way * half, half) if s == far - 1 else pl.ds(0, picks)
        src = x_ref if s == 0 else rows_all.at[origin, window]
        cp = remote(
            src,
            rows_all.at[origin, window],
            ring_s.at[way, s],
            ring_r.at[way, s],
            here.next if way == 0 else here.prev,
        )
        cp.start()
        sends.append(cp)
        waiting[way] = cp

    def columns(t):
        return t * tile + lax.broadcasted_iota(jnp.int32, (picks, tile), 1)

    def span(t):
        return pl.ds(pl.multiple_of(t * tile, tile), tile)

    def fold(x, join):
        out = x[:, :128]
        for k in range(1, tile // 128):
            out = join(out, x[:, k * 128 : (k + 1) * 128])
        return out

    def forward(origin):
        rows = rows_all[origin]
        label = label_ref[origin]

        def product(t, top):
            scores = mm(rows, table[span(t)], NT)
            scores = jnp.where(columns(t) < vocab, scores, masked_score)
            logits[origin, :, span(t)] = scores
            return jnp.maximum(top, fold(scores, jnp.maximum))

        top = lax.fori_loop(0, tiles, product, jnp.full((picks, 128), masked_score, f32))
        top = jnp.max(top, axis=1, keepdims=True)

        def weigh(t, sums):
            total, target = sums
            scores = logits[origin, :, span(t)]
            total = total + fold(jnp.exp(scores - top), jnp.add)
            hit = jnp.where(columns(t) == label, scores, 0.0)
            return total, target + fold(hit, jnp.add)

        zero = jnp.zeros((picks, 128), f32)
        total, target = lax.fori_loop(0, tiles, weigh, (zero, zero))
        log_sum = top + jnp.log(jnp.sum(total, axis=1, keepdims=True))
        target = jnp.sum(target, axis=1, keepdims=True)
        lane = lax.broadcasted_iota(jnp.int32, (picks, 128), 1)
        both = jnp.where(lane == 0, log_sum, target).T
        stats[pl.ds(origin, 1)] = both[0:1]
        stats[pl.ds(n + origin, 1)] = both[1:2]

    rows_all[me] = x_ref[...]
    for way in range(2):
        hop(way, 0)
    load.wait()
    forward(me)
    for s in range(far):
        for way in range(2):
            waiting[way].wait_recv()
            if s < far - 1:
                hop(way, s + 1)
        if s < far - 1:
            forward(here.at(-s - 1))
            forward(here.at(s + 1))
        else:
            forward(here.at(far))

    moves = []
    for k, o in enumerate(others):
        cp = remote(stats, shared.at[me], stat_s.at[k], stat_r.at[k], (here.r, o))
        cp.start()
        moves.append(cp)
    shared[me] = stats[...]
    table_ref[...] = jnp.zeros(table_ref.shape, f32)
    for cp in moves:
        cp.wait_recv()
    top = shared[0, :n]
    for k in range(1, n):
        top = jnp.maximum(top, shared[k, :n])
    total = jnp.exp(shared[0, :n] - top)
    target = shared[0, n:]
    for k in range(1, n):
        total = total + jnp.exp(shared[k, :n] - top)
        target = target + shared[k, n:]
    log_sum = top + jnp.log(total)
    for cp in moves:
        cp.wait_send()
    stats[:n] = log_sum
    stats[n:] = log_sum - target
    mine = stats[pl.ds(n + me, 1)]
    loss_ref[...] = jnp.broadcast_to(jnp.sum(mine, axis=1, keepdims=True), loss_ref.shape)

    def backward(q):
        rows = rows_all[q]
        label = label_ref[q]
        norm = jnp.broadcast_to(stats[pl.ds(q, 1)], (128, picks)).T

        def product(t, out):
            scores = logits[q, :, span(t)]
            parts = [jnp.exp(scores[:, k * 128 : (k + 1) * 128] - norm) for k in range(tile // 128)]
            soft = jnp.concatenate(parts, axis=1)
            grad = (soft - jnp.where(columns(t) == label, 1.0, 0.0)).astype(bf16)
            table_ref[span(t)] += mm(grad, rows, TN)
            return out + mm(grad, table[span(t)])

        return lax.fori_loop(0, tiles, product, jnp.zeros((picks, width), f32))

    ring = {}

    def lane_send(way, h, s, value):
        before = ring.get((way, h, s - 1))
        if before is not None:
            before.wait_recv()
            value = value + got[way, h, s - 1].astype(f32)
        held[way, h, s] = value.astype(bf16)
        cp = remote(
            held.at[way, h, s],
            got.at[way, h, s],
            back_s.at[way, h, s],
            back_r.at[way, h, s],
            here.next if way == 0 else here.prev,
        )
        cp.start()
        ring[way, h, s] = cp

    out = backward(here.at(far))
    lane_send(0, 0, 0, out[:half])
    lane_send(1, 1, 0, out[half:])
    for s in range(1, far):
        for way in range(2):
            d = far - s
            out = backward(here.at(d if way == 0 else -d))
            for h in (1 - way, way):
                lane_send(way, h, s, out[h * half : (h + 1) * half])
    out = backward(me)
    for h in range(2):
        total = out[h * half : (h + 1) * half]
        for way in range(2):
            ring[way, h, far - 1].wait_recv()
            total = total + got[way, h, far - 1].astype(f32)
        picked_ref[pl.ds(h * half, half)] = total
    for cp in sends + list(ring.values()):
        cp.wait_send()


def head_step(mesh_sizes, cid, picked, table, labels, vocab):
    n_rep, n = mesh_sizes
    picks, width = picked.shape
    padded = table.shape[0]
    far = n // 2
    dma = pltpu.SemaphoreType.DMA
    return pl.pallas_call(
        partial(head_kernel, n_rep, n, vocab, 256),
        out_shape=[
            jax.ShapeDtypeStruct((picks, width), f32),
            jax.ShapeDtypeStruct((padded, width), f32),
            jax.ShapeDtypeStruct((8, 128), f32),
        ],
        in_specs=[VMEM, ANY, VMEM],
        out_specs=[VMEM, VMEM, VMEM],
        scratch_shapes=[
            pltpu.VMEM((padded, width), bf16),
            pltpu.VMEM((n, picks, width), bf16),
            pltpu.VMEM((n, picks, padded), f32),
            pltpu.VMEM((2 * n, picks), f32),
            pltpu.VMEM((n, 2 * n, picks), f32),
            pltpu.VMEM((2, 2, far, picks // 2, width), bf16),
            pltpu.VMEM((2, 2, far, picks // 2, width), bf16),
            dma,
            dma((2, far)),
            dma((2, far)),
            dma((n - 1,)),
            dma((n - 1,)),
            dma((2, 2, far)),
            dma((2, 2, far)),
        ],
        compiler_params=params(cid, 60 << 20),
        name="head_step",
    )(picked, table, labels.reshape(n, picks, 1))


class Transport:
    def __init__(self, n_rep, n_fsdp, shard_rows):
        self.sizes = (n_rep, n_fsdp)
        self.kernels = n_rep == 4 and n_fsdp == 8 and shard_rows == 64

    def open(self, cid, shard, table, wanted, facts, gains):
        if self.kernels:
            return open_step(self.sizes, cid, shard, table, wanted, facts, gains)
        asked = lax.all_to_all(wanted, "fsdp", split_axis=0, concat_axis=0, tiled=True)
        rows = jnp.take(table.astype(bf16), asked.reshape(-1), axis=0)
        rows = rows.reshape(wanted.shape[0], wanted.shape[2], table.shape[1])
        return (
            lax.all_gather(shard, "fsdp", axis=1, tiled=True),
            self.spread(cid, rows),
            asked,
            lax.all_gather(facts, "fsdp"),
            lax.all_gather(gains, "fsdp"),
            lax.pmax(facts, ("rep", "fsdp")),
        )

    def spread(self, cid, x):
        if self.kernels:
            return group_exchange(self.sizes, cid, x, True)
        return lax.all_to_all(x, "fsdp", split_axis=0, concat_axis=0, tiled=True)


def body(
    token_ids,
    segment_ids,
    masked_pos,
    labels,
    blocks,
    gains,
    embed,
    embed_m,
    embed_v,
    gains_m,
    gains_v,
    soap_m,
    soap_v,
    left_basis,
    right_basis,
    block_slots,
    step_count,
):
    groups = lax.axis_size("fsdp")
    replicas = lax.axis_size("rep")
    member = lax.axis_index("fsdp")
    replica = lax.axis_index("rep")
    micro_count = token_ids.shape[0]
    pack_length = token_ids.shape[2]
    pick_count = masked_pos.shape[2]
    vocab_rows, model_width = embed.shape
    block_count, shard_rows, _ = blocks.shape
    gain_count = gains.shape[0]
    tokens = micro_count * pack_length
    picks = micro_count * pick_count
    move = Transport(replicas, groups, shard_rows)
    padded_rows = -(-vocab_rows // 768) * 768
    table_low = jnp.pad(embed.astype(bf16), ((0, padded_rows - vocab_rows), (0, 0)))

    ids = token_ids.reshape(tokens)
    index = jnp.arange(tokens, dtype=jnp.int32)
    owner = ids // vocab_rows
    local = ids - owner * vocab_rows
    first_at = jnp.min(jnp.where(ids[:, None] == ids[None, :], index[None, :], tokens), axis=1)
    is_first = first_at == index
    ahead = is_first[None, :] & (owner[:, None] == owner[None, :]) & (index[None, :] < first_at[:, None])
    rank = jnp.sum(ahead.astype(jnp.int32), axis=1)
    most = jnp.max(rank) + 1

    my_labels = labels.reshape(picks // 128, 128)
    facts = jnp.concatenate(
        [my_labels, jnp.full((8 - picks // 128, 128), most, jnp.int32)], axis=0
    )
    gain_pad = jnp.pad(gains, ((0, 8 - gain_count), (0, 128 - gains.shape[1])))
    slots = groups * CAPACITY
    most_rounds = (tokens + CAPACITY - 1) // CAPACITY
    slot_index = jnp.arange(slots, dtype=jnp.int32)

    def slot_of(k):
        here = rank - k * CAPACITY
        return jnp.where((here >= 0) & (here < CAPACITY), owner * CAPACITY + here, -1)

    def wanted_in(slot):
        wanted = jnp.where((slot[None, :] == slot_index[:, None]) & is_first[None, :], local[None, :], 0)
        return jnp.sum(wanted, axis=1).reshape(groups, 1, CAPACITY)

    def placed(slot, rows):
        chosen = (slot[:, None] == slot_index[None, :]).astype(bf16)
        return jnp.dot(chosen, rows.reshape(slots, model_width), preferred_element_type=f32)

    slot = slot_of(0)
    full_blocks, rows, asked, group_facts, gain_rows, most_facts = move.open(
        0, blocks.astype(bf16), embed, wanted_in(slot), facts, gain_pad
    )
    rounds = (most_facts[7, 0] + CAPACITY - 1) // CAPACITY
    all_labels = group_facts[:, : picks // 128].reshape(groups * picks)
    gain_rows = gain_rows[:, :gain_count, : gains.shape[1]].transpose(1, 0, 2).reshape(gain_count, model_width)
    gain_rows = lax.reduce_precision(gain_rows, exponent_bits=8, mantissa_bits=7)
    embedded = placed(slot, rows)
    asked_all = jnp.zeros((most_rounds, slots), jnp.int32).at[0].set(asked.reshape(slots))

    def look(state):
        k, rows_so_far, asked_all = state
        slot = slot_of(k)
        asked = move.spread(1, wanted_in(slot))
        asked_all = lax.dynamic_update_index_in_dim(asked_all, asked.reshape(slots), k, 0)
        rows = jnp.take(table_low, asked.reshape(slots), axis=0).reshape(groups, CAPACITY, model_width)
        return k + 1, rows_so_far + placed(slot, move.spread(2, rows)), asked_all

    _, embedded, asked_all = lax.while_loop(lambda s: s[0] < rounds, look, (jnp.int32(1), embedded, asked_all))

    segments = segment_ids.reshape(micro_count, pack_length)
    stream, first_pull = jax.vjp(layer_norm, embedded, gain_rows[0])
    saved_layers = []
    for layer in range(LAYERS):
        middle, *attention_kept = attend(stream, gain_rows[1 + 2 * layer], full_blocks, layer, segments)
        after, *feed_kept = feed(middle, gain_rows[2 + 2 * layer], full_blocks, layer)
        saved_layers.append((stream, attention_kept, middle, feed_kept))
        stream = after
    final_rows, final_pull = jax.vjp(layer_norm, stream, gain_rows[gain_count - 1])

    positions = masked_pos.reshape(micro_count, pick_count)
    flat_positions = (positions + jnp.arange(micro_count, dtype=jnp.int32)[:, None] * pack_length).reshape(picks)
    picked = jnp.take(final_rows, flat_positions, axis=0).astype(bf16)
    label_local = all_labels - member * vocab_rows
    label_local = jnp.where((label_local >= 0) & (label_local < vocab_rows), label_local, -1)
    if move.kernels:
        grad_picked, grad_table, loss_local = head_step(
            move.sizes, 4, picked, table_low, label_local.reshape(groups, picks), vocab_rows
        )
        loss_local = loss_local[0, 0]
    else:
        all_picked = lax.all_gather(picked, "fsdp", tiled=True)
        logits = jnp.einsum("td,vd->tv", all_picked, table_low[:vocab_rows], preferred_element_type=f32)
        top_value = jnp.max(logits, axis=-1)
        exp_total = jnp.sum(jnp.exp(logits - top_value[:, None]), axis=-1)
        label_hits = jnp.arange(vocab_rows, dtype=jnp.int32)[None, :] == label_local[:, None]
        target = jnp.sum(jnp.where(label_hits, logits, 0.0), axis=-1)
        stats = lax.all_gather(jnp.stack([top_value, exp_total, target]), "fsdp")
        top_all = jnp.max(stats[:, 0], axis=0)
        total_all = jnp.sum(stats[:, 1] * jnp.exp(stats[:, 0] - top_all[None]), axis=0)
        target_all = jnp.sum(stats[:, 2], axis=0)
        entropy = top_all + jnp.log(total_all) - target_all
        loss_local = jnp.sum(lax.dynamic_slice_in_dim(entropy, member * picks, picks))
        grad_logits = (
            jnp.exp(logits - top_all[:, None]) / total_all[:, None] - label_hits.astype(f32)
        ).astype(bf16)
        grad_table = jnp.einsum("tv,td->vd", grad_logits, all_picked, preferred_element_type=f32)
        grad_table = jnp.pad(grad_table, ((0, padded_rows - vocab_rows), (0, 0)))
        grad_picked = jnp.einsum("tv,vd->td", grad_logits, table_low[:vocab_rows], preferred_element_type=f32)
        grad_picked = grad_picked.reshape(groups, picks, model_width)
        grad_picked = lax.psum_scatter(grad_picked, "fsdp", scatter_dimension=0)

    match = flat_positions[None, :] == index[:, None]
    place = jnp.sum(jnp.where(match, jnp.arange(picks, dtype=jnp.int32)[None, :] + 1, 0), axis=1)
    grad_final = jnp.where(
        (place > 0)[:, None], jnp.take(grad_picked, jnp.maximum(place - 1, 0), axis=0), 0.0
    )
    grad_stream, grad_final_gain = final_pull(grad_final)
    gain_grads = [None] * gain_count
    gain_grads[gain_count - 1] = grad_final_gain
    layer_grads = [None] * LAYERS
    for layer in reversed(range(LAYERS)):
        before, attention_kept, middle, feed_kept = saved_layers[layer]
        grad_stream, feed_gain, *grads_feed = feed_back(
            grad_stream, middle, gain_rows[2 + 2 * layer], full_blocks, layer, feed_kept
        )
        grad_stream, attention_gain, grads_attention = attend_back(
            grad_stream, before, gain_rows[1 + 2 * layer], full_blocks, layer, segments, attention_kept
        )
        gain_grads[1 + 2 * layer] = jnp.sum(attention_gain, axis=(0, 1))
        gain_grads[2 + 2 * layer] = jnp.sum(feed_gain, axis=0)
        layer_grads[layer] = [grads_attention] + grads_feed
    grad_embedded, gain_grads[0] = first_pull(grad_stream)
    grad_rows = grad_embedded.astype(bf16)
    row_index = jnp.arange(padded_rows, dtype=jnp.int32)

    def given(cid, k, grad_table):
        chosen = (slot_index[:, None] == slot_of(k)[None, :]).astype(bf16)
        rows = jnp.dot(chosen, grad_rows, preferred_element_type=f32).astype(bf16)
        rows = move.spread(cid, rows.reshape(groups, CAPACITY, model_width)).reshape(slots, model_width)
        asked = lax.dynamic_index_in_dim(asked_all, k, 0, keepdims=False)
        target_rows = (row_index[:, None] == asked[None, :]).astype(bf16)
        return grad_table + jnp.dot(target_rows, rows, preferred_element_type=f32)

    grad_table = given(7, 0, grad_table)
    _, grad_table = lax.while_loop(
        lambda s: s[0] < rounds, lambda s: (s[0] + 1, given(13, s[0], s[1])), (jnp.int32(1), grad_table)
    )
    grad_blocks = [g for grads in layer_grads for g in grads]
    grad_gains = jnp.stack(gain_grads, axis=0)

    position_count = micro_count * replicas * groups * pick_count
    clip_limit = clip_ratio * math.sqrt(position_count)
    steps_done = step_count[0].astype(f32)
    first_fix = 1.0 - beta_first**steps_done
    second_fix = 1.0 - beta_second**steps_done
    slot_cap = soap_m.shape[0]
    slot_total = slot_cap * groups
    named = jnp.arange(slot_total, dtype=jnp.int32)[:, None] == block_slots[None, :]
    taken = jnp.any(named, axis=1)
    block_of = jnp.sum(jnp.where(named, jnp.arange(block_count, dtype=jnp.int32)[None, :], 0), axis=1)

    small = jnp.zeros((8, model_width), f32).at[:gain_count].set(grad_gains)
    small = small.at[7, 0].set(loss_local)
    if move.kernels:
        owned, grad_table, small = settle_gradients(
            move.sizes,
            8,
            grad_blocks,
            grad_table.reshape(4, padded_rows // 4, model_width),
            small,
            block_of,
            taken.astype(jnp.int32),
            slot_cap,
        )
        grad_table = grad_table.reshape(padded_rows, model_width)[:vocab_rows]
        squares = jnp.sum(small[6])
        owned = owned.reshape(slot_cap, model_width, model_width)
    else:
        grad_blocks = jnp.concatenate([g.astype(f32) for g in grad_blocks], axis=0)
        mine = lax.psum_scatter(grad_blocks, "fsdp", scatter_dimension=1, tiled=True)
        mine, grad_table = lax.psum((mine, grad_table[:vocab_rows]), "rep")
        small = lax.psum(small, ("rep", "fsdp"))
        squares = lax.psum(jnp.sum(mine * mine) + jnp.sum(grad_table * grad_table), "fsdp")
        outgoing = jnp.where(taken[:, None, None], jnp.take(mine, block_of, axis=0), 0)
        owned = lax.all_to_all(outgoing, "fsdp", split_axis=0, concat_axis=1, tiled=True)
    loss_all = small[7, 0]
    grad_gains = small[:gain_count]
    grad_norm = jnp.sqrt(squares + jnp.sum(grad_gains * grad_gains))
    factor = jnp.minimum(1.0, clip_limit / grad_norm)
    grad_gains = lax.dynamic_slice_in_dim(grad_gains, member * gains.shape[1], gains.shape[1], axis=1)

    live = lax.dynamic_slice_in_dim(taken, member * slot_cap, slot_cap)
    if move.kernels:
        soap_m_new, soap_v_new, turned = turn_slots(
            replica,
            live,
            jnp.stack([factor, first_fix, second_fix]),
            left_basis,
            right_basis,
            owned,
            soap_m,
            soap_v,
        )
        returned = exchange_slots(move.sizes, 11, turned, False)
        returned = returned.reshape(slot_total, shard_rows, model_width)
    else:
        rotated = jnp.einsum("bji,bjk->bik", left_basis, owned, precision=high)
        rotated = factor * jnp.einsum("bik,bkl->bil", rotated, right_basis, precision=high)
        moment_first, moment_second, rotated_step = adam_moments(soap_m, soap_v, rotated, first_fix, second_fix)
        soap_m_new = jnp.where(live[:, None, None], moment_first, soap_m)
        soap_v_new = jnp.where(live[:, None, None], moment_second, soap_v)
        turned = jnp.einsum("bij,bjk->bik", left_basis, rotated_step, precision=high)
        turned = jnp.einsum("bik,blk->bil", turned, right_basis, precision=high)
        returned = lax.all_to_all(turned, "fsdp", split_axis=1, concat_axis=0, tiled=True)
    update = jnp.take(returned, block_slots, axis=0).astype(f32)
    blocks_new = blocks - step_rate * (update + weight_decay * blocks)

    embed_m_new, embed_v_new, table_step = adam_moments(
        embed_m, embed_v, factor * grad_table, first_fix, second_fix
    )
    embed_new = embed - step_rate * (table_step + weight_decay * embed)
    gains_m_new, gains_v_new, gain_step = adam_moments(
        gains_m, gains_v, factor * grad_gains, first_fix, second_fix
    )
    gains_new = gains - step_rate * gain_step
    loss = (loss_all / position_count).reshape(1)
    return (
        loss,
        grad_norm.reshape(1),
        blocks_new,
        gains_new,
        embed_new,
        embed_m_new,
        embed_v_new,
        gains_m_new,
        gains_v_new,
        soap_m_new,
        soap_v_new,
        blocks_new.astype(bf16),
        embed_new.astype(bf16),
    )


def solution(mesh):
    packs = P(None, ("rep", "fsdp"), None)
    rows = P(None, "fsdp", None)
    columns = P(None, "fsdp")
    table = P("fsdp", None)
    slots = P("fsdp", None, None)
    return jax.shard_map(
        body,
        mesh=mesh,
        in_specs=(packs,) * 4
        + (rows, columns)
        + (table,) * 3
        + (columns,) * 2
        + (slots,) * 4
        + (P(), P()),
        out_specs=(P(), P(), rows, columns)
        + (table,) * 3
        + (columns,) * 2
        + (slots,) * 2
        + (rows, table),
        check_vma=False,
    )
```

```python
from functools import partial
import math

import jax
import jax.numpy as jnp
from jax import lax
from jax.experimental import pallas as pl
from jax.experimental.pallas import tpu as pltpu
from jax.sharding import PartitionSpec as P

HEADS = 8
FF = 2048
LAYERS = 2

norm_epsilon = 1e-05
beta_first = 0.9
beta_second = 0.99
adam_epsilon = 1e-08
step_rate = 0.04
weight_decay = 0.1
clip_ratio = 12.0
masked_score = -1e30
bf16 = jnp.bfloat16
f32 = jnp.float32
highest = lax.Precision.HIGHEST
high = lax.Precision.HIGH
MESH = pl.DeviceIdType.MESH
ANY = pl.BlockSpec(memory_space=pl.ANY)
VMEM = pl.BlockSpec(memory_space=pltpu.VMEM)
CAPACITY = 128


def pick(table, index):
    out = jnp.int32(table[0])
    for k in range(1, len(table)):
        out = jnp.where(index == k, jnp.int32(table[k]), out)
    return out


def ring_order(n):
    nz = 4
    nx = n // nz
    order = []
    for x in range(nx):
        zs = range(1, nz) if x % 2 == 0 else range(nz - 1, 0, -1)
        order += [z * nx + x for z in zs]
    order += [x for x in range(nx - 1, -1, -1)]
    return order


class Place:
    def __init__(self, n_rep, n_fsdp):
        self.r = lax.axis_index("rep")
        self.f = lax.axis_index("fsdp")
        self.n_rep, self.n = n_rep, n_fsdp
        self.c = lax.rem(self.r, 2)
        self.y = self.r // 2
        self.order = ring_order(n_fsdp)
        spot = [self.order.index(k) for k in range(n_fsdp)]
        self.pos = pick(spot, self.f)
        self.core = (self.r + 1 - 2 * self.c, self.f)
        self.next = (self.r, self.at(1))
        self.prev = (self.r, self.at(-1))

    def at(self, step):
        return pick(self.order, lax.rem(self.pos + step + 2 * self.n, self.n))


def enter(peers):
    barrier = pltpu.get_barrier_semaphore()
    for peer in peers:
        pl.semaphore_signal(barrier, inc=1, device_id=peer, device_id_type=MESH)
    pl.semaphore_wait(barrier, len(peers))


def remote(src, dst, send, recv, peer):
    return pltpu.make_async_remote_copy(
        src_ref=src, dst_ref=dst, send_sem=send, recv_sem=recv, device_id=peer, device_id_type=MESH
    )


def params(cid, limit=None):
    return pltpu.CompilerParams(
        collective_id=cid, has_side_effects=True, vmem_limit_bytes=limit
    )


def group_kernel(n_rep, n, spread, x_ref, o_ref, send, recv):
    here = Place(n_rep, n)
    me = here.f
    others = [lax.rem(me + k, n) for k in range(1, n)]
    enter([(here.r, o) for o in others])
    copies = []
    for k, o in enumerate(others):
        src = x_ref.at[o] if spread else x_ref
        cp = remote(src, o_ref.at[me], send.at[k], recv.at[k], (here.r, o))
        cp.start()
        copies.append(cp)
    o_ref[me] = x_ref[me] if spread else x_ref[...]
    for cp in copies:
        cp.wait()


def group_exchange(mesh_sizes, cid, x, spread):
    n_rep, n = mesh_sizes
    shape = x.shape if spread else (n,) + x.shape
    return pl.pallas_call(
        partial(group_kernel, n_rep, n, spread),
        out_shape=jax.ShapeDtypeStruct(shape, x.dtype),
        in_specs=[VMEM],
        out_specs=VMEM,
        scratch_shapes=[pltpu.SemaphoreType.DMA((n - 1,)), pltpu.SemaphoreType.DMA((n - 1,))],
        compiler_params=params(cid),
        name=f"group_{cid}",
    )(x)


def opening_kernel(
    n_rep, n, half, shared, x_ref, t_ref, w_ref, facts_ref, gains_ref, o_ref, rows_ref, asked, facts, gains, most,
    table, index, stage, ready, held, got,
    t_s, ring_s, ring_r, core_s, core_r, y_s, y_r, over_s, over_r, ask_s, ask_r, top_s, top_r, rows_s, rows_r,
):
    here = Place(n_rep, n)
    me = here.f
    ypeer = (lax.rem(here.r + 2, 4), here.f)
    others = [lax.rem(me + k, n) for k in range(1, n)]
    rows = x_ref.shape[1]
    alone = (half - shared) // 2
    enter([(here.r, o) for o in others] + [here.core, ypeer])
    load = pltpu.make_async_copy(t_ref, table, t_s.at[0])
    load.start()
    asks = []
    for k, o in enumerate(others):
        peer = (here.r, o)
        asks.append(remote(w_ref.at[o], asked.at[me], ask_s.at[0, k], ask_r.at[0, k], peer))
        asks.append(remote(facts_ref, facts.at[me], ask_s.at[1, k], ask_r.at[1, k], peer))
        asks.append(remote(gains_ref, gains.at[me], ask_s.at[2, k], ask_r.at[2, k], peer))
    for cp in asks:
        cp.start()

    mine = pl.ds(here.c * half + here.y * alone, alone + shared)
    given = pl.ds(here.c * half + here.y * (alone + shared), alone)
    taken = pl.ds(here.c * half + (1 - here.y) * (alone + shared), alone)
    hops = n // 2
    copies, sends = [], []

    def rows_of(origin, way, s):
        if s == hops - 1:
            return pl.ds(pl.multiple_of(origin * rows + way * (rows // 2), rows // 2), rows // 2)
        return pl.ds(pl.multiple_of(origin * rows, rows), rows)

    own = remote(x_ref, o_ref.at[:, rows_of(here.f, 0, -1)], core_s.at[0, 0], core_r.at[0, 0], here.core)
    own.start()
    copies.append(own)
    waiting = [None, None]
    across = []

    def pass_on(way, s):
        waiting[way].wait_recv()
        where = rows_of(here.at(-s - 1 if way == 0 else s + 1), way, s)
        kept = o_ref.at[given, where]
        cp = remote(kept, kept, y_s.at[way, s], y_r.at[way, s], ypeer)
        cp.start()
        across.append((cp, o_ref.at[taken, where], way, s))
        kept = o_ref.at[mine, where]
        cp = remote(kept, kept, core_s.at[way, s + 1], core_r.at[way, s + 1], here.core)
        cp.start()
        copies.append(cp)

    def hop(way, s):
        where = rows_of(here.at(-s if way == 0 else s), way, s)
        src = x_ref.at[mine] if s == 0 else o_ref.at[mine, where]
        cp = remote(
            src, o_ref.at[mine, where], ring_s.at[way, s], ring_r.at[way, s], here.next if way == 0 else here.prev
        )
        cp.start()
        waiting[way] = cp
        sends.append(cp)

    for way in range(2):
        hop(way, 0)

    asked[me] = w_ref[me]
    facts[me] = facts_ref[...]
    gains[me] = gains_ref[...]
    for cp in asks:
        cp.wait_recv()
    listed = pltpu.make_async_copy(asked, index, t_s.at[1])
    listed.start()
    top = facts[0]
    for k in range(1, n):
        top = jnp.maximum(top, facts[k])
    held[0] = top
    first = remote(held.at[0], got.at[0], top_s.at[0], top_r.at[0], here.core)
    first.start()
    listed.wait()
    load.wait()
    places = rows_ref.shape[1]

    def collect(o):
        def one(i, carry):
            stage[pl.ds(i, 1)] = table[pl.ds(index[o, 0, i], 1)]
            return carry

        lax.fori_loop(0, places, one, 0, unroll=8)
        return stage[...].astype(bf16)

    for k, o in enumerate(others):
        ready[o] = collect(o)
        cp = remote(ready.at[o], rows_ref.at[me], rows_s.at[k], rows_r.at[k], (here.r, o))
        cp.start()
        asks.append(cp)
    rows_ref[me] = collect(me)
    first.wait_recv()
    held[1] = jnp.maximum(top, got[0])
    second = remote(held.at[1], got.at[1], top_s.at[1], top_r.at[1], ypeer)
    second.start()

    for s in range(1, hops):
        for way in range(2):
            pass_on(way, s - 1)
            hop(way, s)
    second.wait_recv()
    most[...] = jnp.maximum(held[1], got[1])
    for way in range(2):
        pass_on(way, hops - 1)
    for cp, kept, way, s in across:
        cp.wait_recv()
        over = remote(kept, kept, over_s.at[way, s], over_r.at[way, s], here.core)
        over.start()
        copies.append(over)
        sends.append(cp)
    for cp in asks[3 * (n - 1) :]:
        cp.wait_recv()
    for cp in asks + [first, second] + sends:
        cp.wait_send()
    for cp in copies:
        cp.wait()


def open_step(mesh_sizes, cid, shard, table, wanted, facts, gains):
    n_rep, n = mesh_sizes
    count, rows, width = shard.shape
    half = count // 2
    places = wanted.shape[2]
    dma = pltpu.SemaphoreType.DMA
    return pl.pallas_call(
        partial(opening_kernel, n_rep, n, half, half - 2 * (half // 3)),
        out_shape=[
            jax.ShapeDtypeStruct((count, rows * n, width), shard.dtype),
            jax.ShapeDtypeStruct((n, places, width), bf16),
            jax.ShapeDtypeStruct(wanted.shape, wanted.dtype),
            jax.ShapeDtypeStruct((n,) + facts.shape, facts.dtype),
            jax.ShapeDtypeStruct((n,) + gains.shape, gains.dtype),
            jax.ShapeDtypeStruct(facts.shape, facts.dtype),
        ],
        in_specs=[ANY, ANY] + [VMEM] * 3,
        out_specs=[ANY] + [VMEM] * 5,
        scratch_shapes=[
            pltpu.VMEM(table.shape, table.dtype),
            pltpu.SMEM(wanted.shape, wanted.dtype),
            pltpu.VMEM((places, width), table.dtype),
            pltpu.VMEM((n, places, width), bf16),
            pltpu.VMEM((2,) + facts.shape, facts.dtype),
            pltpu.VMEM((2,) + facts.shape, facts.dtype),
            dma((2,)),
            dma((2, n // 2)),
            dma((2, n // 2)),
            dma((2, n // 2 + 1)),
            dma((2, n // 2 + 1)),
            dma((2, n // 2)),
            dma((2, n // 2)),
            dma((2, n // 2)),
            dma((2, n // 2)),
            dma((3, n - 1)),
            dma((3, n - 1)),
            dma((2,)),
            dma((2,)),
            dma((n - 1,)),
            dma((n - 1,)),
        ],
        compiler_params=params(cid, 60 << 20),
        name="open_step",
    )(shard, table, wanted, facts, gains)


def squares_row(square):
    row = jnp.sum(square, axis=0, keepdims=True)
    return jnp.where(lax.broadcasted_iota(jnp.int32, square.shape, 0) == 6, row, 0.0)


def reduce_kernel(
    n_rep, n, half, table_rows, each, *refs
):
    g_refs, refs = refs[: 2 * each], refs[2 * each :]
    (
    t_ref, small_ref, block_of, taken, o_ref, to_ref, sum_ref, mine, outgoing, held, hgot, four, fours, squares,
    own, part, got, fin, ysend, ygot, town, tpart, tsend, tgot,
    load_s, core_s, core_r, ring_s, ring_r, y_s, y_r, tload, tcs, tcr, tys, tyr, tos, tor,
    keep, a_s, a_r, f_s, f_r, sum_s, sum_r,
    ) = refs
    here = Place(n_rep, n)
    c, y = here.c, here.y
    ypeer = (lax.rem(here.r + 2, 4), here.f)
    other_c, other_y = 1 - c, 1 - y
    me = here.f
    others = [lax.rem(me + k, n) for k in range(1, n)]
    enter([(here.r, o) for o in others] + [here.core, ypeer])
    far = n // 2

    tl = pltpu.make_async_copy(t_ref.at[pl.ds(c * 2, 2)], town, tload)
    tl.start()
    tc = remote(t_ref.at[pl.ds(other_c * 2, 2)], tpart, tcs, tcr, here.core)
    tc.start()

    spots = {(0, far): 0, (1, far): 0}
    for d in range(far - 1, 0, -1):
        spots[0, d] = 1 + 2 * (far - 1 - d)
        spots[1, d] = 2 + 2 * (far - 1 - d)
    spots[0, 0] = spots[1, 0] = n - 1
    loads, cores = {}, {}
    done = set()
    for (way, d), spot in sorted(spots.items(), key=lambda item: item[1]):
        if spot in done:
            continue
        done.add(spot)
        to = here.f if d == 0 else here.at(d if way == 0 else -d)
        for h in (way, 1 - way):
            loads[spot, h], cores[spot, h] = [], []
            for j in range(each):
                g_ref = g_refs[h * each + j]
                into = pl.ds(j * (half // each), half // each)
                ld = pltpu.make_async_copy(g_ref.at[:, to, :, c], own.at[spot, h, into], load_s.at[spot, h, j])
                ld.start()
                loads[spot, h].append(ld)
                cp = remote(
                    g_ref.at[:, to, :, other_c],
                    part.at[spot, h, into],
                    core_s.at[spot, h, j],
                    core_r.at[spot, h, j],
                    here.core,
                )
                cp.start()
                cores[spot, h].append(cp)

    def ready(spot, h):
        for j in range(each):
            loads[spot, h][j].wait()
            cores[spot, h][j].wait_recv()

    ring = {}

    def came(way, h, s):
        return got.at[way, h, s]

    def lane(way, h, s):
        d = far - s
        spot = spots[way, d]
        ready(spot, h)
        before = ring.get((way, h, s - 1))
        if before is not None:
            before.wait_recv()
        target = own.at[spot, h]

        @pl.loop(0, half)
        def _(b):
            for k in range(2):
                total = own[spot, h, b, k].astype(f32) + part[spot, h, b, k].astype(f32)
                if before is not None:
                    total = total + came(way, h, s - 1)[b, k].astype(f32)
                target[b, k] = total.astype(target.dtype)

        cp = remote(
            target, came(way, h, s), ring_s.at[way, h, s], ring_r.at[way, h, s], here.next if way == 0 else here.prev
        )
        cp.start()
        ring[way, h, s] = cp

    step_rows = 48
    for s in range(far):
        for h_turn in range(2):
            for way in range(2):
                h = way if h_turn == 1 else 1 - way
                if s == far - 1:
                    h = h_turn
                if s == 0 and h_turn == 0:
                    continue
                if s == 1 and h_turn == 0:
                    continue
                lane(way, h, s)
        if s == 0:
            for way in range(2):
                lane(way, 1 - way, 1)
            tl.wait()
            tc.wait_recv()

            @pl.loop(0, table_rows // step_rows)
            def _(i):
                at = pl.ds(pl.multiple_of(i * step_rows, step_rows), step_rows)
                town[y, at] = town[y, at] + tpart[y, at]
                tsend[at] = (town[other_y, at] + tpart[other_y, at]).astype(bf16)

            ty = remote(tsend, tgot, tys, tyr, ypeer)
            ty.start()
        if s == 2:
            ty.wait_recv()

            def add(i, acc):
                at = pl.ds(pl.multiple_of(i * step_rows, step_rows), step_rows)
                total = town[y, at] + tgot[at].astype(f32)
                town[y, at] = total
                square = total * total
                for k in range(step_rows // 8):
                    acc = acc + square[k * 8 : k * 8 + 8]
                return acc

            squares[...] = lax.fori_loop(0, table_rows // step_rows, add, jnp.zeros((8, tgot.shape[1]), f32))
            quarter = c * 2 + y
            near = c * 2 + other_y
            tkeep = pltpu.make_async_copy(town.at[y], to_ref.at[quarter], tload)
            tkeep.start()
            t0 = remote(town.at[y], to_ref.at[quarter], tos.at[0], tor.at[0], ypeer)
            t1 = remote(town.at[y], to_ref.at[quarter], tos.at[1], tor.at[1], here.core)
            t0.start()
            t1.start()
    ys = []
    spot = spots[0, 0]
    for h in range(2):
        ready(spot, h)
        for way in range(2):
            ring[way, h, far - 1].wait_recv()

        @pl.loop(0, half)
        def _(b, h=h):
            for keep in range(2):
                k = y if keep else other_y
                total = own[spot, h, b, k].astype(f32) + part[spot, h, b, k].astype(f32)
                for way in range(2):
                    total = total + got[way, h, far - 1, b, k].astype(f32)
                if keep:
                    fin[h, b] = total
                else:
                    ysend[h, b] = total.astype(bf16)

        cp = remote(ysend.at[h], ygot.at[h], y_s.at[h], y_r.at[h], ypeer)
        cp.start()
        ys.append(cp)

    acc = jnp.zeros((8, fin.shape[-1]), f32)
    for h in range(2):
        ys[h].wait_recv()

        def last(b, acc, h=h):
            total = fin[h, b] + ygot[h, b].astype(f32)
            mine[h * half + b] = total.astype(bf16)
            square = total * total
            return acc + square[:8] + square[8:]

        acc = lax.fori_loop(0, half, last, acc)

    held[0] = small_ref[...] + squares_row(acc + squares[...])
    first = remote(held.at[0], hgot.at[0], sum_s.at[0], sum_r.at[0], here.core)
    first.start()

    cap = o_ref.shape[0]

    @pl.loop(0, n * cap)
    def _(k):
        value = mine[block_of[k]]
        outgoing[k] = jnp.where(taken[k] > 0, value, jnp.zeros_like(value))

    def spot_of(source, r):
        return o_ref.at[:, source, r]

    moves = []
    for k, o in enumerate(others):
        cp = remote(outgoing.at[pl.ds(o * cap, cap)], spot_of(me, here.r), a_s.at[k], a_r.at[k], (here.r, o))
        cp.start()
        moves.append(cp)
    kept = pltpu.make_async_copy(outgoing.at[pl.ds(me * cap, cap)], spot_of(me, here.r), keep)
    kept.start()
    first.wait_recv()
    held[1] = held[0] + hgot[0]
    second = remote(held.at[1], hgot.at[1], sum_s.at[1], sum_r.at[1], ypeer)
    second.start()
    t0.wait_recv()
    t2 = remote(to_ref.at[near], to_ref.at[near], tos.at[2], tor.at[2], here.core)
    t2.start()
    second.wait_recv()
    four[...] = held[1] + hgot[1]
    totals = []
    for k, o in enumerate(others):
        cp = remote(four, fours.at[me], sum_s.at[2 + k], sum_r.at[2 + k], (here.r, o))
        cp.start()
        totals.append(cp)
    fours[me] = four[...]
    beside, distant = [], []
    for k in range(n):
        source = me if k == 0 else lax.rem(me - k + n, n)
        if k == 0:
            kept.wait()
        else:
            moves[k - 1].wait_recv()
        piece = spot_of(source, here.r)
        over = remote(piece, piece, f_s.at[0, k], f_r.at[0, k], ypeer)
        over.start()
        cp = remote(piece, piece, f_s.at[1, k], f_r.at[1, k], here.core)
        cp.start()
        distant.append((over, source))
        beside.append(cp)
    for cp in totals:
        cp.wait_recv()
    total = fours[0]
    for k in range(1, n):
        total = total + fours[k]
    sum_ref[...] = total
    yr = lax.rem(here.r + 2, 4)
    for k, (over, source) in enumerate(distant):
        over.wait_recv()
        piece = spot_of(source, yr)
        cp = remote(piece, piece, f_s.at[2, k], f_r.at[2, k], here.core)
        cp.start()
        beside.append(cp)
    for cp in moves + totals + [first, second] + [over for over, _ in distant]:
        cp.wait_send()
    for cp in beside:
        cp.wait()
    for cp in ys:
        cp.wait_send()
    for cp in ring.values():
        cp.wait_send()
    for group in cores.values():
        for cp in group:
            cp.wait_send()
    tc.wait_send()
    ty.wait_send()
    tkeep.wait()
    t0.wait_send()
    t1.wait()
    t2.wait()


def settle_gradients(mesh_sizes, cid, grads, table, small, block_of, taken, cap):
    n_rep, n = mesh_sizes
    _, depth, width = grads[0].shape
    count = sum(g.shape[0] for g in grads)
    half = count // 2
    each = len(grads) // 2
    far = n // 2
    table_rows = table.shape[1]
    views = [g.reshape(g.shape[0], n, 2, 2, 16, width) for g in grads]
    dma = pltpu.SemaphoreType.DMA
    piece = (half, 2, 16, width)
    smem = pl.BlockSpec(memory_space=pltpu.SMEM)
    like = small.shape
    return pl.pallas_call(
        partial(reduce_kernel, n_rep, n, half, table_rows, each),
        out_shape=[
            jax.ShapeDtypeStruct((cap, n, 4, 16, width), bf16),
            jax.ShapeDtypeStruct(table.shape, f32),
            jax.ShapeDtypeStruct(like, f32),
        ],
        in_specs=[ANY] * (2 * each + 1) + [VMEM, smem, smem],
        out_specs=[ANY, ANY, VMEM],
        scratch_shapes=[
            pltpu.VMEM((count, 16, width), bf16),
            pltpu.VMEM((n * cap, 16, width), bf16),
            pltpu.VMEM((2,) + like, f32),
            pltpu.VMEM((2,) + like, f32),
            pltpu.VMEM(like, f32),
            pltpu.VMEM((n,) + like, f32),
            pltpu.VMEM(like, f32),
            pltpu.VMEM((n, 2) + piece, bf16),
            pltpu.VMEM((n, 2) + piece, bf16),
            pltpu.VMEM((2, 2, far) + piece, bf16),
            pltpu.VMEM((2, half, 16, width), f32),
            pltpu.VMEM((2, half, 16, width), bf16),
            pltpu.VMEM((2, half, 16, width), bf16),
            pltpu.VMEM((2, table_rows, width), f32),
            pltpu.VMEM((2, table_rows, width), f32),
            pltpu.VMEM((table_rows, width), bf16),
            pltpu.VMEM((table_rows, width), bf16),
            dma((n, 2, each)),
            dma((n, 2, each)),
            dma((n, 2, each)),
            dma((2, 2, far)),
            dma((2, 2, far)),
            dma((2,)),
            dma((2,)),
            dma,
            dma,
            dma,
            dma,
            dma,
            dma((3,)),
            dma((3,)),
            dma,
            dma((n - 1,)),
            dma((n - 1,)),
            dma((3, n)),
            dma((3, n)),
            dma((n + 1,)),
            dma((n + 1,)),
        ],
        compiler_params=params(cid, 56 << 20),
        name="settle_gradients",
    )(*views, table, small, block_of, taken)


def slots_kernel(n_rep, n, to_slots, x_ref, o_ref, keep, a_s, a_r, f_s, f_r):
    here = Place(n_rep, n)
    ypeer = (lax.rem(here.r + 2, 4), here.f)
    me = here.f
    others = [lax.rem(me + k, n) for k in range(1, n)]
    enter([(here.r, o) for o in others] + [here.core, ypeer])

    def spot(source, r):
        return o_ref.at[:, source, r] if to_slots else o_ref.at[source, :, r]

    copies = []
    for k, o in enumerate(others):
        cp = remote(x_ref.at[o], spot(me, here.r), a_s.at[k], a_r.at[k], (here.r, o))
        cp.start()
        copies.append(cp)
    own = pltpu.make_async_copy(x_ref.at[me], spot(me, here.r), keep)
    own.start()
    sends, far = [], []
    for k in range(n):
        source = me if k == 0 else lax.rem(me - k + n, n)
        if k == 0:
            own.wait()
        else:
            copies[k - 1].wait_recv()
        held = spot(source, here.r)
        over = remote(held, held, f_s.at[0, k], f_r.at[0, k], ypeer)
        over.start()
        beside = remote(held, held, f_s.at[1, k], f_r.at[1, k], here.core)
        beside.start()
        far.append((over, source))
        sends.append(beside)
    yr = lax.rem(here.r + 2, 4)
    for k, (over, source) in enumerate(far):
        over.wait_recv()
        src = me if k == 0 else lax.rem(me - k + n, n)
        held = spot(src, yr)
        beside = remote(held, held, f_s.at[2, k], f_r.at[2, k], here.core)
        beside.start()
        sends.append(beside)
    for cp in copies:
        cp.wait_send()
    for over, _ in far:
        over.wait_send()
    for cp in sends:
        cp.wait()


def exchange_slots(mesh_sizes, cid, x, to_slots):
    n_rep, n = mesh_sizes
    _, cap, rows, width = x.shape
    shape = (cap, n, 4, rows, width) if to_slots else (n, cap, 4, rows, width)
    dma = pltpu.SemaphoreType.DMA
    return pl.pallas_call(
        partial(slots_kernel, n_rep, n, to_slots),
        out_shape=jax.ShapeDtypeStruct(shape, x.dtype),
        in_specs=[VMEM],
        out_specs=ANY,
        scratch_shapes=[dma, dma((n - 1,)), dma((n - 1,)), dma((3, n)), dma((3, n))],
        compiler_params=params(cid),
        name=f"slots_{cid}",
    )(x)


def layer_norm(inputs, gain_row):
    centre = inputs - jnp.mean(inputs, axis=-1, keepdims=True)
    spread = jnp.mean(centre * centre, axis=-1, keepdims=True)
    return centre * lax.rsqrt(spread + norm_epsilon) * gain_row


def adam_moments(moment_old, second_old, gradient, first_fix, second_fix):
    moment_new = beta_first * moment_old + (1.0 - beta_first) * gradient
    second_new = beta_second * second_old + (1.0 - beta_second) * gradient * gradient
    step_value = moment_new / first_fix / (jnp.sqrt(second_new / second_fix) + adam_epsilon)
    return (moment_new, second_new, step_value)


def head_slopes(head_count):
    return 2.0 ** (-8.0 * (jnp.arange(head_count, dtype=f32) + 1.0) / head_count)


NT = (((1,), (1,)), ((), ()))
TN = (((0,), (0,)), ((), ()))
masked_distance = 1e33


def mm(a, b, dims=None):
    if dims is None:
        return jnp.dot(a, b, preferred_element_type=f32)
    return lax.dot_general(a, b, dims, preferred_element_type=f32)


def norm_parts(x):
    centre = x - jnp.mean(x, axis=-1, keepdims=True)
    spread = jnp.mean(centre * centre, axis=-1, keepdims=True)
    rstd = lax.rsqrt(spread + norm_epsilon)
    return centre * rstd, rstd


def norm_back(x, gain, grad):
    hat, rstd = norm_parts(x)
    inner = grad * gain
    back = inner - jnp.mean(inner, axis=-1, keepdims=True) - hat * jnp.mean(inner * hat, axis=-1, keepdims=True)
    return rstd * back, grad * hat


def fold8(x):
    total = x[:8]
    for k in range(1, x.shape[0] // 8):
        total = total + x[k * 8 : k * 8 + 8]
    return total


def pair_bias(seg_row, seg_col, bias):
    length = bias.shape[0]
    i = lax.broadcasted_iota(jnp.int32, (length, length), 0)
    j = lax.broadcasted_iota(jnp.int32, (length, length), 1)
    apart = jnp.abs(i - j).astype(f32)
    bias[...] = jnp.where(seg_col == seg_row, apart, masked_distance)


def attend_kernel(slopes, x, gain, w, seg_row, seg_col, y, a, qkv, o, lse, bias):
    pair = pl.program_id(1)
    length, width = x.shape
    half = width // HEADS
    two = 2 * half
    rows = ROWS

    @pl.when(pair == 0)
    def _():
        pair_bias(seg_row[0], seg_col[0], bias)

        @pl.loop(0, length // rows)
        def _(i):
            at = pl.ds(pl.multiple_of(i * rows, rows), rows)
            hat, _ = norm_parts(x[at])
            low = (hat * gain[...]).astype(bf16)
            a[at] = low
            for k in range(3):
                part = mm(low, w[k])
                if k == 0:
                    part = part.astype(bf16).astype(f32) * half ** (-0.5)
                qkv[at, k * width : (k + 1) * width] = part.astype(bf16)

    lanes = pl.ds(pl.multiple_of(pair * two, two), two)
    q = qkv[:, pl.ds(pl.multiple_of(pair * two, two), two)]
    k = qkv[:, pl.ds(pl.multiple_of(width + pair * two, two), two)]
    v = qkv[:, pl.ds(pl.multiple_of(2 * width + pair * two, two), two)]
    v_t = v.astype(f32).T.astype(bf16)
    left = lax.broadcasted_iota(jnp.int32, (length, two), 1) < half
    zero = jnp.zeros_like(q)
    out = []
    for e in range(2):
        slope = slopes[2 * pair + e]
        q_e = jnp.where(left, q, zero) if e == 0 else jnp.where(left, zero, q)
        s = mm(k, q_e, NT) - slope * bias[...]
        top = jnp.max(s, axis=0, keepdims=True)
        p = jnp.exp(s - top)
        total = jnp.sum(p, axis=0, keepdims=True)
        low = (p * (1.0 / total)).astype(bf16)
        out.append(mm(v_t, low))
        lse[0, pl.ds(2 * pair + e, 1)] = top + jnp.log(total)
    upper = lax.broadcasted_iota(jnp.int32, (two, length), 0) < half
    o[:, lanes] = jnp.where(upper, out[0], out[1]).T.astype(bf16)

    @pl.when(pair == pl.num_programs(1) - 1)
    def _():
        @pl.loop(0, length // rows)
        def _(i):
            at = pl.ds(pl.multiple_of(i * rows, rows), rows)
            y[at] = x[at] + mm(o[at], w[3])


def attend(x, gain, weights, layer, seg):
    packs, length = seg.shape
    tokens, width = x.shape
    per_layer4 = weights.shape[0] // LAYERS // 4
    slopes = head_slopes(HEADS)
    whole = lambda shape: pl.BlockSpec(shape, lambda m, p: (m,) + (0,) * (len(shape) - 1))
    fixed = lambda shape, at: pl.BlockSpec(shape, lambda m, p: at)
    return pl.pallas_call(
        attend_kernel,
        grid=(packs, HEADS // 2),
        in_specs=[
            pl.BlockSpec(memory_space=pltpu.SMEM),
            whole((length, width)),
            fixed((1, width), (0, 0)),
            fixed((4, width, width), (per_layer4 * layer, 0, 0)),
            whole((1, 1, length)),
            whole((1, length, 1)),
        ],
        out_specs=[
            whole((length, width)),
            whole((length, width)),
            whole((length, 3 * width)),
            whole((length, width)),
            whole((1, HEADS, length)),
        ],
        out_shape=[
            jax.ShapeDtypeStruct((tokens, width), f32),
            jax.ShapeDtypeStruct((tokens, width), bf16),
            jax.ShapeDtypeStruct((tokens, 3 * width), bf16),
            jax.ShapeDtypeStruct((tokens, width), bf16),
            jax.ShapeDtypeStruct((packs, HEADS, length), f32),
        ],
        scratch_shapes=[pltpu.VMEM((length, length), f32)],
        compiler_params=pltpu.CompilerParams(vmem_limit_bytes=48 << 20),
        name="attend",
    )(slopes, x, gain.reshape(1, width), weights, seg.reshape(packs, 1, length), seg.reshape(packs, length, 1))


def attend_back_kernel(
    slopes, dx, x, gain, w, a, qkv, o, lse, seg_row, seg_col, new, dgain, gw, bias, do, dqkv, acc
):
    pack, pair = pl.program_id(0), pl.program_id(1)
    length, width = x.shape
    half = width // HEADS
    two = 2 * half
    rows = ROWS

    @pl.when(pair == 0)
    def _():
        pair_bias(seg_row[0], seg_col[0], bias)

        @pl.loop(0, length // rows)
        def _(i):
            at = pl.ds(pl.multiple_of(i * rows, rows), rows)
            do[at] = mm(dx[at].astype(bf16), w[3], NT).astype(bf16)

        part = mm(o[...], dx[...].astype(bf16), TN)

        @pl.when(pack == 0)
        def _():
            acc[3] = part

        @pl.when(pack > 0)
        def _():
            acc[3] += part

    lanes = [pl.ds(pl.multiple_of(n * width + pair * two, two), two) for n in range(3)]
    q, k, v = [qkv[:, at] for at in lanes]
    do_p = do[:, lanes[0]]
    k_t = k.astype(f32).T.astype(bf16)
    left = lax.broadcasted_iota(jnp.int32, (length, two), 1) < half
    upper = lax.broadcasted_iota(jnp.int32, (two, length), 0) < half
    zero = jnp.zeros_like(q)
    dq, dk, dv = [], [], []
    for e in range(2):
        slope = slopes[2 * pair + e]
        keep = (lambda t: jnp.where(left, t, zero)) if e == 0 else (lambda t: jnp.where(left, zero, t))
        s = mm(k, keep(q), NT) - slope * bias[...]
        p = jnp.exp(s - lse[0, pl.ds(2 * pair + e, 1)])
        dp = mm(v, keep(do_p), NT)
        inner = jnp.sum(p * dp, axis=0, keepdims=True)
        ds = (p * (dp - inner)).astype(bf16)
        dv.append(mm(p.astype(bf16), do_p))
        dk.append(mm(ds, q))
        dq.append(mm(k_t, ds))
    dqkv[:, lanes[0]] = (jnp.where(upper, dq[0], dq[1]).T * half ** (-0.5)).astype(bf16)
    dqkv[:, lanes[1]] = jnp.where(left, dk[0], dk[1]).astype(bf16)
    dqkv[:, lanes[2]] = jnp.where(left, dv[0], dv[1]).astype(bf16)

    @pl.when(pair == pl.num_programs(1) - 1)
    def _():
        def chunk(i, total):
            at = pl.ds(pl.multiple_of(i * rows, rows), rows)
            da = mm(dqkv[at, :width], w[0], NT)
            da = da + mm(dqkv[at, width : 2 * width], w[1], NT)
            da = da + mm(dqkv[at, 2 * width :], w[2], NT)
            back, extra = norm_back(x[at], gain[...], da)
            new[at] = dx[at] + back
            return total + fold8(extra)

        dgain[0] = lax.fori_loop(0, length // rows, chunk, jnp.zeros((8, width), f32))
        for n in range(3):
            part = mm(a[...], dqkv[:, n * width : (n + 1) * width], TN)

            @pl.when(pack == 0)
            def _(part=part, n=n):
                acc[n] = part

            @pl.when(pack > 0)
            def _(part=part, n=n):
                acc[n] += part

    @pl.when((pair == pl.num_programs(1) - 1) & (pack == pl.num_programs(0) - 1))
    def _():
        for n in range(4):
            gw[n] = acc[n].astype(bf16)


def attend_back(dx, x, gain, weights, layer, seg, kept):
    a, qkv, o, lse = kept
    packs, length = seg.shape
    tokens, width = x.shape
    per_layer4 = weights.shape[0] // LAYERS // 4
    whole = lambda shape: pl.BlockSpec(shape, lambda m, p: (m,) + (0,) * (len(shape) - 1))
    fixed = lambda shape, at: pl.BlockSpec(shape, lambda m, p: at)
    return pl.pallas_call(
        attend_back_kernel,
        grid=(packs, HEADS // 2),
        in_specs=[
            pl.BlockSpec(memory_space=pltpu.SMEM),
            whole((length, width)),
            whole((length, width)),
            fixed((1, width), (0, 0)),
            fixed((4, width, width), (per_layer4 * layer, 0, 0)),
            whole((length, width)),
            whole((length, 3 * width)),
            whole((length, width)),
            whole((1, HEADS, length)),
            whole((1, 1, length)),
            whole((1, length, 1)),
        ],
        out_specs=[
            whole((length, width)),
            whole((1, 8, width)),
            fixed((4, width, width), (0, 0, 0)),
        ],
        out_shape=[
            jax.ShapeDtypeStruct((tokens, width), f32),
            jax.ShapeDtypeStruct((packs, 8, width), f32),
            jax.ShapeDtypeStruct((4, width, width), bf16),
        ],
        scratch_shapes=[
            pltpu.VMEM((length, length), f32),
            pltpu.VMEM((length, width), bf16),
            pltpu.VMEM((length, 3 * width), bf16),
            pltpu.VMEM((4, width, width), f32),
        ],
        compiler_params=pltpu.CompilerParams(vmem_limit_bytes=56 << 20),
        name="attend_back",
    )(
        head_slopes(HEADS),
        dx,
        x,
        gain.reshape(1, width),
        weights,
        a,
        qkv,
        o,
        lse,
        seg.reshape(packs, 1, length),
        seg.reshape(packs, length, 1),
    )


ROWS = 512
gelu_c = math.sqrt(2.0 / math.pi)


def feed_kernel(x, gain, wg, wu, wd, y, f, gate, up):
    k = pl.program_id(0)
    tokens = x.shape[0]
    rows = ROWS

    @pl.loop(0, tokens // rows)
    def _(i):
        at = pl.ds(pl.multiple_of(i * rows, rows), rows)

        @pl.when(k == 0)
        def _():
            hat, _ = norm_parts(x[at])
            f[at] = (hat * gain[...]).astype(bf16)
            y[at] = x[at]

        low = f[at]
        g = mm(low, wg[0]).astype(bf16)
        u = mm(low, wu[0]).astype(bf16)
        gate[0, at] = g
        up[0, at] = u
        g, u = g.astype(f32), u.astype(f32)
        cdf = 0.5 * (1.0 + jnp.tanh(gelu_c * (g + 0.044715 * (g * g * g))))
        hidden = (g * cdf * u).astype(bf16)
        y[at] += mm(hidden, wd[0])


def feed(x, gain, weights, layer):
    tokens, width = x.shape
    per_layer = weights.shape[0] // LAYERS
    pieces = FF // width
    fixed = lambda shape: pl.BlockSpec(shape, lambda k: (0,) * len(shape))
    block = lambda skip: pl.BlockSpec((1, width, width), lambda k: (per_layer * layer + skip + k, 0, 0))
    each = pl.BlockSpec((1, tokens, width), lambda k: (k, 0, 0))
    return pl.pallas_call(
        feed_kernel,
        grid=(pieces,),
        in_specs=[fixed((tokens, width)), fixed((1, width)), block(4), block(4 + pieces), block(4 + 2 * pieces)],
        out_specs=[fixed((tokens, width)), fixed((tokens, width)), each, each],
        out_shape=[
            jax.ShapeDtypeStruct((tokens, width), f32),
            jax.ShapeDtypeStruct((tokens, width), bf16),
            jax.ShapeDtypeStruct((pieces, tokens, width), bf16),
            jax.ShapeDtypeStruct((pieces, tokens, width), bf16),
        ],
        compiler_params=pltpu.CompilerParams(vmem_limit_bytes=48 << 20),
        name="feed",
    )(x, gain.reshape(1, width), weights, weights, weights)


def feed_back_kernel(dx, x, gain, wg, wu, wd, f, gate, up, new, dgain, gg, gu, gd, f_t, dz, hid, dg, du):
    k = pl.program_id(0)
    tokens, width = x.shape
    rows = ROWS
    last = pl.num_programs(0) - 1

    @pl.when(k == 0)
    def _():
        @pl.loop(0, tokens // rows)
        def _(i):
            at = pl.ds(pl.multiple_of(i * rows, rows), rows)
            f_t[:, at] = f[at].astype(f32).T.astype(bf16)
            dz[at] = dx[at].astype(bf16)
            new[at] = jnp.zeros((rows, width), f32)

    def chunk(i, total):
        at = pl.ds(pl.multiple_of(i * rows, rows), rows)
        dh = mm(dz[at], wd[0], NT)
        g, u = gate[0, at].astype(f32), up[0, at].astype(f32)
        square = g * g
        t = jnp.tanh(gelu_c * (g + 0.044715 * (square * g)))
        cdf = 0.5 * (1.0 + t)
        act = g * cdf
        slope = cdf + 0.5 * g * (1.0 - t * t) * (gelu_c * (1.0 + 3 * 0.044715 * square))
        hid[at] = (act * u).astype(bf16)
        dgate = (dh * u * slope).astype(bf16)
        dup = (dh * act).astype(bf16)
        dg[at] = dgate
        du[at] = dup
        new[at] += mm(dgate, wg[0], NT) + mm(dup, wu[0], NT)
        return total

    lax.fori_loop(0, tokens // rows, chunk, 0)
    gg[0] = mm(f_t[...], dg[...]).astype(bf16)
    gu[0] = mm(f_t[...], du[...]).astype(bf16)
    gd[0] = mm(hid[...], dz[...], TN).astype(bf16)

    @pl.when(k == last)
    def _():
        def finish(i, total):
            at = pl.ds(pl.multiple_of(i * rows, rows), rows)
            back, extra = norm_back(x[at], gain[...], new[at])
            new[at] = dx[at] + back
            return total + fold8(extra)

        dgain[...] = lax.fori_loop(0, tokens // rows, finish, jnp.zeros((8, width), f32))


def feed_back(dx, x, gain, weights, layer, kept):
    f, gate, up = kept
    tokens, width = x.shape
    per_layer = weights.shape[0] // LAYERS
    pieces = FF // width
    fixed = lambda shape: pl.BlockSpec(shape, lambda k: (0,) * len(shape))
    block = lambda skip: pl.BlockSpec((1, width, width), lambda k: (per_layer * layer + skip + k, 0, 0))
    each = pl.BlockSpec((1, tokens, width), lambda k: (k, 0, 0))
    grad = pl.BlockSpec((1, width, width), lambda k: (k, 0, 0))
    return pl.pallas_call(
        feed_back_kernel,
        grid=(pieces,),
        in_specs=[
            fixed((tokens, width)),
            fixed((tokens, width)),
            fixed((1, width)),
            block(4),
            block(4 + pieces),
            block(4 + 2 * pieces),
            fixed((tokens, width)),
            each,
            each,
        ],
        out_specs=[fixed((tokens, width)), fixed((8, width)), grad, grad, grad],
        out_shape=[
            jax.ShapeDtypeStruct((tokens, width), f32),
            jax.ShapeDtypeStruct((8, width), f32),
        ]
        + [jax.ShapeDtypeStruct((pieces, width, width), bf16)] * 3,
        scratch_shapes=[
            pltpu.VMEM((width, tokens), bf16),
            pltpu.VMEM((tokens, width), bf16),
            pltpu.VMEM((tokens, width), bf16),
            pltpu.VMEM((tokens, width), bf16),
            pltpu.VMEM((tokens, width), bf16),
        ],
        compiler_params=pltpu.CompilerParams(vmem_limit_bytes=56 << 20),
        name="feed_back",
    )(dx, x, gain.reshape(1, width), weights, weights, weights, f, gate, up)


def two_parts(x):
    top = x.astype(bf16)
    return top, (x - top.astype(f32)).astype(bf16)


def mm3(a, b, dims=None):
    (a1, a2), (b1, b2) = a, b
    return mm(a1, b1, dims) + (mm(a1, b2, dims) + mm(a2, b1, dims))


def turn_kernel(scalars, numbers, left, right, some, grad, m, v, m_new, v_new, turned):
    slot = pl.program_id(0)
    factor, first_fix, second_fix = numbers[0], numbers[1], numbers[2]
    bases = two_parts(right[0])
    left_top, left_rest = two_parts(left[0])
    rotated = mm(left_top, grad[0], TN) + mm(left_rest, grad[0], TN)
    rotated = factor * mm3(two_parts(rotated), bases)
    moment, second, step = adam_moments(m[0], v[0], rotated, first_fix, second_fix)
    live = scalars[1 + slot] > 0
    m_new[0] = jnp.where(live, moment, m[0])
    v_new[0] = jnp.where(live, second, v[0])
    groups, _, rows, width = turned.shape
    rows_here = some[...].reshape(groups * rows, width)
    out = mm3(two_parts(rows_here), two_parts(step))
    out = mm3(two_parts(out), bases, NT)
    turned[...] = out.astype(turned.dtype).reshape(turned.shape)


def turn_slots(replica, live, numbers, left, right, grads, m, v):
    cap, width, _ = left.shape
    groups = width // 64
    scalars = jnp.concatenate([replica.reshape(1), live.astype(jnp.int32)])
    view = left.reshape(cap, groups, 4, 16, width)
    whole = pl.BlockSpec((1, width, width), lambda s, scalars: (s, 0, 0))
    grid_spec = pltpu.PrefetchScalarGridSpec(
        num_scalar_prefetch=1,
        grid=(cap,),
        in_specs=[
            pl.BlockSpec(memory_space=pltpu.SMEM),
            whole,
            whole,
            pl.BlockSpec((1, groups, 1, 16, width), lambda s, scalars: (s, 0, scalars[0], 0, 0)),
            whole,
            whole,
            whole,
        ],
        out_specs=[whole, whole, pl.BlockSpec((groups, 1, 16, width), lambda s, scalars: (0, s, 0, 0))],
    )
    return pl.pallas_call(
        turn_kernel,
        grid_spec=grid_spec,
        out_shape=[
            jax.ShapeDtypeStruct(m.shape, f32),
            jax.ShapeDtypeStruct(v.shape, f32),
            jax.ShapeDtypeStruct((groups, cap, 16, width), bf16),
        ],
        compiler_params=pltpu.CompilerParams(vmem_limit_bytes=56 << 20),
        name="turn_slots",
    )(scalars, numbers, left, right, view, grads, m, v)


def head_kernel(
    n_rep, n, vocab, tile, x_ref, e_ref, label_ref, picked_ref, table_ref, loss_ref,
    table, rows_all, logits, stats, shared, held, got,
    load_s, ring_s, ring_r, stat_s, stat_r, back_s, back_r,
):
    here = Place(n_rep, n)
    me = here.f
    others = [lax.rem(me + k, n) for k in range(1, n)]
    enter([(here.r, o) for o in others])
    picks, width = x_ref.shape
    half = picks // 2
    tiles = table.shape[0] // tile
    far = n // 2
    load = pltpu.make_async_copy(e_ref, table, load_s)
    load.start()
    sends = []
    waiting = {}

    def hop(way, s):
        origin = here.at(-s if way == 0 else s)
        window = pl.ds(way * half, half) if s == far - 1 else pl.ds(0, picks)
        src = x_ref if s == 0 else rows_all.at[origin, window]
        cp = remote(
            src,
            rows_all.at[origin, window],
            ring_s.at[way, s],
            ring_r.at[way, s],
            here.next if way == 0 else here.prev,
        )
        cp.start()
        sends.append(cp)
        waiting[way] = cp

    def columns(t, count):
        return t * tile + lax.broadcasted_iota(jnp.int32, (count, tile), 1)

    def span(t):
        return pl.ds(pl.multiple_of(t * tile, tile), tile)

    def stack(ref, origins):
        return jnp.concatenate([ref[o] for o in origins], axis=0)

    def scores_of(origins, t):
        return jnp.concatenate([logits[o, :, span(t)] for o in origins], axis=0)

    def piece(value, i):
        return value[i * picks : (i + 1) * picks]

    def fold(x, join):
        out = x[:, :128]
        for k in range(1, tile // 128):
            out = join(out, x[:, k * 128 : (k + 1) * 128])
        return out

    def forward(*origins):
        rows, label = stack(rows_all, origins), stack(label_ref, origins)
        count = rows.shape[0]

        def product(t, top):
            scores = mm(rows, table[span(t)], NT)
            scores = jnp.where(columns(t, count) < vocab, scores, masked_score)
            for i, o in enumerate(origins):
                logits[o, :, span(t)] = piece(scores, i)
            return jnp.maximum(top, fold(scores, jnp.maximum))

        top = lax.fori_loop(0, tiles, product, jnp.full((count, 128), masked_score, f32))
        top = jnp.max(top, axis=1, keepdims=True)

        def weigh(t, sums):
            total, target = sums
            scores = scores_of(origins, t)
            total = total + fold(jnp.exp(scores - top), jnp.add)
            hit = jnp.where(columns(t, count) == label, scores, 0.0)
            return total, target + fold(hit, jnp.add)

        zero = jnp.zeros((count, 128), f32)
        total, target = lax.fori_loop(0, tiles, weigh, (zero, zero))
        log_sum = top + jnp.log(jnp.sum(total, axis=1, keepdims=True))
        target = jnp.sum(target, axis=1, keepdims=True)
        lane = lax.broadcasted_iota(jnp.int32, (count, 128), 1)
        both = jnp.where(lane == 0, log_sum, target).T
        for i, o in enumerate(origins):
            stats[pl.ds(o, 1)] = both[0:1, i * picks : (i + 1) * picks]
            stats[pl.ds(n + o, 1)] = both[1:2, i * picks : (i + 1) * picks]

    rows_all[me] = x_ref[...]
    for way in range(2):
        hop(way, 0)
    load.wait()
    forward(me)
    for s in range(far):
        for way in range(2):
            waiting[way].wait_recv()
            if s < far - 1:
                hop(way, s + 1)
        if s < far - 1:
            forward(here.at(-s - 1), here.at(s + 1))
        else:
            forward(here.at(far))

    moves = []
    for k, o in enumerate(others):
        cp = remote(stats, shared.at[me], stat_s.at[k], stat_r.at[k], (here.r, o))
        cp.start()
        moves.append(cp)
    shared[me] = stats[...]
    table_ref[...] = jnp.zeros(table_ref.shape, f32)
    for cp in moves:
        cp.wait_recv()
    top = shared[0, :n]
    for k in range(1, n):
        top = jnp.maximum(top, shared[k, :n])
    total = jnp.exp(shared[0, :n] - top)
    target = shared[0, n:]
    for k in range(1, n):
        total = total + jnp.exp(shared[k, :n] - top)
        target = target + shared[k, n:]
    log_sum = top + jnp.log(total)
    for cp in moves:
        cp.wait_send()
    stats[:n] = log_sum
    stats[n:] = log_sum - target
    mine = stats[pl.ds(n + me, 1)]
    loss_ref[...] = jnp.broadcast_to(jnp.sum(mine, axis=1, keepdims=True), loss_ref.shape)

    def backward(*origins):
        rows, label = stack(rows_all, origins), stack(label_ref, origins)
        count = rows.shape[0]
        norm = [jnp.broadcast_to(stats[pl.ds(o, 1)], (128, picks)) for o in origins]
        norm = jnp.concatenate(norm, axis=1).T

        def product(t, out):
            scores = scores_of(origins, t)
            parts = [jnp.exp(scores[:, k * 128 : (k + 1) * 128] - norm) for k in range(tile // 128)]
            soft = jnp.concatenate(parts, axis=1)
            grad = (soft - jnp.where(columns(t, count) == label, 1.0, 0.0)).astype(bf16)
            table_ref[span(t)] += mm(grad, rows, TN)
            return out + mm(grad, table[span(t)])

        return lax.fori_loop(0, tiles, product, jnp.zeros((count, width), f32))

    ring = {}

    def lane_send(way, h, s, value):
        before = ring.get((way, h, s - 1))
        if before is not None:
            before.wait_recv()
            value = value + got[way, h, s - 1].astype(f32)
        held[way, h, s] = value.astype(bf16)
        cp = remote(
            held.at[way, h, s],
            got.at[way, h, s],
            back_s.at[way, h, s],
            back_r.at[way, h, s],
            here.next if way == 0 else here.prev,
        )
        cp.start()
        ring[way, h, s] = cp

    out = backward(here.at(far))
    lane_send(0, 0, 0, out[:half])
    lane_send(1, 1, 0, out[half:])
    for s in range(1, far):
        d = far - s
        out = backward(here.at(d), here.at(-d))
        for turn in range(2):
            for way in range(2):
                h = way if turn == 1 else 1 - way
                lane_send(way, h, s, piece(out, way)[h * half : (h + 1) * half])
    out = backward(me)
    for h in range(2):
        total = out[h * half : (h + 1) * half]
        for way in range(2):
            ring[way, h, far - 1].wait_recv()
            total = total + got[way, h, far - 1].astype(f32)
        picked_ref[pl.ds(h * half, half)] = total
    for cp in sends + list(ring.values()):
        cp.wait_send()


def head_step(mesh_sizes, cid, picked, table, labels, vocab):
    n_rep, n = mesh_sizes
    picks, width = picked.shape
    padded = table.shape[0]
    far = n // 2
    dma = pltpu.SemaphoreType.DMA
    return pl.pallas_call(
        partial(head_kernel, n_rep, n, vocab, 768),
        out_shape=[
            jax.ShapeDtypeStruct((picks, width), f32),
            jax.ShapeDtypeStruct((padded, width), f32),
            jax.ShapeDtypeStruct((8, 128), f32),
        ],
        in_specs=[VMEM, ANY, VMEM],
        out_specs=[VMEM, VMEM, VMEM],
        scratch_shapes=[
            pltpu.VMEM((padded, width), bf16),
            pltpu.VMEM((n, picks, width), bf16),
            pltpu.VMEM((n, picks, padded), f32),
            pltpu.VMEM((2 * n, picks), f32),
            pltpu.VMEM((n, 2 * n, picks), f32),
            pltpu.VMEM((2, 2, far, picks // 2, width), bf16),
            pltpu.VMEM((2, 2, far, picks // 2, width), bf16),
            dma,
            dma((2, far)),
            dma((2, far)),
            dma((n - 1,)),
            dma((n - 1,)),
            dma((2, 2, far)),
            dma((2, 2, far)),
        ],
        compiler_params=params(cid, 60 << 20),
        name="head_step",
    )(picked, table, labels.reshape(n, picks, 1))


class Transport:
    def __init__(self, n_rep, n_fsdp, shard_rows):
        self.sizes = (n_rep, n_fsdp)
        self.kernels = n_rep == 4 and n_fsdp == 8 and shard_rows == 64

    def open(self, cid, shard, table, wanted, facts, gains):
        if self.kernels:
            return open_step(self.sizes, cid, shard, table, wanted, facts, gains)
        asked = lax.all_to_all(wanted, "fsdp", split_axis=0, concat_axis=0, tiled=True)
        rows = jnp.take(table.astype(bf16), asked.reshape(-1), axis=0)
        rows = rows.reshape(wanted.shape[0], wanted.shape[2], table.shape[1])
        return (
            lax.all_gather(shard, "fsdp", axis=1, tiled=True),
            self.spread(cid, rows),
            asked,
            lax.all_gather(facts, "fsdp"),
            lax.all_gather(gains, "fsdp"),
            lax.pmax(facts, ("rep", "fsdp")),
        )

    def spread(self, cid, x):
        if self.kernels:
            return group_exchange(self.sizes, cid, x, True)
        return lax.all_to_all(x, "fsdp", split_axis=0, concat_axis=0, tiled=True)


def body(
    token_ids,
    segment_ids,
    masked_pos,
    labels,
    blocks,
    gains,
    embed,
    embed_m,
    embed_v,
    gains_m,
    gains_v,
    soap_m,
    soap_v,
    left_basis,
    right_basis,
    block_slots,
    step_count,
):
    groups = lax.axis_size("fsdp")
    replicas = lax.axis_size("rep")
    member = lax.axis_index("fsdp")
    replica = lax.axis_index("rep")
    micro_count = token_ids.shape[0]
    pack_length = token_ids.shape[2]
    pick_count = masked_pos.shape[2]
    vocab_rows, model_width = embed.shape
    block_count, shard_rows, _ = blocks.shape
    gain_count = gains.shape[0]
    tokens = micro_count * pack_length
    picks = micro_count * pick_count
    move = Transport(replicas, groups, shard_rows)
    padded_rows = -(-vocab_rows // 768) * 768
    table_low = jnp.pad(embed.astype(bf16), ((0, padded_rows - vocab_rows), (0, 0)))

    ids = token_ids.reshape(tokens)
    index = jnp.arange(tokens, dtype=jnp.int32)
    owner = ids // vocab_rows
    local = ids - owner * vocab_rows
    first_at = jnp.min(jnp.where(ids[:, None] == ids[None, :], index[None, :], tokens), axis=1)
    is_first = first_at == index
    ahead = is_first[None, :] & (owner[:, None] == owner[None, :]) & (index[None, :] < first_at[:, None])
    rank = jnp.sum(ahead.astype(jnp.int32), axis=1)
    most = jnp.max(rank) + 1

    my_labels = labels.reshape(picks // 128, 128)
    facts = jnp.concatenate(
        [my_labels, jnp.full((8 - picks // 128, 128), most, jnp.int32)], axis=0
    )
    gain_pad = jnp.pad(gains, ((0, 8 - gain_count), (0, 128 - gains.shape[1])))
    slots = groups * CAPACITY
    most_rounds = (tokens + CAPACITY - 1) // CAPACITY
    slot_index = jnp.arange(slots, dtype=jnp.int32)

    def slot_of(k):
        here = rank - k * CAPACITY
        return jnp.where((here >= 0) & (here < CAPACITY), owner * CAPACITY + here, -1)

    def wanted_in(slot):
        wanted = jnp.where((slot[None, :] == slot_index[:, None]) & is_first[None, :], local[None, :], 0)
        return jnp.sum(wanted, axis=1).reshape(groups, 1, CAPACITY)

    def placed(slot, rows):
        chosen = (slot[:, None] == slot_index[None, :]).astype(bf16)
        return jnp.dot(chosen, rows.reshape(slots, model_width), preferred_element_type=f32)

    slot = slot_of(0)
    full_blocks, rows, asked, group_facts, gain_rows, most_facts = move.open(
        0, blocks.astype(bf16), embed, wanted_in(slot), facts, gain_pad
    )
    rounds = (most_facts[7, 0] + CAPACITY - 1) // CAPACITY
    all_labels = group_facts[:, : picks // 128].reshape(groups * picks)
    gain_rows = gain_rows[:, :gain_count, : gains.shape[1]].transpose(1, 0, 2).reshape(gain_count, model_width)
    gain_rows = lax.reduce_precision(gain_rows, exponent_bits=8, mantissa_bits=7)
    embedded = placed(slot, rows)
    asked_all = jnp.zeros((most_rounds, slots), jnp.int32).at[0].set(asked.reshape(slots))

    def look(state):
        k, rows_so_far, asked_all = state
        slot = slot_of(k)
        asked = move.spread(1, wanted_in(slot))
        asked_all = lax.dynamic_update_index_in_dim(asked_all, asked.reshape(slots), k, 0)
        rows = jnp.take(table_low, asked.reshape(slots), axis=0).reshape(groups, CAPACITY, model_width)
        return k + 1, rows_so_far + placed(slot, move.spread(2, rows)), asked_all

    _, embedded, asked_all = lax.while_loop(lambda s: s[0] < rounds, look, (jnp.int32(1), embedded, asked_all))

    segments = segment_ids.reshape(micro_count, pack_length)
    stream, first_pull = jax.vjp(layer_norm, embedded, gain_rows[0])
    saved_layers = []
    for layer in range(LAYERS):
        middle, *attention_kept = attend(stream, gain_rows[1 + 2 * layer], full_blocks, layer, segments)
        after, *feed_kept = feed(middle, gain_rows[2 + 2 * layer], full_blocks, layer)
        saved_layers.append((stream, attention_kept, middle, feed_kept))
        stream = after
    final_rows, final_pull = jax.vjp(layer_norm, stream, gain_rows[gain_count - 1])

    positions = masked_pos.reshape(micro_count, pick_count)
    flat_positions = (positions + jnp.arange(micro_count, dtype=jnp.int32)[:, None] * pack_length).reshape(picks)
    picked = jnp.take(final_rows, flat_positions, axis=0).astype(bf16)
    label_local = all_labels - member * vocab_rows
    label_local = jnp.where((label_local >= 0) & (label_local < vocab_rows), label_local, -1)
    if move.kernels:
        grad_picked, grad_table, loss_local = head_step(
            move.sizes, 4, picked, table_low, label_local.reshape(groups, picks), vocab_rows
        )
        loss_local = loss_local[0, 0]
    else:
        all_picked = lax.all_gather(picked, "fsdp", tiled=True)
        logits = jnp.einsum("td,vd->tv", all_picked, table_low[:vocab_rows], preferred_element_type=f32)
        top_value = jnp.max(logits, axis=-1)
        exp_total = jnp.sum(jnp.exp(logits - top_value[:, None]), axis=-1)
        label_hits = jnp.arange(vocab_rows, dtype=jnp.int32)[None, :] == label_local[:, None]
        target = jnp.sum(jnp.where(label_hits, logits, 0.0), axis=-1)
        stats = lax.all_gather(jnp.stack([top_value, exp_total, target]), "fsdp")
        top_all = jnp.max(stats[:, 0], axis=0)
        total_all = jnp.sum(stats[:, 1] * jnp.exp(stats[:, 0] - top_all[None]), axis=0)
        target_all = jnp.sum(stats[:, 2], axis=0)
        entropy = top_all + jnp.log(total_all) - target_all
        loss_local = jnp.sum(lax.dynamic_slice_in_dim(entropy, member * picks, picks))
        grad_logits = (
            jnp.exp(logits - top_all[:, None]) / total_all[:, None] - label_hits.astype(f32)
        ).astype(bf16)
        grad_table = jnp.einsum("tv,td->vd", grad_logits, all_picked, preferred_element_type=f32)
        grad_table = jnp.pad(grad_table, ((0, padded_rows - vocab_rows), (0, 0)))
        grad_picked = jnp.einsum("tv,vd->td", grad_logits, table_low[:vocab_rows], preferred_element_type=f32)
        grad_picked = grad_picked.reshape(groups, picks, model_width)
        grad_picked = lax.psum_scatter(grad_picked, "fsdp", scatter_dimension=0)

    match = flat_positions[None, :] == index[:, None]
    place = jnp.sum(jnp.where(match, jnp.arange(picks, dtype=jnp.int32)[None, :] + 1, 0), axis=1)
    grad_final = jnp.where(
        (place > 0)[:, None], jnp.take(grad_picked, jnp.maximum(place - 1, 0), axis=0), 0.0
    )
    grad_stream, grad_final_gain = final_pull(grad_final)
    gain_grads = [None] * gain_count
    gain_grads[gain_count - 1] = grad_final_gain
    layer_grads = [None] * LAYERS
    for layer in reversed(range(LAYERS)):
        before, attention_kept, middle, feed_kept = saved_layers[layer]
        grad_stream, feed_gain, *grads_feed = feed_back(
            grad_stream, middle, gain_rows[2 + 2 * layer], full_blocks, layer, feed_kept
        )
        grad_stream, attention_gain, grads_attention = attend_back(
            grad_stream, before, gain_rows[1 + 2 * layer], full_blocks, layer, segments, attention_kept
        )
        gain_grads[1 + 2 * layer] = jnp.sum(attention_gain, axis=(0, 1))
        gain_grads[2 + 2 * layer] = jnp.sum(feed_gain, axis=0)
        layer_grads[layer] = [grads_attention] + grads_feed
    grad_embedded, gain_grads[0] = first_pull(grad_stream)
    grad_rows = grad_embedded.astype(bf16)
    row_index = jnp.arange(padded_rows, dtype=jnp.int32)

    def given(cid, k, grad_table):
        chosen = (slot_index[:, None] == slot_of(k)[None, :]).astype(bf16)
        rows = jnp.dot(chosen, grad_rows, preferred_element_type=f32).astype(bf16)
        rows = move.spread(cid, rows.reshape(groups, CAPACITY, model_width)).reshape(slots, model_width)
        asked = lax.dynamic_index_in_dim(asked_all, k, 0, keepdims=False)
        target_rows = (row_index[:, None] == asked[None, :]).astype(bf16)
        return grad_table + jnp.dot(target_rows, rows, preferred_element_type=f32)

    grad_table = given(7, 0, grad_table)
    _, grad_table = lax.while_loop(
        lambda s: s[0] < rounds, lambda s: (s[0] + 1, given(13, s[0], s[1])), (jnp.int32(1), grad_table)
    )
    grad_blocks = [g for grads in layer_grads for g in grads]
    grad_gains = jnp.stack(gain_grads, axis=0)

    position_count = micro_count * replicas * groups * pick_count
    clip_limit = clip_ratio * math.sqrt(position_count)
    steps_done = step_count[0].astype(f32)
    first_fix = 1.0 - beta_first**steps_done
    second_fix = 1.0 - beta_second**steps_done
    slot_cap = soap_m.shape[0]
    slot_total = slot_cap * groups
    named = jnp.arange(slot_total, dtype=jnp.int32)[:, None] == block_slots[None, :]
    taken = jnp.any(named, axis=1)
    block_of = jnp.sum(jnp.where(named, jnp.arange(block_count, dtype=jnp.int32)[None, :], 0), axis=1)

    small = jnp.zeros((8, model_width), f32).at[:gain_count].set(grad_gains)
    small = small.at[7, 0].set(loss_local)
    if move.kernels:
        owned, grad_table, small = settle_gradients(
            move.sizes,
            8,
            grad_blocks,
            grad_table.reshape(4, padded_rows // 4, model_width),
            small,
            block_of,
            taken.astype(jnp.int32),
            slot_cap,
        )
        grad_table = grad_table.reshape(padded_rows, model_width)[:vocab_rows]
        squares = jnp.sum(small[6])
        owned = owned.reshape(slot_cap, model_width, model_width)
    else:
        grad_blocks = jnp.concatenate([g.astype(f32) for g in grad_blocks], axis=0)
        mine = lax.psum_scatter(grad_blocks, "fsdp", scatter_dimension=1, tiled=True)
        mine, grad_table = lax.psum((mine, grad_table[:vocab_rows]), "rep")
        small = lax.psum(small, ("rep", "fsdp"))
        squares = lax.psum(jnp.sum(mine * mine) + jnp.sum(grad_table * grad_table), "fsdp")
        outgoing = jnp.where(taken[:, None, None], jnp.take(mine, block_of, axis=0), 0)
        owned = lax.all_to_all(outgoing, "fsdp", split_axis=0, concat_axis=1, tiled=True)
    loss_all = small[7, 0]
    grad_gains = small[:gain_count]
    grad_norm = jnp.sqrt(squares + jnp.sum(grad_gains * grad_gains))
    factor = jnp.minimum(1.0, clip_limit / grad_norm)
    grad_gains = lax.dynamic_slice_in_dim(grad_gains, member * gains.shape[1], gains.shape[1], axis=1)

    live = lax.dynamic_slice_in_dim(taken, member * slot_cap, slot_cap)
    if move.kernels:
        soap_m_new, soap_v_new, turned = turn_slots(
            replica,
            live,
            jnp.stack([factor, first_fix, second_fix]),
            left_basis,
            right_basis,
            owned,
            soap_m,
            soap_v,
        )
        returned = exchange_slots(move.sizes, 11, turned, False)
        returned = returned.reshape(slot_total, shard_rows, model_width)
    else:
        rotated = jnp.einsum("bji,bjk->bik", left_basis, owned, precision=high)
        rotated = factor * jnp.einsum("bik,bkl->bil", rotated, right_basis, precision=high)
        moment_first, moment_second, rotated_step = adam_moments(soap_m, soap_v, rotated, first_fix, second_fix)
        soap_m_new = jnp.where(live[:, None, None], moment_first, soap_m)
        soap_v_new = jnp.where(live[:, None, None], moment_second, soap_v)
        turned = jnp.einsum("bij,bjk->bik", left_basis, rotated_step, precision=high)
        turned = jnp.einsum("bik,blk->bil", turned, right_basis, precision=high)
        returned = lax.all_to_all(turned, "fsdp", split_axis=1, concat_axis=0, tiled=True)
    update = jnp.take(returned, block_slots, axis=0).astype(f32)
    blocks_new = blocks - step_rate * (update + weight_decay * blocks)

    embed_m_new, embed_v_new, table_step = adam_moments(
        embed_m, embed_v, factor * grad_table, first_fix, second_fix
    )
    embed_new = embed - step_rate * (table_step + weight_decay * embed)
    gains_m_new, gains_v_new, gain_step = adam_moments(
        gains_m, gains_v, factor * grad_gains, first_fix, second_fix
    )
    gains_new = gains - step_rate * gain_step
    loss = (loss_all / position_count).reshape(1)
    return (
        loss,
        grad_norm.reshape(1),
        blocks_new,
        gains_new,
        embed_new,
        embed_m_new,
        embed_v_new,
        gains_m_new,
        gains_v_new,
        soap_m_new,
        soap_v_new,
        blocks_new.astype(bf16),
        embed_new.astype(bf16),
    )


def solution(mesh):
    packs = P(None, ("rep", "fsdp"), None)
    rows = P(None, "fsdp", None)
    columns = P(None, "fsdp")
    table = P("fsdp", None)
    slots = P("fsdp", None, None)
    return jax.shard_map(
        body,
        mesh=mesh,
        in_specs=(packs,) * 4
        + (rows, columns)
        + (table,) * 3
        + (columns,) * 2
        + (slots,) * 4
        + (P(), P()),
        out_specs=(P(), P(), rows, columns)
        + (table,) * 3
        + (columns,) * 2
        + (slots,) * 2
        + (rows, table),
        check_vma=False,
    )
```

```python
from functools import partial
import math

import jax
import jax.numpy as jnp
from jax import lax
from jax.experimental import pallas as pl
from jax.experimental.pallas import tpu as pltpu
from jax.sharding import PartitionSpec as P

HEADS = 8
FF = 2048
LAYERS = 2

norm_epsilon = 1e-05
beta_first = 0.9
beta_second = 0.99
adam_epsilon = 1e-08
step_rate = 0.04
weight_decay = 0.1
clip_ratio = 12.0
masked_score = -1e30
bf16 = jnp.bfloat16
f32 = jnp.float32
highest = lax.Precision.HIGHEST
high = lax.Precision.HIGH
MESH = pl.DeviceIdType.MESH
ANY = pl.BlockSpec(memory_space=pl.ANY)
VMEM = pl.BlockSpec(memory_space=pltpu.VMEM)
CAPACITY = 128


def pick(table, index):
    out = jnp.int32(table[0])
    for k in range(1, len(table)):
        out = jnp.where(index == k, jnp.int32(table[k]), out)
    return out


def ring_order(n):
    nz = 4
    nx = n // nz
    order = []
    for x in range(nx):
        zs = range(1, nz) if x % 2 == 0 else range(nz - 1, 0, -1)
        order += [z * nx + x for z in zs]
    order += [x for x in range(nx - 1, -1, -1)]
    return order


class Place:
    def __init__(self, n_rep, n_fsdp):
        self.r = lax.axis_index("rep")
        self.f = lax.axis_index("fsdp")
        self.n_rep, self.n = n_rep, n_fsdp
        self.c = lax.rem(self.r, 2)
        self.y = self.r // 2
        self.order = ring_order(n_fsdp)
        spot = [self.order.index(k) for k in range(n_fsdp)]
        self.pos = pick(spot, self.f)
        self.core = (self.r + 1 - 2 * self.c, self.f)
        self.next = (self.r, self.at(1))
        self.prev = (self.r, self.at(-1))

    def at(self, step):
        return pick(self.order, lax.rem(self.pos + step + 2 * self.n, self.n))


def enter(peers):
    barrier = pltpu.get_barrier_semaphore()
    for peer in peers:
        pl.semaphore_signal(barrier, inc=1, device_id=peer, device_id_type=MESH)
    pl.semaphore_wait(barrier, len(peers))


def remote(src, dst, send, recv, peer):
    return pltpu.make_async_remote_copy(
        src_ref=src, dst_ref=dst, send_sem=send, recv_sem=recv, device_id=peer, device_id_type=MESH
    )


def params(cid, limit=None):
    return pltpu.CompilerParams(
        collective_id=cid, has_side_effects=True, vmem_limit_bytes=limit
    )


def group_kernel(n_rep, n, spread, x_ref, o_ref, send, recv):
    here = Place(n_rep, n)
    me = here.f
    others = [lax.rem(me + k, n) for k in range(1, n)]
    enter([(here.r, o) for o in others])
    copies = []
    for k, o in enumerate(others):
        src = x_ref.at[o] if spread else x_ref
        cp = remote(src, o_ref.at[me], send.at[k], recv.at[k], (here.r, o))
        cp.start()
        copies.append(cp)
    o_ref[me] = x_ref[me] if spread else x_ref[...]
    for cp in copies:
        cp.wait()


def group_exchange(mesh_sizes, cid, x, spread):
    n_rep, n = mesh_sizes
    shape = x.shape if spread else (n,) + x.shape
    return pl.pallas_call(
        partial(group_kernel, n_rep, n, spread),
        out_shape=jax.ShapeDtypeStruct(shape, x.dtype),
        in_specs=[VMEM],
        out_specs=VMEM,
        scratch_shapes=[pltpu.SemaphoreType.DMA((n - 1,)), pltpu.SemaphoreType.DMA((n - 1,))],
        compiler_params=params(cid),
        name=f"group_{cid}",
    )(x)


def distinct(here, n, capacity, ids_row, ids_col, own_row, own_col, local_col, rank_ref, first_ref, ask):
    tokens = ids_col.shape[0]
    step = 128
    lane = lax.broadcasted_iota(jnp.int32, (1, tokens), 1)

    def rows_at(t):
        return pl.ds(pl.multiple_of(t * step, step), step)

    def place(t, width):
        return t * step + lax.broadcasted_iota(jnp.int32, (step, width), 0)

    def earliest(t, first):
        same = ids_col[rows_at(t)] == ids_row[...]
        return jnp.minimum(first, jnp.min(jnp.where(same, place(t, tokens), tokens), axis=0, keepdims=True))

    first_row = lax.fori_loop(0, tokens // step, earliest, jnp.full((1, tokens), tokens, jnp.int32))
    member = jnp.where(first_row == lane, own_row[...], -1)

    def number(t, carry):
        wanted, most = carry
        at = rows_at(t)
        same = ids_col[at] == ids_row[...]
        first = jnp.min(jnp.where(same, lane, tokens), axis=1, keepdims=True)
        ahead = (member == own_col[at]) & (lane < first)
        rank = jnp.sum(jnp.where(ahead, 1, 0), axis=1, keepdims=True)
        rank_ref[at] = rank
        first_ref[at] = first
        slot = jnp.where((first == place(t, 1)) & (rank < capacity), own_col[at] * capacity + rank, -1)
        slots = lax.broadcasted_iota(jnp.int32, (1, n * capacity), 1)
        wanted = wanted + jnp.sum(jnp.where(slot == slots, local_col[at], 0), axis=0, keepdims=True)
        return wanted, jnp.maximum(most, jnp.max(rank, axis=0, keepdims=True))

    start = (jnp.zeros((1, n * capacity), jnp.int32), jnp.zeros((1, 1), jnp.int32))
    wanted, most = lax.fori_loop(0, tokens // step, number, start)
    for o in range(n):
        ask[o] = wanted[:, o * capacity : (o + 1) * capacity]
    return most + 1


def opening_kernel(
    n_rep, n, half, shared,
    x_ref, t_ref, ids_row, ids_col, own_row, own_col, local_col, facts_ref, gains_ref,
    o_ref, rows_ref, asked, facts, gains, most, rank_ref, first_ref, low_ref,
    table, low, index, ask, fact, stage, ready, held, got,
    t_s, ring_s, ring_r, core_s, core_r, y_s, y_r, over_s, over_r, ask_s, ask_r, top_s, top_r, rows_s, rows_r,
):
    here = Place(n_rep, n)
    me = here.f
    ypeer = (lax.rem(here.r + 2, 4), here.f)
    others = [lax.rem(me + k, n) for k in range(1, n)]
    rows = x_ref.shape[1]
    part = rows // 2
    alone = (half - shared) // 2
    enter([(here.r, o) for o in others] + [here.core, ypeer])
    vocab = t_ref.shape[0]
    load = pltpu.make_async_copy(t_ref, table.at[pl.ds(0, vocab)], t_s.at[0])
    load.start()
    table[vocab:] = jnp.zeros((table.shape[0] - vocab, table.shape[1]), table.dtype)

    mine = pl.ds(here.c * half + here.y * alone, alone + shared)
    given = pl.ds(here.c * half + here.y * (alone + shared), alone)
    taken = pl.ds(here.c * half + (1 - here.y) * (alone + shared), alone)
    hops = n // 2
    copies, sends = [], []

    def rows_of(origin, lane):
        return pl.ds(pl.multiple_of(origin * rows + lane * part, part), part)

    own = remote(
        x_ref, o_ref.at[:, pl.ds(pl.multiple_of(me * rows, rows), rows)], core_s.at[0, 0, 0], core_r.at[0, 0, 0], here.core
    )
    waiting = {}
    across = []

    def pass_on(way, s, lane):
        waiting[way, s, lane].wait_recv()
        where = rows_of(here.at(-s - 1 if way == 0 else s + 1), lane)
        kept = o_ref.at[given, where]
        cp = remote(kept, kept, y_s.at[way, s, lane], y_r.at[way, s, lane], ypeer)
        cp.start()
        across.append((cp, o_ref.at[taken, where], way, s, lane))
        kept = o_ref.at[mine, where]
        cp = remote(kept, kept, core_s.at[way, s + 1, lane], core_r.at[way, s + 1, lane], here.core)
        cp.start()
        copies.append(cp)

    def hop(way, s, lane):
        where = rows_of(here.at(-s if way == 0 else s), lane)
        src = x_ref.at[mine, pl.ds(lane * part, part)] if s == 0 else o_ref.at[mine, where]
        cp = remote(
            src,
            o_ref.at[mine, where],
            ring_s.at[way, s, lane],
            ring_r.at[way, s, lane],
            here.next if way == 0 else here.prev,
        )
        cp.start()
        waiting[way, s, lane] = cp
        sends.append(cp)

    for way in range(2):
        hop(way, 0, way)
    for way in range(2):
        hop(way, 0, 1 - way)
    own.start()
    copies.append(own)

    count = distinct(
        here, n, ask.shape[2], ids_row, ids_col, own_row, own_col, local_col, rank_ref, first_ref, ask
    )
    line = lax.broadcasted_iota(jnp.int32, fact.shape, 0)
    fact[...] = jnp.where(line == fact.shape[0] - 1, count, facts_ref[...])
    asks = []
    for k, o in enumerate(others):
        peer = (here.r, o)
        asks.append(remote(ask.at[o], asked.at[me], ask_s.at[0, k], ask_r.at[0, k], peer))
        asks.append(remote(fact, facts.at[me], ask_s.at[1, k], ask_r.at[1, k], peer))
        asks.append(remote(gains_ref, gains.at[me], ask_s.at[2, k], ask_r.at[2, k], peer))
    for cp in asks:
        cp.start()
    asked[me] = ask[me]
    facts[me] = fact[...]
    gains[me] = gains_ref[...]
    for cp in asks:
        cp.wait_recv()
    listed = pltpu.make_async_copy(asked, index, t_s.at[1])
    listed.start()
    top = facts[0]
    for k in range(1, n):
        top = jnp.maximum(top, facts[k])
    held[0] = top
    first = remote(held.at[0], got.at[0], top_s.at[0], top_r.at[0], here.core)
    first.start()
    listed.wait()
    load.wait()
    places = rows_ref.shape[1]

    def collect(o):
        def one(i, carry):
            stage[pl.ds(i, 1)] = table[pl.ds(index[o, 0, i], 1)]
            return carry

        lax.fori_loop(0, places, one, 0, unroll=8)
        return stage[...].astype(bf16)

    for k, o in enumerate(others):
        ready[o] = collect(o)
        cp = remote(ready.at[o], rows_ref.at[me], rows_s.at[k], rows_r.at[k], (here.r, o))
        cp.start()
        asks.append(cp)
    for way in range(2):
        pass_on(way, 0, way)
        hop(way, 1, way)
    for way in range(2):
        pass_on(way, 0, 1 - way)
        hop(way, 1, 1 - way)
    rows_ref[me] = collect(me)
    first.wait_recv()
    held[1] = jnp.maximum(top, got[0])
    second = remote(held.at[1], got.at[1], top_s.at[1], top_r.at[1], ypeer)
    second.start()

    step = 96

    @pl.loop(0, table.shape[0] // step)
    def _(i):
        at = pl.ds(pl.multiple_of(i * step, step), step)
        low[at] = table[at].astype(bf16)

    put = pltpu.make_async_copy(low, low_ref, t_s.at[0])
    put.start()

    for s in range(2, hops):
        for way in range(2):
            pass_on(way, s - 1, way)
            hop(way, s, way)
        for way in range(2):
            pass_on(way, s - 1, 1 - way)
            if s < hops - 1:
                hop(way, s, 1 - way)
    second.wait_recv()
    most[...] = jnp.maximum(held[1], got[1])
    for way in range(2):
        pass_on(way, hops - 1, way)
    for cp, kept, way, s, lane in across:
        cp.wait_recv()
        over = remote(kept, kept, over_s.at[way, s, lane], over_r.at[way, s, lane], here.core)
        over.start()
        copies.append(over)
        sends.append(cp)
    for cp in asks[3 * (n - 1) :]:
        cp.wait_recv()
    for cp in asks + [first, second] + sends:
        cp.wait_send()
    for cp in copies:
        cp.wait()
    put.wait()


def open_step(mesh_sizes, cid, shard, table, ids, owner, local, facts, gains, padded):
    n_rep, n = mesh_sizes
    count, rows, width = shard.shape
    tokens = ids.shape[0]
    half = count // 2
    hops = n // 2
    dma = pltpu.SemaphoreType.DMA
    wanted = (n, 1, CAPACITY)
    like = facts.shape
    i32 = jnp.int32
    return pl.pallas_call(
        partial(opening_kernel, n_rep, n, half, half - 2 * (half // 3)),
        out_shape=[
            jax.ShapeDtypeStruct((count, rows * n, width), shard.dtype),
            jax.ShapeDtypeStruct((n, CAPACITY, width), bf16),
            jax.ShapeDtypeStruct(wanted, i32),
            jax.ShapeDtypeStruct((n,) + like, i32),
            jax.ShapeDtypeStruct((n,) + gains.shape, gains.dtype),
            jax.ShapeDtypeStruct(like, i32),
            jax.ShapeDtypeStruct((tokens, 1), i32),
            jax.ShapeDtypeStruct((tokens, 1), i32),
            jax.ShapeDtypeStruct((padded, width), bf16),
        ],
        in_specs=[ANY, ANY] + [VMEM] * 7,
        out_specs=[ANY] + [VMEM] * 7 + [ANY],
        scratch_shapes=[
            pltpu.VMEM((padded, width), f32),
            pltpu.VMEM((padded, width), bf16),
            pltpu.SMEM(wanted, i32),
            pltpu.VMEM(wanted, i32),
            pltpu.VMEM(like, i32),
            pltpu.VMEM((CAPACITY, width), f32),
            pltpu.VMEM((n, CAPACITY, width), bf16),
            pltpu.VMEM((2,) + like, i32),
            pltpu.VMEM((2,) + like, i32),
            dma((2,)),
            dma((2, hops, 2)),
            dma((2, hops, 2)),
            dma((2, hops + 1, 2)),
            dma((2, hops + 1, 2)),
            dma((2, hops, 2)),
            dma((2, hops, 2)),
            dma((2, hops, 2)),
            dma((2, hops, 2)),
            dma((3, n - 1)),
            dma((3, n - 1)),
            dma((2,)),
            dma((2,)),
            dma((n - 1,)),
            dma((n - 1,)),
        ],
        compiler_params=params(cid, 60 << 20),
        name="open_step",
    )(
        shard,
        table,
        ids.reshape(1, tokens),
        ids.reshape(tokens, 1),
        owner.reshape(1, tokens),
        owner.reshape(tokens, 1),
        local.reshape(tokens, 1),
        facts,
        gains,
    )


def squares_row(square):
    row = jnp.sum(square, axis=0, keepdims=True)
    return jnp.where(lax.broadcasted_iota(jnp.int32, square.shape, 0) == 6, row, 0.0)


def reduce_kernel(
    n_rep, n, half, table_rows, each, *refs
):
    g_refs, refs = refs[: 2 * each], refs[2 * each :]
    (
    t_ref, small_ref, block_of, taken, o_ref, to_ref, sum_ref, mine, outgoing, held, hgot, four, fours, squares,
    own, part, got, fin, ysend, ygot, town, tpart, tsend, tgot,
    load_s, core_s, core_r, ring_s, ring_r, y_s, y_r, tload, tcs, tcr, tys, tyr, tos, tor,
    keep, a_s, a_r, f_s, f_r, sum_s, sum_r,
    ) = refs
    here = Place(n_rep, n)
    c, y = here.c, here.y
    ypeer = (lax.rem(here.r + 2, 4), here.f)
    other_c, other_y = 1 - c, 1 - y
    me = here.f
    others = [lax.rem(me + k, n) for k in range(1, n)]
    enter([(here.r, o) for o in others] + [here.core, ypeer])
    far = n // 2

    tl = pltpu.make_async_copy(t_ref.at[pl.ds(c * 2, 2)], town, tload)
    tl.start()
    tc = remote(t_ref.at[pl.ds(other_c * 2, 2)], tpart, tcs, tcr, here.core)
    tc.start()

    spots = {(0, far): 0, (1, far): 0}
    for d in range(far - 1, 0, -1):
        spots[0, d] = 1 + 2 * (far - 1 - d)
        spots[1, d] = 2 + 2 * (far - 1 - d)
    spots[0, 0] = spots[1, 0] = n - 1
    loads, cores = {}, {}
    done = set()
    for (way, d), spot in sorted(spots.items(), key=lambda item: item[1]):
        if spot in done:
            continue
        done.add(spot)
        to = here.f if d == 0 else here.at(d if way == 0 else -d)
        for h in (way, 1 - way):
            loads[spot, h], cores[spot, h] = [], []
            for j in range(each):
                g_ref = g_refs[h * each + j]
                into = pl.ds(j * (half // each), half // each)
                ld = pltpu.make_async_copy(g_ref.at[:, to, :, c], own.at[spot, h, into], load_s.at[spot, h, j])
                ld.start()
                loads[spot, h].append(ld)
                cp = remote(
                    g_ref.at[:, to, :, other_c],
                    part.at[spot, h, into],
                    core_s.at[spot, h, j],
                    core_r.at[spot, h, j],
                    here.core,
                )
                cp.start()
                cores[spot, h].append(cp)

    def ready(spot, h):
        for j in range(each):
            loads[spot, h][j].wait()
            cores[spot, h][j].wait_recv()

    ring = {}

    def came(way, h, s):
        return got.at[way, h, s]

    def lane(way, h, s):
        d = far - s
        spot = spots[way, d]
        ready(spot, h)
        before = ring.get((way, h, s - 1))
        if before is not None:
            before.wait_recv()
        target = own.at[spot, h]

        @pl.loop(0, half)
        def _(b):
            for k in range(2):
                total = own[spot, h, b, k].astype(f32) + part[spot, h, b, k].astype(f32)
                if before is not None:
                    total = total + came(way, h, s - 1)[b, k].astype(f32)
                target[b, k] = total.astype(target.dtype)

        cp = remote(
            target, came(way, h, s), ring_s.at[way, h, s], ring_r.at[way, h, s], here.next if way == 0 else here.prev
        )
        cp.start()
        ring[way, h, s] = cp

    step_rows = 48
    for s in range(far):
        for h_turn in range(2):
            for way in range(2):
                h = way if h_turn == 1 else 1 - way
                if s == far - 1:
                    h = h_turn
                if s == 0 and h_turn == 0:
                    continue
                if s == 1 and h_turn == 0:
                    continue
                lane(way, h, s)
        if s == 0:
            for way in range(2):
                lane(way, 1 - way, 1)
            tl.wait()
            tc.wait_recv()

            @pl.loop(0, table_rows // step_rows)
            def _(i):
                at = pl.ds(pl.multiple_of(i * step_rows, step_rows), step_rows)
                town[y, at] = town[y, at] + tpart[y, at]
                tsend[at] = (town[other_y, at] + tpart[other_y, at]).astype(bf16)

            ty = remote(tsend, tgot, tys, tyr, ypeer)
            ty.start()
        if s == 2:
            ty.wait_recv()

            def add(i, acc):
                at = pl.ds(pl.multiple_of(i * step_rows, step_rows), step_rows)
                total = town[y, at] + tgot[at].astype(f32)
                town[y, at] = total
                square = total * total
                for k in range(step_rows // 8):
                    acc = acc + square[k * 8 : k * 8 + 8]
                return acc

            squares[...] = lax.fori_loop(0, table_rows // step_rows, add, jnp.zeros((8, tgot.shape[1]), f32))
            quarter = c * 2 + y
            near = c * 2 + other_y
            tkeep = pltpu.make_async_copy(town.at[y], to_ref.at[quarter], tload)
            tkeep.start()
            t0 = remote(town.at[y], to_ref.at[quarter], tos.at[0], tor.at[0], ypeer)
            t1 = remote(town.at[y], to_ref.at[quarter], tos.at[1], tor.at[1], here.core)
            t0.start()
            t1.start()
    ys = []
    spot = spots[0, 0]
    for h in range(2):
        ready(spot, h)
        for way in range(2):
            ring[way, h, far - 1].wait_recv()

        @pl.loop(0, half)
        def _(b, h=h):
            for keep in range(2):
                k = y if keep else other_y
                total = own[spot, h, b, k].astype(f32) + part[spot, h, b, k].astype(f32)
                for way in range(2):
                    total = total + got[way, h, far - 1, b, k].astype(f32)
                if keep:
                    fin[h, b] = total
                else:
                    ysend[h, b] = total.astype(bf16)

        cp = remote(ysend.at[h], ygot.at[h], y_s.at[h], y_r.at[h], ypeer)
        cp.start()
        ys.append(cp)

    acc = jnp.zeros((8, fin.shape[-1]), f32)
    for h in range(2):
        ys[h].wait_recv()

        def last(b, acc, h=h):
            total = fin[h, b] + ygot[h, b].astype(f32)
            mine[h * half + b] = total.astype(bf16)
            square = total * total
            return acc + square[:8] + square[8:]

        acc = lax.fori_loop(0, half, last, acc)

    held[0] = small_ref[...] + squares_row(acc + squares[...])
    first = remote(held.at[0], hgot.at[0], sum_s.at[0], sum_r.at[0], here.core)
    first.start()

    cap = o_ref.shape[0]

    @pl.loop(0, n * cap)
    def _(k):
        value = mine[block_of[k]]
        outgoing[k] = jnp.where(taken[k] > 0, value, jnp.zeros_like(value))

    def spot_of(source, r):
        return o_ref.at[:, source, r]

    moves = []
    for k, o in enumerate(others):
        cp = remote(outgoing.at[pl.ds(o * cap, cap)], spot_of(me, here.r), a_s.at[k], a_r.at[k], (here.r, o))
        cp.start()
        moves.append(cp)
    kept = pltpu.make_async_copy(outgoing.at[pl.ds(me * cap, cap)], spot_of(me, here.r), keep)
    kept.start()
    first.wait_recv()
    held[1] = held[0] + hgot[0]
    second = remote(held.at[1], hgot.at[1], sum_s.at[1], sum_r.at[1], ypeer)
    second.start()
    t0.wait_recv()
    t2 = remote(to_ref.at[near], to_ref.at[near], tos.at[2], tor.at[2], here.core)
    t2.start()
    second.wait_recv()
    four[...] = held[1] + hgot[1]
    totals = []
    for k, o in enumerate(others):
        cp = remote(four, fours.at[me], sum_s.at[2 + k], sum_r.at[2 + k], (here.r, o))
        cp.start()
        totals.append(cp)
    fours[me] = four[...]
    beside, distant = [], []
    for k in range(n):
        source = me if k == 0 else lax.rem(me - k + n, n)
        if k == 0:
            kept.wait()
        else:
            moves[k - 1].wait_recv()
        piece = spot_of(source, here.r)
        over = remote(piece, piece, f_s.at[0, k], f_r.at[0, k], ypeer)
        over.start()
        cp = remote(piece, piece, f_s.at[1, k], f_r.at[1, k], here.core)
        cp.start()
        distant.append((over, source))
        beside.append(cp)
    for cp in totals:
        cp.wait_recv()
    total = fours[0]
    for k in range(1, n):
        total = total + fours[k]
    sum_ref[...] = total
    yr = lax.rem(here.r + 2, 4)
    for k, (over, source) in enumerate(distant):
        over.wait_recv()
        piece = spot_of(source, yr)
        cp = remote(piece, piece, f_s.at[2, k], f_r.at[2, k], here.core)
        cp.start()
        beside.append(cp)
    for cp in moves + totals + [first, second] + [over for over, _ in distant]:
        cp.wait_send()
    for cp in beside:
        cp.wait()
    for cp in ys:
        cp.wait_send()
    for cp in ring.values():
        cp.wait_send()
    for group in cores.values():
        for cp in group:
            cp.wait_send()
    tc.wait_send()
    ty.wait_send()
    tkeep.wait()
    t0.wait_send()
    t1.wait()
    t2.wait()


def settle_gradients(mesh_sizes, cid, grads, table, small, block_of, taken, cap):
    n_rep, n = mesh_sizes
    _, depth, width = grads[0].shape
    count = sum(g.shape[0] for g in grads)
    half = count // 2
    each = len(grads) // 2
    far = n // 2
    table_rows = table.shape[1]
    views = [g.reshape(g.shape[0], n, 2, 2, 16, width) for g in grads]
    dma = pltpu.SemaphoreType.DMA
    piece = (half, 2, 16, width)
    smem = pl.BlockSpec(memory_space=pltpu.SMEM)
    like = small.shape
    return pl.pallas_call(
        partial(reduce_kernel, n_rep, n, half, table_rows, each),
        out_shape=[
            jax.ShapeDtypeStruct((cap, n, 4, 16, width), bf16),
            jax.ShapeDtypeStruct(table.shape, f32),
            jax.ShapeDtypeStruct(like, f32),
        ],
        in_specs=[ANY] * (2 * each + 1) + [VMEM, smem, smem],
        out_specs=[ANY, ANY, VMEM],
        scratch_shapes=[
            pltpu.VMEM((count, 16, width), bf16),
            pltpu.VMEM((n * cap, 16, width), bf16),
            pltpu.VMEM((2,) + like, f32),
            pltpu.VMEM((2,) + like, f32),
            pltpu.VMEM(like, f32),
            pltpu.VMEM((n,) + like, f32),
            pltpu.VMEM(like, f32),
            pltpu.VMEM((n, 2) + piece, bf16),
            pltpu.VMEM((n, 2) + piece, bf16),
            pltpu.VMEM((2, 2, far) + piece, bf16),
            pltpu.VMEM((2, half, 16, width), f32),
            pltpu.VMEM((2, half, 16, width), bf16),
            pltpu.VMEM((2, half, 16, width), bf16),
            pltpu.VMEM((2, table_rows, width), f32),
            pltpu.VMEM((2, table_rows, width), f32),
            pltpu.VMEM((table_rows, width), bf16),
            pltpu.VMEM((table_rows, width), bf16),
            dma((n, 2, each)),
            dma((n, 2, each)),
            dma((n, 2, each)),
            dma((2, 2, far)),
            dma((2, 2, far)),
            dma((2,)),
            dma((2,)),
            dma,
            dma,
            dma,
            dma,
            dma,
            dma((3,)),
            dma((3,)),
            dma,
            dma((n - 1,)),
            dma((n - 1,)),
            dma((3, n)),
            dma((3, n)),
            dma((n + 1,)),
            dma((n + 1,)),
        ],
        compiler_params=params(cid, 56 << 20),
        name="settle_gradients",
    )(*views, table, small, block_of, taken)


def slots_kernel(n_rep, n, to_slots, x_ref, o_ref, keep, a_s, a_r, f_s, f_r):
    here = Place(n_rep, n)
    ypeer = (lax.rem(here.r + 2, 4), here.f)
    me = here.f
    others = [lax.rem(me + k, n) for k in range(1, n)]
    enter([(here.r, o) for o in others] + [here.core, ypeer])

    def spot(source, r):
        return o_ref.at[:, source, r] if to_slots else o_ref.at[source, :, r]

    copies = []
    for k, o in enumerate(others):
        cp = remote(x_ref.at[o], spot(me, here.r), a_s.at[k], a_r.at[k], (here.r, o))
        cp.start()
        copies.append(cp)
    own = pltpu.make_async_copy(x_ref.at[me], spot(me, here.r), keep)
    own.start()
    sends, far = [], []
    for k in range(n):
        source = me if k == 0 else lax.rem(me - k + n, n)
        if k == 0:
            own.wait()
        else:
            copies[k - 1].wait_recv()
        held = spot(source, here.r)
        over = remote(held, held, f_s.at[0, k], f_r.at[0, k], ypeer)
        over.start()
        beside = remote(held, held, f_s.at[1, k], f_r.at[1, k], here.core)
        beside.start()
        far.append((over, source))
        sends.append(beside)
    yr = lax.rem(here.r + 2, 4)
    for k, (over, source) in enumerate(far):
        over.wait_recv()
        src = me if k == 0 else lax.rem(me - k + n, n)
        held = spot(src, yr)
        beside = remote(held, held, f_s.at[2, k], f_r.at[2, k], here.core)
        beside.start()
        sends.append(beside)
    for cp in copies:
        cp.wait_send()
    for over, _ in far:
        over.wait_send()
    for cp in sends:
        cp.wait()


def exchange_slots(mesh_sizes, cid, x, to_slots):
    n_rep, n = mesh_sizes
    _, cap, rows, width = x.shape
    shape = (cap, n, 4, rows, width) if to_slots else (n, cap, 4, rows, width)
    dma = pltpu.SemaphoreType.DMA
    return pl.pallas_call(
        partial(slots_kernel, n_rep, n, to_slots),
        out_shape=jax.ShapeDtypeStruct(shape, x.dtype),
        in_specs=[VMEM],
        out_specs=ANY,
        scratch_shapes=[dma, dma((n - 1,)), dma((n - 1,)), dma((3, n)), dma((3, n))],
        compiler_params=params(cid),
        name=f"slots_{cid}",
    )(x)


def layer_norm(inputs, gain_row):
    centre = inputs - jnp.mean(inputs, axis=-1, keepdims=True)
    spread = jnp.mean(centre * centre, axis=-1, keepdims=True)
    return centre * lax.rsqrt(spread + norm_epsilon) * gain_row


def adam_moments(moment_old, second_old, gradient, first_fix, second_fix):
    moment_new = beta_first * moment_old + (1.0 - beta_first) * gradient
    second_new = beta_second * second_old + (1.0 - beta_second) * gradient * gradient
    step_value = moment_new / first_fix / (jnp.sqrt(second_new / second_fix) + adam_epsilon)
    return (moment_new, second_new, step_value)


def head_slopes(head_count):
    return 2.0 ** (-8.0 * (jnp.arange(head_count, dtype=f32) + 1.0) / head_count)


NT = (((1,), (1,)), ((), ()))
TN = (((0,), (0,)), ((), ()))
masked_distance = 1e33


def mm(a, b, dims=None):
    if dims is None:
        return jnp.dot(a, b, preferred_element_type=f32)
    return lax.dot_general(a, b, dims, preferred_element_type=f32)


def norm_parts(x):
    centre = x - jnp.mean(x, axis=-1, keepdims=True)
    spread = jnp.mean(centre * centre, axis=-1, keepdims=True)
    rstd = lax.rsqrt(spread + norm_epsilon)
    return centre * rstd, rstd


def norm_back(x, gain, grad):
    hat, rstd = norm_parts(x)
    inner = grad * gain
    back = inner - jnp.mean(inner, axis=-1, keepdims=True) - hat * jnp.mean(inner * hat, axis=-1, keepdims=True)
    return rstd * back, grad * hat


def fold8(x):
    total = x[:8]
    for k in range(1, x.shape[0] // 8):
        total = total + x[k * 8 : k * 8 + 8]
    return total


def pair_bias(seg_row, seg_col, bias):
    length = bias.shape[0]
    i = lax.broadcasted_iota(jnp.int32, (length, length), 0)
    j = lax.broadcasted_iota(jnp.int32, (length, length), 1)
    apart = jnp.abs(i - j).astype(f32)
    bias[...] = jnp.where(seg_col == seg_row, apart, masked_distance)


def attend_kernel(slopes, x, gain, w, seg_row, seg_col, y, a, qkv, o, lse, bias):
    pair = pl.program_id(1)
    length, width = x.shape
    half = width // HEADS
    two = 2 * half
    rows = ROWS

    @pl.when(pair == 0)
    def _():
        pair_bias(seg_row[0], seg_col[0], bias)

        @pl.loop(0, length // rows)
        def _(i):
            at = pl.ds(pl.multiple_of(i * rows, rows), rows)
            hat, _ = norm_parts(x[at])
            low = (hat * gain[...]).astype(bf16)
            a[at] = low
            for k in range(3):
                part = mm(low, w[k])
                if k == 0:
                    part = part.astype(bf16).astype(f32) * half ** (-0.5)
                qkv[at, k * width : (k + 1) * width] = part.astype(bf16)

    lanes = pl.ds(pl.multiple_of(pair * two, two), two)
    q = qkv[:, pl.ds(pl.multiple_of(pair * two, two), two)]
    k = qkv[:, pl.ds(pl.multiple_of(width + pair * two, two), two)]
    v = qkv[:, pl.ds(pl.multiple_of(2 * width + pair * two, two), two)]
    v_t = v.astype(f32).T.astype(bf16)
    left = lax.broadcasted_iota(jnp.int32, (length, two), 1) < half
    zero = jnp.zeros_like(q)
    out = []
    for e in range(2):
        slope = slopes[2 * pair + e]
        q_e = jnp.where(left, q, zero) if e == 0 else jnp.where(left, zero, q)
        s = mm(k, q_e, NT) - slope * bias[...]
        top = jnp.max(s, axis=0, keepdims=True)
        p = jnp.exp(s - top)
        total = jnp.sum(p, axis=0, keepdims=True)
        low = (p * (1.0 / total)).astype(bf16)
        out.append(mm(v_t, low))
        lse[0, pl.ds(2 * pair + e, 1)] = top + jnp.log(total)
    upper = lax.broadcasted_iota(jnp.int32, (two, length), 0) < half
    o[:, lanes] = jnp.where(upper, out[0], out[1]).T.astype(bf16)

    @pl.when(pair == pl.num_programs(1) - 1)
    def _():
        @pl.loop(0, length // rows)
        def _(i):
            at = pl.ds(pl.multiple_of(i * rows, rows), rows)
            y[at] = x[at] + mm(o[at], w[3])


def attend(x, gain, weights, layer, seg):
    packs, length = seg.shape
    tokens, width = x.shape
    per_layer4 = weights.shape[0] // LAYERS // 4
    slopes = head_slopes(HEADS)
    whole = lambda shape: pl.BlockSpec(shape, lambda m, p: (m,) + (0,) * (len(shape) - 1))
    fixed = lambda shape, at: pl.BlockSpec(shape, lambda m, p: at)
    return pl.pallas_call(
        attend_kernel,
        grid=(packs, HEADS // 2),
        in_specs=[
            pl.BlockSpec(memory_space=pltpu.SMEM),
            whole((length, width)),
            fixed((1, width), (0, 0)),
            fixed((4, width, width), (per_layer4 * layer, 0, 0)),
            whole((1, 1, length)),
            whole((1, length, 1)),
        ],
        out_specs=[
            whole((length, width)),
            whole((length, width)),
            whole((length, 3 * width)),
            whole((length, width)),
            whole((1, HEADS, length)),
        ],
        out_shape=[
            jax.ShapeDtypeStruct((tokens, width), f32),
            jax.ShapeDtypeStruct((tokens, width), bf16),
            jax.ShapeDtypeStruct((tokens, 3 * width), bf16),
            jax.ShapeDtypeStruct((tokens, width), bf16),
            jax.ShapeDtypeStruct((packs, HEADS, length), f32),
        ],
        scratch_shapes=[pltpu.VMEM((length, length), f32)],
        compiler_params=pltpu.CompilerParams(vmem_limit_bytes=48 << 20),
        name="attend",
    )(slopes, x, gain.reshape(1, width), weights, seg.reshape(packs, 1, length), seg.reshape(packs, length, 1))


def attend_back_kernel(
    slopes, dx, x, gain, w, a, qkv, o, lse, seg_row, seg_col, new, dgain, gw, bias, do, dqkv, acc
):
    pack, pair = pl.program_id(0), pl.program_id(1)
    length, width = x.shape
    half = width // HEADS
    two = 2 * half
    rows = ROWS

    @pl.when(pair == 0)
    def _():
        pair_bias(seg_row[0], seg_col[0], bias)

        @pl.loop(0, length // rows)
        def _(i):
            at = pl.ds(pl.multiple_of(i * rows, rows), rows)
            do[at] = mm(dx[at].astype(bf16), w[3], NT).astype(bf16)

        part = mm(o[...], dx[...].astype(bf16), TN)

        @pl.when(pack == 0)
        def _():
            acc[3] = part

        @pl.when(pack > 0)
        def _():
            acc[3] += part

    lanes = [pl.ds(pl.multiple_of(n * width + pair * two, two), two) for n in range(3)]
    q, k, v = [qkv[:, at] for at in lanes]
    do_p = do[:, lanes[0]]
    k_t = k.astype(f32).T.astype(bf16)
    left = lax.broadcasted_iota(jnp.int32, (length, two), 1) < half
    upper = lax.broadcasted_iota(jnp.int32, (two, length), 0) < half
    zero = jnp.zeros_like(q)
    dq, dk, dv = [], [], []
    for e in range(2):
        slope = slopes[2 * pair + e]
        keep = (lambda t: jnp.where(left, t, zero)) if e == 0 else (lambda t: jnp.where(left, zero, t))
        s = mm(k, keep(q), NT) - slope * bias[...]
        p = jnp.exp(s - lse[0, pl.ds(2 * pair + e, 1)])
        dp = mm(v, keep(do_p), NT)
        inner = jnp.sum(p * dp, axis=0, keepdims=True)
        ds = (p * (dp - inner)).astype(bf16)
        dv.append(mm(p.astype(bf16), do_p))
        dk.append(mm(ds, q))
        dq.append(mm(k_t, ds))
    dqkv[:, lanes[0]] = (jnp.where(upper, dq[0], dq[1]).T * half ** (-0.5)).astype(bf16)
    dqkv[:, lanes[1]] = jnp.where(left, dk[0], dk[1]).astype(bf16)
    dqkv[:, lanes[2]] = jnp.where(left, dv[0], dv[1]).astype(bf16)

    @pl.when(pair == pl.num_programs(1) - 1)
    def _():
        def chunk(i, total):
            at = pl.ds(pl.multiple_of(i * rows, rows), rows)
            da = mm(dqkv[at, :width], w[0], NT)
            da = da + mm(dqkv[at, width : 2 * width], w[1], NT)
            da = da + mm(dqkv[at, 2 * width :], w[2], NT)
            back, extra = norm_back(x[at], gain[...], da)
            new[at] = dx[at] + back
            return total + fold8(extra)

        dgain[0] = lax.fori_loop(0, length // rows, chunk, jnp.zeros((8, width), f32))
        for n in range(3):
            part = mm(a[...], dqkv[:, n * width : (n + 1) * width], TN)

            @pl.when(pack == 0)
            def _(part=part, n=n):
                acc[n] = part

            @pl.when(pack > 0)
            def _(part=part, n=n):
                acc[n] += part

    @pl.when((pair == pl.num_programs(1) - 1) & (pack == pl.num_programs(0) - 1))
    def _():
        for n in range(4):
            gw[n] = acc[n].astype(bf16)


def attend_back(dx, x, gain, weights, layer, seg, kept):
    a, qkv, o, lse = kept
    packs, length = seg.shape
    tokens, width = x.shape
    per_layer4 = weights.shape[0] // LAYERS // 4
    whole = lambda shape: pl.BlockSpec(shape, lambda m, p: (m,) + (0,) * (len(shape) - 1))
    fixed = lambda shape, at: pl.BlockSpec(shape, lambda m, p: at)
    return pl.pallas_call(
        attend_back_kernel,
        grid=(packs, HEADS // 2),
        in_specs=[
            pl.BlockSpec(memory_space=pltpu.SMEM),
            whole((length, width)),
            whole((length, width)),
            fixed((1, width), (0, 0)),
            fixed((4, width, width), (per_layer4 * layer, 0, 0)),
            whole((length, width)),
            whole((length, 3 * width)),
            whole((length, width)),
            whole((1, HEADS, length)),
            whole((1, 1, length)),
            whole((1, length, 1)),
        ],
        out_specs=[
            whole((length, width)),
            whole((1, 8, width)),
            fixed((4, width, width), (0, 0, 0)),
        ],
        out_shape=[
            jax.ShapeDtypeStruct((tokens, width), f32),
            jax.ShapeDtypeStruct((packs, 8, width), f32),
            jax.ShapeDtypeStruct((4, width, width), bf16),
        ],
        scratch_shapes=[
            pltpu.VMEM((length, length), f32),
            pltpu.VMEM((length, width), bf16),
            pltpu.VMEM((length, 3 * width), bf16),
            pltpu.VMEM((4, width, width), f32),
        ],
        compiler_params=pltpu.CompilerParams(vmem_limit_bytes=56 << 20),
        name="attend_back",
    )(
        head_slopes(HEADS),
        dx,
        x,
        gain.reshape(1, width),
        weights,
        a,
        qkv,
        o,
        lse,
        seg.reshape(packs, 1, length),
        seg.reshape(packs, length, 1),
    )


ROWS = 512
gelu_c = math.sqrt(2.0 / math.pi)


def feed_kernel(x, gain, wg, wu, wd, y, f, gate, up):
    k = pl.program_id(0)
    tokens = x.shape[0]
    rows = ROWS

    @pl.loop(0, tokens // rows)
    def _(i):
        at = pl.ds(pl.multiple_of(i * rows, rows), rows)

        @pl.when(k == 0)
        def _():
            hat, _ = norm_parts(x[at])
            f[at] = (hat * gain[...]).astype(bf16)
            y[at] = x[at]

        low = f[at]
        g = mm(low, wg[0]).astype(bf16)
        u = mm(low, wu[0]).astype(bf16)
        gate[0, at] = g
        up[0, at] = u
        g, u = g.astype(f32), u.astype(f32)
        cdf = 0.5 * (1.0 + jnp.tanh(gelu_c * (g + 0.044715 * (g * g * g))))
        hidden = (g * cdf * u).astype(bf16)
        y[at] += mm(hidden, wd[0])


def feed(x, gain, weights, layer):
    tokens, width = x.shape
    per_layer = weights.shape[0] // LAYERS
    pieces = FF // width
    fixed = lambda shape: pl.BlockSpec(shape, lambda k: (0,) * len(shape))
    block = lambda skip: pl.BlockSpec((1, width, width), lambda k: (per_layer * layer + skip + k, 0, 0))
    each = pl.BlockSpec((1, tokens, width), lambda k: (k, 0, 0))
    return pl.pallas_call(
        feed_kernel,
        grid=(pieces,),
        in_specs=[fixed((tokens, width)), fixed((1, width)), block(4), block(4 + pieces), block(4 + 2 * pieces)],
        out_specs=[fixed((tokens, width)), fixed((tokens, width)), each, each],
        out_shape=[
            jax.ShapeDtypeStruct((tokens, width), f32),
            jax.ShapeDtypeStruct((tokens, width), bf16),
            jax.ShapeDtypeStruct((pieces, tokens, width), bf16),
            jax.ShapeDtypeStruct((pieces, tokens, width), bf16),
        ],
        compiler_params=pltpu.CompilerParams(vmem_limit_bytes=48 << 20),
        name="feed",
    )(x, gain.reshape(1, width), weights, weights, weights)


def feed_back_kernel(dx, x, gain, wg, wu, wd, f, gate, up, new, dgain, gg, gu, gd, f_t, dz, hid, dg, du):
    k = pl.program_id(0)
    tokens, width = x.shape
    rows = ROWS
    last = pl.num_programs(0) - 1

    @pl.when(k == 0)
    def _():
        @pl.loop(0, tokens // rows)
        def _(i):
            at = pl.ds(pl.multiple_of(i * rows, rows), rows)
            f_t[:, at] = f[at].astype(f32).T.astype(bf16)
            dz[at] = dx[at].astype(bf16)
            new[at] = jnp.zeros((rows, width), f32)

    def chunk(i, total):
        at = pl.ds(pl.multiple_of(i * rows, rows), rows)
        dh = mm(dz[at], wd[0], NT)
        g, u = gate[0, at].astype(f32), up[0, at].astype(f32)
        square = g * g
        t = jnp.tanh(gelu_c * (g + 0.044715 * (square * g)))
        cdf = 0.5 * (1.0 + t)
        act = g * cdf
        slope = cdf + 0.5 * g * (1.0 - t * t) * (gelu_c * (1.0 + 3 * 0.044715 * square))
        hid[at] = (act * u).astype(bf16)
        dgate = (dh * u * slope).astype(bf16)
        dup = (dh * act).astype(bf16)
        dg[at] = dgate
        du[at] = dup
        new[at] += mm(dgate, wg[0], NT) + mm(dup, wu[0], NT)
        return total

    lax.fori_loop(0, tokens // rows, chunk, 0)
    gg[0] = mm(f_t[...], dg[...]).astype(bf16)
    gu[0] = mm(f_t[...], du[...]).astype(bf16)
    gd[0] = mm(hid[...], dz[...], TN).astype(bf16)

    @pl.when(k == last)
    def _():
        def finish(i, total):
            at = pl.ds(pl.multiple_of(i * rows, rows), rows)
            back, extra = norm_back(x[at], gain[...], new[at])
            new[at] = dx[at] + back
            return total + fold8(extra)

        dgain[...] = lax.fori_loop(0, tokens // rows, finish, jnp.zeros((8, width), f32))


def feed_back(dx, x, gain, weights, layer, kept):
    f, gate, up = kept
    tokens, width = x.shape
    per_layer = weights.shape[0] // LAYERS
    pieces = FF // width
    fixed = lambda shape: pl.BlockSpec(shape, lambda k: (0,) * len(shape))
    block = lambda skip: pl.BlockSpec((1, width, width), lambda k: (per_layer * layer + skip + k, 0, 0))
    each = pl.BlockSpec((1, tokens, width), lambda k: (k, 0, 0))
    grad = pl.BlockSpec((1, width, width), lambda k: (k, 0, 0))
    return pl.pallas_call(
        feed_back_kernel,
        grid=(pieces,),
        in_specs=[
            fixed((tokens, width)),
            fixed((tokens, width)),
            fixed((1, width)),
            block(4),
            block(4 + pieces),
            block(4 + 2 * pieces),
            fixed((tokens, width)),
            each,
            each,
        ],
        out_specs=[fixed((tokens, width)), fixed((8, width)), grad, grad, grad],
        out_shape=[
            jax.ShapeDtypeStruct((tokens, width), f32),
            jax.ShapeDtypeStruct((8, width), f32),
        ]
        + [jax.ShapeDtypeStruct((pieces, width, width), bf16)] * 3,
        scratch_shapes=[
            pltpu.VMEM((width, tokens), bf16),
            pltpu.VMEM((tokens, width), bf16),
            pltpu.VMEM((tokens, width), bf16),
            pltpu.VMEM((tokens, width), bf16),
            pltpu.VMEM((tokens, width), bf16),
        ],
        compiler_params=pltpu.CompilerParams(vmem_limit_bytes=56 << 20),
        name="feed_back",
    )(dx, x, gain.reshape(1, width), weights, weights, weights, f, gate, up)


def two_parts(x):
    top = x.astype(bf16)
    return top, (x - top.astype(f32)).astype(bf16)


def mm3(a, b, dims=None):
    (a1, a2), (b1, b2) = a, b
    return mm(a1, b1, dims) + (mm(a1, b2, dims) + mm(a2, b1, dims))


def turn_kernel(scalars, numbers, left, right, some, grad, m, v, m_new, v_new, turned):
    slot = pl.program_id(0)
    factor, first_fix, second_fix = numbers[0], numbers[1], numbers[2]
    bases = two_parts(right[0])
    left_top, left_rest = two_parts(left[0])
    rotated = mm(left_top, grad[0], TN) + mm(left_rest, grad[0], TN)
    rotated = factor * mm3(two_parts(rotated), bases)
    moment, second, step = adam_moments(m[0], v[0], rotated, first_fix, second_fix)
    live = scalars[1 + slot] > 0
    m_new[0] = jnp.where(live, moment, m[0])
    v_new[0] = jnp.where(live, second, v[0])
    groups, _, rows, width = turned.shape
    rows_here = some[...].reshape(groups * rows, width)
    out = mm3(two_parts(rows_here), two_parts(step))
    out = mm3(two_parts(out), bases, NT)
    turned[...] = out.astype(turned.dtype).reshape(turned.shape)


def turn_slots(replica, live, numbers, left, right, grads, m, v):
    cap, width, _ = left.shape
    groups = width // 64
    scalars = jnp.concatenate([replica.reshape(1), live.astype(jnp.int32)])
    view = left.reshape(cap, groups, 4, 16, width)
    whole = pl.BlockSpec((1, width, width), lambda s, scalars: (s, 0, 0))
    grid_spec = pltpu.PrefetchScalarGridSpec(
        num_scalar_prefetch=1,
        grid=(cap,),
        in_specs=[
            pl.BlockSpec(memory_space=pltpu.SMEM),
            whole,
            whole,
            pl.BlockSpec((1, groups, 1, 16, width), lambda s, scalars: (s, 0, scalars[0], 0, 0)),
            whole,
            whole,
            whole,
        ],
        out_specs=[whole, whole, pl.BlockSpec((groups, 1, 16, width), lambda s, scalars: (0, s, 0, 0))],
    )
    return pl.pallas_call(
        turn_kernel,
        grid_spec=grid_spec,
        out_shape=[
            jax.ShapeDtypeStruct(m.shape, f32),
            jax.ShapeDtypeStruct(v.shape, f32),
            jax.ShapeDtypeStruct((groups, cap, 16, width), bf16),
        ],
        compiler_params=pltpu.CompilerParams(vmem_limit_bytes=56 << 20),
        name="turn_slots",
    )(scalars, numbers, left, right, view, grads, m, v)


def head_kernel(
    n_rep, n, vocab, tile, x_ref, e_ref, label_ref, picked_ref, table_ref, loss_ref,
    table, rows_all, logits, stats, shared, held, got,
    load_s, ring_s, ring_r, stat_s, stat_r, back_s, back_r,
):
    here = Place(n_rep, n)
    me = here.f
    others = [lax.rem(me + k, n) for k in range(1, n)]
    enter([(here.r, o) for o in others])
    picks, width = x_ref.shape
    half = picks // 2
    tiles = table.shape[0] // tile
    far = n // 2
    load = pltpu.make_async_copy(e_ref, table, load_s)
    load.start()
    sends = []
    waiting = {}

    def hop(way, s):
        origin = here.at(-s if way == 0 else s)
        window = pl.ds(way * half, half) if s == far - 1 else pl.ds(0, picks)
        src = x_ref if s == 0 else rows_all.at[origin, window]
        cp = remote(
            src,
            rows_all.at[origin, window],
            ring_s.at[way, s],
            ring_r.at[way, s],
            here.next if way == 0 else here.prev,
        )
        cp.start()
        sends.append(cp)
        waiting[way] = cp

    def columns(t, count):
        return t * tile + lax.broadcasted_iota(jnp.int32, (count, tile), 1)

    def span(t):
        return pl.ds(pl.multiple_of(t * tile, tile), tile)

    def stack(ref, origins):
        return jnp.concatenate([ref[o] for o in origins], axis=0)

    def scores_of(origins, t):
        return jnp.concatenate([logits[o, :, span(t)] for o in origins], axis=0)

    def piece(value, i):
        return value[i * picks : (i + 1) * picks]

    def fold(x, join):
        out = x[:, :128]
        for k in range(1, tile // 128):
            out = join(out, x[:, k * 128 : (k + 1) * 128])
        return out

    def forward(*origins):
        rows, label = stack(rows_all, origins), stack(label_ref, origins)
        count = rows.shape[0]

        def product(t, top):
            scores = mm(rows, table[span(t)], NT)
            scores = jnp.where(columns(t, count) < vocab, scores, masked_score)
            for i, o in enumerate(origins):
                logits[o, :, span(t)] = piece(scores, i)
            return jnp.maximum(top, fold(scores, jnp.maximum))

        top = lax.fori_loop(0, tiles, product, jnp.full((count, 128), masked_score, f32))
        top = jnp.max(top, axis=1, keepdims=True)

        def weigh(t, sums):
            total, target = sums
            scores = scores_of(origins, t)
            total = total + fold(jnp.exp(scores - top), jnp.add)
            hit = jnp.where(columns(t, count) == label, scores, 0.0)
            return total, target + fold(hit, jnp.add)

        zero = jnp.zeros((count, 128), f32)
        total, target = lax.fori_loop(0, tiles, weigh, (zero, zero))
        log_sum = top + jnp.log(jnp.sum(total, axis=1, keepdims=True))
        target = jnp.sum(target, axis=1, keepdims=True)
        lane = lax.broadcasted_iota(jnp.int32, (count, 128), 1)
        both = jnp.where(lane == 0, log_sum, target).T
        for i, o in enumerate(origins):
            stats[pl.ds(o, 1)] = both[0:1, i * picks : (i + 1) * picks]
            stats[pl.ds(n + o, 1)] = both[1:2, i * picks : (i + 1) * picks]

    rows_all[me] = x_ref[...]
    for way in range(2):
        hop(way, 0)
    load.wait()
    forward(me)
    for s in range(far):
        for way in range(2):
            waiting[way].wait_recv()
            if s < far - 1:
                hop(way, s + 1)
        if s < far - 1:
            forward(here.at(-s - 1), here.at(s + 1))
        else:
            forward(here.at(far))

    moves = []
    for k, o in enumerate(others):
        cp = remote(stats, shared.at[me], stat_s.at[k], stat_r.at[k], (here.r, o))
        cp.start()
        moves.append(cp)
    shared[me] = stats[...]
    table_ref[...] = jnp.zeros(table_ref.shape, f32)
    for cp in moves:
        cp.wait_recv()
    top = shared[0, :n]
    for k in range(1, n):
        top = jnp.maximum(top, shared[k, :n])
    total = jnp.exp(shared[0, :n] - top)
    target = shared[0, n:]
    for k in range(1, n):
        total = total + jnp.exp(shared[k, :n] - top)
        target = target + shared[k, n:]
    log_sum = top + jnp.log(total)
    for cp in moves:
        cp.wait_send()
    stats[:n] = log_sum
    stats[n:] = log_sum - target
    mine = stats[pl.ds(n + me, 1)]
    loss_ref[...] = jnp.broadcast_to(jnp.sum(mine, axis=1, keepdims=True), loss_ref.shape)

    def backward(*origins):
        rows, label = stack(rows_all, origins), stack(label_ref, origins)
        count = rows.shape[0]
        norm = [jnp.broadcast_to(stats[pl.ds(o, 1)], (128, picks)) for o in origins]
        norm = jnp.concatenate(norm, axis=1).T

        def product(t, out):
            scores = scores_of(origins, t)
            parts = [jnp.exp(scores[:, k * 128 : (k + 1) * 128] - norm) for k in range(tile // 128)]
            soft = jnp.concatenate(parts, axis=1)
            grad = (soft - jnp.where(columns(t, count) == label, 1.0, 0.0)).astype(bf16)
            table_ref[span(t)] += mm(grad, rows, TN)
            return out + mm(grad, table[span(t)])

        return lax.fori_loop(0, tiles, product, jnp.zeros((count, width), f32))

    ring = {}

    def lane_send(way, h, s, value):
        before = ring.get((way, h, s - 1))
        if before is not None:
            before.wait_recv()
            value = value + got[way, h, s - 1].astype(f32)
        held[way, h, s] = value.astype(bf16)
        cp = remote(
            held.at[way, h, s],
            got.at[way, h, s],
            back_s.at[way, h, s],
            back_r.at[way, h, s],
            here.next if way == 0 else here.prev,
        )
        cp.start()
        ring[way, h, s] = cp

    out = backward(here.at(far))
    lane_send(0, 0, 0, out[:half])
    lane_send(1, 1, 0, out[half:])
    for s in range(1, far):
        d = far - s
        out = backward(here.at(d), here.at(-d))
        for turn in range(2):
            for way in range(2):
                h = way if turn == 1 else 1 - way
                lane_send(way, h, s, piece(out, way)[h * half : (h + 1) * half])
    out = backward(me)
    for h in range(2):
        total = out[h * half : (h + 1) * half]
        for way in range(2):
            ring[way, h, far - 1].wait_recv()
            total = total + got[way, h, far - 1].astype(f32)
        picked_ref[pl.ds(h * half, half)] = total
    for cp in sends + list(ring.values()):
        cp.wait_send()


def head_step(mesh_sizes, cid, picked, table, labels, vocab):
    n_rep, n = mesh_sizes
    picks, width = picked.shape
    padded = table.shape[0]
    far = n // 2
    dma = pltpu.SemaphoreType.DMA
    return pl.pallas_call(
        partial(head_kernel, n_rep, n, vocab, 768),
        out_shape=[
            jax.ShapeDtypeStruct((picks, width), f32),
            jax.ShapeDtypeStruct((padded, width), f32),
            jax.ShapeDtypeStruct((8, 128), f32),
        ],
        in_specs=[VMEM, ANY, VMEM],
        out_specs=[VMEM, VMEM, VMEM],
        scratch_shapes=[
            pltpu.VMEM((padded, width), bf16),
            pltpu.VMEM((n, picks, width), bf16),
            pltpu.VMEM((n, picks, padded), f32),
            pltpu.VMEM((2 * n, picks), f32),
            pltpu.VMEM((n, 2 * n, picks), f32),
            pltpu.VMEM((2, 2, far, picks // 2, width), bf16),
            pltpu.VMEM((2, 2, far, picks // 2, width), bf16),
            dma,
            dma((2, far)),
            dma((2, far)),
            dma((n - 1,)),
            dma((n - 1,)),
            dma((2, 2, far)),
            dma((2, 2, far)),
        ],
        compiler_params=params(cid, 60 << 20),
        name="head_step",
    )(picked, table, labels.reshape(n, picks, 1))


class Transport:
    def __init__(self, n_rep, n_fsdp, shard_rows):
        self.sizes = (n_rep, n_fsdp)
        self.kernels = n_rep == 4 and n_fsdp == 8 and shard_rows == 64

    def open(self, cid, shard, table, ids, owner, local, facts, gains, padded):
        if self.kernels:
            return open_step(self.sizes, cid, shard, table, ids, owner, local, facts, gains, padded)
        tokens = ids.shape[0]
        groups = self.sizes[1]
        index = jnp.arange(tokens, dtype=jnp.int32)
        first_at = jnp.min(jnp.where(ids[:, None] == ids[None, :], index[None, :], tokens), axis=1)
        is_first = first_at == index
        ahead = is_first[None, :] & (owner[:, None] == owner[None, :]) & (index[None, :] < first_at[:, None])
        rank = jnp.sum(ahead.astype(jnp.int32), axis=1)
        facts = facts.at[facts.shape[0] - 1].set(jnp.max(rank) + 1)
        slot = jnp.where(is_first & (rank < CAPACITY), owner * CAPACITY + rank, -1)
        slot_index = jnp.arange(groups * CAPACITY, dtype=jnp.int32)
        wanted = jnp.sum(jnp.where(slot[None, :] == slot_index[:, None], local[None, :], 0), axis=1)
        wanted = wanted.reshape(groups, 1, CAPACITY)
        asked = lax.all_to_all(wanted, "fsdp", split_axis=0, concat_axis=0, tiled=True)
        low = jnp.pad(table.astype(bf16), ((0, padded - table.shape[0]), (0, 0)))
        rows = jnp.take(low, asked.reshape(-1), axis=0).reshape(groups, CAPACITY, table.shape[1])
        return (
            lax.all_gather(shard, "fsdp", axis=1, tiled=True),
            self.spread(cid, rows),
            asked,
            lax.all_gather(facts, "fsdp"),
            lax.all_gather(gains, "fsdp"),
            lax.pmax(facts, ("rep", "fsdp")),
            rank,
            first_at,
            low,
        )

    def spread(self, cid, x):
        if self.kernels:
            return group_exchange(self.sizes, cid, x, True)
        return lax.all_to_all(x, "fsdp", split_axis=0, concat_axis=0, tiled=True)


def body(
    token_ids,
    segment_ids,
    masked_pos,
    labels,
    blocks,
    gains,
    embed,
    embed_m,
    embed_v,
    gains_m,
    gains_v,
    soap_m,
    soap_v,
    left_basis,
    right_basis,
    block_slots,
    step_count,
):
    groups = lax.axis_size("fsdp")
    replicas = lax.axis_size("rep")
    member = lax.axis_index("fsdp")
    replica = lax.axis_index("rep")
    micro_count = token_ids.shape[0]
    pack_length = token_ids.shape[2]
    pick_count = masked_pos.shape[2]
    vocab_rows, model_width = embed.shape
    block_count, shard_rows, _ = blocks.shape
    gain_count = gains.shape[0]
    tokens = micro_count * pack_length
    picks = micro_count * pick_count
    move = Transport(replicas, groups, shard_rows)
    padded_rows = -(-vocab_rows // 768) * 768

    ids = token_ids.reshape(tokens)
    index = jnp.arange(tokens, dtype=jnp.int32)
    owner = ids // vocab_rows
    local = ids - owner * vocab_rows
    my_labels = labels.reshape(picks // 128, 128)
    facts = jnp.pad(my_labels, ((0, 8 - my_labels.shape[0]), (0, 0)))
    gain_pad = jnp.pad(gains, ((0, 8 - gain_count), (0, 128 - gains.shape[1])))
    full_blocks, rows, asked, group_facts, gain_rows, most_facts, rank, first_at, table_low = move.open(
        0, blocks.astype(bf16), embed, ids, owner, local, facts, gain_pad, padded_rows
    )
    rank, is_first = rank.reshape(tokens), first_at.reshape(tokens) == index
    slots = groups * CAPACITY
    most_rounds = (tokens + CAPACITY - 1) // CAPACITY
    slot_index = jnp.arange(slots, dtype=jnp.int32)

    def slot_of(k):
        here = rank - k * CAPACITY
        return jnp.where((here >= 0) & (here < CAPACITY), owner * CAPACITY + here, -1)

    def wanted_in(slot):
        wanted = jnp.where((slot[None, :] == slot_index[:, None]) & is_first[None, :], local[None, :], 0)
        return jnp.sum(wanted, axis=1).reshape(groups, 1, CAPACITY)

    def placed(slot, rows):
        chosen = (slot[:, None] == slot_index[None, :]).astype(bf16)
        return jnp.dot(chosen, rows.reshape(slots, model_width), preferred_element_type=f32)

    slot = slot_of(0)
    rounds = (most_facts[7, 0] + CAPACITY - 1) // CAPACITY
    all_labels = group_facts[:, : picks // 128].reshape(groups * picks)
    gain_rows = gain_rows[:, :gain_count, : gains.shape[1]].transpose(1, 0, 2).reshape(gain_count, model_width)
    gain_rows = lax.reduce_precision(gain_rows, exponent_bits=8, mantissa_bits=7)
    embedded = placed(slot, rows)
    asked_all = jnp.zeros((most_rounds, slots), jnp.int32).at[0].set(asked.reshape(slots))

    def look(state):
        k, rows_so_far, asked_all = state
        slot = slot_of(k)
        asked = move.spread(1, wanted_in(slot))
        asked_all = lax.dynamic_update_index_in_dim(asked_all, asked.reshape(slots), k, 0)
        rows = jnp.take(table_low, asked.reshape(slots), axis=0).reshape(groups, CAPACITY, model_width)
        return k + 1, rows_so_far + placed(slot, move.spread(2, rows)), asked_all

    _, embedded, asked_all = lax.while_loop(lambda s: s[0] < rounds, look, (jnp.int32(1), embedded, asked_all))

    segments = segment_ids.reshape(micro_count, pack_length)
    stream, first_pull = jax.vjp(layer_norm, embedded, gain_rows[0])
    saved_layers = []
    for layer in range(LAYERS):
        middle, *attention_kept = attend(stream, gain_rows[1 + 2 * layer], full_blocks, layer, segments)
        after, *feed_kept = feed(middle, gain_rows[2 + 2 * layer], full_blocks, layer)
        saved_layers.append((stream, attention_kept, middle, feed_kept))
        stream = after
    final_rows, final_pull = jax.vjp(layer_norm, stream, gain_rows[gain_count - 1])

    positions = masked_pos.reshape(micro_count, pick_count)
    flat_positions = (positions + jnp.arange(micro_count, dtype=jnp.int32)[:, None] * pack_length).reshape(picks)
    picked = jnp.take(final_rows, flat_positions, axis=0).astype(bf16)
    label_local = all_labels - member * vocab_rows
    label_local = jnp.where((label_local >= 0) & (label_local < vocab_rows), label_local, -1)
    if move.kernels:
        grad_picked, grad_table, loss_local = head_step(
            move.sizes, 4, picked, table_low, label_local.reshape(groups, picks), vocab_rows
        )
        loss_local = loss_local[0, 0]
    else:
        all_picked = lax.all_gather(picked, "fsdp", tiled=True)
        logits = jnp.einsum("td,vd->tv", all_picked, table_low[:vocab_rows], preferred_element_type=f32)
        top_value = jnp.max(logits, axis=-1)
        exp_total = jnp.sum(jnp.exp(logits - top_value[:, None]), axis=-1)
        label_hits = jnp.arange(vocab_rows, dtype=jnp.int32)[None, :] == label_local[:, None]
        target = jnp.sum(jnp.where(label_hits, logits, 0.0), axis=-1)
        stats = lax.all_gather(jnp.stack([top_value, exp_total, target]), "fsdp")
        top_all = jnp.max(stats[:, 0], axis=0)
        total_all = jnp.sum(stats[:, 1] * jnp.exp(stats[:, 0] - top_all[None]), axis=0)
        target_all = jnp.sum(stats[:, 2], axis=0)
        entropy = top_all + jnp.log(total_all) - target_all
        loss_local = jnp.sum(lax.dynamic_slice_in_dim(entropy, member * picks, picks))
        grad_logits = (
            jnp.exp(logits - top_all[:, None]) / total_all[:, None] - label_hits.astype(f32)
        ).astype(bf16)
        grad_table = jnp.einsum("tv,td->vd", grad_logits, all_picked, preferred_element_type=f32)
        grad_table = jnp.pad(grad_table, ((0, padded_rows - vocab_rows), (0, 0)))
        grad_picked = jnp.einsum("tv,vd->td", grad_logits, table_low[:vocab_rows], preferred_element_type=f32)
        grad_picked = grad_picked.reshape(groups, picks, model_width)
        grad_picked = lax.psum_scatter(grad_picked, "fsdp", scatter_dimension=0)

    match = flat_positions[None, :] == index[:, None]
    place = jnp.sum(jnp.where(match, jnp.arange(picks, dtype=jnp.int32)[None, :] + 1, 0), axis=1)
    grad_final = jnp.where(
        (place > 0)[:, None], jnp.take(grad_picked, jnp.maximum(place - 1, 0), axis=0), 0.0
    )
    grad_stream, grad_final_gain = final_pull(grad_final)
    gain_grads = [None] * gain_count
    gain_grads[gain_count - 1] = grad_final_gain
    layer_grads = [None] * LAYERS
    for layer in reversed(range(LAYERS)):
        before, attention_kept, middle, feed_kept = saved_layers[layer]
        grad_stream, feed_gain, *grads_feed = feed_back(
            grad_stream, middle, gain_rows[2 + 2 * layer], full_blocks, layer, feed_kept
        )
        grad_stream, attention_gain, grads_attention = attend_back(
            grad_stream, before, gain_rows[1 + 2 * layer], full_blocks, layer, segments, attention_kept
        )
        gain_grads[1 + 2 * layer] = jnp.sum(attention_gain, axis=(0, 1))
        gain_grads[2 + 2 * layer] = jnp.sum(feed_gain, axis=0)
        layer_grads[layer] = [grads_attention] + grads_feed
    grad_embedded, gain_grads[0] = first_pull(grad_stream)
    grad_rows = grad_embedded.astype(bf16)
    row_index = jnp.arange(padded_rows, dtype=jnp.int32)

    def given(cid, k, grad_table):
        chosen = (slot_index[:, None] == slot_of(k)[None, :]).astype(bf16)
        rows = jnp.dot(chosen, grad_rows, preferred_element_type=f32).astype(bf16)
        rows = move.spread(cid, rows.reshape(groups, CAPACITY, model_width)).reshape(slots, model_width)
        asked = lax.dynamic_index_in_dim(asked_all, k, 0, keepdims=False)
        target_rows = (row_index[:, None] == asked[None, :]).astype(bf16)
        return grad_table + jnp.dot(target_rows, rows, preferred_element_type=f32)

    grad_table = given(7, 0, grad_table)
    _, grad_table = lax.while_loop(
        lambda s: s[0] < rounds, lambda s: (s[0] + 1, given(13, s[0], s[1])), (jnp.int32(1), grad_table)
    )
    grad_blocks = [g for grads in layer_grads for g in grads]
    grad_gains = jnp.stack(gain_grads, axis=0)

    position_count = micro_count * replicas * groups * pick_count
    clip_limit = clip_ratio * math.sqrt(position_count)
    steps_done = step_count[0].astype(f32)
    first_fix = 1.0 - beta_first**steps_done
    second_fix = 1.0 - beta_second**steps_done
    slot_cap = soap_m.shape[0]
    slot_total = slot_cap * groups
    named = jnp.arange(slot_total, dtype=jnp.int32)[:, None] == block_slots[None, :]
    taken = jnp.any(named, axis=1)
    block_of = jnp.sum(jnp.where(named, jnp.arange(block_count, dtype=jnp.int32)[None, :], 0), axis=1)

    small = jnp.zeros((8, model_width), f32).at[:gain_count].set(grad_gains)
    small = small.at[7, 0].set(loss_local)
    if move.kernels:
        owned, grad_table, small = settle_gradients(
            move.sizes,
            8,
            grad_blocks,
            grad_table.reshape(4, padded_rows // 4, model_width),
            small,
            block_of,
            taken.astype(jnp.int32),
            slot_cap,
        )
        grad_table = grad_table.reshape(padded_rows, model_width)[:vocab_rows]
        squares = jnp.sum(small[6])
        owned = owned.reshape(slot_cap, model_width, model_width)
    else:
        grad_blocks = jnp.concatenate([g.astype(f32) for g in grad_blocks], axis=0)
        mine = lax.psum_scatter(grad_blocks, "fsdp", scatter_dimension=1, tiled=True)
        mine, grad_table = lax.psum((mine, grad_table[:vocab_rows]), "rep")
        small = lax.psum(small, ("rep", "fsdp"))
        squares = lax.psum(jnp.sum(mine * mine) + jnp.sum(grad_table * grad_table), "fsdp")
        outgoing = jnp.where(taken[:, None, None], jnp.take(mine, block_of, axis=0), 0)
        owned = lax.all_to_all(outgoing, "fsdp", split_axis=0, concat_axis=1, tiled=True)
    loss_all = small[7, 0]
    grad_gains = small[:gain_count]
    grad_norm = jnp.sqrt(squares + jnp.sum(grad_gains * grad_gains))
    factor = jnp.minimum(1.0, clip_limit / grad_norm)
    grad_gains = lax.dynamic_slice_in_dim(grad_gains, member * gains.shape[1], gains.shape[1], axis=1)

    live = lax.dynamic_slice_in_dim(taken, member * slot_cap, slot_cap)
    if move.kernels:
        soap_m_new, soap_v_new, turned = turn_slots(
            replica,
            live,
            jnp.stack([factor, first_fix, second_fix]),
            left_basis,
            right_basis,
            owned,
            soap_m,
            soap_v,
        )
        returned = exchange_slots(move.sizes, 11, turned, False)
        returned = returned.reshape(slot_total, shard_rows, model_width)
    else:
        rotated = jnp.einsum("bji,bjk->bik", left_basis, owned, precision=high)
        rotated = factor * jnp.einsum("bik,bkl->bil", rotated, right_basis, precision=high)
        moment_first, moment_second, rotated_step = adam_moments(soap_m, soap_v, rotated, first_fix, second_fix)
        soap_m_new = jnp.where(live[:, None, None], moment_first, soap_m)
        soap_v_new = jnp.where(live[:, None, None], moment_second, soap_v)
        turned = jnp.einsum("bij,bjk->bik", left_basis, rotated_step, precision=high)
        turned = jnp.einsum("bik,blk->bil", turned, right_basis, precision=high)
        returned = lax.all_to_all(turned, "fsdp", split_axis=1, concat_axis=0, tiled=True)
    update = jnp.take(returned, block_slots, axis=0).astype(f32)
    blocks_new = blocks - step_rate * (update + weight_decay * blocks)

    embed_m_new, embed_v_new, table_step = adam_moments(
        embed_m, embed_v, factor * grad_table, first_fix, second_fix
    )
    embed_new = embed - step_rate * (table_step + weight_decay * embed)
    gains_m_new, gains_v_new, gain_step = adam_moments(
        gains_m, gains_v, factor * grad_gains, first_fix, second_fix
    )
    gains_new = gains - step_rate * gain_step
    loss = (loss_all / position_count).reshape(1)
    return (
        loss,
        grad_norm.reshape(1),
        blocks_new,
        gains_new,
        embed_new,
        embed_m_new,
        embed_v_new,
        gains_m_new,
        gains_v_new,
        soap_m_new,
        soap_v_new,
        blocks_new.astype(bf16),
        embed_new.astype(bf16),
    )


def solution(mesh):
    packs = P(None, ("rep", "fsdp"), None)
    rows = P(None, "fsdp", None)
    columns = P(None, "fsdp")
    table = P("fsdp", None)
    slots = P("fsdp", None, None)
    return jax.shard_map(
        body,
        mesh=mesh,
        in_specs=(packs,) * 4
        + (rows, columns)
        + (table,) * 3
        + (columns,) * 2
        + (slots,) * 4
        + (P(), P()),
        out_specs=(P(), P(), rows, columns)
        + (table,) * 3
        + (columns,) * 2
        + (slots,) * 2
        + (rows, table),
        check_vma=False,
    )
```

```python
from functools import partial
import math

import jax
import jax.numpy as jnp
from jax import lax
from jax.experimental import pallas as pl
from jax.experimental.pallas import tpu as pltpu
from jax.sharding import PartitionSpec as P

HEADS = 8
FF = 2048
LAYERS = 2

norm_epsilon = 1e-05
beta_first = 0.9
beta_second = 0.99
adam_epsilon = 1e-08
step_rate = 0.04
weight_decay = 0.1
clip_ratio = 12.0
masked_score = -1e30
bf16 = jnp.bfloat16
f32 = jnp.float32
highest = lax.Precision.HIGHEST
high = lax.Precision.HIGH
MESH = pl.DeviceIdType.MESH
ANY = pl.BlockSpec(memory_space=pl.ANY)
VMEM = pl.BlockSpec(memory_space=pltpu.VMEM)
CAPACITY = 128


def pick(table, index):
    out = jnp.int32(table[0])
    for k in range(1, len(table)):
        out = jnp.where(index == k, jnp.int32(table[k]), out)
    return out


def ring_order(n):
    nz = 4
    nx = n // nz
    order = []
    for x in range(nx):
        zs = range(1, nz) if x % 2 == 0 else range(nz - 1, 0, -1)
        order += [z * nx + x for z in zs]
    order += [x for x in range(nx - 1, -1, -1)]
    return order


class Place:
    def __init__(self, n_rep, n_fsdp):
        self.r = lax.axis_index("rep")
        self.f = lax.axis_index("fsdp")
        self.n_rep, self.n = n_rep, n_fsdp
        self.c = lax.rem(self.r, 2)
        self.y = self.r // 2
        self.order = ring_order(n_fsdp)
        spot = [self.order.index(k) for k in range(n_fsdp)]
        self.pos = pick(spot, self.f)
        self.core = (self.r + 1 - 2 * self.c, self.f)
        self.next = (self.r, self.at(1))
        self.prev = (self.r, self.at(-1))

    def at(self, step):
        return pick(self.order, lax.rem(self.pos + step + 2 * self.n, self.n))


def enter(peers):
    barrier = pltpu.get_barrier_semaphore()
    for peer in peers:
        pl.semaphore_signal(barrier, inc=1, device_id=peer, device_id_type=MESH)
    pl.semaphore_wait(barrier, len(peers))


def remote(src, dst, send, recv, peer):
    return pltpu.make_async_remote_copy(
        src_ref=src, dst_ref=dst, send_sem=send, recv_sem=recv, device_id=peer, device_id_type=MESH
    )


def params(cid, limit=None):
    return pltpu.CompilerParams(
        collective_id=cid, has_side_effects=True, vmem_limit_bytes=limit
    )


def group_kernel(n_rep, n, spread, x_ref, o_ref, send, recv):
    here = Place(n_rep, n)
    me = here.f
    others = [lax.rem(me + k, n) for k in range(1, n)]
    enter([(here.r, o) for o in others])
    copies = []
    for k, o in enumerate(others):
        src = x_ref.at[o] if spread else x_ref
        cp = remote(src, o_ref.at[me], send.at[k], recv.at[k], (here.r, o))
        cp.start()
        copies.append(cp)
    o_ref[me] = x_ref[me] if spread else x_ref[...]
    for cp in copies:
        cp.wait()


def group_exchange(mesh_sizes, cid, x, spread):
    n_rep, n = mesh_sizes
    shape = x.shape if spread else (n,) + x.shape
    return pl.pallas_call(
        partial(group_kernel, n_rep, n, spread),
        out_shape=jax.ShapeDtypeStruct(shape, x.dtype),
        in_specs=[VMEM],
        out_specs=VMEM,
        scratch_shapes=[pltpu.SemaphoreType.DMA((n - 1,)), pltpu.SemaphoreType.DMA((n - 1,))],
        compiler_params=params(cid),
        name=f"group_{cid}",
    )(x)


def distinct(here, n, capacity, ids_row, ids_col, own_row, own_col, local_col, rank_ref, first_ref, ask):
    tokens = ids_col.shape[0]
    step = 128
    lane = lax.broadcasted_iota(jnp.int32, (1, tokens), 1)

    def rows_at(t):
        return pl.ds(pl.multiple_of(t * step, step), step)

    def place(t, width):
        return t * step + lax.broadcasted_iota(jnp.int32, (step, width), 0)

    def earliest(t, first):
        same = ids_col[rows_at(t)] == ids_row[...]
        return jnp.minimum(first, jnp.min(jnp.where(same, place(t, tokens), tokens), axis=0, keepdims=True))

    first_row = lax.fori_loop(0, tokens // step, earliest, jnp.full((1, tokens), tokens, jnp.int32))
    member = jnp.where(first_row == lane, own_row[...], -1)

    def number(t, carry):
        wanted, most = carry
        at = rows_at(t)
        same = ids_col[at] == ids_row[...]
        first = jnp.min(jnp.where(same, lane, tokens), axis=1, keepdims=True)
        ahead = (member == own_col[at]) & (lane < first)
        rank = jnp.sum(jnp.where(ahead, 1, 0), axis=1, keepdims=True)
        rank_ref[at] = rank
        first_ref[at] = first
        slot = jnp.where((first == place(t, 1)) & (rank < capacity), own_col[at] * capacity + rank, -1)
        slots = lax.broadcasted_iota(jnp.int32, (1, n * capacity), 1)
        wanted = wanted + jnp.sum(jnp.where(slot == slots, local_col[at], 0), axis=0, keepdims=True)
        return wanted, jnp.maximum(most, jnp.max(rank, axis=0, keepdims=True))

    start = (jnp.zeros((1, n * capacity), jnp.int32), jnp.zeros((1, 1), jnp.int32))
    wanted, most = lax.fori_loop(0, tokens // step, number, start)
    for o in range(n):
        ask[o] = wanted[:, o * capacity : (o + 1) * capacity]
    return most + 1


def opening_kernel(
    n_rep, n, half, shared,
    x_ref, t_ref, ids_row, ids_col, own_row, own_col, local_col, facts_ref, gains_ref,
    o_ref, rows_ref, asked, facts, gains, most, rank_ref, first_ref, low_ref,
    table, low, index, ask, fact, stage, ready, held, got,
    t_s, ring_s, ring_r, core_s, core_r, y_s, y_r, over_s, over_r, ask_s, ask_r, top_s, top_r, rows_s, rows_r,
):
    here = Place(n_rep, n)
    me = here.f
    ypeer = (lax.rem(here.r + 2, 4), here.f)
    others = [lax.rem(me + k, n) for k in range(1, n)]
    rows = x_ref.shape[1]
    part = rows // 2
    alone = (half - shared) // 2
    enter([(here.r, o) for o in others] + [here.core, ypeer])
    vocab = t_ref.shape[0]
    load = pltpu.make_async_copy(t_ref, table.at[pl.ds(0, vocab)], t_s.at[0])
    load.start()
    table[vocab:] = jnp.zeros((table.shape[0] - vocab, table.shape[1]), table.dtype)

    mine = pl.ds(here.c * half + here.y * alone, alone + shared)
    given = pl.ds(here.c * half + here.y * (alone + shared), alone)
    taken = pl.ds(here.c * half + (1 - here.y) * (alone + shared), alone)
    hops = n // 2
    copies, sends = [], []

    def rows_of(origin, lane):
        return pl.ds(pl.multiple_of(origin * rows + lane * part, part), part)

    own = remote(
        x_ref, o_ref.at[:, pl.ds(pl.multiple_of(me * rows, rows), rows)], core_s.at[0, 0, 0], core_r.at[0, 0, 0], here.core
    )
    waiting = {}
    across = []

    def pass_on(way, s, lane):
        waiting[way, s, lane].wait_recv()
        where = rows_of(here.at(-s - 1 if way == 0 else s + 1), lane)
        kept = o_ref.at[given, where]
        cp = remote(kept, kept, y_s.at[way, s, lane], y_r.at[way, s, lane], ypeer)
        cp.start()
        across.append((cp, o_ref.at[taken, where], way, s, lane))
        kept = o_ref.at[mine, where]
        cp = remote(kept, kept, core_s.at[way, s + 1, lane], core_r.at[way, s + 1, lane], here.core)
        cp.start()
        copies.append(cp)

    def hop(way, s, lane):
        where = rows_of(here.at(-s if way == 0 else s), lane)
        src = x_ref.at[mine, pl.ds(lane * part, part)] if s == 0 else o_ref.at[mine, where]
        cp = remote(
            src,
            o_ref.at[mine, where],
            ring_s.at[way, s, lane],
            ring_r.at[way, s, lane],
            here.next if way == 0 else here.prev,
        )
        cp.start()
        waiting[way, s, lane] = cp
        sends.append(cp)

    for way in range(2):
        hop(way, 0, way)
    for way in range(2):
        hop(way, 0, 1 - way)
    own.start()
    copies.append(own)

    count = distinct(
        here, n, ask.shape[2], ids_row, ids_col, own_row, own_col, local_col, rank_ref, first_ref, ask
    )
    line = lax.broadcasted_iota(jnp.int32, fact.shape, 0)
    fact[...] = jnp.where(line == fact.shape[0] - 1, count, facts_ref[...])
    asks = []
    for k, o in enumerate(others):
        peer = (here.r, o)
        asks.append(remote(ask.at[o], asked.at[me], ask_s.at[0, k], ask_r.at[0, k], peer))
        asks.append(remote(fact, facts.at[me], ask_s.at[1, k], ask_r.at[1, k], peer))
        asks.append(remote(gains_ref, gains.at[me], ask_s.at[2, k], ask_r.at[2, k], peer))
    for cp in asks:
        cp.start()
    asked[me] = ask[me]
    facts[me] = fact[...]
    gains[me] = gains_ref[...]
    for cp in asks:
        cp.wait_recv()
    listed = pltpu.make_async_copy(asked, index, t_s.at[1])
    listed.start()
    top = facts[0]
    for k in range(1, n):
        top = jnp.maximum(top, facts[k])
    held[0] = top
    first = remote(held.at[0], got.at[0], top_s.at[0], top_r.at[0], here.core)
    first.start()
    listed.wait()
    load.wait()
    places = rows_ref.shape[1]

    def collect(o):
        def one(i, carry):
            stage[pl.ds(i, 1)] = table[pl.ds(index[o, 0, i], 1)]
            return carry

        lax.fori_loop(0, places, one, 0, unroll=8)
        return stage[...].astype(bf16)

    for k, o in enumerate(others):
        ready[o] = collect(o)
        cp = remote(ready.at[o], rows_ref.at[me], rows_s.at[k], rows_r.at[k], (here.r, o))
        cp.start()
        asks.append(cp)
    for way in range(2):
        pass_on(way, 0, way)
        hop(way, 1, way)
    for way in range(2):
        pass_on(way, 0, 1 - way)
        hop(way, 1, 1 - way)
    rows_ref[me] = collect(me)
    first.wait_recv()
    held[1] = jnp.maximum(top, got[0])
    second = remote(held.at[1], got.at[1], top_s.at[1], top_r.at[1], ypeer)
    second.start()

    step = 96

    @pl.loop(0, table.shape[0] // step)
    def _(i):
        at = pl.ds(pl.multiple_of(i * step, step), step)
        low[at] = table[at].astype(bf16)

    put = pltpu.make_async_copy(low, low_ref, t_s.at[0])
    put.start()

    for s in range(2, hops):
        for way in range(2):
            pass_on(way, s - 1, way)
            hop(way, s, way)
        for way in range(2):
            pass_on(way, s - 1, 1 - way)
            if s < hops - 1:
                hop(way, s, 1 - way)
    second.wait_recv()
    most[...] = jnp.maximum(held[1], got[1])
    for way in range(2):
        pass_on(way, hops - 1, way)
    for cp, kept, way, s, lane in across:
        cp.wait_recv()
        over = remote(kept, kept, over_s.at[way, s, lane], over_r.at[way, s, lane], here.core)
        over.start()
        copies.append(over)
        sends.append(cp)
    for cp in asks[3 * (n - 1) :]:
        cp.wait_recv()
    for cp in asks + [first, second] + sends:
        cp.wait_send()
    for cp in copies:
        cp.wait()
    put.wait()


def open_step(mesh_sizes, cid, shard, table, ids, owner, local, facts, gains, padded):
    n_rep, n = mesh_sizes
    count, rows, width = shard.shape
    tokens = ids.shape[0]
    half = count // 2
    hops = n // 2
    dma = pltpu.SemaphoreType.DMA
    wanted = (n, 1, CAPACITY)
    like = facts.shape
    i32 = jnp.int32
    return pl.pallas_call(
        partial(opening_kernel, n_rep, n, half, half - 2 * (half // 3)),
        out_shape=[
            jax.ShapeDtypeStruct((count, rows * n, width), shard.dtype),
            jax.ShapeDtypeStruct((n, CAPACITY, width), bf16),
            jax.ShapeDtypeStruct(wanted, i32),
            jax.ShapeDtypeStruct((n,) + like, i32),
            jax.ShapeDtypeStruct((n,) + gains.shape, gains.dtype),
            jax.ShapeDtypeStruct(like, i32),
            jax.ShapeDtypeStruct((tokens, 1), i32),
            jax.ShapeDtypeStruct((tokens, 1), i32),
            jax.ShapeDtypeStruct((padded, width), bf16),
        ],
        in_specs=[ANY, ANY] + [VMEM] * 7,
        out_specs=[ANY] + [VMEM] * 7 + [ANY],
        scratch_shapes=[
            pltpu.VMEM((padded, width), f32),
            pltpu.VMEM((padded, width), bf16),
            pltpu.SMEM(wanted, i32),
            pltpu.VMEM(wanted, i32),
            pltpu.VMEM(like, i32),
            pltpu.VMEM((CAPACITY, width), f32),
            pltpu.VMEM((n, CAPACITY, width), bf16),
            pltpu.VMEM((2,) + like, i32),
            pltpu.VMEM((2,) + like, i32),
            dma((2,)),
            dma((2, hops, 2)),
            dma((2, hops, 2)),
            dma((2, hops + 1, 2)),
            dma((2, hops + 1, 2)),
            dma((2, hops, 2)),
            dma((2, hops, 2)),
            dma((2, hops, 2)),
            dma((2, hops, 2)),
            dma((3, n - 1)),
            dma((3, n - 1)),
            dma((2,)),
            dma((2,)),
            dma((n - 1,)),
            dma((n - 1,)),
        ],
        compiler_params=params(cid, 60 << 20),
        name="open_step",
    )(
        shard,
        table,
        ids.reshape(1, tokens),
        ids.reshape(tokens, 1),
        owner.reshape(1, tokens),
        owner.reshape(tokens, 1),
        local.reshape(tokens, 1),
        facts,
        gains,
    )


def squares_row(square):
    row = jnp.sum(square, axis=0, keepdims=True)
    return jnp.where(lax.broadcasted_iota(jnp.int32, square.shape, 0) == 6, row, 0.0)


def reduce_kernel(
    n_rep, n, half, table_rows, each, *refs
):
    g_refs, refs = refs[: 2 * each], refs[2 * each :]
    (
    t_ref, small_ref, block_of, taken, o_ref, to_ref, sum_ref, mine, outgoing, held, hgot, four, fours, squares,
    own, part, got, fin, ysend, ygot, town, tpart, tsend, tgot,
    load_s, core_s, core_r, ring_s, ring_r, y_s, y_r, tload, tcs, tcr, tys, tyr, tos, tor,
    keep, a_s, a_r, f_s, f_r, sum_s, sum_r,
    ) = refs
    here = Place(n_rep, n)
    c, y = here.c, here.y
    ypeer = (lax.rem(here.r + 2, 4), here.f)
    other_c, other_y = 1 - c, 1 - y
    me = here.f
    others = [lax.rem(me + k, n) for k in range(1, n)]
    enter([(here.r, o) for o in others] + [here.core, ypeer])
    far = n // 2

    tl = pltpu.make_async_copy(t_ref.at[pl.ds(c * 2, 2)], town, tload)
    tl.start()
    tc = remote(t_ref.at[pl.ds(other_c * 2, 2)], tpart, tcs, tcr, here.core)
    tc.start()

    spots = {(0, far): 0, (1, far): 0}
    for d in range(far - 1, 0, -1):
        spots[0, d] = 1 + 2 * (far - 1 - d)
        spots[1, d] = 2 + 2 * (far - 1 - d)
    spots[0, 0] = spots[1, 0] = n - 1
    loads, cores = {}, {}
    done = set()
    for (way, d), spot in sorted(spots.items(), key=lambda item: item[1]):
        if spot in done:
            continue
        done.add(spot)
        to = here.f if d == 0 else here.at(d if way == 0 else -d)
        for h in (way, 1 - way):
            loads[spot, h], cores[spot, h] = [], []
            for j in range(each):
                g_ref = g_refs[h * each + j]
                into = pl.ds(j * (half // each), half // each)
                ld = pltpu.make_async_copy(g_ref.at[:, to, :, c], own.at[spot, h, into], load_s.at[spot, h, j])
                ld.start()
                loads[spot, h].append(ld)
                cp = remote(
                    g_ref.at[:, to, :, other_c],
                    part.at[spot, h, into],
                    core_s.at[spot, h, j],
                    core_r.at[spot, h, j],
                    here.core,
                )
                cp.start()
                cores[spot, h].append(cp)

    def ready(spot, h):
        for j in range(each):
            loads[spot, h][j].wait()
            cores[spot, h][j].wait_recv()

    ring = {}

    def came(way, h, s):
        return got.at[way, h, s]

    def lane(way, h, s):
        d = far - s
        spot = spots[way, d]
        ready(spot, h)
        before = ring.get((way, h, s - 1))
        if before is not None:
            before.wait_recv()
        target = own.at[spot, h]

        @pl.loop(0, half)
        def _(b):
            for k in range(2):
                total = own[spot, h, b, k].astype(f32) + part[spot, h, b, k].astype(f32)
                if before is not None:
                    total = total + came(way, h, s - 1)[b, k].astype(f32)
                target[b, k] = total.astype(target.dtype)

        cp = remote(
            target, came(way, h, s), ring_s.at[way, h, s], ring_r.at[way, h, s], here.next if way == 0 else here.prev
        )
        cp.start()
        ring[way, h, s] = cp

    step_rows = 48
    for s in range(far):
        for h_turn in range(2):
            for way in range(2):
                h = way if h_turn == 1 else 1 - way
                if s == far - 1:
                    h = h_turn
                if s == 0 and h_turn == 0:
                    continue
                if s == 1 and h_turn == 0:
                    continue
                lane(way, h, s)
        if s == 0:
            for way in range(2):
                lane(way, 1 - way, 1)
            tl.wait()
            tc.wait_recv()

            @pl.loop(0, table_rows // step_rows)
            def _(i):
                at = pl.ds(pl.multiple_of(i * step_rows, step_rows), step_rows)
                town[y, at] = town[y, at] + tpart[y, at]
                tsend[at] = (town[other_y, at] + tpart[other_y, at]).astype(bf16)

            ty = remote(tsend, tgot, tys, tyr, ypeer)
            ty.start()
        if s == 2:
            ty.wait_recv()

            def add(i, acc):
                at = pl.ds(pl.multiple_of(i * step_rows, step_rows), step_rows)
                total = town[y, at] + tgot[at].astype(f32)
                town[y, at] = total
                square = total * total
                for k in range(step_rows // 8):
                    acc = acc + square[k * 8 : k * 8 + 8]
                return acc

            squares[...] = lax.fori_loop(0, table_rows // step_rows, add, jnp.zeros((8, tgot.shape[1]), f32))
            quarter = c * 2 + y
            near = c * 2 + other_y
            tkeep = pltpu.make_async_copy(town.at[y], to_ref.at[quarter], tload)
            tkeep.start()
            t0 = remote(town.at[y], to_ref.at[quarter], tos.at[0], tor.at[0], ypeer)
            t1 = remote(town.at[y], to_ref.at[quarter], tos.at[1], tor.at[1], here.core)
            t0.start()
            t1.start()
    ys = []
    spot = spots[0, 0]
    for h in range(2):
        ready(spot, h)
        for way in range(2):
            ring[way, h, far - 1].wait_recv()

        @pl.loop(0, half)
        def _(b, h=h):
            for keep in range(2):
                k = y if keep else other_y
                total = own[spot, h, b, k].astype(f32) + part[spot, h, b, k].astype(f32)
                for way in range(2):
                    total = total + got[way, h, far - 1, b, k].astype(f32)
                if keep:
                    fin[h, b] = total
                else:
                    ysend[h, b] = total.astype(bf16)

        cp = remote(ysend.at[h], ygot.at[h], y_s.at[h], y_r.at[h], ypeer)
        cp.start()
        ys.append(cp)

    acc = jnp.zeros((8, fin.shape[-1]), f32)
    for h in range(2):
        ys[h].wait_recv()

        def last(b, acc, h=h):
            total = fin[h, b] + ygot[h, b].astype(f32)
            mine[h * half + b] = total.astype(bf16)
            square = total * total
            return acc + square[:8] + square[8:]

        acc = lax.fori_loop(0, half, last, acc)

    held[0] = small_ref[...] + squares_row(acc + squares[...])
    first = remote(held.at[0], hgot.at[0], sum_s.at[0], sum_r.at[0], here.core)
    first.start()

    cap = o_ref.shape[0]

    @pl.loop(0, n * cap)
    def _(k):
        value = mine[block_of[k]]
        outgoing[k] = jnp.where(taken[k] > 0, value, jnp.zeros_like(value))

    def spot_of(source, r):
        return o_ref.at[:, source, r]

    moves = []
    for k, o in enumerate(others):
        cp = remote(outgoing.at[pl.ds(o * cap, cap)], spot_of(me, here.r), a_s.at[k], a_r.at[k], (here.r, o))
        cp.start()
        moves.append(cp)
    kept = pltpu.make_async_copy(outgoing.at[pl.ds(me * cap, cap)], spot_of(me, here.r), keep)
    kept.start()
    first.wait_recv()
    held[1] = held[0] + hgot[0]
    second = remote(held.at[1], hgot.at[1], sum_s.at[1], sum_r.at[1], ypeer)
    second.start()
    t0.wait_recv()
    t2 = remote(to_ref.at[near], to_ref.at[near], tos.at[2], tor.at[2], here.core)
    t2.start()
    second.wait_recv()
    four[...] = held[1] + hgot[1]
    totals = []
    for k, o in enumerate(others):
        cp = remote(four, fours.at[me], sum_s.at[2 + k], sum_r.at[2 + k], (here.r, o))
        cp.start()
        totals.append(cp)
    fours[me] = four[...]
    beside, distant = [], []
    for k in range(n):
        source = me if k == 0 else lax.rem(me - k + n, n)
        if k == 0:
            kept.wait()
        else:
            moves[k - 1].wait_recv()
        piece = spot_of(source, here.r)
        over = remote(piece, piece, f_s.at[0, k], f_r.at[0, k], ypeer)
        over.start()
        cp = remote(piece, piece, f_s.at[1, k], f_r.at[1, k], here.core)
        cp.start()
        distant.append((over, source))
        beside.append(cp)
    for cp in totals:
        cp.wait_recv()
    total = fours[0]
    for k in range(1, n):
        total = total + fours[k]
    sum_ref[...] = total
    yr = lax.rem(here.r + 2, 4)
    for k, (over, source) in enumerate(distant):
        over.wait_recv()
        piece = spot_of(source, yr)
        cp = remote(piece, piece, f_s.at[2, k], f_r.at[2, k], here.core)
        cp.start()
        beside.append(cp)
    for cp in moves + totals + [first, second] + [over for over, _ in distant]:
        cp.wait_send()
    for cp in beside:
        cp.wait()
    for cp in ys:
        cp.wait_send()
    for cp in ring.values():
        cp.wait_send()
    for group in cores.values():
        for cp in group:
            cp.wait_send()
    tc.wait_send()
    ty.wait_send()
    tkeep.wait()
    t0.wait_send()
    t1.wait()
    t2.wait()


def settle_gradients(mesh_sizes, cid, grads, table, small, block_of, taken, cap):
    n_rep, n = mesh_sizes
    _, depth, width = grads[0].shape
    count = sum(g.shape[0] for g in grads)
    half = count // 2
    each = len(grads) // 2
    far = n // 2
    table_rows = table.shape[1]
    views = [g.reshape(g.shape[0], n, 2, 2, 16, width) for g in grads]
    dma = pltpu.SemaphoreType.DMA
    piece = (half, 2, 16, width)
    smem = pl.BlockSpec(memory_space=pltpu.SMEM)
    like = small.shape
    return pl.pallas_call(
        partial(reduce_kernel, n_rep, n, half, table_rows, each),
        out_shape=[
            jax.ShapeDtypeStruct((cap, n, 4, 16, width), bf16),
            jax.ShapeDtypeStruct(table.shape, f32),
            jax.ShapeDtypeStruct(like, f32),
        ],
        in_specs=[ANY] * (2 * each + 1) + [VMEM, smem, smem],
        out_specs=[ANY, ANY, VMEM],
        scratch_shapes=[
            pltpu.VMEM((count, 16, width), bf16),
            pltpu.VMEM((n * cap, 16, width), bf16),
            pltpu.VMEM((2,) + like, f32),
            pltpu.VMEM((2,) + like, f32),
            pltpu.VMEM(like, f32),
            pltpu.VMEM((n,) + like, f32),
            pltpu.VMEM(like, f32),
            pltpu.VMEM((n, 2) + piece, bf16),
            pltpu.VMEM((n, 2) + piece, bf16),
            pltpu.VMEM((2, 2, far) + piece, bf16),
            pltpu.VMEM((2, half, 16, width), f32),
            pltpu.VMEM((2, half, 16, width), bf16),
            pltpu.VMEM((2, half, 16, width), bf16),
            pltpu.VMEM((2, table_rows, width), f32),
            pltpu.VMEM((2, table_rows, width), f32),
            pltpu.VMEM((table_rows, width), bf16),
            pltpu.VMEM((table_rows, width), bf16),
            dma((n, 2, each)),
            dma((n, 2, each)),
            dma((n, 2, each)),
            dma((2, 2, far)),
            dma((2, 2, far)),
            dma((2,)),
            dma((2,)),
            dma,
            dma,
            dma,
            dma,
            dma,
            dma((3,)),
            dma((3,)),
            dma,
            dma((n - 1,)),
            dma((n - 1,)),
            dma((3, n)),
            dma((3, n)),
            dma((n + 1,)),
            dma((n + 1,)),
        ],
        compiler_params=params(cid, 56 << 20),
        name="settle_gradients",
    )(*views, table, small, block_of, taken)


def return_kernel(
    n_rep, n, vocab, x_ref, numbers, g_ref, e_ref, m_ref, v_ref, o_ref, e_new, m_new, v_new, low_new,
    fetched, made, made_low, keep, a_s, a_r, f_s, f_r, in_s, out_s,
):
    here = Place(n_rep, n)
    ypeer = (lax.rem(here.r + 2, 4), here.f)
    me = here.f
    others = [lax.rem(me + k, n) for k in range(1, n)]
    chunk = fetched.shape[2]
    strip = 48
    chunks = -(-vocab // chunk)

    def extent(t):
        return min(chunk, vocab - t * chunk)

    def fetch(t):
        spot, size = t % 2, extent(t)
        loads = [
            pltpu.make_async_copy(
                ref.at[pl.ds(t * chunk, size)], fetched.at[spot, k, pl.ds(0, size)], in_s.at[spot, k]
            )
            for k, ref in enumerate((g_ref, e_ref, m_ref, v_ref))
        ]
        for ld in loads:
            ld.start()
        return loads

    def store(t):
        spot, size = t % 2, extent(t)
        puts = [
            pltpu.make_async_copy(
                made.at[spot, k, pl.ds(0, size)], ref.at[pl.ds(t * chunk, size)], out_s.at[spot, k]
            )
            for k, ref in enumerate((e_new, m_new, v_new))
        ]
        puts.append(
            pltpu.make_async_copy(
                made_low.at[spot, pl.ds(0, size)], low_new.at[pl.ds(t * chunk, size)], out_s.at[spot, 3]
            )
        )
        for cp in puts:
            cp.start()
        return puts

    loads = {t: fetch(t) for t in range(min(2, chunks))}
    enter([(here.r, o) for o in others] + [here.core, ypeer])

    def piece(source, r):
        return o_ref.at[source, :, r]

    copies = []
    for k, o in enumerate(others):
        cp = remote(x_ref.at[o], piece(me, here.r), a_s.at[k], a_r.at[k], (here.r, o))
        cp.start()
        copies.append(cp)
    own = pltpu.make_async_copy(x_ref.at[me], piece(me, here.r), keep)
    own.start()
    sends, far = [], []
    yr = lax.rem(here.r + 2, 4)

    def source_of(k):
        return me if k == 0 else lax.rem(me - k + n, n)

    def forward(k):
        if k == 0:
            own.wait()
        else:
            copies[k - 1].wait_recv()
        held = piece(source_of(k), here.r)
        over = remote(held, held, f_s.at[0, k], f_r.at[0, k], ypeer)
        over.start()
        beside = remote(held, held, f_s.at[1, k], f_r.at[1, k], here.core)
        beside.start()
        far.append(over)
        sends.append(beside)

    def finish(k):
        far[k].wait_recv()
        held = piece(source_of(k), yr)
        beside = remote(held, held, f_s.at[2, k], f_r.at[2, k], here.core)
        beside.start()
        sends.append(beside)

    factor, first_scale, second_scale = numbers[0], numbers[1], numbers[2]
    puts = {}
    lag = 5
    for t in range(chunks):
        spot = t % 2
        for ld in loads[t]:
            ld.wait()
        if t >= 2:
            for cp in puts[t - 2]:
                cp.wait()

        @pl.loop(0, -(-extent(t) // strip))
        def _(i, spot=spot):
            at = pl.ds(pl.multiple_of(i * strip, strip), strip)
            grad = factor * fetched[spot, 0, at]
            old = fetched[spot, 1, at]
            moment = beta_first * fetched[spot, 2, at] + (1.0 - beta_first) * grad
            second = beta_second * fetched[spot, 3, at] + (1.0 - beta_second) * grad * grad
            step = moment * first_scale / (jnp.sqrt(second * second_scale) + adam_epsilon)
            value = old - step_rate * (step + weight_decay * old)
            made[spot, 0, at] = value
            made[spot, 1, at] = moment
            made[spot, 2, at] = second
            made_low[spot, at] = value.astype(bf16)

        puts[t] = store(t)
        if t + 2 < chunks:
            loads[t + 2] = fetch(t + 2)
        if t < n:
            forward(t)
        if lag <= t < n + lag:
            finish(t - lag)
    for k in range(chunks, n):
        forward(k)
    for k in range(max(0, chunks - lag), n):
        finish(k)
    for t in range(max(0, chunks - 2), chunks):
        for cp in puts[t]:
            cp.wait()
    for cp in copies + far:
        cp.wait_send()
    for cp in sends:
        cp.wait()


def return_slots(mesh_sizes, cid, x, numbers, grad_table, embed, embed_m, embed_v):
    n_rep, n = mesh_sizes
    _, cap, rows, width = x.shape
    vocab = embed.shape[0]
    chunk = 432
    dma = pltpu.SemaphoreType.DMA
    return pl.pallas_call(
        partial(return_kernel, n_rep, n, vocab),
        out_shape=[jax.ShapeDtypeStruct((n, cap, 4, rows, width), x.dtype)]
        + [jax.ShapeDtypeStruct(embed.shape, f32)] * 3
        + [jax.ShapeDtypeStruct(embed.shape, bf16)],
        in_specs=[VMEM, pl.BlockSpec(memory_space=pltpu.SMEM)] + [ANY] * 4,
        out_specs=[ANY] * 5,
        scratch_shapes=[
            pltpu.VMEM((2, 4, chunk, width), f32),
            pltpu.VMEM((2, 3, chunk, width), f32),
            pltpu.VMEM((2, chunk, width), bf16),
            dma,
            dma((n - 1,)),
            dma((n - 1,)),
            dma((3, n)),
            dma((3, n)),
            dma((2, 4)),
            dma((2, 4)),
        ],
        compiler_params=params(cid, 48 << 20),
        name="return_slots",
    )(x, numbers, grad_table, embed, embed_m, embed_v)


def layer_norm(inputs, gain_row):
    centre = inputs - jnp.mean(inputs, axis=-1, keepdims=True)
    spread = jnp.mean(centre * centre, axis=-1, keepdims=True)
    return centre * lax.rsqrt(spread + norm_epsilon) * gain_row


def adam_moments(moment_old, second_old, gradient, first_fix, second_fix):
    moment_new = beta_first * moment_old + (1.0 - beta_first) * gradient
    second_new = beta_second * second_old + (1.0 - beta_second) * gradient * gradient
    step_value = moment_new / first_fix / (jnp.sqrt(second_new / second_fix) + adam_epsilon)
    return (moment_new, second_new, step_value)


def head_slopes(head_count):
    return 2.0 ** (-8.0 * (jnp.arange(head_count, dtype=f32) + 1.0) / head_count)


NT = (((1,), (1,)), ((), ()))
TN = (((0,), (0,)), ((), ()))
masked_distance = 1e33


def mm(a, b, dims=None):
    if dims is None:
        return jnp.dot(a, b, preferred_element_type=f32)
    return lax.dot_general(a, b, dims, preferred_element_type=f32)


def norm_parts(x):
    centre = x - jnp.mean(x, axis=-1, keepdims=True)
    spread = jnp.mean(centre * centre, axis=-1, keepdims=True)
    rstd = lax.rsqrt(spread + norm_epsilon)
    return centre * rstd, rstd


def norm_back(x, gain, grad):
    hat, rstd = norm_parts(x)
    inner = grad * gain
    back = inner - jnp.mean(inner, axis=-1, keepdims=True) - hat * jnp.mean(inner * hat, axis=-1, keepdims=True)
    return rstd * back, grad * hat


def fold8(x):
    total = x[:8]
    for k in range(1, x.shape[0] // 8):
        total = total + x[k * 8 : k * 8 + 8]
    return total


def pair_bias(seg_row, seg_col, bias):
    length = bias.shape[0]
    i = lax.broadcasted_iota(jnp.int32, (length, length), 0)
    j = lax.broadcasted_iota(jnp.int32, (length, length), 1)
    apart = jnp.abs(i - j).astype(f32)
    bias[...] = jnp.where(seg_col == seg_row, apart, masked_distance)


def attend_kernel(slopes, x, gain, w, seg_row, seg_col, y, a, qkv, o, lse, bias):
    pair = pl.program_id(1)
    length, width = x.shape
    half = width // HEADS
    two = 2 * half
    rows = ROWS

    @pl.when(pair == 0)
    def _():
        pair_bias(seg_row[0], seg_col[0], bias)

        @pl.loop(0, length // rows)
        def _(i):
            at = pl.ds(pl.multiple_of(i * rows, rows), rows)
            hat, _ = norm_parts(x[at])
            low = (hat * gain[...]).astype(bf16)
            a[at] = low
            for k in range(3):
                part = mm(low, w[k])
                if k == 0:
                    part = part.astype(bf16).astype(f32) * half ** (-0.5)
                qkv[at, k * width : (k + 1) * width] = part.astype(bf16)

    lanes = pl.ds(pl.multiple_of(pair * two, two), two)
    q = qkv[:, pl.ds(pl.multiple_of(pair * two, two), two)]
    k = qkv[:, pl.ds(pl.multiple_of(width + pair * two, two), two)]
    v = qkv[:, pl.ds(pl.multiple_of(2 * width + pair * two, two), two)]
    v_t = v.astype(f32).T.astype(bf16)
    left = lax.broadcasted_iota(jnp.int32, (length, two), 1) < half
    zero = jnp.zeros_like(q)
    out = []
    for e in range(2):
        slope = slopes[2 * pair + e]
        q_e = jnp.where(left, q, zero) if e == 0 else jnp.where(left, zero, q)
        s = mm(k, q_e, NT) - slope * bias[...]
        top = jnp.max(s, axis=0, keepdims=True)
        p = jnp.exp(s - top)
        total = jnp.sum(p, axis=0, keepdims=True)
        low = (p * (1.0 / total)).astype(bf16)
        out.append(mm(v_t, low))
        lse[0, pl.ds(2 * pair + e, 1)] = top + jnp.log(total)
    upper = lax.broadcasted_iota(jnp.int32, (two, length), 0) < half
    o[:, lanes] = jnp.where(upper, out[0], out[1]).T.astype(bf16)

    @pl.when(pair == pl.num_programs(1) - 1)
    def _():
        @pl.loop(0, length // rows)
        def _(i):
            at = pl.ds(pl.multiple_of(i * rows, rows), rows)
            y[at] = x[at] + mm(o[at], w[3])


def attend(x, gain, weights, layer, seg):
    packs, length = seg.shape
    tokens, width = x.shape
    per_layer4 = weights.shape[0] // LAYERS // 4
    slopes = head_slopes(HEADS)
    whole = lambda shape: pl.BlockSpec(shape, lambda m, p: (m,) + (0,) * (len(shape) - 1))
    fixed = lambda shape, at: pl.BlockSpec(shape, lambda m, p: at)
    return pl.pallas_call(
        attend_kernel,
        grid=(packs, HEADS // 2),
        in_specs=[
            pl.BlockSpec(memory_space=pltpu.SMEM),
            whole((length, width)),
            fixed((1, width), (0, 0)),
            fixed((4, width, width), (per_layer4 * layer, 0, 0)),
            whole((1, 1, length)),
            whole((1, length, 1)),
        ],
        out_specs=[
            whole((length, width)),
            whole((length, width)),
            whole((length, 3 * width)),
            whole((length, width)),
            whole((1, HEADS, length)),
        ],
        out_shape=[
            jax.ShapeDtypeStruct((tokens, width), f32),
            jax.ShapeDtypeStruct((tokens, width), bf16),
            jax.ShapeDtypeStruct((tokens, 3 * width), bf16),
            jax.ShapeDtypeStruct((tokens, width), bf16),
            jax.ShapeDtypeStruct((packs, HEADS, length), f32),
        ],
        scratch_shapes=[pltpu.VMEM((length, length), f32)],
        compiler_params=pltpu.CompilerParams(vmem_limit_bytes=48 << 20),
        name="attend",
    )(slopes, x, gain.reshape(1, width), weights, seg.reshape(packs, 1, length), seg.reshape(packs, length, 1))


def attend_back_kernel(
    slopes, dx, x, gain, w, a, qkv, o, lse, seg_row, seg_col, new, dgain, gw, bias, do, dqkv, acc
):
    pack, pair = pl.program_id(0), pl.program_id(1)
    length, width = x.shape
    half = width // HEADS
    two = 2 * half
    rows = ROWS

    @pl.when(pair == 0)
    def _():
        pair_bias(seg_row[0], seg_col[0], bias)

        @pl.loop(0, length // rows)
        def _(i):
            at = pl.ds(pl.multiple_of(i * rows, rows), rows)
            do[at] = mm(dx[at].astype(bf16), w[3], NT).astype(bf16)

        part = mm(o[...], dx[...].astype(bf16), TN)

        @pl.when(pack == 0)
        def _():
            acc[3] = part

        @pl.when(pack > 0)
        def _():
            acc[3] += part

    lanes = [pl.ds(pl.multiple_of(n * width + pair * two, two), two) for n in range(3)]
    q, k, v = [qkv[:, at] for at in lanes]
    do_p = do[:, lanes[0]]
    k_t = k.astype(f32).T.astype(bf16)
    left = lax.broadcasted_iota(jnp.int32, (length, two), 1) < half
    upper = lax.broadcasted_iota(jnp.int32, (two, length), 0) < half
    zero = jnp.zeros_like(q)
    dq, dk, dv = [], [], []
    for e in range(2):
        slope = slopes[2 * pair + e]
        keep = (lambda t: jnp.where(left, t, zero)) if e == 0 else (lambda t: jnp.where(left, zero, t))
        s = mm(k, keep(q), NT) - slope * bias[...]
        p = jnp.exp(s - lse[0, pl.ds(2 * pair + e, 1)])
        dp = mm(v, keep(do_p), NT)
        inner = jnp.sum(p * dp, axis=0, keepdims=True)
        ds = (p * (dp - inner)).astype(bf16)
        dv.append(mm(p.astype(bf16), do_p))
        dk.append(mm(ds, q))
        dq.append(mm(k_t, ds))
    dqkv[:, lanes[0]] = (jnp.where(upper, dq[0], dq[1]).T * half ** (-0.5)).astype(bf16)
    dqkv[:, lanes[1]] = jnp.where(left, dk[0], dk[1]).astype(bf16)
    dqkv[:, lanes[2]] = jnp.where(left, dv[0], dv[1]).astype(bf16)

    @pl.when(pair == pl.num_programs(1) - 1)
    def _():
        def chunk(i, total):
            at = pl.ds(pl.multiple_of(i * rows, rows), rows)
            da = mm(dqkv[at, :width], w[0], NT)
            da = da + mm(dqkv[at, width : 2 * width], w[1], NT)
            da = da + mm(dqkv[at, 2 * width :], w[2], NT)
            back, extra = norm_back(x[at], gain[...], da)
            new[at] = dx[at] + back
            return total + fold8(extra)

        dgain[0] = lax.fori_loop(0, length // rows, chunk, jnp.zeros((8, width), f32))
        for n in range(3):
            part = mm(a[...], dqkv[:, n * width : (n + 1) * width], TN)

            @pl.when(pack == 0)
            def _(part=part, n=n):
                acc[n] = part

            @pl.when(pack > 0)
            def _(part=part, n=n):
                acc[n] += part

    @pl.when((pair == pl.num_programs(1) - 1) & (pack == pl.num_programs(0) - 1))
    def _():
        for n in range(4):
            gw[n] = acc[n].astype(bf16)


def attend_back(dx, x, gain, weights, layer, seg, kept):
    a, qkv, o, lse = kept
    packs, length = seg.shape
    tokens, width = x.shape
    per_layer4 = weights.shape[0] // LAYERS // 4
    whole = lambda shape: pl.BlockSpec(shape, lambda m, p: (m,) + (0,) * (len(shape) - 1))
    fixed = lambda shape, at: pl.BlockSpec(shape, lambda m, p: at)
    return pl.pallas_call(
        attend_back_kernel,
        grid=(packs, HEADS // 2),
        in_specs=[
            pl.BlockSpec(memory_space=pltpu.SMEM),
            whole((length, width)),
            whole((length, width)),
            fixed((1, width), (0, 0)),
            fixed((4, width, width), (per_layer4 * layer, 0, 0)),
            whole((length, width)),
            whole((length, 3 * width)),
            whole((length, width)),
            whole((1, HEADS, length)),
            whole((1, 1, length)),
            whole((1, length, 1)),
        ],
        out_specs=[
            whole((length, width)),
            whole((1, 8, width)),
            fixed((4, width, width), (0, 0, 0)),
        ],
        out_shape=[
            jax.ShapeDtypeStruct((tokens, width), f32),
            jax.ShapeDtypeStruct((packs, 8, width), f32),
            jax.ShapeDtypeStruct((4, width, width), bf16),
        ],
        scratch_shapes=[
            pltpu.VMEM((length, length), f32),
            pltpu.VMEM((length, width), bf16),
            pltpu.VMEM((length, 3 * width), bf16),
            pltpu.VMEM((4, width, width), f32),
        ],
        compiler_params=pltpu.CompilerParams(vmem_limit_bytes=56 << 20),
        name="attend_back",
    )(
        head_slopes(HEADS),
        dx,
        x,
        gain.reshape(1, width),
        weights,
        a,
        qkv,
        o,
        lse,
        seg.reshape(packs, 1, length),
        seg.reshape(packs, length, 1),
    )


ROWS = 512
gelu_c = math.sqrt(2.0 / math.pi)


def feed_kernel(x, gain, wg, wu, wd, y, f, gate, up):
    k = pl.program_id(0)
    tokens = x.shape[0]
    rows = ROWS

    @pl.loop(0, tokens // rows)
    def _(i):
        at = pl.ds(pl.multiple_of(i * rows, rows), rows)

        @pl.when(k == 0)
        def _():
            hat, _ = norm_parts(x[at])
            f[at] = (hat * gain[...]).astype(bf16)
            y[at] = x[at]

        low = f[at]
        g = mm(low, wg[0]).astype(bf16)
        u = mm(low, wu[0]).astype(bf16)
        gate[0, at] = g
        up[0, at] = u
        g, u = g.astype(f32), u.astype(f32)
        cdf = 0.5 * (1.0 + jnp.tanh(gelu_c * (g + 0.044715 * (g * g * g))))
        hidden = (g * cdf * u).astype(bf16)
        y[at] += mm(hidden, wd[0])


def feed(x, gain, weights, layer):
    tokens, width = x.shape
    per_layer = weights.shape[0] // LAYERS
    pieces = FF // width
    fixed = lambda shape: pl.BlockSpec(shape, lambda k: (0,) * len(shape))
    block = lambda skip: pl.BlockSpec((1, width, width), lambda k: (per_layer * layer + skip + k, 0, 0))
    each = pl.BlockSpec((1, tokens, width), lambda k: (k, 0, 0))
    return pl.pallas_call(
        feed_kernel,
        grid=(pieces,),
        in_specs=[fixed((tokens, width)), fixed((1, width)), block(4), block(4 + pieces), block(4 + 2 * pieces)],
        out_specs=[fixed((tokens, width)), fixed((tokens, width)), each, each],
        out_shape=[
            jax.ShapeDtypeStruct((tokens, width), f32),
            jax.ShapeDtypeStruct((tokens, width), bf16),
            jax.ShapeDtypeStruct((pieces, tokens, width), bf16),
            jax.ShapeDtypeStruct((pieces, tokens, width), bf16),
        ],
        compiler_params=pltpu.CompilerParams(vmem_limit_bytes=48 << 20),
        name="feed",
    )(x, gain.reshape(1, width), weights, weights, weights)


def feed_back_kernel(dx, x, gain, wg, wu, wd, f, gate, up, new, dgain, gg, gu, gd, f_t, dz, hid, dg, du):
    k = pl.program_id(0)
    tokens, width = x.shape
    rows = ROWS
    last = pl.num_programs(0) - 1

    @pl.when(k == 0)
    def _():
        @pl.loop(0, tokens // rows)
        def _(i):
            at = pl.ds(pl.multiple_of(i * rows, rows), rows)
            f_t[:, at] = f[at].astype(f32).T.astype(bf16)
            dz[at] = dx[at].astype(bf16)
            new[at] = jnp.zeros((rows, width), f32)

    def chunk(i, total):
        at = pl.ds(pl.multiple_of(i * rows, rows), rows)
        dh = mm(dz[at], wd[0], NT)
        g, u = gate[0, at].astype(f32), up[0, at].astype(f32)
        square = g * g
        t = jnp.tanh(gelu_c * (g + 0.044715 * (square * g)))
        cdf = 0.5 * (1.0 + t)
        act = g * cdf
        slope = cdf + 0.5 * g * (1.0 - t * t) * (gelu_c * (1.0 + 3 * 0.044715 * square))
        hid[at] = (act * u).astype(bf16)
        dgate = (dh * u * slope).astype(bf16)
        dup = (dh * act).astype(bf16)
        dg[at] = dgate
        du[at] = dup
        new[at] += mm(dgate, wg[0], NT) + mm(dup, wu[0], NT)
        return total

    lax.fori_loop(0, tokens // rows, chunk, 0)
    gg[0] = mm(f_t[...], dg[...]).astype(bf16)
    gu[0] = mm(f_t[...], du[...]).astype(bf16)
    gd[0] = mm(hid[...], dz[...], TN).astype(bf16)

    @pl.when(k == last)
    def _():
        def finish(i, total):
            at = pl.ds(pl.multiple_of(i * rows, rows), rows)
            back, extra = norm_back(x[at], gain[...], new[at])
            new[at] = dx[at] + back
            return total + fold8(extra)

        dgain[...] = lax.fori_loop(0, tokens // rows, finish, jnp.zeros((8, width), f32))


def feed_back(dx, x, gain, weights, layer, kept):
    f, gate, up = kept
    tokens, width = x.shape
    per_layer = weights.shape[0] // LAYERS
    pieces = FF // width
    fixed = lambda shape: pl.BlockSpec(shape, lambda k: (0,) * len(shape))
    block = lambda skip: pl.BlockSpec((1, width, width), lambda k: (per_layer * layer + skip + k, 0, 0))
    each = pl.BlockSpec((1, tokens, width), lambda k: (k, 0, 0))
    grad = pl.BlockSpec((1, width, width), lambda k: (k, 0, 0))
    return pl.pallas_call(
        feed_back_kernel,
        grid=(pieces,),
        in_specs=[
            fixed((tokens, width)),
            fixed((tokens, width)),
            fixed((1, width)),
            block(4),
            block(4 + pieces),
            block(4 + 2 * pieces),
            fixed((tokens, width)),
            each,
            each,
        ],
        out_specs=[fixed((tokens, width)), fixed((8, width)), grad, grad, grad],
        out_shape=[
            jax.ShapeDtypeStruct((tokens, width), f32),
            jax.ShapeDtypeStruct((8, width), f32),
        ]
        + [jax.ShapeDtypeStruct((pieces, width, width), bf16)] * 3,
        scratch_shapes=[
            pltpu.VMEM((width, tokens), bf16),
            pltpu.VMEM((tokens, width), bf16),
            pltpu.VMEM((tokens, width), bf16),
            pltpu.VMEM((tokens, width), bf16),
            pltpu.VMEM((tokens, width), bf16),
        ],
        compiler_params=pltpu.CompilerParams(vmem_limit_bytes=56 << 20),
        name="feed_back",
    )(dx, x, gain.reshape(1, width), weights, weights, weights, f, gate, up)


def two_parts(x):
    top = x.astype(bf16)
    return top, (x - top.astype(f32)).astype(bf16)


def mm3(a, b, dims=None):
    (a1, a2), (b1, b2) = a, b
    return mm(a1, b1, dims) + (mm(a1, b2, dims) + mm(a2, b1, dims))


def turn_kernel(scalars, numbers, left, right, some, grad, m, v, m_new, v_new, turned):
    slot = pl.program_id(0)
    factor, first_fix, second_fix = numbers[0], numbers[1], numbers[2]
    bases = two_parts(right[0])
    left_top, left_rest = two_parts(left[0])
    rotated = mm(left_top, grad[0], TN) + mm(left_rest, grad[0], TN)
    rotated = factor * mm3(two_parts(rotated), bases)
    moment, second, step = adam_moments(m[0], v[0], rotated, first_fix, second_fix)
    live = scalars[1 + slot] > 0
    m_new[0] = jnp.where(live, moment, m[0])
    v_new[0] = jnp.where(live, second, v[0])
    groups, _, rows, width = turned.shape
    rows_here = some[...].reshape(groups * rows, width)
    out = mm3(two_parts(rows_here), two_parts(step))
    out = mm3(two_parts(out), bases, NT)
    turned[...] = out.astype(turned.dtype).reshape(turned.shape)


def turn_slots(replica, live, numbers, left, right, grads, m, v):
    cap, width, _ = left.shape
    groups = width // 64
    scalars = jnp.concatenate([replica.reshape(1), live.astype(jnp.int32)])
    view = left.reshape(cap, groups, 4, 16, width)
    whole = pl.BlockSpec((1, width, width), lambda s, scalars: (s, 0, 0))
    grid_spec = pltpu.PrefetchScalarGridSpec(
        num_scalar_prefetch=1,
        grid=(cap,),
        in_specs=[
            pl.BlockSpec(memory_space=pltpu.SMEM),
            whole,
            whole,
            pl.BlockSpec((1, groups, 1, 16, width), lambda s, scalars: (s, 0, scalars[0], 0, 0)),
            whole,
            whole,
            whole,
        ],
        out_specs=[whole, whole, pl.BlockSpec((groups, 1, 16, width), lambda s, scalars: (0, s, 0, 0))],
    )
    return pl.pallas_call(
        turn_kernel,
        grid_spec=grid_spec,
        out_shape=[
            jax.ShapeDtypeStruct(m.shape, f32),
            jax.ShapeDtypeStruct(v.shape, f32),
            jax.ShapeDtypeStruct((groups, cap, 16, width), bf16),
        ],
        compiler_params=pltpu.CompilerParams(vmem_limit_bytes=56 << 20),
        name="turn_slots",
    )(scalars, numbers, left, right, view, grads, m, v)


def head_kernel(
    n_rep, n, vocab, tile, x_ref, e_ref, label_ref, picked_ref, table_ref, loss_ref,
    table, rows_all, logits, stats, shared, held, got,
    load_s, ring_s, ring_r, stat_s, stat_r, back_s, back_r,
):
    here = Place(n_rep, n)
    me = here.f
    others = [lax.rem(me + k, n) for k in range(1, n)]
    enter([(here.r, o) for o in others])
    picks, width = x_ref.shape
    half = picks // 2
    tiles = table.shape[0] // tile
    far = n // 2
    load = pltpu.make_async_copy(e_ref, table, load_s)
    load.start()
    sends = []
    waiting = {}

    def hop(way, s):
        origin = here.at(-s if way == 0 else s)
        window = pl.ds(way * half, half) if s == far - 1 else pl.ds(0, picks)
        src = x_ref if s == 0 else rows_all.at[origin, window]
        cp = remote(
            src,
            rows_all.at[origin, window],
            ring_s.at[way, s],
            ring_r.at[way, s],
            here.next if way == 0 else here.prev,
        )
        cp.start()
        sends.append(cp)
        waiting[way] = cp

    def columns(t, count):
        return t * tile + lax.broadcasted_iota(jnp.int32, (count, tile), 1)

    def span(t):
        return pl.ds(pl.multiple_of(t * tile, tile), tile)

    def stack(ref, origins):
        return jnp.concatenate([ref[o] for o in origins], axis=0)

    def scores_of(origins, t):
        return jnp.concatenate([logits[o, :, span(t)] for o in origins], axis=0)

    def piece(value, i):
        return value[i * picks : (i + 1) * picks]

    def fold(x, join):
        out = x[:, :128]
        for k in range(1, tile // 128):
            out = join(out, x[:, k * 128 : (k + 1) * 128])
        return out

    def forward(*origins):
        rows, label = stack(rows_all, origins), stack(label_ref, origins)
        count = rows.shape[0]

        def product(t, top):
            scores = mm(rows, table[span(t)], NT)
            scores = jnp.where(columns(t, count) < vocab, scores, masked_score)
            for i, o in enumerate(origins):
                logits[o, :, span(t)] = piece(scores, i)
            return jnp.maximum(top, fold(scores, jnp.maximum))

        top = lax.fori_loop(0, tiles, product, jnp.full((count, 128), masked_score, f32))
        top = jnp.max(top, axis=1, keepdims=True)

        def weigh(t, sums):
            total, target = sums
            scores = scores_of(origins, t)
            total = total + fold(jnp.exp(scores - top), jnp.add)
            hit = jnp.where(columns(t, count) == label, scores, 0.0)
            return total, target + fold(hit, jnp.add)

        zero = jnp.zeros((count, 128), f32)
        total, target = lax.fori_loop(0, tiles, weigh, (zero, zero))
        log_sum = top + jnp.log(jnp.sum(total, axis=1, keepdims=True))
        target = jnp.sum(target, axis=1, keepdims=True)
        lane = lax.broadcasted_iota(jnp.int32, (count, 128), 1)
        both = jnp.where(lane == 0, log_sum, target).T
        for i, o in enumerate(origins):
            stats[pl.ds(o, 1)] = both[0:1, i * picks : (i + 1) * picks]
            stats[pl.ds(n + o, 1)] = both[1:2, i * picks : (i + 1) * picks]

    rows_all[me] = x_ref[...]
    for way in range(2):
        hop(way, 0)
    load.wait()
    forward(me)
    for s in range(far):
        for way in range(2):
            waiting[way].wait_recv()
            if s < far - 1:
                hop(way, s + 1)
        if s < far - 1:
            forward(here.at(-s - 1), here.at(s + 1))
        else:
            forward(here.at(far))

    moves = []
    for k, o in enumerate(others):
        cp = remote(stats, shared.at[me], stat_s.at[k], stat_r.at[k], (here.r, o))
        cp.start()
        moves.append(cp)
    shared[me] = stats[...]
    table_ref[...] = jnp.zeros(table_ref.shape, f32)
    for cp in moves:
        cp.wait_recv()
    top = shared[0, :n]
    for k in range(1, n):
        top = jnp.maximum(top, shared[k, :n])
    total = jnp.exp(shared[0, :n] - top)
    target = shared[0, n:]
    for k in range(1, n):
        total = total + jnp.exp(shared[k, :n] - top)
        target = target + shared[k, n:]
    log_sum = top + jnp.log(total)
    for cp in moves:
        cp.wait_send()
    stats[:n] = log_sum
    stats[n:] = log_sum - target
    mine = stats[pl.ds(n + me, 1)]
    loss_ref[...] = jnp.broadcast_to(jnp.sum(mine, axis=1, keepdims=True), loss_ref.shape)

    def backward(*origins):
        rows, label = stack(rows_all, origins), stack(label_ref, origins)
        count = rows.shape[0]
        norm = [jnp.broadcast_to(stats[pl.ds(o, 1)], (128, picks)) for o in origins]
        norm = jnp.concatenate(norm, axis=1).T

        def product(t, out):
            scores = scores_of(origins, t)
            parts = [jnp.exp(scores[:, k * 128 : (k + 1) * 128] - norm) for k in range(tile // 128)]
            soft = jnp.concatenate(parts, axis=1)
            grad = (soft - jnp.where(columns(t, count) == label, 1.0, 0.0)).astype(bf16)
            table_ref[span(t)] += mm(grad, rows, TN)
            return out + mm(grad, table[span(t)])

        return lax.fori_loop(0, tiles, product, jnp.zeros((count, width), f32))

    ring = {}

    def lane_send(way, h, s, value):
        before = ring.get((way, h, s - 1))
        if before is not None:
            before.wait_recv()
            value = value + got[way, h, s - 1].astype(f32)
        held[way, h, s] = value.astype(bf16)
        cp = remote(
            held.at[way, h, s],
            got.at[way, h, s],
            back_s.at[way, h, s],
            back_r.at[way, h, s],
            here.next if way == 0 else here.prev,
        )
        cp.start()
        ring[way, h, s] = cp

    out = backward(here.at(far))
    lane_send(0, 0, 0, out[:half])
    lane_send(1, 1, 0, out[half:])
    for s in range(1, far):
        d = far - s
        out = backward(here.at(d), here.at(-d))
        for turn in range(2):
            for way in range(2):
                h = way if turn == 1 else 1 - way
                lane_send(way, h, s, piece(out, way)[h * half : (h + 1) * half])
    out = backward(me)
    for h in range(2):
        total = out[h * half : (h + 1) * half]
        for way in range(2):
            ring[way, h, far - 1].wait_recv()
            total = total + got[way, h, far - 1].astype(f32)
        picked_ref[pl.ds(h * half, half)] = total
    for cp in sends + list(ring.values()):
        cp.wait_send()


def head_step(mesh_sizes, cid, picked, table, labels, vocab):
    n_rep, n = mesh_sizes
    picks, width = picked.shape
    padded = table.shape[0]
    far = n // 2
    dma = pltpu.SemaphoreType.DMA
    return pl.pallas_call(
        partial(head_kernel, n_rep, n, vocab, 768),
        out_shape=[
            jax.ShapeDtypeStruct((picks, width), f32),
            jax.ShapeDtypeStruct((padded, width), f32),
            jax.ShapeDtypeStruct((8, 128), f32),
        ],
        in_specs=[VMEM, ANY, VMEM],
        out_specs=[VMEM, VMEM, VMEM],
        scratch_shapes=[
            pltpu.VMEM((padded, width), bf16),
            pltpu.VMEM((n, picks, width), bf16),
            pltpu.VMEM((n, picks, padded), f32),
            pltpu.VMEM((2 * n, picks), f32),
            pltpu.VMEM((n, 2 * n, picks), f32),
            pltpu.VMEM((2, 2, far, picks // 2, width), bf16),
            pltpu.VMEM((2, 2, far, picks // 2, width), bf16),
            dma,
            dma((2, far)),
            dma((2, far)),
            dma((n - 1,)),
            dma((n - 1,)),
            dma((2, 2, far)),
            dma((2, 2, far)),
        ],
        compiler_params=params(cid, 60 << 20),
        name="head_step",
    )(picked, table, labels.reshape(n, picks, 1))


class Transport:
    def __init__(self, n_rep, n_fsdp, shard_rows):
        self.sizes = (n_rep, n_fsdp)
        self.kernels = n_rep == 4 and n_fsdp == 8 and shard_rows == 64

    def open(self, cid, shard, table, ids, owner, local, facts, gains, padded):
        if self.kernels:
            return open_step(self.sizes, cid, shard, table, ids, owner, local, facts, gains, padded)
        tokens = ids.shape[0]
        groups = self.sizes[1]
        index = jnp.arange(tokens, dtype=jnp.int32)
        first_at = jnp.min(jnp.where(ids[:, None] == ids[None, :], index[None, :], tokens), axis=1)
        is_first = first_at == index
        ahead = is_first[None, :] & (owner[:, None] == owner[None, :]) & (index[None, :] < first_at[:, None])
        rank = jnp.sum(ahead.astype(jnp.int32), axis=1)
        facts = facts.at[facts.shape[0] - 1].set(jnp.max(rank) + 1)
        slot = jnp.where(is_first & (rank < CAPACITY), owner * CAPACITY + rank, -1)
        slot_index = jnp.arange(groups * CAPACITY, dtype=jnp.int32)
        wanted = jnp.sum(jnp.where(slot[None, :] == slot_index[:, None], local[None, :], 0), axis=1)
        wanted = wanted.reshape(groups, 1, CAPACITY)
        asked = lax.all_to_all(wanted, "fsdp", split_axis=0, concat_axis=0, tiled=True)
        low = jnp.pad(table.astype(bf16), ((0, padded - table.shape[0]), (0, 0)))
        rows = jnp.take(low, asked.reshape(-1), axis=0).reshape(groups, CAPACITY, table.shape[1])
        return (
            lax.all_gather(shard, "fsdp", axis=1, tiled=True),
            self.spread(cid, rows),
            asked,
            lax.all_gather(facts, "fsdp"),
            lax.all_gather(gains, "fsdp"),
            lax.pmax(facts, ("rep", "fsdp")),
            rank,
            first_at,
            low,
        )

    def spread(self, cid, x):
        if self.kernels:
            return group_exchange(self.sizes, cid, x, True)
        return lax.all_to_all(x, "fsdp", split_axis=0, concat_axis=0, tiled=True)


def body(
    token_ids,
    segment_ids,
    masked_pos,
    labels,
    blocks,
    gains,
    embed,
    embed_m,
    embed_v,
    gains_m,
    gains_v,
    soap_m,
    soap_v,
    left_basis,
    right_basis,
    block_slots,
    step_count,
):
    groups = lax.axis_size("fsdp")
    replicas = lax.axis_size("rep")
    member = lax.axis_index("fsdp")
    replica = lax.axis_index("rep")
    micro_count = token_ids.shape[0]
    pack_length = token_ids.shape[2]
    pick_count = masked_pos.shape[2]
    vocab_rows, model_width = embed.shape
    block_count, shard_rows, _ = blocks.shape
    gain_count = gains.shape[0]
    tokens = micro_count * pack_length
    picks = micro_count * pick_count
    move = Transport(replicas, groups, shard_rows)
    padded_rows = -(-vocab_rows // 768) * 768

    ids = token_ids.reshape(tokens)
    index = jnp.arange(tokens, dtype=jnp.int32)
    owner = ids // vocab_rows
    local = ids - owner * vocab_rows
    my_labels = labels.reshape(picks // 128, 128)
    facts = jnp.pad(my_labels, ((0, 8 - my_labels.shape[0]), (0, 0)))
    gain_pad = jnp.pad(gains, ((0, 8 - gain_count), (0, 128 - gains.shape[1])))
    full_blocks, rows, asked, group_facts, gain_rows, most_facts, rank, first_at, table_low = move.open(
        0, blocks.astype(bf16), embed, ids, owner, local, facts, gain_pad, padded_rows
    )
    rank, is_first = rank.reshape(tokens), first_at.reshape(tokens) == index
    slots = groups * CAPACITY
    most_rounds = (tokens + CAPACITY - 1) // CAPACITY
    slot_index = jnp.arange(slots, dtype=jnp.int32)

    def slot_of(k):
        here = rank - k * CAPACITY
        return jnp.where((here >= 0) & (here < CAPACITY), owner * CAPACITY + here, -1)

    def wanted_in(slot):
        wanted = jnp.where((slot[None, :] == slot_index[:, None]) & is_first[None, :], local[None, :], 0)
        return jnp.sum(wanted, axis=1).reshape(groups, 1, CAPACITY)

    def placed(slot, rows):
        chosen = (slot[:, None] == slot_index[None, :]).astype(bf16)
        return jnp.dot(chosen, rows.reshape(slots, model_width), preferred_element_type=f32)

    slot = slot_of(0)
    rounds = (most_facts[7, 0] + CAPACITY - 1) // CAPACITY
    all_labels = group_facts[:, : picks // 128].reshape(groups * picks)
    gain_rows = gain_rows[:, :gain_count, : gains.shape[1]].transpose(1, 0, 2).reshape(gain_count, model_width)
    gain_rows = lax.reduce_precision(gain_rows, exponent_bits=8, mantissa_bits=7)
    embedded = placed(slot, rows)
    asked_all = jnp.zeros((most_rounds, slots), jnp.int32).at[0].set(asked.reshape(slots))

    def look(state):
        k, rows_so_far, asked_all = state
        slot = slot_of(k)
        asked = move.spread(1, wanted_in(slot))
        asked_all = lax.dynamic_update_index_in_dim(asked_all, asked.reshape(slots), k, 0)
        rows = jnp.take(table_low, asked.reshape(slots), axis=0).reshape(groups, CAPACITY, model_width)
        return k + 1, rows_so_far + placed(slot, move.spread(2, rows)), asked_all

    _, embedded, asked_all = lax.while_loop(lambda s: s[0] < rounds, look, (jnp.int32(1), embedded, asked_all))

    segments = segment_ids.reshape(micro_count, pack_length)
    stream, first_pull = jax.vjp(layer_norm, embedded, gain_rows[0])
    saved_layers = []
    for layer in range(LAYERS):
        middle, *attention_kept = attend(stream, gain_rows[1 + 2 * layer], full_blocks, layer, segments)
        after, *feed_kept = feed(middle, gain_rows[2 + 2 * layer], full_blocks, layer)
        saved_layers.append((stream, attention_kept, middle, feed_kept))
        stream = after
    final_rows, final_pull = jax.vjp(layer_norm, stream, gain_rows[gain_count - 1])

    positions = masked_pos.reshape(micro_count, pick_count)
    flat_positions = (positions + jnp.arange(micro_count, dtype=jnp.int32)[:, None] * pack_length).reshape(picks)
    picked = jnp.take(final_rows, flat_positions, axis=0).astype(bf16)
    label_local = all_labels - member * vocab_rows
    label_local = jnp.where((label_local >= 0) & (label_local < vocab_rows), label_local, -1)
    if move.kernels:
        grad_picked, grad_table, loss_local = head_step(
            move.sizes, 4, picked, table_low, label_local.reshape(groups, picks), vocab_rows
        )
        loss_local = loss_local[0, 0]
    else:
        all_picked = lax.all_gather(picked, "fsdp", tiled=True)
        logits = jnp.einsum("td,vd->tv", all_picked, table_low[:vocab_rows], preferred_element_type=f32)
        top_value = jnp.max(logits, axis=-1)
        exp_total = jnp.sum(jnp.exp(logits - top_value[:, None]), axis=-1)
        label_hits = jnp.arange(vocab_rows, dtype=jnp.int32)[None, :] == label_local[:, None]
        target = jnp.sum(jnp.where(label_hits, logits, 0.0), axis=-1)
        stats = lax.all_gather(jnp.stack([top_value, exp_total, target]), "fsdp")
        top_all = jnp.max(stats[:, 0], axis=0)
        total_all = jnp.sum(stats[:, 1] * jnp.exp(stats[:, 0] - top_all[None]), axis=0)
        target_all = jnp.sum(stats[:, 2], axis=0)
        entropy = top_all + jnp.log(total_all) - target_all
        loss_local = jnp.sum(lax.dynamic_slice_in_dim(entropy, member * picks, picks))
        grad_logits = (
            jnp.exp(logits - top_all[:, None]) / total_all[:, None] - label_hits.astype(f32)
        ).astype(bf16)
        grad_table = jnp.einsum("tv,td->vd", grad_logits, all_picked, preferred_element_type=f32)
        grad_table = jnp.pad(grad_table, ((0, padded_rows - vocab_rows), (0, 0)))
        grad_picked = jnp.einsum("tv,vd->td", grad_logits, table_low[:vocab_rows], preferred_element_type=f32)
        grad_picked = grad_picked.reshape(groups, picks, model_width)
        grad_picked = lax.psum_scatter(grad_picked, "fsdp", scatter_dimension=0)

    match = flat_positions[None, :] == index[:, None]
    place = jnp.sum(jnp.where(match, jnp.arange(picks, dtype=jnp.int32)[None, :] + 1, 0), axis=1)
    grad_final = jnp.where(
        (place > 0)[:, None], jnp.take(grad_picked, jnp.maximum(place - 1, 0), axis=0), 0.0
    )
    grad_stream, grad_final_gain = final_pull(grad_final)
    gain_grads = [None] * gain_count
    gain_grads[gain_count - 1] = grad_final_gain
    layer_grads = [None] * LAYERS
    for layer in reversed(range(LAYERS)):
        before, attention_kept, middle, feed_kept = saved_layers[layer]
        grad_stream, feed_gain, *grads_feed = feed_back(
            grad_stream, middle, gain_rows[2 + 2 * layer], full_blocks, layer, feed_kept
        )
        grad_stream, attention_gain, grads_attention = attend_back(
            grad_stream, before, gain_rows[1 + 2 * layer], full_blocks, layer, segments, attention_kept
        )
        gain_grads[1 + 2 * layer] = jnp.sum(attention_gain, axis=(0, 1))
        gain_grads[2 + 2 * layer] = jnp.sum(feed_gain, axis=0)
        layer_grads[layer] = [grads_attention] + grads_feed
    grad_embedded, gain_grads[0] = first_pull(grad_stream)
    grad_rows = grad_embedded.astype(bf16)
    row_index = jnp.arange(padded_rows, dtype=jnp.int32)

    def given(cid, k, grad_table):
        chosen = (slot_index[:, None] == slot_of(k)[None, :]).astype(bf16)
        rows = jnp.dot(chosen, grad_rows, preferred_element_type=f32).astype(bf16)
        rows = move.spread(cid, rows.reshape(groups, CAPACITY, model_width)).reshape(slots, model_width)
        asked = lax.dynamic_index_in_dim(asked_all, k, 0, keepdims=False)
        target_rows = (row_index[:, None] == asked[None, :]).astype(bf16)
        return grad_table + jnp.dot(target_rows, rows, preferred_element_type=f32)

    grad_table = given(7, 0, grad_table)
    _, grad_table = lax.while_loop(
        lambda s: s[0] < rounds, lambda s: (s[0] + 1, given(13, s[0], s[1])), (jnp.int32(1), grad_table)
    )
    grad_blocks = [g for grads in layer_grads for g in grads]
    grad_gains = jnp.stack(gain_grads, axis=0)

    position_count = micro_count * replicas * groups * pick_count
    clip_limit = clip_ratio * math.sqrt(position_count)
    steps_done = step_count[0].astype(f32)
    first_fix = 1.0 - beta_first**steps_done
    second_fix = 1.0 - beta_second**steps_done
    slot_cap = soap_m.shape[0]
    slot_total = slot_cap * groups
    named = jnp.arange(slot_total, dtype=jnp.int32)[:, None] == block_slots[None, :]
    taken = jnp.any(named, axis=1)
    block_of = jnp.sum(jnp.where(named, jnp.arange(block_count, dtype=jnp.int32)[None, :], 0), axis=1)

    small = jnp.zeros((8, model_width), f32).at[:gain_count].set(grad_gains)
    small = small.at[7, 0].set(loss_local)
    if move.kernels:
        owned, grad_table, small = settle_gradients(
            move.sizes,
            8,
            grad_blocks,
            grad_table.reshape(4, padded_rows // 4, model_width),
            small,
            block_of,
            taken.astype(jnp.int32),
            slot_cap,
        )
        grad_table = grad_table.reshape(padded_rows, model_width)
        squares = jnp.sum(small[6])
        owned = owned.reshape(slot_cap, model_width, model_width)
    else:
        grad_blocks = jnp.concatenate([g.astype(f32) for g in grad_blocks], axis=0)
        mine = lax.psum_scatter(grad_blocks, "fsdp", scatter_dimension=1, tiled=True)
        mine, grad_table = lax.psum((mine, grad_table[:vocab_rows]), "rep")
        small = lax.psum(small, ("rep", "fsdp"))
        squares = lax.psum(jnp.sum(mine * mine) + jnp.sum(grad_table * grad_table), "fsdp")
        outgoing = jnp.where(taken[:, None, None], jnp.take(mine, block_of, axis=0), 0)
        owned = lax.all_to_all(outgoing, "fsdp", split_axis=0, concat_axis=1, tiled=True)
    loss_all = small[7, 0]
    grad_gains = small[:gain_count]
    grad_norm = jnp.sqrt(squares + jnp.sum(grad_gains * grad_gains))
    factor = jnp.minimum(1.0, clip_limit / grad_norm)
    grad_gains = lax.dynamic_slice_in_dim(grad_gains, member * gains.shape[1], gains.shape[1], axis=1)

    live = lax.dynamic_slice_in_dim(taken, member * slot_cap, slot_cap)
    if move.kernels:
        soap_m_new, soap_v_new, turned = turn_slots(
            replica,
            live,
            jnp.stack([factor, first_fix, second_fix]),
            left_basis,
            right_basis,
            owned,
            soap_m,
            soap_v,
        )
        returned, embed_new, embed_m_new, embed_v_new, embed_new_low = return_slots(
            move.sizes,
            11,
            turned,
            jnp.stack([factor, 1.0 / first_fix, 1.0 / second_fix]),
            grad_table,
            embed,
            embed_m,
            embed_v,
        )
        returned = returned.reshape(slot_total, shard_rows, model_width)
    else:
        rotated = jnp.einsum("bji,bjk->bik", left_basis, owned, precision=high)
        rotated = factor * jnp.einsum("bik,bkl->bil", rotated, right_basis, precision=high)
        moment_first, moment_second, rotated_step = adam_moments(soap_m, soap_v, rotated, first_fix, second_fix)
        soap_m_new = jnp.where(live[:, None, None], moment_first, soap_m)
        soap_v_new = jnp.where(live[:, None, None], moment_second, soap_v)
        turned = jnp.einsum("bij,bjk->bik", left_basis, rotated_step, precision=high)
        turned = jnp.einsum("bik,blk->bil", turned, right_basis, precision=high)
        returned = lax.all_to_all(turned, "fsdp", split_axis=1, concat_axis=0, tiled=True)
        embed_m_new, embed_v_new, table_step = adam_moments(
            embed_m, embed_v, factor * grad_table, first_fix, second_fix
        )
        embed_new = embed - step_rate * (table_step + weight_decay * embed)
        embed_new_low = embed_new.astype(bf16)
    update = jnp.take(returned, block_slots, axis=0).astype(f32)
    blocks_new = blocks - step_rate * (update + weight_decay * blocks)

    gains_m_new, gains_v_new, gain_step = adam_moments(
        gains_m, gains_v, factor * grad_gains, first_fix, second_fix
    )
    gains_new = gains - step_rate * gain_step
    loss = (loss_all / position_count).reshape(1)
    return (
        loss,
        grad_norm.reshape(1),
        blocks_new,
        gains_new,
        embed_new,
        embed_m_new,
        embed_v_new,
        gains_m_new,
        gains_v_new,
        soap_m_new,
        soap_v_new,
        blocks_new.astype(bf16),
        embed_new_low,
    )


def solution(mesh):
    packs = P(None, ("rep", "fsdp"), None)
    rows = P(None, "fsdp", None)
    columns = P(None, "fsdp")
    table = P("fsdp", None)
    slots = P("fsdp", None, None)
    return jax.shard_map(
        body,
        mesh=mesh,
        in_specs=(packs,) * 4
        + (rows, columns)
        + (table,) * 3
        + (columns,) * 2
        + (slots,) * 4
        + (P(), P()),
        out_specs=(P(), P(), rows, columns)
        + (table,) * 3
        + (columns,) * 2
        + (slots,) * 2
        + (rows, table),
        check_vma=False,
    )
```
